32 devices in a mesh: expert: 16 (over z, y, x), tensor: 2 (over core).
Axes of the slice: x: 2, y: 2, z: 4, core: 2. Of those that a mesh axis runs over, the one named last changes fastest.
Arguments:
- layer_in: float32 [2048, 2048], P('expert'), may hold values from -20 to 20
- norm1_gain: bfloat16 [2048], P('expert'), may hold values from 0.5 to 1.5
- q_weight: bfloat16 [2048, 3072], P('expert', 'tensor'), may hold values from -0.125 to 0.125
- kva_weight: bfloat16 [2048, 576], P('expert'), may hold values from -0.125 to 0.125
- kv_gain: bfloat16 [512], P('expert'), may hold values from 0.5 to 1.5
- kvb_weight: bfloat16 [512, 4096], P('expert', 'tensor'), may hold values from -0.25 to 0.25
- o_weight: bfloat16 [2048, 2048], P('tensor', 'expert'), may hold values from -0.5 to 0.5
- norm2_gain: bfloat16 [2048], P('expert'), may hold values from 0.5 to 1.5
- router_weight: bfloat16 [2048, 16], P('expert'), may hold values from -0.25 to 0.25
- shared_gate: bfloat16 [2048, 2816], P('expert', 'tensor'), may hold values from -0.125 to 0.125
- shared_up: bfloat16 [2048, 2816], P('expert', 'tensor'), may hold values from -0.125 to 0.125
- shared_down: bfloat16 [2816, 2048], P('tensor', 'expert'), may hold values from -0.109375 to 0.109375
- expert_gate: bfloat16 [16, 2048, 1408], P('expert', None, 'tensor'), may hold values from -0.125 to 0.125
- expert_up: bfloat16 [16, 2048, 1408], P('expert', None, 'tensor'), may hold values from -0.125 to 0.125
- expert_down: bfloat16 [16, 1408, 2048], P('expert', 'tensor'), may hold values from -0.625 to 0.625
- routes: int32 [2048, 6], P('expert'), may hold values from 0 to 15, all different within a row; in each aligned block of 128 rows (0 to 127, 128 to 255, ...) at most 64 rows name the same one
- out_grad: float32 [2048, 2048], P('expert'), may hold values from -6 to 6
Outputs:
- layer_out: float32 [2048, 2048], P('expert')
- x_grad: float32 [2048, 2048], P('expert')
- norm1_gain_grad: float32 [2048], P('expert')
- q_grad: float32 [2048, 3072], P('expert', 'tensor')
- kva_grad: float32 [2048, 576], P('expert')
- kv_gain_grad: float32 [512], P('expert')
- kvb_grad: float32 [512, 4096], P('expert', 'tensor')
- o_grad: float32 [2048, 2048], P('tensor', 'expert')
- norm2_gain_grad: float32 [2048], P('expert')
- router_grad: float32 [2048, 16], P('expert')
- shared_gate_grad: float32 [2048, 2816], P('expert', 'tensor')
- shared_up_grad: float32 [2048, 2816], P('expert', 'tensor')
- shared_down_grad: float32 [2816, 2048], P('tensor', 'expert')
- expert_gate_grad: float32 [16, 2048, 1408], P('expert', None, 'tensor')
- expert_up_grad: float32 [16, 2048, 1408], P('expert', None, 'tensor')
- expert_down_grad: float32 [16, 1408, 2048], P('expert', 'tensor')
The draws below stay inside these ranges and needn't reach their ends.
Inputs may be any that keep to these rules, and one draw needn't show every extreme that they name: `routes`: each row names 6 different experts; in the rows of one device no expert is named by more than 64 rows, a bound that some block reaches.
All inputs are finite; a program needn't handle non-finite values.
Results may differ from the reference program's by a relative error of at most 0.02.
Values may be sent and summed in bfloat16 or wider, within the bound.
A program may use at most 256 MiB of HBM per device.

```python
import math
import jax
import jax.numpy as jnp
import numpy as np
from jax import lax

D = 2048
H = 16
DN = 128
DR = 64
DQK = 192
DL = 512
DV = 128
FE = 1408
FS = 2816
TOPK = 6
EXPERTS = 16
SEQ = 128
TOKENS = 2048
CAP = 64
N_EXPERT = 16
N_TENSOR = 2


def draw_layer_in(key, part):
    key_rows, key_vals = jax.random.split(key, 2)
    scales = jnp.exp(jax.random.uniform(key_rows, (TOKENS, 1), jnp.float32, jnp.log(0.4), jnp.log(4.0)))
    entries = jax.random.normal(key_vals, (TOKENS, D), jnp.float32)
    return jnp.clip(entries, -5.0, 5.0) * scales


def shard_levels(own_key, shape, cuts, smallest, largest):
    def one(axis_at, parts):
        steps = jax.random.uniform(jax.random.fold_in(jax.random.fold_in(own_key, 6), axis_at), (parts,), jnp.float32, smallest / len(cuts), largest / len(cuts))
        return jnp.repeat(jnp.exp(steps), shape[axis_at] // parts).reshape((-1,) + (1,) * (len(shape) - axis_at - 1))

    loudness = one(*cuts[0])
    for cut in cuts[1:]:
        loudness = loudness * one(*cut)
    return loudness


def deal_out(key, own, number, rows, count, top, bound, skew):
    sequence = jax.random.permutation(key, count)
    crowded, usual = shares(count, rows * top, bound, skew, True), shares(count, rows * top, bound, skew, False)
    places = jnp.arange(count)

    def named(sizes, rotation):
        used = int((sizes > 0).sum())
        fixed = max(1, used // 4)
        passed = fixed + (places - fixed + rotation * (used - fixed)) % max(1, count - fixed)
        return jnp.zeros((count,), jnp.int32).at[sequence[jnp.where(places < fixed, places, passed)]].set(jnp.asarray(sizes, jnp.int32))

    sizes = jnp.where(number % 4 == 0, named(crowded, number // 4), named(usual, number - number // 4 - 1))
    mixed = jax.random.permutation(jax.random.fold_in(own, 3), count)
    donor, taker = mixed[0:count // 2 * 2:2], mixed[1:count // 2 * 2:2]
    slack = jnp.minimum(sizes[donor] - 1, bound - sizes[taker]) // 2
    slack = jnp.where((donor == sequence[0]) | (taker == sequence[0]) | (sizes[taker] == 0), 0, jnp.maximum(slack, 0))
    passed = jax.random.randint(jax.random.fold_in(own, 4), (count // 2,), 0, 1 << 20) % (slack + 1)
    sizes = sizes.at[donor].add(-passed).at[taker].add(passed)
    labels = jnp.searchsorted(jnp.cumsum(sizes), jnp.arange(rows * top), side="right").astype(jnp.int32)
    grid = labels.reshape(top, rows).T
    grid = grid[jax.random.permutation(jax.random.fold_in(own, 1), rows)]
    rotation = jax.random.randint(jax.random.fold_in(own, 2), (rows, 1), 0, top)
    return jnp.take_along_axis(grid, (jnp.arange(top)[None, :] + rotation) % top, axis=1)


def shares(amount, total, most, slope, full):
    portions = [(1 << 20) // math.isqrt(rank ** slope) + 1 for rank in range(1, amount + 1)]
    largest = most if full else min(most, max(-(-total // amount), total * portions[0] // sum(portions)))
    least = 1 if total - largest >= amount - 1 else 0
    counts, rest = [largest] + [least] * (amount - 1), total - largest - least * (amount - 1)
    while rest > 0:
        candidates = [i for i in range(1, amount) if counts[i] < largest] or [i for i in range(1, amount) if counts[i] < most]
        whole, left = sum([portions[i] for i in candidates]), rest
        for i in candidates:
            addition = min(most - counts[i], max(1, left * portions[i] // whole), rest)
            counts[i] = counts[i] + addition
            rest = rest - addition
    return np.array(counts)


def normal_values(rng, extent, deviation, limit, cuts=(), kind=jnp.bfloat16):
    values = deviation * jax.random.normal(rng, extent, jnp.float32)
    if cuts:
        values = values * shard_levels(rng, extent, cuts, -0.22, 0.18)
    return jnp.clip(values, -limit, limit).astype(kind)


def setup_inputs(seed: int = 0) -> dict:
    key_list = jax.random.split(jax.random.key(seed), 18)
    layer_in = draw_layer_in(jax.random.fold_in(key_list[17], 71), 0)
    norm1_gain = jnp.clip(1.0 + 0.1 * jax.random.normal(key_list[1], (D,), jnp.float32), 0.5, 1.5).astype(jnp.bfloat16)
    q_weight = normal_values(key_list[2], (D, H * DQK), D ** -0.5, 0.125, ((0, 16), (1, 2)))
    kva_weight = normal_values(key_list[3], (D, DL + DR), D ** -0.5, 0.125, ((0, 16),))
    kv_gain = jnp.clip(1.0 + 0.1 * jax.random.normal(key_list[4], (DL,), jnp.float32), 0.5, 1.5).astype(jnp.bfloat16)
    kvb_weight = normal_values(key_list[5], (DL, H * (DN + DV)), DL ** -0.5, 0.25, ((0, 16), (1, 2)))
    o_weight = normal_values(key_list[6], (H * DV, D), (H * DV // 16) ** -0.5, 0.5, ((0, 2), (1, 16)))
    norm2_gain = jnp.clip(1.0 + 0.1 * jax.random.normal(key_list[7], (D,), jnp.float32), 0.5, 1.5).astype(jnp.bfloat16)
    router_weight = normal_values(key_list[8], (D, EXPERTS), (D // 4) ** -0.5, 0.25, ((0, 16),))
    shared_gate = normal_values(key_list[9], (D, FS), D ** -0.5, 0.125, ((0, 16), (1, 2)))
    shared_up = normal_values(key_list[10], (D, FS), D ** -0.5, 0.125, ((0, 16), (1, 2)))
    shared_down = normal_values(key_list[11], (FS, D), FS ** -0.5, 0.109375, ((0, 2), (1, 16)))
    expert_gate = normal_values(key_list[12], (EXPERTS, D, FE), D ** -0.5, 0.125, ((0, 16), (2, 2)))
    expert_up = normal_values(key_list[13], (EXPERTS, D, FE), D ** -0.5, 0.125, ((0, 16), (2, 2)))
    expert_down = normal_values(key_list[14], (EXPERTS, FE, D), (FE // 16) ** -0.5, 0.625, ((0, 16), (1, 2)))
    routes_keys = jax.random.split(jax.random.fold_in(key_list[15], 1), TOKENS // SEQ)
    routes_turns = jax.random.permutation(jax.random.fold_in(key_list[15], 3), TOKENS // SEQ)
    routes = jax.vmap(lambda own, number: deal_out(jax.random.fold_in(key_list[15], 2), own, number, SEQ, EXPERTS, TOPK, CAP, 2))(routes_keys, routes_turns).reshape((TOKENS, TOPK))
    out_grad = normal_values(key_list[16], (TOKENS, D), 1.0, 6.0, ((0, 16),), jnp.float32)
    return {"layer_in": layer_in, "norm1_gain": norm1_gain, "q_weight": q_weight, "kva_weight": kva_weight, "kv_gain": kv_gain, "kvb_weight": kvb_weight, "o_weight": o_weight, "norm2_gain": norm2_gain, "router_weight": router_weight, "shared_gate": shared_gate, "shared_up": shared_up, "shared_down": shared_down, "expert_gate": expert_gate, "expert_up": expert_up, "expert_down": expert_down, "routes": routes, "out_grad": out_grad}


norm_eps = 1e-06

def rms_scale(inputs):
    return lax.rsqrt(lax.optimization_barrier(jnp.mean(inputs * inputs, axis=-1, keepdims=True)) + norm_eps)

def rope_tables(length, rot_width):
    half_width = rot_width // 2
    frequency = 10000.0 ** (-jnp.arange(half_width).astype(jnp.float32) / half_width)
    angles = jnp.arange(length).astype(jnp.float32)[:, None] * frequency[None, :]
    return (jnp.cos(angles), jnp.sin(angles))

def rotate(inputs, cosine, sine_part):
    half_width = inputs.shape[-1] // 2
    first_half = inputs[..., :half_width]
    second_half = inputs[..., half_width:]
    return jnp.concatenate([first_half * cosine - second_half * sine_part, second_half * cosine + first_half * sine_part], axis=-1)

def rotate_back(inputs, cosine, sine_part):
    half_width = inputs.shape[-1] // 2
    first_half = inputs[..., :half_width]
    second_half = inputs[..., half_width:]
    return jnp.concatenate([first_half * cosine + second_half * sine_part, second_half * cosine - first_half * sine_part], axis=-1)

def silu_grad(pre_act):
    sigmoid_val = jax.nn.sigmoid(pre_act)
    return sigmoid_val * (1.0 + pre_act * (1.0 - sigmoid_val))

def masked_scores(query_blk, key_rows, first_row):
    scores = jnp.einsum('qhd,khd->hqk', query_blk.astype(jnp.float32), key_rows.astype(jnp.float32)) * DQK ** (-0.5)
    row_pos = first_row + jnp.arange(query_blk.shape[0], dtype=jnp.int32)
    col_pos = jnp.arange(key_rows.shape[0], dtype=jnp.int32)
    return jnp.where(col_pos[None, None, :] <= row_pos[None, :, None], scores, -1e+30)

def attend(query_rows, key_rows, value_rows):
    seq_len = query_rows.shape[0]
    blk_rows = min(seq_len, 512)

    def one_block(block_index):
        first_row = (block_index * blk_rows).astype(jnp.int32)
        query_blk = lax.dynamic_slice_in_dim(query_rows, first_row, blk_rows, 0)
        scores = masked_scores(query_blk, key_rows, first_row)
        row_max = lax.optimization_barrier(jnp.max(scores, axis=-1, keepdims=True))
        log_total = row_max + jnp.log(lax.optimization_barrier(jnp.sum(jnp.exp(scores - row_max), axis=-1, keepdims=True)))
        att_weights = jnp.exp(scores - log_total).astype(jnp.bfloat16)
        mixed_blk = jnp.einsum('hqk,khd->qhd', att_weights.astype(jnp.float32), value_rows.astype(jnp.float32)).astype(jnp.bfloat16)
        return (mixed_blk, log_total)
    mixed_heads, log_totals = lax.map(one_block, jnp.arange(seq_len // blk_rows, dtype=jnp.int32))
    return (mixed_heads.reshape(seq_len, query_rows.shape[1], value_rows.shape[2]), log_totals)

def attend_back(query_rows, key_rows, value_rows, log_totals, mixed_grad):
    seq_len, head_count = (query_rows.shape[0], query_rows.shape[1])
    blk_rows = min(seq_len, 512)

    def one_block(running, block_index):
        key_acc, value_acc = running
        first_row = (block_index * blk_rows).astype(jnp.int32)
        query_blk = lax.dynamic_slice_in_dim(query_rows, first_row, blk_rows, 0)
        grad_blk = lax.dynamic_slice_in_dim(mixed_grad, first_row, blk_rows, 0)
        scores = masked_scores(query_blk, key_rows, first_row)
        att_probs = jnp.exp(scores - log_totals[block_index])
        att_weights = att_probs.astype(jnp.bfloat16)
        value_acc = value_acc + jnp.einsum('hqk,qhd->khd', att_weights.astype(jnp.float32), grad_blk.astype(jnp.float32))
        prob_grad = jnp.einsum('qhd,khd->hqk', grad_blk.astype(jnp.float32), value_rows.astype(jnp.float32))
        row_delta = lax.optimization_barrier(jnp.sum(att_probs * prob_grad, axis=-1, keepdims=True))
        score_delta = (att_probs * (prob_grad - row_delta) * DQK ** (-0.5)).astype(jnp.bfloat16)
        query_grad = jnp.einsum('hqk,khd->qhd', score_delta.astype(jnp.float32), key_rows.astype(jnp.float32))
        key_acc = key_acc + jnp.einsum('hqk,qhd->khd', score_delta.astype(jnp.float32), query_blk.astype(jnp.float32))
        return ((key_acc, value_acc), query_grad)
    zero_start = (jnp.zeros((seq_len, head_count, DQK), jnp.float32), jnp.zeros((seq_len, head_count, DV), jnp.float32))
    (key_grad, value_grad), query_grad = lax.scan(one_block, zero_start, jnp.arange(seq_len // blk_rows, dtype=jnp.int32))
    return (query_grad.reshape(seq_len, head_count, DQK), key_grad, value_grad)

def attention_forward(seq_in, norm1_gain, q_weight, kva_weight, kv_gain, kvb_weight):
    seq_len = seq_in.shape[0]
    head_count = q_weight.shape[1] // DQK
    cosine, sine_part = rope_tables(seq_len, DR)
    stat_one = rms_scale(seq_in)
    unit_one = seq_in * stat_one
    normed1 = (unit_one * norm1_gain.astype(jnp.float32)).astype(jnp.bfloat16)
    query_full = jnp.dot(normed1, q_weight, preferred_element_type=jnp.float32).reshape(seq_len, head_count, DQK)
    query_rows = jnp.concatenate([query_full[..., :DN], rotate(query_full[..., DN:], cosine[:, None, :], sine_part[:, None, :])], axis=-1).astype(jnp.bfloat16)
    latent_full = jnp.dot(normed1, kva_weight, preferred_element_type=jnp.float32)
    latent_stat = rms_scale(latent_full[:, :DL])
    latent_unit = latent_full[:, :DL] * latent_stat
    latent = (latent_unit * kv_gain.astype(jnp.float32)).astype(jnp.bfloat16)
    rot_key = rotate(latent_full[:, DL:], cosine, sine_part).astype(jnp.bfloat16)
    key_value = jnp.dot(latent, kvb_weight, preferred_element_type=jnp.float32).astype(jnp.bfloat16).reshape(seq_len, head_count, DN + DV)
    key_rows = jnp.concatenate([key_value[..., :DN], jnp.broadcast_to(rot_key[:, None, :], (seq_len, head_count, DR))], axis=-1)
    value_rows = key_value[..., DN:]
    mixed_heads, log_totals = attend(query_rows, key_rows, value_rows)
    return (stat_one, unit_one, normed1, query_rows, latent_stat, latent_unit, latent, key_rows, value_rows, mixed_heads, log_totals, cosine, sine_part)

def reference(layer_in, norm1_gain, q_weight, kva_weight, kv_gain, kvb_weight, o_weight, norm2_gain, router_weight, shared_gate, shared_up, shared_down, expert_gate, expert_up, expert_down, routes, out_grad):
    seqs_in = layer_in.reshape(N_EXPERT, SEQ, D)

    def forward_seq(running, seq_in):
        pieces = attention_forward(seq_in, norm1_gain, q_weight, kva_weight, kv_gain, kvb_weight)
        attn_out = jnp.dot(pieces[9].reshape(SEQ, H * DV), o_weight, preferred_element_type=jnp.float32)
        return (running, seq_in + attn_out)
    _, hidden_state = lax.scan(forward_seq, None, seqs_in)
    hidden_state = hidden_state.reshape(TOKENS, D)
    stat_two = rms_scale(hidden_state)
    unit_two = hidden_state * stat_two
    normed2 = (unit_two * norm2_gain.astype(jnp.float32)).astype(jnp.bfloat16)
    logits = jnp.dot(normed2, router_weight, preferred_element_type=jnp.float32)
    router_probs = jax.nn.softmax(logits, axis=-1)
    route_onehot = (routes[:, :, None] == jnp.arange(EXPERTS, dtype=jnp.int32)[None, None, :]).astype(jnp.float32)
    route_weight = jnp.einsum('tke,te->tk', route_onehot, router_probs)
    shared_pre_gate = jnp.dot(normed2, shared_gate, preferred_element_type=jnp.float32)
    shared_pre_up = jnp.dot(normed2, shared_up, preferred_element_type=jnp.float32)
    shared_act = (jax.nn.silu(shared_pre_gate) * shared_pre_up).astype(jnp.bfloat16)
    shared_out = jnp.dot(shared_act, shared_down, preferred_element_type=jnp.float32)
    out_rows = out_grad.astype(jnp.bfloat16)
    shared_down_grad = jnp.dot(shared_act.T, out_rows, preferred_element_type=jnp.float32)
    shared_hidden_grad = jnp.dot(out_rows, shared_down.T, preferred_element_type=jnp.float32)
    shared_gate_delta = (shared_hidden_grad * shared_pre_up * silu_grad(shared_pre_gate)).astype(jnp.bfloat16)
    shared_up_delta = (shared_hidden_grad * jax.nn.silu(shared_pre_gate)).astype(jnp.bfloat16)
    shared_gate_grad = jnp.dot(normed2.T, shared_gate_delta, preferred_element_type=jnp.float32)
    shared_up_grad = jnp.dot(normed2.T, shared_up_delta, preferred_element_type=jnp.float32)
    normed2_grad = jnp.dot(shared_gate_delta, shared_gate.T, preferred_element_type=jnp.float32) + jnp.dot(shared_up_delta, shared_up.T, preferred_element_type=jnp.float32)
    flat_routes = routes.reshape(N_EXPERT, SEQ * TOPK)
    flat_hot = (flat_routes[:, :, None] == jnp.arange(EXPERTS, dtype=jnp.int32)[None, None, :]).astype(jnp.int32)
    slot_pos = (lax.optimization_barrier(jnp.sum(jnp.cumsum(flat_hot, axis=1) * flat_hot, axis=-1)) - 1).astype(jnp.int32)
    buffer_pos = (jnp.arange(N_EXPERT, dtype=jnp.int32)[:, None] * CAP + slot_pos).reshape(-1).astype(jnp.int32)
    assign_ids = jnp.arange(TOKENS * TOPK, dtype=jnp.int32)
    token_table = jnp.full((EXPERTS, N_EXPERT * CAP), TOKENS, jnp.int32).at[flat_routes.reshape(-1), buffer_pos].set((assign_ids // TOPK).astype(jnp.int32))
    route_table = jnp.zeros((EXPERTS, N_EXPERT * CAP), jnp.int32).at[flat_routes.reshape(-1), buffer_pos].set((assign_ids % TOPK).astype(jnp.int32))
    normed2_pad = jnp.concatenate([normed2, jnp.zeros((1, D), jnp.bfloat16)], axis=0)
    weight_pad = jnp.concatenate([route_weight, jnp.zeros((1, TOPK), jnp.float32)], axis=0)
    grad_pad = jnp.concatenate([out_grad, jnp.zeros((1, D), jnp.float32)], axis=0)
    block_width = FE // N_TENSOR
    slot_rows = N_EXPERT * CAP

    def expert_step(running, step_input):
        routed_sum, row_grad_sum, route_grad = running
        gate_w, up_w, down_w, token_ids, route_ids = step_input
        rows_in = normed2_pad[token_ids]
        slot_weight = weight_pad[token_ids, route_ids]
        slot_grad = grad_pad[token_ids]
        routed_cot = (slot_weight[:, None] * slot_grad).astype(jnp.bfloat16)
        expert_out = jnp.zeros((slot_rows, D), jnp.float32)
        row_grad = jnp.zeros((slot_rows, D), jnp.float32)
        gate_grads, up_grads, down_grads = ([], [], [])
        for block_index in range(N_TENSOR):
            low_col = block_index * block_width
            gate_blk = gate_w[:, low_col:low_col + block_width]
            up_blk = up_w[:, low_col:low_col + block_width]
            down_blk = down_w[low_col:low_col + block_width]
            pre_gate = jnp.dot(rows_in, gate_blk, preferred_element_type=jnp.float32)
            pre_up = jnp.dot(rows_in, up_blk, preferred_element_type=jnp.float32)
            expert_act = (jax.nn.silu(pre_gate) * pre_up).astype(jnp.bfloat16)
            block_out = lax.optimization_barrier(jnp.dot(expert_act, down_blk, preferred_element_type=jnp.float32).astype(jnp.bfloat16))
            expert_out = expert_out + block_out.astype(jnp.float32)
            hidden_grad = jnp.dot(routed_cot, down_blk.T, preferred_element_type=jnp.float32)
            gate_delta = (hidden_grad * pre_up * silu_grad(pre_gate)).astype(jnp.bfloat16)
            up_delta = (hidden_grad * jax.nn.silu(pre_gate)).astype(jnp.bfloat16)
            down_grads.append(jnp.dot(expert_act.T, routed_cot, preferred_element_type=jnp.float32))
            gate_grads.append(jnp.dot(rows_in.T, gate_delta, preferred_element_type=jnp.float32))
            up_grads.append(jnp.dot(rows_in.T, up_delta, preferred_element_type=jnp.float32))
            block_row = lax.optimization_barrier((jnp.dot(gate_delta, gate_blk.T, preferred_element_type=jnp.float32) + jnp.dot(up_delta, up_blk.T, preferred_element_type=jnp.float32)).astype(jnp.bfloat16))
            row_grad = row_grad + block_row.astype(jnp.float32)
        routed_sum = routed_sum.at[token_ids].add(slot_weight[:, None] * expert_out)
        route_grad = route_grad.at[token_ids, route_ids].add(lax.optimization_barrier(jnp.sum(slot_grad * expert_out, axis=-1)))
        row_grad_sum = row_grad_sum.at[token_ids].add(row_grad)
        return ((routed_sum, row_grad_sum, route_grad), (jnp.concatenate(gate_grads, axis=1), jnp.concatenate(up_grads, axis=1), jnp.concatenate(down_grads, axis=0)))
    zero_start = (jnp.zeros((TOKENS + 1, D), jnp.float32), jnp.zeros((TOKENS + 1, D), jnp.float32), jnp.zeros((TOKENS + 1, TOPK), jnp.float32))
    (routed_sum, row_grad_sum, route_grad), (expert_gate_grad, expert_up_grad, expert_down_grad) = lax.scan(expert_step, zero_start, (expert_gate, expert_up, expert_down, token_table, route_table))
    layer_out = hidden_state + routed_sum[:TOKENS] + shared_out
    prob_grad = jnp.einsum('tk,tke->te', route_grad[:TOKENS], route_onehot)
    logit_delta = (router_probs * (prob_grad - lax.optimization_barrier(jnp.sum(router_probs * prob_grad, axis=-1, keepdims=True)))).astype(jnp.bfloat16)
    router_grad = jnp.dot(normed2.T, logit_delta, preferred_element_type=jnp.float32)
    normed2_grad = normed2_grad + row_grad_sum[:TOKENS] + jnp.dot(logit_delta, router_weight.T, preferred_element_type=jnp.float32)
    norm2_gain_grad = lax.optimization_barrier(jnp.sum(normed2_grad * unit_two, axis=0))
    scaled_two = normed2_grad * norm2_gain.astype(jnp.float32)
    hidden_grad = out_grad + stat_two * (scaled_two - unit_two * lax.optimization_barrier(jnp.mean(scaled_two * unit_two, axis=-1, keepdims=True)))
    seqs_hidden_grad = hidden_grad.reshape(N_EXPERT, SEQ, D)

    def backward_seq(running, step_input):
        gain1_acc, q_acc, kva_acc, kvgain_acc, kvb_acc, o_acc = running
        seq_in, seq_grad = step_input
        stat_one, unit_one, normed1, query_rows, latent_stat, latent_unit, latent, key_rows, value_rows, mixed_heads, log_totals, cosine, sine_part = attention_forward(seq_in, norm1_gain, q_weight, kva_weight, kv_gain, kvb_weight)
        hidden_rows = seq_grad.astype(jnp.bfloat16)
        o_acc = o_acc + jnp.dot(mixed_heads.reshape(SEQ, H * DV).T, hidden_rows, preferred_element_type=jnp.float32)
        mixed_grad = jnp.dot(hidden_rows, o_weight.T, preferred_element_type=jnp.float32).astype(jnp.bfloat16).reshape(SEQ, H, DV)
        query_grad, key_grad, value_grad = attend_back(query_rows, key_rows, value_rows, log_totals, mixed_grad)
        query_delta = jnp.concatenate([query_grad[..., :DN], rotate_back(query_grad[..., DN:], cosine[:, None, :], sine_part[:, None, :])], axis=-1).astype(jnp.bfloat16).reshape(SEQ, H * DQK)
        kv_delta = jnp.concatenate([key_grad[..., :DN], value_grad], axis=-1).astype(jnp.bfloat16).reshape(SEQ, H * (DN + DV))
        rot_grad = rotate_back(lax.optimization_barrier(jnp.sum(key_grad[..., DN:], axis=1)), cosine, sine_part)
        latent_grad = jnp.dot(kv_delta, kvb_weight.T, preferred_element_type=jnp.float32)
        kvgain_acc = kvgain_acc + lax.optimization_barrier(jnp.sum(latent_grad * latent_unit, axis=0))
        scaled_lat = latent_grad * kv_gain.astype(jnp.float32)
        latent_back = latent_stat * (scaled_lat - latent_unit * lax.optimization_barrier(jnp.mean(scaled_lat * latent_unit, axis=-1, keepdims=True)))
        latent_delta = jnp.concatenate([latent_back, rot_grad], axis=-1).astype(jnp.bfloat16)
        q_acc = q_acc + jnp.dot(normed1.T, query_delta, preferred_element_type=jnp.float32)
        kva_acc = kva_acc + jnp.dot(normed1.T, latent_delta, preferred_element_type=jnp.float32)
        kvb_acc = kvb_acc + jnp.dot(latent.T, kv_delta, preferred_element_type=jnp.float32)
        normed1_grad = jnp.dot(query_delta, q_weight.T, preferred_element_type=jnp.float32) + jnp.dot(latent_delta, kva_weight.T, preferred_element_type=jnp.float32)
        gain1_acc = gain1_acc + lax.optimization_barrier(jnp.sum(normed1_grad * unit_one, axis=0))
        scaled_one = normed1_grad * norm1_gain.astype(jnp.float32)
        seq_x_grad = seq_grad + stat_one * (scaled_one - unit_one * lax.optimization_barrier(jnp.mean(scaled_one * unit_one, axis=-1, keepdims=True)))
        return ((gain1_acc, q_acc, kva_acc, kvgain_acc, kvb_acc, o_acc), seq_x_grad)
    zero_grads = (jnp.zeros((D,), jnp.float32), jnp.zeros((D, H * DQK), jnp.float32), jnp.zeros((D, DL + DR), jnp.float32), jnp.zeros((DL,), jnp.float32), jnp.zeros((DL, H * (DN + DV)), jnp.float32), jnp.zeros((H * DV, D), jnp.float32))
    (norm1_gain_grad, q_grad, kva_grad, kv_gain_grad, kvb_grad, o_grad), x_grad = lax.scan(backward_seq, zero_grads, (seqs_in, seqs_hidden_grad))
    x_grad = x_grad.reshape(TOKENS, D)
    return (layer_out, x_grad, norm1_gain_grad, q_grad, kva_grad, kv_gain_grad, kvb_grad, o_grad, norm2_gain_grad, router_grad, shared_gate_grad, shared_up_grad, shared_down_grad, expert_gate_grad, expert_up_grad, expert_down_grad)
```

```python
import functools

import jax
import jax.numpy as jnp
from jax import lax
from jax.experimental import pallas as pl
from jax.experimental.pallas import tpu as pltpu
from jax.sharding import PartitionSpec as P

DN = 128
DR = 64
DQK = 192
DV = 128
TOPK = 6
LANES = 128


norm_eps = 1e-06


def rms_scale(inputs):
    return lax.rsqrt(jnp.mean(inputs * inputs, axis=-1, keepdims=True) + norm_eps)


def rope_tables(length, rot_width):
    half_width = rot_width // 2
    frequency = 10000.0 ** (-jnp.arange(half_width).astype(jnp.float32) / half_width)
    angles = jnp.arange(length).astype(jnp.float32)[:, None] * frequency[None, :]
    return (jnp.cos(angles), jnp.sin(angles))


def rotate(inputs, cosine, sine_part):
    half_width = inputs.shape[-1] // 2
    first_half = inputs[..., :half_width]
    second_half = inputs[..., half_width:]
    return jnp.concatenate(
        [
            first_half * cosine - second_half * sine_part,
            second_half * cosine + first_half * sine_part,
        ],
        axis=-1,
    )


def rotate_back(inputs, cosine, sine_part):
    return rotate(inputs, cosine, -sine_part)


def silu_grad(pre_act):
    sigmoid_val = jax.nn.sigmoid(pre_act)
    return sigmoid_val * (1.0 + pre_act * (1.0 - sigmoid_val))


def fdot(left, right):
    return jnp.dot(left, right, preferred_element_type=jnp.float32)


def fsum(spec, left, right):
    return jnp.einsum(spec, left, right, preferred_element_type=jnp.float32)


EXPERT, TENSOR = "expert", "tensor"
MESH = pl.DeviceIdType.MESH
DMA = pltpu.SemaphoreType.DMA


def guarded(cond, body):
    if cond is None:
        body()
    else:
        pl.when(cond)(body)


def remote(src, dst, send, recv, target):
    return pltpu.make_async_remote_copy(
        src_ref=src, dst_ref=dst, send_sem=send, recv_sem=recv, device_id=target, device_id_type=MESH
    )


def part_rows(start, size):
    return pl.ds(pl.multiple_of(start, size), size)


class Place:
    def __init__(self):
        self.groups = lax.axis_size(EXPERT)
        self.chip = lax.axis_index(EXPERT)
        self.core = lax.axis_index(TENSOR)
        self.here = lax.rem(self.chip, 4)
        self.there_x = self.here + 1 - 2 * lax.rem(self.here, 2)
        self.there_y = self.here + 2 - 4 * (self.here // 2)
        self.across = 3 - self.here
        base = self.chip - self.here
        self.by_x = {EXPERT: base + self.there_x}
        self.by_y = {EXPERT: base + self.there_y}
        self.above = {EXPERT: self.chip + 4}
        self.below = {EXPERT: self.chip - 4}
        self.mate = {TENSOR: 1 - self.core}

    def partner(self, j):
        return lax.rem(self.chip + j, self.groups)


def level_steps(level, planes, far_first):
    order = [(0, 0)] + [(d, s) for d in range(1, planes) for s in (-1, 1)]
    steps = []
    for distance, side in order[::-1] if far_first else order:
        lev = level + side * distance
        steps.append((lev, side, None if distance == 0 else ((lev >= 0) & (lev < planes))))
    return steps


class Swap:
    reach = 0

    def __init__(self, blocks, vmem_result=False):
        groups = blocks.shape[0]
        self.ins = [(blocks, pltpu.VMEM)]
        self.outs = [
            (
                jax.ShapeDtypeStruct(blocks.shape, blocks.dtype),
                pltpu.VMEM if vmem_result else pl.ANY,
            )
        ]
        self.scratch = [DMA, DMA((groups,)), DMA((groups,))]

    def bind(self, place, ins, outs, scratch):
        self.place, self.groups = place, place.groups
        self.source, self.result = ins[0], outs[0]
        self.own_sem, self.send_sem, self.recv_sem = scratch

    def copy(self, j, src, dst):
        return remote(
            self.source.at[src],
            self.result.at[dst],
            self.send_sem.at[j],
            self.recv_sem.at[j],
            {EXPERT: self.place.partner(j)},
        )

    def own(self):
        chip = self.place.chip
        return pltpu.make_async_copy(self.source.at[chip], self.result.at[chip], self.own_sem)

    def begin(self):
        self.own().start()
        for j in range(1, self.groups):
            self.copy(j, self.place.partner(j), self.place.chip).start()

    def middle(self):
        return []

    def end(self):
        self.own().wait()
        for j in range(1, self.groups):
            self.copy(j, self.place.chip, self.place.partner(self.groups - j)).wait_recv()
            self.copy(j, self.place.partner(j), self.place.chip).wait_send()


class Gather:
    def __init__(self, arrays, planes):
        count, slots = len(arrays), planes * 4
        self.planes, self.count, self.reach = planes, count, planes
        self.ins = [(a, pltpu.VMEM) for a in arrays]
        self.outs = [(jax.ShapeDtypeStruct((slots,) + a.shape, a.dtype), pl.ANY) for a in arrays]
        by_level, by_slot = DMA((count, planes)), DMA((count, slots))
        self.scratch = [DMA((count,))] + [by_level] * 5 + [by_slot] + [by_level] * 6 + [by_slot]

    def bind(self, place, ins, outs, scratch):
        self.place, self.sources, self.results = place, ins, outs
        self.level = lax.rem(place.chip // 4, self.planes)
        self.has_up, self.has_down = self.level < self.planes - 1, self.level > 0
        self.own_sem = scratch[0]
        self.in_z, self.in_x, self.in_y, self.in_a, self.in_b, self.in_p = scratch[1:7]
        self.out_up, self.out_down, self.out_x, self.out_y = scratch[7:11]
        self.out_a, self.out_b, self.out_p = scratch[11:14]
        self.steps = level_steps(self.level, self.planes, False)

    def move(self, a, slot, part, send, recv, target, own=False, whose=None):
        half = self.sources[a].shape[0] // 2
        whose = self.place.core if whose is None else whose
        if part is None:
            rows = part_rows(whose * half, half)
        else:
            rows = part_rows(whose * half + part * (half // 2), half // 2)
        dst = self.results[a].at[slot, rows]
        return remote(self.sources[a].at[rows] if own else dst, dst, send, recv, target)

    def along_z(self, a, lev, own, up):
        sems = self.out_up if up else self.out_down
        target = self.place.above if up else self.place.below
        slot = lev * 4 + self.place.here
        return self.move(a, slot, None, sems.at[a, lev], self.in_z.at[a, lev], target, own)

    def along_x(self, a, lev, slot, own=False):
        return self.move(
            a, slot, None, self.out_x.at[a, lev], self.in_x.at[a, lev], self.place.by_x, own
        )

    def along_y(self, a, lev, slot, own=False):
        return self.move(
            a, slot, None, self.out_y.at[a, lev], self.in_y.at[a, lev], self.place.by_y, own
        )

    def corner_x(self, a, lev, slot):
        return self.move(
            a, slot, 0, self.out_a.at[a, lev], self.in_a.at[a, lev], self.place.by_x
        )

    def corner_y(self, a, lev, slot):
        return self.move(
            a, slot, 1, self.out_b.at[a, lev], self.in_b.at[a, lev], self.place.by_y
        )

    def share(self, a, slot, whose=None):
        return self.move(
            a, slot, None, self.out_p.at[a, slot], self.in_p.at[a, slot], self.place.mate, whose=whose
        )

    def own(self, a):
        slot = self.level * 4 + self.place.here
        return pltpu.make_async_copy(self.sources[a], self.results[a].at[slot], self.own_sem.at[a])

    def begin(self):
        for a in range(self.count):
            self.own(a).start()
        self.first(*self.steps[0])

    def first(self, lev, side, cond):
        def body():
            for a in range(self.count):
                own, slot = side == 0, lev * 4 + self.place.here
                if side != 0:
                    self.along_z(a, lev, own, True).wait_recv()
                if side <= 0:
                    pl.when(self.has_up)(lambda a=a: self.along_z(a, lev, own, True).start())
                if side >= 0:
                    pl.when(self.has_down)(lambda a=a: self.along_z(a, lev, own, False).start())
                self.along_x(a, lev, slot, own).start()
                self.along_y(a, lev, slot, own).start()
                if side != 0:
                    self.share(a, slot).start()

        guarded(cond, body)

    def second(self, lev, side, cond):
        def body():
            for a in range(self.count):
                slot = lev * 4 + self.place.there_y
                self.along_y(a, lev, slot).wait_recv()
                self.corner_x(a, lev, slot).start()
                self.share(a, slot).start()
                slot = lev * 4 + self.place.there_x
                self.along_x(a, lev, slot).wait_recv()
                self.corner_y(a, lev, slot).start()
                self.share(a, slot).start()

        guarded(cond, body)

    def third(self, lev, side, cond):
        def body():
            for a in range(self.count):
                slot = lev * 4 + self.place.across
                self.corner_x(a, lev, slot).wait_recv()
                self.corner_y(a, lev, slot).wait_recv()
                self.share(a, slot).start()

        guarded(cond, body)

    def middle(self):
        steps, calls = self.steps, []
        for i in range(1, len(steps) + 2):

            def call(i=i):
                if i < len(steps):
                    self.first(*steps[i])
                if 0 <= i - 1 < len(steps):
                    self.second(*steps[i - 1])
                if 0 <= i - 2 < len(steps):
                    self.third(*steps[i - 2])

            calls.append(call)
        return calls

    def end(self):
        place = self.place

        def finish(lev, side, cond):
            def body():
                for a in range(self.count):
                    own, slot = side == 0, lev * 4 + place.here
                    if side <= 0:
                        pl.when(self.has_up)(
                            lambda a=a: self.along_z(a, lev, own, True).wait_send()
                        )
                    if side >= 0:
                        pl.when(self.has_down)(
                            lambda a=a: self.along_z(a, lev, own, False).wait_send()
                        )
                    self.along_x(a, lev, slot, own).wait_send()
                    self.along_y(a, lev, slot, own).wait_send()
                    self.corner_x(a, lev, lev * 4 + place.there_y).wait_send()
                    self.corner_y(a, lev, lev * 4 + place.there_x).wait_send()
                    spots = [] if side == 0 else [slot]
                    for other in (place.there_y, place.there_x, place.across):
                        spots.append(lev * 4 + other)
                    for spot in spots:
                        self.share(a, spot).wait_send()
                        self.share(a, spot, 1 - place.core).wait_recv()

            guarded(cond, body)

        for step in self.steps:
            finish(*step)
        for a in range(self.count):
            self.own(a).wait()


class NormGather(Gather):
    def __init__(self, rows, gains, gain_row, planes):
        super().__init__([jax.ShapeDtypeStruct(rows.shape, jnp.bfloat16)], planes)
        self.ins = [(rows, pltpu.VMEM)]
        self.scratch = self.scratch + [pltpu.VMEM(rows.shape, jnp.bfloat16)]
        self.gains, self.gain_row = gains, gain_row

    def bind(self, place, ins, outs, scratch):
        super().bind(place, [scratch[-1]], outs, scratch[:-1])
        self.rows = ins[0]

    def begin(self):
        self.gains.end()
        rows = self.rows[...]
        stat = lax.rsqrt(jnp.mean(rows * rows, axis=-1, keepdims=True) + norm_eps)
        cols = rows.shape[1] // self.place.groups
        for j in range(self.place.groups):
            at = slice(j * cols, (j + 1) * cols)
            gain = self.gains.result[j, self.gain_row : self.gain_row + 1, :].astype(jnp.float32)
            self.sources[0][:, at] = (rows[:, at] * stat * gain).astype(jnp.bfloat16)
        super().begin()


class Reduce:
    def __init__(self, operands, produce, slots, block, width, scratch=(), prepare=None):
        planes, rows, kind = slots // 4, block // 2, jnp.bfloat16
        self.planes, self.reach = planes, planes
        self.ins = [(a, pltpu.VMEM) for a in operands]
        self.outs = [(jax.ShapeDtypeStruct((block, width), jnp.float32), pltpu.VMEM)]
        self.own_scratch, self.produce, self.prepare = len(scratch), produce, prepare
        by_level = DMA((planes,))
        self.scratch = (
            list(scratch)
            + [pltpu.VMEM((slots, block, width), kind), pltpu.VMEM((slots, rows, width), kind)]
            + [pltpu.VMEM((planes, rows // 2, width), kind)] * 2
            + [pltpu.VMEM((planes, rows, width), kind)] * 4
            + [DMA((slots,))]
            + [by_level] * 6
            + [DMA, DMA((slots,))]
            + [by_level] * 5
            + [DMA]
        )

    def bind(self, place, ins, outs, scratch):
        self.place, self.out = place, outs[0]
        self.refs = list(ins) + list(scratch[: self.own_scratch])
        scratch = scratch[self.own_scratch :]
        self.part, self.mine = scratch[:2]
        self.from_a, self.from_b, self.from_x, self.from_y = scratch[2:6]
        self.from_up, self.from_down = scratch[6:8]
        self.in_p, self.in_a, self.in_b, self.in_x, self.in_y = scratch[8:13]
        self.in_up, self.in_down, self.in_m, self.out_p = scratch[13:17]
        self.out_a, self.out_b, self.out_x, self.out_y, self.out_z, self.out_m = scratch[17:]
        self.level = lax.rem(place.chip // 4, self.planes)
        self.has_up, self.has_down = self.level < self.planes - 1, self.level > 0
        self.steps = level_steps(self.level, self.planes, True)
        self.rows = self.part.shape[1] // 2
        self.half = self.rows // 2

    def swap(self, slot):
        theirs = part_rows((1 - self.place.core) * self.rows, self.rows)
        return remote(
            self.part.at[slot, theirs],
            self.mine.at[slot],
            self.out_p.at[slot],
            self.in_p.at[slot],
            self.place.mate,
        )

    def add_into(self, dst, terms, first, size):
        step = 16

        @pl.loop(0, size // step)
        def _(i):
            at = first + i * step
            total = None
            for term, shift in terms:
                block = term[part_rows(at + shift, step), :].astype(jnp.float32)
                total = block if total is None else total + block
            dst[part_rows(at, step), :] = total.astype(dst.dtype)

    def send_a(self, lev):
        src = self.mine.at[lev * 4 + self.place.across, pl.ds(0, self.half)]
        return remote(
            src, self.from_a.at[lev], self.out_a.at[lev], self.in_a.at[lev], self.place.by_x
        )

    def send_b(self, lev):
        src = self.mine.at[lev * 4 + self.place.across, pl.ds(self.half, self.half)]
        return remote(
            src, self.from_b.at[lev], self.out_b.at[lev], self.in_b.at[lev], self.place.by_y
        )

    def send_y(self, lev):
        src = self.mine.at[lev * 4 + self.place.there_y]
        return remote(
            src, self.from_y.at[lev], self.out_y.at[lev], self.in_y.at[lev], self.place.by_y
        )

    def send_x(self, lev):
        src = self.mine.at[lev * 4 + self.place.there_x]
        return remote(
            src, self.from_x.at[lev], self.out_x.at[lev], self.in_x.at[lev], self.place.by_x
        )

    def send_up(self, lev):
        src = self.mine.at[lev * 4 + self.place.here]
        return remote(
            src, self.from_down.at[lev], self.out_z.at[lev], self.in_down.at[lev], self.place.above
        )

    def send_down(self, lev):
        src = self.mine.at[lev * 4 + self.place.here]
        return remote(
            src, self.from_up.at[lev], self.out_z.at[lev], self.in_up.at[lev], self.place.below
        )

    def make(self, lev, side, cond):
        def body():
            for spot in (self.place.across, self.place.there_y, self.place.there_x, self.place.here):
                slot = lev * 4 + spot
                self.produce(self.part, slot, self.refs)
                self.swap(slot).start()

        guarded(cond, body)

    def join(self, slot):
        self.swap(slot).wait_recv()
        mine = self.mine.at[slot]
        terms = [(mine, 0), (self.part.at[slot], self.place.core * self.rows)]
        self.add_into(mine, terms, 0, self.rows)

    def first(self, lev, side, cond):
        def body():
            self.join(lev * 4 + self.place.across)
            self.send_a(lev).start()
            self.send_b(lev).start()
            self.join(lev * 4 + self.place.there_y)
            self.join(lev * 4 + self.place.there_x)

        guarded(cond, body)

    def second(self, lev, side, cond):
        def body():
            mine = self.mine.at[lev * 4 + self.place.there_y]
            self.send_a(lev).wait_recv()
            self.add_into(mine, [(mine, 0), (self.from_a.at[lev], 0)], 0, self.half)
            self.send_y(lev).start()
            mine = self.mine.at[lev * 4 + self.place.there_x]
            self.send_b(lev).wait_recv()
            self.add_into(mine, [(mine, 0), (self.from_b.at[lev], -self.half)], self.half, self.half)
            self.send_x(lev).start()
            self.join(lev * 4 + self.place.here)

        guarded(cond, body)

    def third(self, lev, side, cond):
        rows, out = self.rows, self.out

        def body():
            mine = self.mine.at[lev * 4 + self.place.here]
            self.send_y(lev).wait_recv()
            self.send_x(lev).wait_recv()
            terms = [(mine, 0), (self.from_y.at[lev], 0), (self.from_x.at[lev], 0)]
            if side == 0:
                own = out.at[part_rows(self.place.core * rows, rows)]
                self.add_into(own, terms, 0, rows)

                @pl.when(self.has_up)
                def _():
                    self.send_down(lev).wait_recv()
                    self.add_into(own, [(own, 0), (self.from_up.at[lev], 0)], 0, rows)

                @pl.when(self.has_down)
                def _():
                    self.send_up(lev).wait_recv()
                    self.add_into(own, [(own, 0), (self.from_down.at[lev], 0)], 0, rows)
            else:
                down = side < 0
                has_more = self.has_up if down else self.has_down
                relay = self.send_down if down else self.send_up
                more = self.from_up if down else self.from_down
                self.add_into(mine, terms, 0, rows)

                @pl.when(has_more)
                def _():
                    relay(lev).wait_recv()
                    self.add_into(mine, [(mine, 0), (more.at[lev], 0)], 0, rows)

                relay(lev).start()

        guarded(cond, body)

    def begin(self):
        if self.prepare is not None:
            self.prepare(self.refs)
        self.make(*self.steps[0])

    def middle(self):
        steps, calls = self.steps, []
        for i in range(len(steps) + 2):

            def call(i=i):
                if i + 1 < len(steps):
                    self.make(*steps[i + 1])
                if i < len(steps):
                    self.first(*steps[i])
                if 0 <= i - 1 < len(steps):
                    self.second(*steps[i - 1])
                if 0 <= i - 2 < len(steps):
                    self.third(*steps[i - 2])

            calls.append(call)
        return calls

    def hand(self, whose):
        spot = part_rows(whose * self.rows, self.rows)
        return remote(self.out.at[spot], self.out.at[spot], self.out_m, self.in_m, self.place.mate)

    def end(self):
        self.hand(self.place.core).start()

        def finish(lev, side, cond):
            def body():
                for spot in range(4):
                    self.swap(lev * 4 + spot).wait_send()
                for send in (self.send_a, self.send_b, self.send_y, self.send_x):
                    send(lev).wait_send()
                if side < 0:
                    self.send_down(lev).wait_send()
                if side > 0:
                    self.send_up(lev).wait_send()

            guarded(cond, body)

        for step in self.steps:
            finish(*step)
        self.hand(self.place.core).wait_send()
        self.hand(1 - self.place.core).wait_recv()


def greet(place, ops):
    barrier = pltpu.get_barrier_semaphore()
    expected = 1

    def call(target):
        pl.semaphore_signal(barrier, inc=1, device_id=target, device_id_type=MESH)

    call(place.mate)
    if any(op.reach == 0 for op in ops):
        for j in range(1, place.groups):
            call({EXPERT: place.partner(j)})
        expected += place.groups - 1
    else:
        call(place.by_x)
        call(place.by_y)
        planes = max(op.reach for op in ops)
        level = lax.rem(place.chip // 4, planes)
        has_up, has_down = level < planes - 1, level > 0
        pl.when(has_up)(lambda: call(place.above))
        pl.when(has_down)(lambda: call(place.below))
        expected += 2 + has_up.astype(jnp.int32) + has_down.astype(jnp.int32)
    pl.semaphore_wait(barrier, expected)


def chip_kernel(ops, *refs):
    place = Place()
    n_in = sum(len(op.ins) for op in ops)
    n_out = sum(len(op.outs) for op in ops)
    ins, outs, scratch = refs[:n_in], refs[n_in : n_in + n_out], refs[n_in + n_out :]
    for op in ops:
        op.bind(place, ins[: len(op.ins)], outs[: len(op.outs)], scratch[: len(op.scratch)])
        ins, outs = ins[len(op.ins) :], outs[len(op.outs) :]
        scratch = scratch[len(op.scratch) :]
    greet(place, ops)
    for op in ops:
        op.begin()
    queues = [op.middle() for op in ops]
    for i in range(max(len(q) for q in queues)):
        for queue in queues:
            if i < len(queue):
                queue[i]()
    ended = [op.gains for op in ops if isinstance(op, NormGather)]
    for op in ops:
        if op not in ended:
            op.end()


def exchange(ops, ident):
    ins = [pair for op in ops for pair in op.ins]
    outs = [pair for op in ops for pair in op.outs]
    moved = sum(a.size * a.dtype.itemsize for a, _ in ins + outs)
    results = pl.pallas_call(
        functools.partial(chip_kernel, ops),
        out_shape=[shape for shape, _ in outs],
        in_specs=[pl.BlockSpec(memory_space=space) for _, space in ins],
        out_specs=[pl.BlockSpec(memory_space=space) for _, space in outs],
        scratch_shapes=[entry for op in ops for entry in op.scratch],
        compiler_params=pltpu.CompilerParams(
            collective_id=ident, has_side_effects=True, vmem_limit_bytes=60 << 20
        ),
        cost_estimate=pl.CostEstimate(flops=0, bytes_accessed=moved, transcendentals=0),
    )(*[a for a, _ in ins])
    split = []
    for op in ops:
        split.append(results[: len(op.outs)])
        results = results[len(op.outs) :]
    return split


def general_scores(query_blk, key_rows, first_row):
    scores = jnp.einsum(
        "qhd,khd->hqk", query_blk, key_rows, preferred_element_type=jnp.float32
    ) * DQK ** (-0.5)
    row_pos = first_row + jnp.arange(query_blk.shape[0], dtype=jnp.int32)
    col_pos = jnp.arange(key_rows.shape[0], dtype=jnp.int32)
    return jnp.where(col_pos[None, None, :] <= row_pos[None, :, None], scores, -1e30)


def attend(query_rows, key_rows, value_rows):
    seq_len = query_rows.shape[0]
    blk_rows = min(seq_len, 512)

    def one_block(block_index):
        first_row = block_index * blk_rows
        scores = general_scores(query_rows, key_rows, first_row)
        row_max = jnp.max(scores, axis=-1, keepdims=True)
        log_total = row_max + jnp.log(jnp.sum(jnp.exp(scores - row_max), axis=-1, keepdims=True))
        att_weights = jnp.exp(scores - log_total).astype(jnp.bfloat16)
        mixed_blk = jnp.einsum(
            "hqk,khd->qhd", att_weights, value_rows, preferred_element_type=jnp.float32
        ).astype(jnp.bfloat16)
        return (mixed_blk, log_total)

    mixed_heads, log_totals = lax.map(one_block, jnp.arange(seq_len // blk_rows, dtype=jnp.int32))
    return (mixed_heads.reshape(seq_len, query_rows.shape[1], value_rows.shape[2]), log_totals)


def attend_back(query_rows, key_rows, value_rows, log_totals, mixed_grad):
    seq_len, head_count = (query_rows.shape[0], query_rows.shape[1])
    blk_rows = min(seq_len, 512)

    def one_block(running, block_index):
        key_acc, value_acc = running
        first_row = block_index * blk_rows
        scores = general_scores(query_rows, key_rows, first_row)
        att_probs = jnp.exp(scores - log_totals[block_index])
        att_weights = att_probs.astype(jnp.bfloat16)
        value_acc = value_acc + jnp.einsum(
            "hqk,qhd->khd", att_weights, mixed_grad, preferred_element_type=jnp.float32
        )
        prob_grad = jnp.einsum(
            "qhd,khd->hqk", mixed_grad, value_rows, preferred_element_type=jnp.float32
        )
        row_delta = jnp.sum(att_probs * prob_grad, axis=-1, keepdims=True)
        score_delta = (att_probs * (prob_grad - row_delta) * DQK ** (-0.5)).astype(jnp.bfloat16)
        query_grad = jnp.einsum(
            "hqk,khd->qhd", score_delta, key_rows, preferred_element_type=jnp.float32
        )
        key_acc = key_acc + jnp.einsum(
            "hqk,qhd->khd", score_delta, query_rows, preferred_element_type=jnp.float32
        )
        return ((key_acc, value_acc), query_grad)

    zero_start = (
        jnp.zeros((seq_len, head_count, DQK), jnp.float32),
        jnp.zeros((seq_len, head_count, DV), jnp.float32),
    )
    (key_grad, value_grad), query_grad = lax.scan(
        one_block, zero_start, jnp.arange(seq_len // blk_rows, dtype=jnp.int32)
    )
    return (query_grad.reshape(seq_len, head_count, DQK), key_grad, value_grad)


def attention_forward(seq_in, gain_one, query_w, latent_w, gain_kv, kvup_w):
    seq_len = seq_in.shape[0]
    head_count = query_w.shape[1] // DQK
    cosine, sine_part = rope_tables(seq_len, DR)
    stat_one = rms_scale(seq_in)
    unit_one = seq_in * stat_one
    normed1 = (unit_one * gain_one.astype(jnp.float32)).astype(jnp.bfloat16)
    query_full = jnp.dot(normed1, query_w, preferred_element_type=jnp.float32).reshape(
        seq_len, head_count, DQK
    )
    query_rows = jnp.concatenate(
        [
            query_full[..., :DN],
            rotate(query_full[..., DN:], cosine[:, None, :], sine_part[:, None, :]),
        ],
        axis=-1,
    ).astype(jnp.bfloat16)
    latent_full = jnp.dot(normed1, latent_w, preferred_element_type=jnp.float32)
    latent_stat = rms_scale(latent_full[:, : kvup_w.shape[0]])
    latent_unit = latent_full[:, : kvup_w.shape[0]] * latent_stat
    latent = (latent_unit * gain_kv.astype(jnp.float32)).astype(jnp.bfloat16)
    rot_key = rotate(latent_full[:, kvup_w.shape[0] :], cosine, sine_part).astype(jnp.bfloat16)
    key_value = (
        jnp.dot(latent, kvup_w, preferred_element_type=jnp.float32)
        .astype(jnp.bfloat16)
        .reshape(seq_len, head_count, DN + DV)
    )
    key_rows = jnp.concatenate(
        [key_value[..., :DN], jnp.broadcast_to(rot_key[:, None, :], (seq_len, head_count, DR))],
        axis=-1,
    )
    value_rows = key_value[..., DN:]
    mixed_heads, log_totals = attend(query_rows, key_rows, value_rows)
    return (
        stat_one,
        unit_one,
        normed1,
        query_rows,
        latent_stat,
        latent_unit,
        latent,
        key_rows,
        value_rows,
        mixed_heads,
        log_totals,
        cosine,
        sine_part,
    )


def general(
    layer_in,
    norm1_gain,
    q_weight,
    kva_weight,
    kv_gain,
    kvb_weight,
    o_weight,
    norm2_gain,
    router_weight,
    shared_gate,
    shared_up,
    shared_down,
    expert_gate,
    expert_up,
    expert_down,
    routes,
    out_grad,
):
    groups = lax.axis_size(EXPERT)
    seq_len, width = layer_in.shape
    local_experts = expert_gate.shape[0]
    expert_count = local_experts * groups
    capacity = seq_len * TOPK * 4 // (3 * expert_count)
    rows_total = expert_count * capacity
    (
        gain_one,
        query_w,
        latent_w,
        gain_kv,
        kvup_w,
        output_w,
        gain_two,
        route_w,
        gate_sh,
        up_sh,
        down_sh,
    ) = (
        lax.all_gather(norm1_gain, EXPERT, axis=0, tiled=True),
        lax.all_gather(q_weight, EXPERT, axis=0, tiled=True),
        lax.all_gather(kva_weight, EXPERT, axis=0, tiled=True),
        lax.all_gather(kv_gain, EXPERT, axis=0, tiled=True),
        lax.all_gather(kvb_weight, EXPERT, axis=0, tiled=True),
        lax.all_gather(o_weight, EXPERT, axis=1, tiled=True),
        lax.all_gather(norm2_gain, EXPERT, axis=0, tiled=True),
        lax.all_gather(router_weight, EXPERT, axis=0, tiled=True),
        lax.all_gather(shared_gate, EXPERT, axis=0, tiled=True),
        lax.all_gather(shared_up, EXPERT, axis=0, tiled=True),
        lax.all_gather(shared_down, EXPERT, axis=1, tiled=True),
    )
    (
        stat_one,
        unit_one,
        normed1,
        query_rows,
        latent_stat,
        latent_unit,
        latent,
        key_rows,
        value_rows,
        mixed_heads,
        log_totals,
        cosine,
        sine_part,
    ) = attention_forward(layer_in, gain_one, query_w, latent_w, gain_kv, kvup_w)
    head_count = query_rows.shape[1]
    mixed_flat = mixed_heads.reshape(seq_len, head_count * DV)
    attn_part = jnp.dot(mixed_flat, output_w, preferred_element_type=jnp.float32)
    hidden_state = layer_in + lax.psum(attn_part, TENSOR)
    stat_two = rms_scale(hidden_state)
    unit_two = hidden_state * stat_two
    normed2 = (unit_two * gain_two.astype(jnp.float32)).astype(jnp.bfloat16)
    router_probs = jax.nn.softmax(
        jnp.dot(normed2, route_w, preferred_element_type=jnp.float32), axis=-1
    )
    route_onehot = (
        routes[:, :, None] == jnp.arange(expert_count, dtype=jnp.int32)[None, None, :]
    ).astype(jnp.float32)
    route_weight = jnp.einsum("tke,te->tk", route_onehot, router_probs)
    flat_hot = route_onehot.reshape(seq_len * TOPK, expert_count).astype(jnp.int32)
    slot_pos = jnp.sum(jnp.cumsum(flat_hot, axis=0) * flat_hot, axis=-1) - 1
    buffer_pos = routes.reshape(-1) * capacity + slot_pos

    def to_owners(assigned):
        buffer = jnp.zeros((rows_total, width), jnp.bfloat16).at[buffer_pos].set(assigned)
        buffer = buffer.reshape(groups, local_experts * capacity, width)
        arrived = lax.all_to_all(buffer, EXPERT, split_axis=0, concat_axis=0, tiled=True)
        return (
            arrived.reshape(groups, local_experts, capacity, width)
            .transpose(1, 0, 2, 3)
            .reshape(local_experts, groups * capacity, width)
        )

    def to_sources(results):
        arranged = (
            results.reshape(local_experts, groups, capacity, width)
            .transpose(1, 0, 2, 3)
            .reshape(groups, local_experts * capacity, width)
        )
        arrived = lax.all_to_all(arranged, EXPERT, split_axis=0, concat_axis=0, tiled=True)
        return arrived.reshape(rows_total, width)[buffer_pos].reshape(seq_len, TOPK, width)

    rows_in = to_owners(jnp.repeat(normed2, TOPK, axis=0))
    pre_gate = jnp.einsum("emd,edf->emf", rows_in, expert_gate, preferred_element_type=jnp.float32)
    pre_up = jnp.einsum("emd,edf->emf", rows_in, expert_up, preferred_element_type=jnp.float32)
    expert_act = (jax.nn.silu(pre_gate) * pre_up).astype(jnp.bfloat16)
    block_out = jnp.einsum(
        "emf,efd->emd", expert_act, expert_down, preferred_element_type=jnp.float32
    ).astype(jnp.bfloat16)
    expert_out = to_sources(block_out)
    routed_part = jnp.einsum(
        "tk,tkd->td", route_weight, expert_out, preferred_element_type=jnp.float32
    )
    shared_pre_gate = jnp.dot(normed2, gate_sh, preferred_element_type=jnp.float32)
    shared_pre_up = jnp.dot(normed2, up_sh, preferred_element_type=jnp.float32)
    shared_act = (jax.nn.silu(shared_pre_gate) * shared_pre_up).astype(jnp.bfloat16)
    shared_part = jnp.dot(shared_act, down_sh, preferred_element_type=jnp.float32)
    layer_out = hidden_state + lax.psum(
        (routed_part + shared_part).astype(jnp.bfloat16), TENSOR
    ).astype(jnp.float32)
    out_rows = out_grad.astype(jnp.bfloat16)
    routed_cot = (
        (route_weight[:, :, None] * out_grad[:, None, :])
        .astype(jnp.bfloat16)
        .reshape(seq_len * TOPK, width)
    )
    cot_in = to_owners(routed_cot)
    route_grad_part = jnp.einsum(
        "tkd,td->tk", expert_out, out_grad, preferred_element_type=jnp.float32
    )
    hidden_grad_ex = jnp.einsum(
        "emd,efd->emf", cot_in, expert_down, preferred_element_type=jnp.float32
    )
    gate_delta = (hidden_grad_ex * pre_up * silu_grad(pre_gate)).astype(jnp.bfloat16)
    up_delta = (hidden_grad_ex * jax.nn.silu(pre_gate)).astype(jnp.bfloat16)
    expert_down_grad = jnp.einsum(
        "emf,emd->efd", expert_act, cot_in, preferred_element_type=jnp.float32
    )
    expert_gate_grad = jnp.einsum(
        "emd,emf->edf", rows_in, gate_delta, preferred_element_type=jnp.float32
    )
    expert_up_grad = jnp.einsum(
        "emd,emf->edf", rows_in, up_delta, preferred_element_type=jnp.float32
    )
    row_block = (
        jnp.einsum("emf,edf->emd", gate_delta, expert_gate, preferred_element_type=jnp.float32)
        + jnp.einsum("emf,edf->emd", up_delta, expert_up, preferred_element_type=jnp.float32)
    ).astype(jnp.bfloat16)
    row_grad = to_sources(row_block)
    shared_down_grad = jnp.dot(shared_act.T, out_rows, preferred_element_type=jnp.float32)
    shared_hidden_grad = jnp.dot(out_rows, down_sh.T, preferred_element_type=jnp.float32)
    shared_gate_delta = (shared_hidden_grad * shared_pre_up * silu_grad(shared_pre_gate)).astype(
        jnp.bfloat16
    )
    shared_up_delta = (shared_hidden_grad * jax.nn.silu(shared_pre_gate)).astype(jnp.bfloat16)
    shared_gate_grad = jnp.dot(normed2.T, shared_gate_delta, preferred_element_type=jnp.float32)
    shared_up_grad = jnp.dot(normed2.T, shared_up_delta, preferred_element_type=jnp.float32)
    normed2_part = (
        jnp.sum(row_grad, axis=1, dtype=jnp.float32)
        + jnp.dot(shared_gate_delta, gate_sh.T, preferred_element_type=jnp.float32)
        + jnp.dot(shared_up_delta, up_sh.T, preferred_element_type=jnp.float32)
    )
    normed2_grad, route_grad = lax.psum((normed2_part, route_grad_part), TENSOR)
    prob_grad = jnp.einsum("tk,tke->te", route_grad, route_onehot)
    logit_delta = (
        router_probs * (prob_grad - jnp.sum(router_probs * prob_grad, axis=-1, keepdims=True))
    ).astype(jnp.bfloat16)
    router_grad = jnp.dot(normed2.T, logit_delta, preferred_element_type=jnp.float32)
    normed2_grad = normed2_grad + jnp.dot(
        logit_delta, route_w.T, preferred_element_type=jnp.float32
    )
    norm2_gain_grad = jnp.sum(normed2_grad * unit_two, axis=0)
    scaled_two = normed2_grad * gain_two.astype(jnp.float32)
    hidden_grad = out_grad + stat_two * (
        scaled_two - unit_two * jnp.mean(scaled_two * unit_two, axis=-1, keepdims=True)
    )
    hidden_rows = hidden_grad.astype(jnp.bfloat16)
    o_grad = jnp.dot(mixed_flat.T, hidden_rows, preferred_element_type=jnp.float32)
    mixed_grad = (
        jnp.dot(hidden_rows, output_w.T, preferred_element_type=jnp.float32)
        .astype(jnp.bfloat16)
        .reshape(seq_len, head_count, DV)
    )
    query_grad, key_grad, value_grad = attend_back(
        query_rows, key_rows, value_rows, log_totals, mixed_grad
    )
    query_delta = (
        jnp.concatenate(
            [
                query_grad[..., :DN],
                rotate_back(query_grad[..., DN:], cosine[:, None, :], sine_part[:, None, :]),
            ],
            axis=-1,
        )
        .astype(jnp.bfloat16)
        .reshape(seq_len, head_count * DQK)
    )
    kv_delta = (
        jnp.concatenate([key_grad[..., :DN], value_grad], axis=-1)
        .astype(jnp.bfloat16)
        .reshape(seq_len, head_count * (DN + DV))
    )
    q_grad = jnp.dot(normed1.T, query_delta, preferred_element_type=jnp.float32)
    kvb_grad = jnp.dot(latent.T, kv_delta, preferred_element_type=jnp.float32)
    latent_part = jnp.dot(kv_delta, kvup_w.T, preferred_element_type=jnp.float32)
    rot_part = jnp.sum(key_grad[..., DN:], axis=1)
    normed1_part = jnp.dot(query_delta, query_w.T, preferred_element_type=jnp.float32)
    latent_grad, rot_sum, normed1_query = (
        lax.psum(latent_part.astype(jnp.bfloat16), TENSOR).astype(jnp.float32),
        lax.psum(rot_part.astype(jnp.bfloat16), TENSOR).astype(jnp.float32),
        lax.psum(normed1_part.astype(jnp.bfloat16), TENSOR).astype(jnp.float32),
    )
    kv_gain_grad = jnp.sum(latent_grad * latent_unit, axis=0)
    scaled_lat = latent_grad * gain_kv.astype(jnp.float32)
    latent_back = latent_stat * (
        scaled_lat - latent_unit * jnp.mean(scaled_lat * latent_unit, axis=-1, keepdims=True)
    )
    latent_delta = jnp.concatenate(
        [latent_back, rotate_back(rot_sum, cosine, sine_part)], axis=-1
    ).astype(jnp.bfloat16)
    kva_grad = jnp.dot(normed1.T, latent_delta, preferred_element_type=jnp.float32)
    normed1_grad = normed1_query + jnp.dot(
        latent_delta, latent_w.T, preferred_element_type=jnp.float32
    )
    norm1_gain_grad = jnp.sum(normed1_grad * unit_one, axis=0)
    scaled_one = normed1_grad * gain_one.astype(jnp.float32)
    x_grad = hidden_grad + stat_one * (
        scaled_one - unit_one * jnp.mean(scaled_one * unit_one, axis=-1, keepdims=True)
    )
    (
        norm1_gain_grad,
        q_grad,
        kva_grad,
        kv_gain_grad,
        kvb_grad,
        o_grad,
        norm2_gain_grad,
        router_grad,
        shared_gate_grad,
        shared_up_grad,
        shared_down_grad,
    ) = (
        lax.psum_scatter(norm1_gain_grad, EXPERT, scatter_dimension=0, tiled=True),
        lax.psum_scatter(q_grad, EXPERT, scatter_dimension=0, tiled=True),
        lax.psum_scatter(kva_grad, EXPERT, scatter_dimension=0, tiled=True),
        lax.psum_scatter(kv_gain_grad, EXPERT, scatter_dimension=0, tiled=True),
        lax.psum_scatter(kvb_grad, EXPERT, scatter_dimension=0, tiled=True),
        lax.psum_scatter(o_grad, EXPERT, scatter_dimension=1, tiled=True),
        lax.psum_scatter(norm2_gain_grad, EXPERT, scatter_dimension=0, tiled=True),
        lax.psum_scatter(router_grad, EXPERT, scatter_dimension=0, tiled=True),
        lax.psum_scatter(shared_gate_grad, EXPERT, scatter_dimension=0, tiled=True),
        lax.psum_scatter(shared_up_grad, EXPERT, scatter_dimension=0, tiled=True),
        lax.psum_scatter(shared_down_grad, EXPERT, scatter_dimension=1, tiled=True),
    )
    return (
        layer_out,
        x_grad,
        norm1_gain_grad,
        q_grad,
        kva_grad,
        kv_gain_grad,
        kvb_grad,
        o_grad,
        norm2_gain_grad,
        router_grad,
        shared_gate_grad,
        shared_up_grad,
        shared_down_grad,
        expert_gate_grad,
        expert_up_grad,
        expert_down_grad,
    )


def fits(groups, heads, block, width):
    return groups % heads == 0 and heads % 4 == 0 and block % 64 == 0 and 4 * groups * block * width <= 24 << 20


def masked_scores(query_rows, key_rows):
    scores = fsum("sqd,skd->sqk", query_rows, key_rows) * DQK ** (-0.5)
    places = jnp.arange(query_rows.shape[1], dtype=jnp.int32)
    return jnp.where(places[None, None, :] <= places[None, :, None], scores, -1e30)


def to_blocks(grad_rows, groups):
    rows, width = grad_rows.shape
    return grad_rows.reshape(rows, groups, width // groups).transpose(1, 0, 2).astype(jnp.bfloat16)


def from_blocks(blocks):
    groups, rows, width = blocks.shape
    return blocks.transpose(1, 0, 2).reshape(rows, groups * width)


def widen(rows, width):
    return jnp.pad(rows, [(0, 0)] * (rows.ndim - 1) + [(0, width - rows.shape[-1])])


def by_heads(
    layer_in,
    norm1_gain,
    q_weight,
    kva_weight,
    kv_gain,
    kvb_weight,
    o_weight,
    norm2_gain,
    router_weight,
    shared_gate,
    shared_up,
    shared_down,
    expert_gate,
    expert_up,
    expert_down,
    routes,
    out_grad,
):
    groups = lax.axis_size(EXPERT)
    chip = lax.axis_index(EXPERT)
    seq_len, width = layer_in.shape
    capacity = seq_len * TOPK * 4 // (3 * groups)
    heads = q_weight.shape[1] // DQK
    copies = groups // heads
    head = lax.rem(chip, heads)
    own_cols = kva_weight.shape[0]
    lat_rows, lat_width = kvb_weight.shape[0], kvb_weight.shape[0] * groups
    hidden = shared_gate.shape[1] // groups
    bf16 = jnp.bfloat16

    kv_block = lat_rows * (DN + DV) // own_cols
    head_parts = jnp.concatenate(
        [
            q_weight.reshape(own_cols, heads, DQK).transpose(1, 2, 0),
            kvb_weight.reshape(lat_rows, heads, DN + DV)
            .transpose(1, 0, 2)
            .reshape(heads, kv_block, own_cols),
            o_weight.reshape(heads, DV, own_cols),
        ],
        axis=1,
    )
    shared_parts = jnp.concatenate(
        [
            shared_gate.reshape(own_cols, groups, hidden).transpose(1, 2, 0),
            shared_up.reshape(own_cols, groups, hidden).transpose(1, 2, 0),
            shared_down.reshape(groups, hidden, own_cols),
        ],
        axis=1,
    )
    small = jnp.concatenate(
        [
            router_weight.T,
            norm1_gain[None, :],
            norm2_gain[None, :],
            widen(kv_gain[None, :], own_cols),
        ],
        axis=0,
    )
    small = jnp.pad(small, [(0, -small.shape[0] % 16), (0, 0)])
    at_kv = DQK
    at_o = at_kv + kv_block
    at_gate = at_o + DV
    planes, all_planes = heads // 4, groups // 4
    small_swap = Swap(jnp.broadcast_to(small[None], (groups,) + small.shape), True)
    (small_all,), (got,), (latent_w,), (normed1_all,) = exchange(
        [
            small_swap,
            Swap(jnp.tile(head_parts, (copies, 1, 1))),
            Gather([kva_weight], all_planes),
            NormGather(layer_in, small_swap, groups, planes),
        ],
        1,
    )
    query_wt = from_blocks(got[:, :at_kv])
    kvup_w = got[:, at_kv:at_o].reshape(lat_width, DN + DV)
    output_w = from_blocks(got[:, at_o:at_gate])
    route_wt = from_blocks(small_all[:, :groups])
    gain_one = small_all[:, groups].reshape(width).astype(jnp.float32)
    gain_two = small_all[:, groups + 1].reshape(width).astype(jnp.float32)
    gain_kv = small_all[:, groups + 2, :lat_rows].reshape(lat_width).astype(jnp.float32)
    latent_w = latent_w.reshape(width, kva_weight.shape[1])
    stat_one = rms_scale(layer_in)
    unit_one = layer_in * stat_one
    normed1_all = normed1_all.reshape(heads * seq_len, width)

    cosine, sine_part = rope_tables(seq_len, DR)
    by_seq = (heads, seq_len, -1)
    query_full = fsum("td,qd->tq", normed1_all, query_wt).reshape(by_seq)
    query_rows = jnp.concatenate(
        [query_full[..., :DN], rotate(query_full[..., DN:], cosine, sine_part)], axis=-1
    ).astype(bf16)
    latent_full = fdot(normed1_all, latent_w)
    latent_stat = rms_scale(latent_full[:, :lat_width])
    latent_unit = latent_full[:, :lat_width] * latent_stat
    latent = (latent_unit * gain_kv).astype(bf16)
    rot_key = rotate(latent_full[:, lat_width:].reshape(by_seq), cosine, sine_part).astype(bf16)
    key_value = fdot(latent, kvup_w).astype(bf16).reshape(by_seq)
    key_rows = jnp.concatenate([key_value[..., :DN], rot_key], axis=-1)
    value_rows = key_value[..., DN:]
    scores = masked_scores(query_rows, key_rows)
    row_max = jnp.max(scores, axis=-1, keepdims=True)
    log_totals = row_max + jnp.log(jnp.sum(jnp.exp(scores - row_max), axis=-1, keepdims=True))
    att_probs = jnp.exp(scores - log_totals)
    att_weights = att_probs.astype(bf16)
    mixed = fsum("sqk,skd->sqd", att_weights, value_rows).astype(bf16)
    mixed_flat = mixed.reshape(heads * seq_len, DV)
    out_rows = out_grad.astype(bf16)

    def attn_part(part, slot, refs):
        product = fdot(refs[0][slot], refs[1][...])
        part[slot] = product.astype(bf16)

    (shared_got,), (out_all,), (attn_sum,) = exchange(
        [
            Swap(shared_parts),
            Gather([out_rows], all_planes),
            Reduce([mixed, output_w], attn_part, heads, seq_len, width),
        ],
        2,
    )
    gate_sht = from_blocks(shared_got[:, :hidden])
    up_sht = from_blocks(shared_got[:, hidden : 2 * hidden])
    down_sh = from_blocks(shared_got[:, 2 * hidden :])
    out_flat = out_all.reshape(groups * seq_len, width)
    hidden_state = layer_in + attn_sum

    stat_two = rms_scale(hidden_state)
    unit_two = hidden_state * stat_two
    normed2 = (unit_two * gain_two).astype(bf16)
    router_probs = jax.nn.softmax(fsum("td,ed->te", normed2, route_wt), axis=-1)
    experts = jnp.arange(groups, dtype=jnp.int32)
    chosen = jnp.any(routes[:, :, None] == experts[None, None, :], axis=1)
    marked = widen(jnp.where(chosen, router_probs, -1.0), -(-groups // LANES) * LANES)
    ((normed2_all, marked_all),) = exchange([Gather([normed2, marked], all_planes)], 3)
    here = lax.dynamic_index_in_dim(marked_all, chip, 2, keepdims=False)
    normed2_flat = normed2_all.reshape(groups * seq_len, width)

    routed = here >= 0.0
    order = jnp.cumsum(routed.astype(jnp.int32), axis=1) - 1
    slots = jnp.arange(capacity, dtype=jnp.int32)
    picks = (routed[:, None, :] & (order[:, None, :] == slots[None, :, None])).astype(bf16)
    weight_rows = jnp.sum(picks.astype(jnp.float32) * here[:, None, :], axis=-1).reshape(-1, 1)
    rows_in = fsum("skt,std->skd", picks, normed2_all).astype(bf16).reshape(-1, width)
    grad_rows = fsum("skt,std->skd", picks, out_all).reshape(-1, width)
    cot_in = (weight_rows * grad_rows).astype(bf16)
    gate_w, up_w, down_w = expert_gate[0], expert_up[0], expert_down[0]
    pre_gate = fdot(rows_in, gate_w)
    pre_up = fdot(rows_in, up_w)
    expert_act = (jax.nn.silu(pre_gate) * pre_up).astype(bf16)
    block_out = fdot(expert_act, down_w).astype(bf16).astype(jnp.float32)
    hidden_grad_ex = fsum("md,fd->mf", cot_in, down_w)
    gate_delta = (hidden_grad_ex * pre_up * silu_grad(pre_gate)).astype(bf16)
    up_delta = (hidden_grad_ex * jax.nn.silu(pre_gate)).astype(bf16)
    expert_down_grad = fsum("mf,md->fd", expert_act, cot_in)[None]
    expert_gate_grad = fsum("md,mf->df", rows_in, gate_delta)[None]
    expert_up_grad = fsum("md,mf->df", rows_in, up_delta)[None]
    row_block = (
        fsum("mf,df->md", gate_delta, gate_w) + fsum("mf,df->md", up_delta, up_w)
    ).astype(bf16)
    route_grad_rows = jnp.sum(grad_rows * block_out, axis=-1).reshape(groups, capacity)
    by_slot = (groups, capacity, width)
    out_block = (weight_rows * block_out).astype(bf16).reshape(by_slot)
    route_grad = jnp.sum(picks.astype(jnp.float32) * route_grad_rows[:, :, None], axis=1)
    route_part = (route_grad[:, :, None] * (experts == chip)).astype(bf16)
    route_part = widen(route_part, marked.shape[1])

    shared_pre_gate = fsum("fd,td->ft", gate_sht, normed2_flat)
    shared_pre_up = fsum("fd,td->ft", up_sht, normed2_flat)
    shared_act = (jax.nn.silu(shared_pre_gate) * shared_pre_up).astype(bf16)
    shared_hidden_grad = fsum("fd,td->ft", down_sh, out_flat)
    shared_gate_delta = (shared_hidden_grad * shared_pre_up * silu_grad(shared_pre_gate)).astype(bf16)
    shared_up_delta = (shared_hidden_grad * jax.nn.silu(shared_pre_gate)).astype(bf16)
    shared_grads = jnp.concatenate(
        [
            to_blocks(fdot(shared_gate_delta, normed2_flat), groups),
            to_blocks(fdot(shared_up_delta, normed2_flat), groups),
            to_blocks(fdot(shared_act, out_flat), groups),
        ],
        axis=1,
    )
    room = -(-hidden // 16) * 16

    def stacked(pieces):
        return jnp.concatenate(
            [jnp.pad(x, [(0, room - hidden)] + [(0, 0)] * (x.ndim - 1)) for x in pieces], axis=0
        )

    def left_side(pieces):
        rows = stacked(pieces).reshape(-1, groups, seq_len).transpose(1, 0, 2)
        return jnp.concatenate([picks, rows], axis=1)

    def expert_parts(part, slot, refs):
        for k, start in ((0, 0), (1, width)):
            left, own, held = refs[k], refs[2 + k], refs[7 + k]
            held[:capacity] = own[slot]
            for col in range(0, width, 512):
                product = lax.dot_general(
                    left[slot],
                    held[:, col : col + 512],
                    (((0,), (0,)), ((), ())),
                    preferred_element_type=jnp.float32,
                )
                part[slot, :, start + col : start + col + 512] = product.astype(bf16)
        part[slot, :, 2 * width :] = refs[6][slot]

    def hold_shared(refs):
        refs[7][capacity:] = refs[4][...]
        refs[8][capacity:] = refs[5][...]

    ((summed,),) = exchange(
        [
            Reduce(
                [
                    left_side([shared_act]),
                    left_side([shared_gate_delta, shared_up_delta]),
                    out_block,
                    row_block.reshape(by_slot),
                    stacked([down_sh]),
                    stacked([gate_sht, up_sht]),
                    route_part,
                ],
                expert_parts,
                groups,
                seq_len,
                2 * width + marked.shape[1],
                [
                    pltpu.VMEM((capacity + room, width), bf16),
                    pltpu.VMEM((capacity + 2 * room, width), bf16),
                ],
                hold_shared,
            )
        ],
        4,
    )
    layer_out = hidden_state + summed[:, :width]
    prob_grad = summed[:, 2 * width : 2 * width + groups]
    logit_delta = (
        router_probs * (prob_grad - jnp.sum(router_probs * prob_grad, axis=-1, keepdims=True))
    ).astype(bf16)
    normed2_grad = summed[:, width : 2 * width] + fdot(logit_delta, route_wt)
    router_gradt = fsum("te,td->ed", logit_delta, normed2)
    norm2_gain_grad = jnp.sum(normed2_grad * unit_two, axis=0)
    scaled_two = normed2_grad * gain_two
    hidden_grad = out_grad + stat_two * (
        scaled_two - unit_two * jnp.mean(scaled_two * unit_two, axis=-1, keepdims=True)
    )

    hidden_rows = hidden_grad.astype(bf16)
    ((hidden_all,),) = exchange([Gather([hidden_rows], planes)], 5)
    hidden_all = hidden_all.reshape(heads * seq_len, width)
    o_grad = fdot(lax.optimization_barrier(mixed_flat.T), hidden_all)
    mixed_grad = fsum("td,vd->tv", hidden_all, output_w).astype(bf16).reshape(by_seq)
    value_grad = fsum("sqk,sqd->skd", att_weights, mixed_grad)
    dprob = fsum("sqd,skd->sqk", mixed_grad, value_rows)
    row_delta = jnp.sum(att_probs * dprob, axis=-1, keepdims=True)
    score_delta = (att_probs * (dprob - row_delta) * DQK ** (-0.5)).astype(bf16)
    query_grad = fsum("sqk,skd->sqd", score_delta, key_rows)
    key_grad = fsum("sqk,sqd->skd", score_delta, query_rows)
    query_delta = (
        jnp.concatenate(
            [query_grad[..., :DN], rotate_back(query_grad[..., DN:], cosine, sine_part)], axis=-1
        )
        .astype(bf16)
    )
    kv_delta = (
        jnp.concatenate([key_grad[..., :DN], value_grad], axis=-1)
        .astype(bf16)
    )

    def back_part(part, slot, refs):
        for col in range(0, width, 512):
            product = fdot(refs[0][slot], refs[1][:, col : col + 512])
            part[slot, :, col : col + 512] = product.astype(bf16)
        product = fdot(refs[2][slot], refs[3][...])
        part[slot, :, width : width + lat_width] = product.astype(bf16)
        part[slot, :, width + lat_width :] = refs[4][slot]

    (owned_early,), (back,) = exchange(
        [
            Swap(jnp.concatenate([shared_grads, to_blocks(o_grad, groups)], axis=1)),
            Reduce(
                [
                    query_delta,
                    query_wt,
                    kv_delta,
                    kvup_w.T,
                    widen(key_grad[..., DN:], LANES).astype(bf16),
                ],
                back_part,
                heads,
                seq_len,
                width + lat_width + LANES,
            ),
        ],
        6,
    )
    normed1_query = back[:, :width]
    latent_grad = back[:, width : width + lat_width]
    rot_sum = back[:, width + lat_width : width + lat_width + DR]

    def own_rows(rows):
        return lax.dynamic_slice_in_dim(rows, head * seq_len, seq_len, 0)

    own_unit, own_stat = own_rows(latent_unit), own_rows(latent_stat)
    kv_gain_grad = jnp.sum(latent_grad * own_unit, axis=0)
    scaled_lat = latent_grad * gain_kv
    latent_back = own_stat * (
        scaled_lat - own_unit * jnp.mean(scaled_lat * own_unit, axis=-1, keepdims=True)
    )
    latent_delta = jnp.concatenate(
        [latent_back, rotate_back(rot_sum, cosine, sine_part)], axis=-1
    ).astype(bf16)
    query_delta_t = lax.optimization_barrier(query_delta.reshape(heads * seq_len, DQK).T)
    kv_flat = kv_delta.reshape(heads * seq_len, DN + DV)
    latent_t = lax.optimization_barrier(latent.T)
    (owned_heads,), (latent_delta_all,) = exchange(
        [
            Swap(
                jnp.concatenate(
                    [
                        to_blocks(fdot(query_delta_t, normed1_all), groups),
                        fdot(latent_t, kv_flat).astype(bf16).reshape(groups, kv_block, own_cols),
                    ],
                    axis=1,
                )
            ),
            Gather([latent_delta], planes),
        ],
        7,
    )
    latent_delta_all = latent_delta_all.reshape(heads * seq_len, -1)
    normed1_grad = normed1_query + fsum("tl,dl->td", latent_delta, latent_w)
    norm1_gain_grad = jnp.sum(normed1_grad * unit_one, axis=0)
    scaled_one = normed1_grad * gain_one
    x_grad = hidden_grad + stat_one * (
        scaled_one - unit_one * jnp.mean(scaled_one * unit_one, axis=-1, keepdims=True)
    )

    share = latent_delta_all.shape[1] // heads
    latent_share = lax.dynamic_slice_in_dim(latent_delta_all, head * share, share, 1)
    kva_blocks = to_blocks(fdot(lax.optimization_barrier(latent_share.T), normed1_all), groups)

    def by_owner(row):
        return widen(row.reshape(groups, 1, -1), own_cols)

    small_grads = jnp.concatenate(
        [
            router_gradt.reshape(groups, groups, own_cols).transpose(1, 0, 2),
            by_owner(norm1_gain_grad),
            by_owner(norm2_gain_grad),
            by_owner(kv_gain_grad),
        ],
        axis=1,
    )
    small_grads = jnp.pad(small_grads, [(0, 0), (0, -small_grads.shape[1] % 8), (0, 0)])
    kva_blocks = jnp.pad(kva_blocks, [(0, 0), (0, -share % 16), (0, 0)])
    (owned_share,), (owned_small,) = exchange([Swap(kva_blocks), Swap(small_grads)], 8)
    small_sums = jnp.sum(owned_small, axis=0)

    def over_copies(blocks):
        blocks = blocks.astype(jnp.float32).reshape((copies, heads) + blocks.shape[1:])
        return jnp.sum(blocks, axis=0)

    of_heads = over_copies(owned_heads)
    q_grad = of_heads[:, :at_kv].transpose(2, 0, 1).reshape(own_cols, heads * DQK)
    kvb_grad = (
        of_heads[:, at_kv:]
        .reshape(heads, lat_rows, DN + DV)
        .transpose(1, 0, 2)
        .reshape(lat_rows, heads * (DN + DV))
    )
    own_o_grad = over_copies(owned_early[:, 3 * hidden :]).reshape(heads * DV, own_cols)
    kva_grad = over_copies(owned_share)[:, :share].reshape(heads * share, own_cols).T
    of_shared = owned_early[:, : 3 * hidden].astype(jnp.float32)

    def columns(blocks):
        return blocks.reshape(groups * hidden, own_cols)

    shared_gate_grad = columns(of_shared[:, :hidden]).T
    shared_up_grad = columns(of_shared[:, hidden : 2 * hidden]).T
    shared_down_grad = columns(of_shared[:, 2 * hidden :])
    router_grad = small_sums[:groups].T
    return (
        layer_out,
        x_grad,
        small_sums[groups],
        q_grad,
        kva_grad,
        small_sums[groups + 2, :lat_rows],
        kvb_grad,
        own_o_grad,
        small_sums[groups + 1],
        router_grad,
        shared_gate_grad,
        shared_up_grad,
        shared_down_grad,
        expert_gate_grad,
        expert_up_grad,
        expert_down_grad,
    )


def on_device(layer_in, *rest):
    groups, heads = lax.axis_size(EXPERT), rest[1].shape[1] // DQK
    one_each = rest[11].shape[0] == 1
    if one_each and fits(groups, heads, *layer_in.shape):
        return by_heads(layer_in, *rest)
    return general(layer_in, *rest)


def solution(mesh):
    in_specs = (
        P(EXPERT, None),
        P(EXPERT),
        P(EXPERT, TENSOR),
        P(EXPERT, None),
        P(EXPERT),
        P(EXPERT, TENSOR),
        P(TENSOR, EXPERT),
        P(EXPERT),
        P(EXPERT, None),
        P(EXPERT, TENSOR),
        P(EXPERT, TENSOR),
        P(TENSOR, EXPERT),
        P(EXPERT, None, TENSOR),
        P(EXPERT, None, TENSOR),
        P(EXPERT, TENSOR, None),
        P(EXPERT, None),
        P(EXPERT, None),
    )
    out_specs = (
        P(EXPERT, None),
        P(EXPERT, None),
        P(EXPERT),
        P(EXPERT, TENSOR),
        P(EXPERT, None),
        P(EXPERT),
        P(EXPERT, TENSOR),
        P(TENSOR, EXPERT),
        P(EXPERT),
        P(EXPERT, None),
        P(EXPERT, TENSOR),
        P(EXPERT, TENSOR),
        P(TENSOR, EXPERT),
        P(EXPERT, None, TENSOR),
        P(EXPERT, None, TENSOR),
        P(EXPERT, TENSOR, None),
    )
    return jax.shard_map(
        on_device, mesh=mesh, in_specs=in_specs, out_specs=out_specs, check_vma=False
    )
```

```python
import functools

import jax
import jax.numpy as jnp
from jax import lax
from jax.experimental import pallas as pl
from jax.experimental.pallas import tpu as pltpu
from jax.sharding import PartitionSpec as P

DN = 128
DR = 64
DQK = 192
DV = 128
TOPK = 6
LANES = 128


norm_eps = 1e-06


def rms_scale(inputs):
    return lax.rsqrt(jnp.mean(inputs * inputs, axis=-1, keepdims=True) + norm_eps)


def rope_tables(length, rot_width):
    half_width = rot_width // 2
    frequency = 10000.0 ** (-jnp.arange(half_width).astype(jnp.float32) / half_width)
    angles = jnp.arange(length).astype(jnp.float32)[:, None] * frequency[None, :]
    return (jnp.cos(angles), jnp.sin(angles))


def rotate(inputs, cosine, sine_part):
    half_width = inputs.shape[-1] // 2
    first_half = inputs[..., :half_width]
    second_half = inputs[..., half_width:]
    return jnp.concatenate(
        [
            first_half * cosine - second_half * sine_part,
            second_half * cosine + first_half * sine_part,
        ],
        axis=-1,
    )


def rotate_back(inputs, cosine, sine_part):
    return rotate(inputs, cosine, -sine_part)


def silu_grad(pre_act):
    sigmoid_val = jax.nn.sigmoid(pre_act)
    return sigmoid_val * (1.0 + pre_act * (1.0 - sigmoid_val))


def fdot(left, right):
    return jnp.dot(left, right, preferred_element_type=jnp.float32)


def dot_nt(left, right):
    return lax.dot_general(
        left, right, (((1,), (1,)), ((), ())), preferred_element_type=jnp.float32
    )


def fsum(spec, left, right):
    return jnp.einsum(spec, left, right, preferred_element_type=jnp.float32)


EXPERT, TENSOR = "expert", "tensor"
MESH = pl.DeviceIdType.MESH
DMA = pltpu.SemaphoreType.DMA


def guarded(cond, body):
    if cond is None:
        body()
    else:
        pl.when(cond)(body)


def remote(src, dst, send, recv, target):
    return pltpu.make_async_remote_copy(
        src_ref=src, dst_ref=dst, send_sem=send, recv_sem=recv, device_id=target, device_id_type=MESH
    )


def part_rows(start, size):
    return pl.ds(pl.multiple_of(start, size), size)


class Place:
    def __init__(self):
        self.groups = lax.axis_size(EXPERT)
        self.chip = lax.axis_index(EXPERT)
        self.core = lax.axis_index(TENSOR)
        self.here = lax.rem(self.chip, 4)
        self.there_x = self.here + 1 - 2 * lax.rem(self.here, 2)
        self.there_y = self.here + 2 - 4 * (self.here // 2)
        self.across = 3 - self.here
        base = self.chip - self.here
        self.by_x = {EXPERT: base + self.there_x}
        self.by_y = {EXPERT: base + self.there_y}
        self.above = {EXPERT: self.chip + 4}
        self.below = {EXPERT: self.chip - 4}
        self.mate = {TENSOR: 1 - self.core}

    def partner(self, j):
        return lax.rem(self.chip + j, self.groups)


def level_steps(level, planes, far_first):
    order = [(0, 0)] + [(d, s) for d in range(1, planes) for s in (-1, 1)]
    steps = []
    for distance, side in order[::-1] if far_first else order:
        lev = level + side * distance
        steps.append((lev, side, None if distance == 0 else ((lev >= 0) & (lev < planes))))
    return steps


class Swap:
    reach = 0

    def __init__(self, blocks, vmem_result=False, pace=2):
        groups = blocks.shape[0]
        self.pace = groups if vmem_result else pace
        self.ins = [(blocks, pltpu.VMEM)]
        self.outs = [
            (
                jax.ShapeDtypeStruct(blocks.shape, blocks.dtype),
                pltpu.VMEM if vmem_result else pl.ANY,
            )
        ]
        self.scratch = [DMA, DMA((groups,)), DMA((groups,))]

    def bind(self, place, ins, outs, scratch):
        self.place, self.groups = place, place.groups
        self.source, self.result = ins[0], outs[0]
        self.own_sem, self.send_sem, self.recv_sem = scratch

    def copy(self, j, src, dst):
        return remote(
            self.source.at[src],
            self.result.at[dst],
            self.send_sem.at[j],
            self.recv_sem.at[j],
            {EXPERT: self.place.partner(j)},
        )

    def own(self):
        chip = self.place.chip
        return pltpu.make_async_copy(self.source.at[chip], self.result.at[chip], self.own_sem)

    def send(self, first):
        for j in range(first, min(first + self.pace, self.groups)):
            self.copy(j, self.place.partner(j), self.place.chip).start()

    def begin(self):
        self.own().start()
        self.send(1)

    def middle(self):
        firsts = range(1 + self.pace, self.groups, self.pace)
        return [functools.partial(self.send, first) for first in firsts]

    def end(self):
        self.own().wait()
        for j in range(1, self.groups):
            self.copy(j, self.place.chip, self.place.partner(self.groups - j)).wait_recv()
            self.copy(j, self.place.partner(j), self.place.chip).wait_send()


class Gather:
    def __init__(self, arrays, planes):
        count, slots = len(arrays), planes * 4
        self.planes, self.count, self.reach = planes, count, planes
        self.ins = [(a, pltpu.VMEM) for a in arrays]
        self.outs = [(jax.ShapeDtypeStruct((slots,) + a.shape, a.dtype), pl.ANY) for a in arrays]
        by_level, by_slot = DMA((count, planes)), DMA((count, slots))
        self.scratch = [DMA((count,))] + [by_level] * 5 + [by_slot] + [by_level] * 6 + [by_slot]

    def bind(self, place, ins, outs, scratch):
        self.place, self.sources, self.results = place, ins, outs
        self.level = lax.rem(place.chip // 4, self.planes)
        self.has_up, self.has_down = self.level < self.planes - 1, self.level > 0
        self.own_sem = scratch[0]
        self.in_z, self.in_x, self.in_y, self.in_a, self.in_b, self.in_p = scratch[1:7]
        self.out_up, self.out_down, self.out_x, self.out_y = scratch[7:11]
        self.out_a, self.out_b, self.out_p = scratch[11:14]
        self.steps = level_steps(self.level, self.planes, False)

    def move(self, a, slot, part, send, recv, target, own=False, whose=None):
        half = self.sources[a].shape[0] // 2
        whose = self.place.core if whose is None else whose
        if part is None:
            rows = part_rows(whose * half, half)
        else:
            rows = part_rows(whose * half + part * (half // 2), half // 2)
        dst = self.results[a].at[slot, rows]
        return remote(self.sources[a].at[rows] if own else dst, dst, send, recv, target)

    def along_z(self, a, lev, own, up):
        sems = self.out_up if up else self.out_down
        target = self.place.above if up else self.place.below
        slot = lev * 4 + self.place.here
        return self.move(a, slot, None, sems.at[a, lev], self.in_z.at[a, lev], target, own)

    def along_x(self, a, lev, slot, own=False):
        return self.move(
            a, slot, None, self.out_x.at[a, lev], self.in_x.at[a, lev], self.place.by_x, own
        )

    def along_y(self, a, lev, slot, own=False):
        return self.move(
            a, slot, None, self.out_y.at[a, lev], self.in_y.at[a, lev], self.place.by_y, own
        )

    def corner_x(self, a, lev, slot):
        return self.move(
            a, slot, 0, self.out_a.at[a, lev], self.in_a.at[a, lev], self.place.by_x
        )

    def corner_y(self, a, lev, slot):
        return self.move(
            a, slot, 1, self.out_b.at[a, lev], self.in_b.at[a, lev], self.place.by_y
        )

    def share(self, a, slot, whose=None):
        return self.move(
            a, slot, None, self.out_p.at[a, slot], self.in_p.at[a, slot], self.place.mate, whose=whose
        )

    def own(self, a):
        slot = self.level * 4 + self.place.here
        return pltpu.make_async_copy(self.sources[a], self.results[a].at[slot], self.own_sem.at[a])

    def begin(self):
        for a in range(self.count):
            self.own(a).start()
        self.first(*self.steps[0])

    def first(self, lev, side, cond):
        def body():
            for a in range(self.count):
                own, slot = side == 0, lev * 4 + self.place.here
                if side != 0:
                    self.along_z(a, lev, own, True).wait_recv()
                if side <= 0:
                    pl.when(self.has_up)(lambda a=a: self.along_z(a, lev, own, True).start())
                if side >= 0:
                    pl.when(self.has_down)(lambda a=a: self.along_z(a, lev, own, False).start())
                self.along_x(a, lev, slot, own).start()
                self.along_y(a, lev, slot, own).start()
                if side != 0:
                    self.share(a, slot).start()

        guarded(cond, body)

    def second(self, lev, side, cond):
        def body():
            for a in range(self.count):
                slot = lev * 4 + self.place.there_y
                self.along_y(a, lev, slot).wait_recv()
                self.corner_x(a, lev, slot).start()
                self.share(a, slot).start()
                slot = lev * 4 + self.place.there_x
                self.along_x(a, lev, slot).wait_recv()
                self.corner_y(a, lev, slot).start()
                self.share(a, slot).start()

        guarded(cond, body)

    def third(self, lev, side, cond):
        def body():
            for a in range(self.count):
                slot = lev * 4 + self.place.across
                self.corner_x(a, lev, slot).wait_recv()
                self.corner_y(a, lev, slot).wait_recv()
                self.share(a, slot).start()

        guarded(cond, body)

    def middle(self):
        steps, calls = self.steps, []
        for i in range(1, len(steps) + 2):

            def call(i=i):
                if i < len(steps):
                    self.first(*steps[i])
                if 0 <= i - 1 < len(steps):
                    self.second(*steps[i - 1])
                if 0 <= i - 2 < len(steps):
                    self.third(*steps[i - 2])

            calls.append(call)
        return calls

    def end(self):
        place = self.place

        def finish(lev, side, cond):
            def body():
                for a in range(self.count):
                    own, slot = side == 0, lev * 4 + place.here
                    if side <= 0:
                        pl.when(self.has_up)(
                            lambda a=a: self.along_z(a, lev, own, True).wait_send()
                        )
                    if side >= 0:
                        pl.when(self.has_down)(
                            lambda a=a: self.along_z(a, lev, own, False).wait_send()
                        )
                    self.along_x(a, lev, slot, own).wait_send()
                    self.along_y(a, lev, slot, own).wait_send()
                    self.corner_x(a, lev, lev * 4 + place.there_y).wait_send()
                    self.corner_y(a, lev, lev * 4 + place.there_x).wait_send()
                    spots = [] if side == 0 else [slot]
                    for other in (place.there_y, place.there_x, place.across):
                        spots.append(lev * 4 + other)
                    for spot in spots:
                        self.share(a, spot).wait_send()
                        self.share(a, spot, 1 - place.core).wait_recv()

            guarded(cond, body)

        for step in self.steps:
            finish(*step)
        for a in range(self.count):
            self.own(a).wait()


class NormGather(Gather):
    def __init__(self, rows, gains, gain_row, planes):
        super().__init__([jax.ShapeDtypeStruct(rows.shape, jnp.bfloat16)], planes)
        self.ins = [(rows, pltpu.VMEM)]
        self.scratch = self.scratch + [pltpu.VMEM(rows.shape, jnp.bfloat16)]
        self.gains, self.gain_row = gains, gain_row

    def bind(self, place, ins, outs, scratch):
        super().bind(place, [scratch[-1]], outs, scratch[:-1])
        self.rows = ins[0]

    def begin(self):
        self.gains.end()
        rows = self.rows[...]
        stat = lax.rsqrt(jnp.mean(rows * rows, axis=-1, keepdims=True) + norm_eps)
        cols = rows.shape[1] // self.place.groups
        for j in range(self.place.groups):
            at = slice(j * cols, (j + 1) * cols)
            gain = self.gains.result[j, self.gain_row : self.gain_row + 1, :].astype(jnp.float32)
            self.sources[0][:, at] = (rows[:, at] * stat * gain).astype(jnp.bfloat16)
        super().begin()


class Reduce:
    def __init__(
        self, operands, produce, slots, block, width, scratch=(), prepare=None, extra=(), prelude=None
    ):
        planes, rows, kind = slots // 4, block // 2, jnp.bfloat16
        self.planes, self.reach = planes, planes
        self.ins = [(a, pltpu.VMEM) for a in operands]
        self.outs = [(jax.ShapeDtypeStruct((block, width), jnp.float32), pltpu.VMEM)]
        self.outs += [(shape, pltpu.VMEM) for shape in extra]
        self.own_scratch, self.produce, self.prepare = len(scratch), produce, prepare
        self.prelude = prelude
        by_level = DMA((planes,))
        self.scratch = (
            list(scratch)
            + [pltpu.VMEM((slots, block, width), kind), pltpu.VMEM((slots, rows, width), kind)]
            + [pltpu.VMEM((planes, rows // 2, width), kind)] * 2
            + [pltpu.VMEM((planes, rows, width), kind)] * 4
            + [DMA((slots,))]
            + [by_level] * 6
            + [DMA, DMA((slots,))]
            + [by_level] * 5
            + [DMA]
        )

    def bind(self, place, ins, outs, scratch):
        self.place, self.out = place, outs[0]
        self.refs = list(ins) + list(outs[1:]) + list(scratch[: self.own_scratch])
        scratch = scratch[self.own_scratch :]
        self.part, self.mine = scratch[:2]
        self.from_a, self.from_b, self.from_x, self.from_y = scratch[2:6]
        self.from_up, self.from_down = scratch[6:8]
        self.in_p, self.in_a, self.in_b, self.in_x, self.in_y = scratch[8:13]
        self.in_up, self.in_down, self.in_m, self.out_p = scratch[13:17]
        self.out_a, self.out_b, self.out_x, self.out_y, self.out_z, self.out_m = scratch[17:]
        self.level = lax.rem(place.chip // 4, self.planes)
        self.has_up, self.has_down = self.level < self.planes - 1, self.level > 0
        self.steps = level_steps(self.level, self.planes, True)
        self.rows = self.part.shape[1] // 2
        self.half = self.rows // 2

    def swap(self, slot):
        theirs = part_rows((1 - self.place.core) * self.rows, self.rows)
        return remote(
            self.part.at[slot, theirs],
            self.mine.at[slot],
            self.out_p.at[slot],
            self.in_p.at[slot],
            self.place.mate,
        )

    def add_into(self, dst, terms, first, size):
        step = 16

        @pl.loop(0, size // step)
        def _(i):
            at = first + i * step
            total = None
            for term, shift in terms:
                block = term[part_rows(at + shift, step), :].astype(jnp.float32)
                total = block if total is None else total + block
            dst[part_rows(at, step), :] = total.astype(dst.dtype)

    def send_a(self, lev):
        src = self.mine.at[lev * 4 + self.place.across, pl.ds(0, self.half)]
        return remote(
            src, self.from_a.at[lev], self.out_a.at[lev], self.in_a.at[lev], self.place.by_x
        )

    def send_b(self, lev):
        src = self.mine.at[lev * 4 + self.place.across, pl.ds(self.half, self.half)]
        return remote(
            src, self.from_b.at[lev], self.out_b.at[lev], self.in_b.at[lev], self.place.by_y
        )

    def send_y(self, lev):
        src = self.mine.at[lev * 4 + self.place.there_y]
        return remote(
            src, self.from_y.at[lev], self.out_y.at[lev], self.in_y.at[lev], self.place.by_y
        )

    def send_x(self, lev):
        src = self.mine.at[lev * 4 + self.place.there_x]
        return remote(
            src, self.from_x.at[lev], self.out_x.at[lev], self.in_x.at[lev], self.place.by_x
        )

    def send_up(self, lev):
        src = self.mine.at[lev * 4 + self.place.here]
        return remote(
            src, self.from_down.at[lev], self.out_z.at[lev], self.in_down.at[lev], self.place.above
        )

    def send_down(self, lev):
        src = self.mine.at[lev * 4 + self.place.here]
        return remote(
            src, self.from_up.at[lev], self.out_z.at[lev], self.in_up.at[lev], self.place.below
        )

    def make(self, lev, side, cond):
        def body():
            for spot in (self.place.across, self.place.there_y, self.place.there_x, self.place.here):
                slot = lev * 4 + spot
                self.produce(self.part, slot, self.refs)
                self.swap(slot).start()

        guarded(cond, body)

    def join(self, slot):
        self.swap(slot).wait_recv()
        mine = self.mine.at[slot]
        terms = [(mine, 0), (self.part.at[slot], self.place.core * self.rows)]
        self.add_into(mine, terms, 0, self.rows)

    def first(self, lev, side, cond):
        def body():
            self.join(lev * 4 + self.place.across)
            self.send_a(lev).start()
            self.send_b(lev).start()
            self.join(lev * 4 + self.place.there_y)
            self.join(lev * 4 + self.place.there_x)

        guarded(cond, body)

    def second(self, lev, side, cond):
        def body():
            mine = self.mine.at[lev * 4 + self.place.there_y]
            self.send_a(lev).wait_recv()
            self.add_into(mine, [(mine, 0), (self.from_a.at[lev], 0)], 0, self.half)
            self.send_y(lev).start()
            mine = self.mine.at[lev * 4 + self.place.there_x]
            self.send_b(lev).wait_recv()
            self.add_into(mine, [(mine, 0), (self.from_b.at[lev], -self.half)], self.half, self.half)
            self.send_x(lev).start()
            self.join(lev * 4 + self.place.here)

        guarded(cond, body)

    def third(self, lev, side, cond):
        rows, out = self.rows, self.out

        def body():
            mine = self.mine.at[lev * 4 + self.place.here]
            self.send_y(lev).wait_recv()
            self.send_x(lev).wait_recv()
            terms = [(mine, 0), (self.from_y.at[lev], 0), (self.from_x.at[lev], 0)]
            if side == 0:
                own = out.at[part_rows(self.place.core * rows, rows)]
                self.add_into(own, terms, 0, rows)

                @pl.when(self.has_up)
                def _():
                    self.send_down(lev).wait_recv()
                    self.add_into(own, [(own, 0), (self.from_up.at[lev], 0)], 0, rows)

                @pl.when(self.has_down)
                def _():
                    self.send_up(lev).wait_recv()
                    self.add_into(own, [(own, 0), (self.from_down.at[lev], 0)], 0, rows)
            else:
                down = side < 0
                has_more = self.has_up if down else self.has_down
                relay = self.send_down if down else self.send_up
                more = self.from_up if down else self.from_down
                self.add_into(mine, terms, 0, rows)

                @pl.when(has_more)
                def _():
                    relay(lev).wait_recv()
                    self.add_into(mine, [(mine, 0), (more.at[lev], 0)], 0, rows)

                relay(lev).start()

        guarded(cond, body)

    def begin(self):
        if self.prepare is not None:
            self.prepare(self.refs)
        if self.prelude is None:
            self.make(*self.steps[0])

    def middle(self):
        steps, calls = self.steps, []
        if self.prelude is not None:
            calls += self.prelude(self.refs)
            calls.append(lambda: self.make(*steps[0]))
        for i in range(len(steps) + 2):

            def call(i=i):
                if i + 1 < len(steps):
                    self.make(*steps[i + 1])
                if i < len(steps):
                    self.first(*steps[i])
                if 0 <= i - 1 < len(steps):
                    self.second(*steps[i - 1])
                if 0 <= i - 2 < len(steps):
                    self.third(*steps[i - 2])

            calls.append(call)
        return calls

    def hand(self, whose):
        spot = part_rows(whose * self.rows, self.rows)
        return remote(self.out.at[spot], self.out.at[spot], self.out_m, self.in_m, self.place.mate)

    def end(self):
        self.hand(self.place.core).start()

        def finish(lev, side, cond):
            def body():
                for spot in range(4):
                    self.swap(lev * 4 + spot).wait_send()
                for send in (self.send_a, self.send_b, self.send_y, self.send_x):
                    send(lev).wait_send()
                if side < 0:
                    self.send_down(lev).wait_send()
                if side > 0:
                    self.send_up(lev).wait_send()

            guarded(cond, body)

        for step in self.steps:
            finish(*step)
        self.hand(self.place.core).wait_send()
        self.hand(1 - self.place.core).wait_recv()


def greet(place, ops):
    barrier = pltpu.get_barrier_semaphore()
    expected = 1

    def call(target):
        pl.semaphore_signal(barrier, inc=1, device_id=target, device_id_type=MESH)

    call(place.mate)
    if any(op.reach == 0 for op in ops):
        for j in range(1, place.groups):
            call({EXPERT: place.partner(j)})
        expected += place.groups - 1
    else:
        call(place.by_x)
        call(place.by_y)
        planes = max(op.reach for op in ops)
        level = lax.rem(place.chip // 4, planes)
        has_up, has_down = level < planes - 1, level > 0
        pl.when(has_up)(lambda: call(place.above))
        pl.when(has_down)(lambda: call(place.below))
        expected += 2 + has_up.astype(jnp.int32) + has_down.astype(jnp.int32)
    pl.semaphore_wait(barrier, expected)


def chip_kernel(ops, *refs):
    place = Place()
    n_in = sum(len(op.ins) for op in ops)
    n_out = sum(len(op.outs) for op in ops)
    ins, outs, scratch = refs[:n_in], refs[n_in : n_in + n_out], refs[n_in + n_out :]
    for op in ops:
        op.bind(place, ins[: len(op.ins)], outs[: len(op.outs)], scratch[: len(op.scratch)])
        ins, outs = ins[len(op.ins) :], outs[len(op.outs) :]
        scratch = scratch[len(op.scratch) :]
    greet(place, ops)
    for op in ops:
        op.begin()
    queues = [op.middle() for op in ops]
    for i in range(max(len(q) for q in queues)):
        for queue in queues:
            if i < len(queue):
                queue[i]()
    ended = [op.gains for op in ops if isinstance(op, NormGather)]
    for op in ops:
        if op not in ended:
            op.end()


def exchange(ops, ident):
    ins = [pair for op in ops for pair in op.ins]
    outs = [pair for op in ops for pair in op.outs]
    moved = sum(a.size * a.dtype.itemsize for a, _ in ins + outs)
    results = pl.pallas_call(
        functools.partial(chip_kernel, ops),
        out_shape=[shape for shape, _ in outs],
        in_specs=[pl.BlockSpec(memory_space=space) for _, space in ins],
        out_specs=[pl.BlockSpec(memory_space=space) for _, space in outs],
        scratch_shapes=[entry for op in ops for entry in op.scratch],
        compiler_params=pltpu.CompilerParams(
            collective_id=ident, has_side_effects=True, vmem_limit_bytes=60 << 20
        ),
        cost_estimate=pl.CostEstimate(flops=0, bytes_accessed=moved, transcendentals=0),
    )(*[a for a, _ in ins])
    split = []
    for op in ops:
        split.append(results[: len(op.outs)])
        results = results[len(op.outs) :]
    return split


def general_scores(query_blk, key_rows, first_row):
    scores = jnp.einsum(
        "qhd,khd->hqk", query_blk, key_rows, preferred_element_type=jnp.float32
    ) * DQK ** (-0.5)
    row_pos = first_row + jnp.arange(query_blk.shape[0], dtype=jnp.int32)
    col_pos = jnp.arange(key_rows.shape[0], dtype=jnp.int32)
    return jnp.where(col_pos[None, None, :] <= row_pos[None, :, None], scores, -1e30)


def attend(query_rows, key_rows, value_rows):
    seq_len = query_rows.shape[0]
    blk_rows = min(seq_len, 512)

    def one_block(block_index):
        first_row = block_index * blk_rows
        scores = general_scores(query_rows, key_rows, first_row)
        row_max = jnp.max(scores, axis=-1, keepdims=True)
        log_total = row_max + jnp.log(jnp.sum(jnp.exp(scores - row_max), axis=-1, keepdims=True))
        att_weights = jnp.exp(scores - log_total).astype(jnp.bfloat16)
        mixed_blk = jnp.einsum(
            "hqk,khd->qhd", att_weights, value_rows, preferred_element_type=jnp.float32
        ).astype(jnp.bfloat16)
        return (mixed_blk, log_total)

    mixed_heads, log_totals = lax.map(one_block, jnp.arange(seq_len // blk_rows, dtype=jnp.int32))
    return (mixed_heads.reshape(seq_len, query_rows.shape[1], value_rows.shape[2]), log_totals)


def attend_back(query_rows, key_rows, value_rows, log_totals, mixed_grad):
    seq_len, head_count = (query_rows.shape[0], query_rows.shape[1])
    blk_rows = min(seq_len, 512)

    def one_block(running, block_index):
        key_acc, value_acc = running
        first_row = block_index * blk_rows
        scores = general_scores(query_rows, key_rows, first_row)
        att_probs = jnp.exp(scores - log_totals[block_index])
        att_weights = att_probs.astype(jnp.bfloat16)
        value_acc = value_acc + jnp.einsum(
            "hqk,qhd->khd", att_weights, mixed_grad, preferred_element_type=jnp.float32
        )
        prob_grad = jnp.einsum(
            "qhd,khd->hqk", mixed_grad, value_rows, preferred_element_type=jnp.float32
        )
        row_delta = jnp.sum(att_probs * prob_grad, axis=-1, keepdims=True)
        score_delta = (att_probs * (prob_grad - row_delta) * DQK ** (-0.5)).astype(jnp.bfloat16)
        query_grad = jnp.einsum(
            "hqk,khd->qhd", score_delta, key_rows, preferred_element_type=jnp.float32
        )
        key_acc = key_acc + jnp.einsum(
            "hqk,qhd->khd", score_delta, query_rows, preferred_element_type=jnp.float32
        )
        return ((key_acc, value_acc), query_grad)

    zero_start = (
        jnp.zeros((seq_len, head_count, DQK), jnp.float32),
        jnp.zeros((seq_len, head_count, DV), jnp.float32),
    )
    (key_grad, value_grad), query_grad = lax.scan(
        one_block, zero_start, jnp.arange(seq_len // blk_rows, dtype=jnp.int32)
    )
    return (query_grad.reshape(seq_len, head_count, DQK), key_grad, value_grad)


def attention_forward(seq_in, gain_one, query_w, latent_w, gain_kv, kvup_w):
    seq_len = seq_in.shape[0]
    head_count = query_w.shape[1] // DQK
    cosine, sine_part = rope_tables(seq_len, DR)
    stat_one = rms_scale(seq_in)
    unit_one = seq_in * stat_one
    normed1 = (unit_one * gain_one.astype(jnp.float32)).astype(jnp.bfloat16)
    query_full = jnp.dot(normed1, query_w, preferred_element_type=jnp.float32).reshape(
        seq_len, head_count, DQK
    )
    query_rows = jnp.concatenate(
        [
            query_full[..., :DN],
            rotate(query_full[..., DN:], cosine[:, None, :], sine_part[:, None, :]),
        ],
        axis=-1,
    ).astype(jnp.bfloat16)
    latent_full = jnp.dot(normed1, latent_w, preferred_element_type=jnp.float32)
    latent_stat = rms_scale(latent_full[:, : kvup_w.shape[0]])
    latent_unit = latent_full[:, : kvup_w.shape[0]] * latent_stat
    latent = (latent_unit * gain_kv.astype(jnp.float32)).astype(jnp.bfloat16)
    rot_key = rotate(latent_full[:, kvup_w.shape[0] :], cosine, sine_part).astype(jnp.bfloat16)
    key_value = (
        jnp.dot(latent, kvup_w, preferred_element_type=jnp.float32)
        .astype(jnp.bfloat16)
        .reshape(seq_len, head_count, DN + DV)
    )
    key_rows = jnp.concatenate(
        [key_value[..., :DN], jnp.broadcast_to(rot_key[:, None, :], (seq_len, head_count, DR))],
        axis=-1,
    )
    value_rows = key_value[..., DN:]
    mixed_heads, log_totals = attend(query_rows, key_rows, value_rows)
    return (
        stat_one,
        unit_one,
        normed1,
        query_rows,
        latent_stat,
        latent_unit,
        latent,
        key_rows,
        value_rows,
        mixed_heads,
        log_totals,
        cosine,
        sine_part,
    )


def general(
    layer_in,
    norm1_gain,
    q_weight,
    kva_weight,
    kv_gain,
    kvb_weight,
    o_weight,
    norm2_gain,
    router_weight,
    shared_gate,
    shared_up,
    shared_down,
    expert_gate,
    expert_up,
    expert_down,
    routes,
    out_grad,
):
    groups = lax.axis_size(EXPERT)
    seq_len, width = layer_in.shape
    local_experts = expert_gate.shape[0]
    expert_count = local_experts * groups
    capacity = seq_len * TOPK * 4 // (3 * expert_count)
    rows_total = expert_count * capacity
    (
        gain_one,
        query_w,
        latent_w,
        gain_kv,
        kvup_w,
        output_w,
        gain_two,
        route_w,
        gate_sh,
        up_sh,
        down_sh,
    ) = (
        lax.all_gather(norm1_gain, EXPERT, axis=0, tiled=True),
        lax.all_gather(q_weight, EXPERT, axis=0, tiled=True),
        lax.all_gather(kva_weight, EXPERT, axis=0, tiled=True),
        lax.all_gather(kv_gain, EXPERT, axis=0, tiled=True),
        lax.all_gather(kvb_weight, EXPERT, axis=0, tiled=True),
        lax.all_gather(o_weight, EXPERT, axis=1, tiled=True),
        lax.all_gather(norm2_gain, EXPERT, axis=0, tiled=True),
        lax.all_gather(router_weight, EXPERT, axis=0, tiled=True),
        lax.all_gather(shared_gate, EXPERT, axis=0, tiled=True),
        lax.all_gather(shared_up, EXPERT, axis=0, tiled=True),
        lax.all_gather(shared_down, EXPERT, axis=1, tiled=True),
    )
    (
        stat_one,
        unit_one,
        normed1,
        query_rows,
        latent_stat,
        latent_unit,
        latent,
        key_rows,
        value_rows,
        mixed_heads,
        log_totals,
        cosine,
        sine_part,
    ) = attention_forward(layer_in, gain_one, query_w, latent_w, gain_kv, kvup_w)
    head_count = query_rows.shape[1]
    mixed_flat = mixed_heads.reshape(seq_len, head_count * DV)
    attn_part = jnp.dot(mixed_flat, output_w, preferred_element_type=jnp.float32)
    hidden_state = layer_in + lax.psum(attn_part, TENSOR)
    stat_two = rms_scale(hidden_state)
    unit_two = hidden_state * stat_two
    normed2 = (unit_two * gain_two.astype(jnp.float32)).astype(jnp.bfloat16)
    router_probs = jax.nn.softmax(
        jnp.dot(normed2, route_w, preferred_element_type=jnp.float32), axis=-1
    )
    route_onehot = (
        routes[:, :, None] == jnp.arange(expert_count, dtype=jnp.int32)[None, None, :]
    ).astype(jnp.float32)
    route_weight = jnp.einsum("tke,te->tk", route_onehot, router_probs)
    flat_hot = route_onehot.reshape(seq_len * TOPK, expert_count).astype(jnp.int32)
    slot_pos = jnp.sum(jnp.cumsum(flat_hot, axis=0) * flat_hot, axis=-1) - 1
    buffer_pos = routes.reshape(-1) * capacity + slot_pos

    def to_owners(assigned):
        buffer = jnp.zeros((rows_total, width), jnp.bfloat16).at[buffer_pos].set(assigned)
        buffer = buffer.reshape(groups, local_experts * capacity, width)
        arrived = lax.all_to_all(buffer, EXPERT, split_axis=0, concat_axis=0, tiled=True)
        return (
            arrived.reshape(groups, local_experts, capacity, width)
            .transpose(1, 0, 2, 3)
            .reshape(local_experts, groups * capacity, width)
        )

    def to_sources(results):
        arranged = (
            results.reshape(local_experts, groups, capacity, width)
            .transpose(1, 0, 2, 3)
            .reshape(groups, local_experts * capacity, width)
        )
        arrived = lax.all_to_all(arranged, EXPERT, split_axis=0, concat_axis=0, tiled=True)
        return arrived.reshape(rows_total, width)[buffer_pos].reshape(seq_len, TOPK, width)

    rows_in = to_owners(jnp.repeat(normed2, TOPK, axis=0))
    pre_gate = jnp.einsum("emd,edf->emf", rows_in, expert_gate, preferred_element_type=jnp.float32)
    pre_up = jnp.einsum("emd,edf->emf", rows_in, expert_up, preferred_element_type=jnp.float32)
    expert_act = (jax.nn.silu(pre_gate) * pre_up).astype(jnp.bfloat16)
    block_out = jnp.einsum(
        "emf,efd->emd", expert_act, expert_down, preferred_element_type=jnp.float32
    ).astype(jnp.bfloat16)
    expert_out = to_sources(block_out)
    routed_part = jnp.einsum(
        "tk,tkd->td", route_weight, expert_out, preferred_element_type=jnp.float32
    )
    shared_pre_gate = jnp.dot(normed2, gate_sh, preferred_element_type=jnp.float32)
    shared_pre_up = jnp.dot(normed2, up_sh, preferred_element_type=jnp.float32)
    shared_act = (jax.nn.silu(shared_pre_gate) * shared_pre_up).astype(jnp.bfloat16)
    shared_part = jnp.dot(shared_act, down_sh, preferred_element_type=jnp.float32)
    layer_out = hidden_state + lax.psum(
        (routed_part + shared_part).astype(jnp.bfloat16), TENSOR
    ).astype(jnp.float32)
    out_rows = out_grad.astype(jnp.bfloat16)
    routed_cot = (
        (route_weight[:, :, None] * out_grad[:, None, :])
        .astype(jnp.bfloat16)
        .reshape(seq_len * TOPK, width)
    )
    cot_in = to_owners(routed_cot)
    route_grad_part = jnp.einsum(
        "tkd,td->tk", expert_out, out_grad, preferred_element_type=jnp.float32
    )
    hidden_grad_ex = jnp.einsum(
        "emd,efd->emf", cot_in, expert_down, preferred_element_type=jnp.float32
    )
    gate_delta = (hidden_grad_ex * pre_up * silu_grad(pre_gate)).astype(jnp.bfloat16)
    up_delta = (hidden_grad_ex * jax.nn.silu(pre_gate)).astype(jnp.bfloat16)
    expert_down_grad = jnp.einsum(
        "emf,emd->efd", expert_act, cot_in, preferred_element_type=jnp.float32
    )
    expert_gate_grad = jnp.einsum(
        "emd,emf->edf", rows_in, gate_delta, preferred_element_type=jnp.float32
    )
    expert_up_grad = jnp.einsum(
        "emd,emf->edf", rows_in, up_delta, preferred_element_type=jnp.float32
    )
    row_block = (
        jnp.einsum("emf,edf->emd", gate_delta, expert_gate, preferred_element_type=jnp.float32)
        + jnp.einsum("emf,edf->emd", up_delta, expert_up, preferred_element_type=jnp.float32)
    ).astype(jnp.bfloat16)
    row_grad = to_sources(row_block)
    shared_down_grad = jnp.dot(shared_act.T, out_rows, preferred_element_type=jnp.float32)
    shared_hidden_grad = jnp.dot(out_rows, down_sh.T, preferred_element_type=jnp.float32)
    shared_gate_delta = (shared_hidden_grad * shared_pre_up * silu_grad(shared_pre_gate)).astype(
        jnp.bfloat16
    )
    shared_up_delta = (shared_hidden_grad * jax.nn.silu(shared_pre_gate)).astype(jnp.bfloat16)
    shared_gate_grad = jnp.dot(normed2.T, shared_gate_delta, preferred_element_type=jnp.float32)
    shared_up_grad = jnp.dot(normed2.T, shared_up_delta, preferred_element_type=jnp.float32)
    normed2_part = (
        jnp.sum(row_grad, axis=1, dtype=jnp.float32)
        + jnp.dot(shared_gate_delta, gate_sh.T, preferred_element_type=jnp.float32)
        + jnp.dot(shared_up_delta, up_sh.T, preferred_element_type=jnp.float32)
    )
    normed2_grad, route_grad = lax.psum((normed2_part, route_grad_part), TENSOR)
    prob_grad = jnp.einsum("tk,tke->te", route_grad, route_onehot)
    logit_delta = (
        router_probs * (prob_grad - jnp.sum(router_probs * prob_grad, axis=-1, keepdims=True))
    ).astype(jnp.bfloat16)
    router_grad = jnp.dot(normed2.T, logit_delta, preferred_element_type=jnp.float32)
    normed2_grad = normed2_grad + jnp.dot(
        logit_delta, route_w.T, preferred_element_type=jnp.float32
    )
    norm2_gain_grad = jnp.sum(normed2_grad * unit_two, axis=0)
    scaled_two = normed2_grad * gain_two.astype(jnp.float32)
    hidden_grad = out_grad + stat_two * (
        scaled_two - unit_two * jnp.mean(scaled_two * unit_two, axis=-1, keepdims=True)
    )
    hidden_rows = hidden_grad.astype(jnp.bfloat16)
    o_grad = jnp.dot(mixed_flat.T, hidden_rows, preferred_element_type=jnp.float32)
    mixed_grad = (
        jnp.dot(hidden_rows, output_w.T, preferred_element_type=jnp.float32)
        .astype(jnp.bfloat16)
        .reshape(seq_len, head_count, DV)
    )
    query_grad, key_grad, value_grad = attend_back(
        query_rows, key_rows, value_rows, log_totals, mixed_grad
    )
    query_delta = (
        jnp.concatenate(
            [
                query_grad[..., :DN],
                rotate_back(query_grad[..., DN:], cosine[:, None, :], sine_part[:, None, :]),
            ],
            axis=-1,
        )
        .astype(jnp.bfloat16)
        .reshape(seq_len, head_count * DQK)
    )
    kv_delta = (
        jnp.concatenate([key_grad[..., :DN], value_grad], axis=-1)
        .astype(jnp.bfloat16)
        .reshape(seq_len, head_count * (DN + DV))
    )
    q_grad = jnp.dot(normed1.T, query_delta, preferred_element_type=jnp.float32)
    kvb_grad = jnp.dot(latent.T, kv_delta, preferred_element_type=jnp.float32)
    latent_part = jnp.dot(kv_delta, kvup_w.T, preferred_element_type=jnp.float32)
    rot_part = jnp.sum(key_grad[..., DN:], axis=1)
    normed1_part = jnp.dot(query_delta, query_w.T, preferred_element_type=jnp.float32)
    latent_grad, rot_sum, normed1_query = (
        lax.psum(latent_part.astype(jnp.bfloat16), TENSOR).astype(jnp.float32),
        lax.psum(rot_part.astype(jnp.bfloat16), TENSOR).astype(jnp.float32),
        lax.psum(normed1_part.astype(jnp.bfloat16), TENSOR).astype(jnp.float32),
    )
    kv_gain_grad = jnp.sum(latent_grad * latent_unit, axis=0)
    scaled_lat = latent_grad * gain_kv.astype(jnp.float32)
    latent_back = latent_stat * (
        scaled_lat - latent_unit * jnp.mean(scaled_lat * latent_unit, axis=-1, keepdims=True)
    )
    latent_delta = jnp.concatenate(
        [latent_back, rotate_back(rot_sum, cosine, sine_part)], axis=-1
    ).astype(jnp.bfloat16)
    kva_grad = jnp.dot(normed1.T, latent_delta, preferred_element_type=jnp.float32)
    normed1_grad = normed1_query + jnp.dot(
        latent_delta, latent_w.T, preferred_element_type=jnp.float32
    )
    norm1_gain_grad = jnp.sum(normed1_grad * unit_one, axis=0)
    scaled_one = normed1_grad * gain_one.astype(jnp.float32)
    x_grad = hidden_grad + stat_one * (
        scaled_one - unit_one * jnp.mean(scaled_one * unit_one, axis=-1, keepdims=True)
    )
    (
        norm1_gain_grad,
        q_grad,
        kva_grad,
        kv_gain_grad,
        kvb_grad,
        o_grad,
        norm2_gain_grad,
        router_grad,
        shared_gate_grad,
        shared_up_grad,
        shared_down_grad,
    ) = (
        lax.psum_scatter(norm1_gain_grad, EXPERT, scatter_dimension=0, tiled=True),
        lax.psum_scatter(q_grad, EXPERT, scatter_dimension=0, tiled=True),
        lax.psum_scatter(kva_grad, EXPERT, scatter_dimension=0, tiled=True),
        lax.psum_scatter(kv_gain_grad, EXPERT, scatter_dimension=0, tiled=True),
        lax.psum_scatter(kvb_grad, EXPERT, scatter_dimension=0, tiled=True),
        lax.psum_scatter(o_grad, EXPERT, scatter_dimension=1, tiled=True),
        lax.psum_scatter(norm2_gain_grad, EXPERT, scatter_dimension=0, tiled=True),
        lax.psum_scatter(router_grad, EXPERT, scatter_dimension=0, tiled=True),
        lax.psum_scatter(shared_gate_grad, EXPERT, scatter_dimension=0, tiled=True),
        lax.psum_scatter(shared_up_grad, EXPERT, scatter_dimension=0, tiled=True),
        lax.psum_scatter(shared_down_grad, EXPERT, scatter_dimension=1, tiled=True),
    )
    return (
        layer_out,
        x_grad,
        norm1_gain_grad,
        q_grad,
        kva_grad,
        kv_gain_grad,
        kvb_grad,
        o_grad,
        norm2_gain_grad,
        router_grad,
        shared_gate_grad,
        shared_up_grad,
        shared_down_grad,
        expert_gate_grad,
        expert_up_grad,
        expert_down_grad,
    )


def fits(groups, heads, block, width):
    return groups % heads == 0 and heads % 4 == 0 and block % 64 == 0 and width == groups * LANES and 4 * groups * block * width <= 24 << 20


def masked_scores(query_rows, key_rows):
    scores = fsum("sqd,skd->sqk", query_rows, key_rows) * DQK ** (-0.5)
    places = jnp.arange(query_rows.shape[1], dtype=jnp.int32)
    return jnp.where(places[None, None, :] <= places[None, :, None], scores, -1e30)


def to_blocks(grad_rows, groups):
    rows, width = grad_rows.shape
    kept = lax.optimization_barrier(grad_rows.astype(jnp.bfloat16))
    return kept.reshape(rows, groups, width // groups).transpose(1, 0, 2)


def from_blocks(blocks):
    groups, rows, width = blocks.shape
    return blocks.transpose(1, 0, 2).reshape(rows, groups * width)


def widen(rows, width):
    return jnp.pad(rows, [(0, 0)] * (rows.ndim - 1) + [(0, width - rows.shape[-1])])


def by_heads(
    layer_in,
    norm1_gain,
    q_weight,
    kva_weight,
    kv_gain,
    kvb_weight,
    o_weight,
    norm2_gain,
    router_weight,
    shared_gate,
    shared_up,
    shared_down,
    expert_gate,
    expert_up,
    expert_down,
    routes,
    out_grad,
):
    groups = lax.axis_size(EXPERT)
    chip = lax.axis_index(EXPERT)
    seq_len, width = layer_in.shape
    capacity = seq_len * TOPK * 4 // (3 * groups)
    heads = q_weight.shape[1] // DQK
    copies = groups // heads
    head = lax.rem(chip, heads)
    own_cols = kva_weight.shape[0]
    lat_rows, lat_width = kvb_weight.shape[0], kvb_weight.shape[0] * groups
    hidden = shared_gate.shape[1] // groups
    bf16 = jnp.bfloat16

    kv_halves = (DN + DV) // own_cols
    kv_block = lat_rows * kv_halves
    head_parts = jnp.concatenate(
        [
            q_weight.reshape(own_cols, heads, DQK).transpose(1, 2, 0),
            kvb_weight.reshape(lat_rows, heads, kv_halves, own_cols)
            .transpose(1, 2, 0, 3)
            .reshape(heads, kv_block, own_cols),
            o_weight.reshape(heads, DV, own_cols),
        ],
        axis=1,
    )
    shared_parts = jnp.concatenate(
        [
            shared_gate.reshape(own_cols, groups, hidden).transpose(1, 2, 0),
            shared_up.reshape(own_cols, groups, hidden).transpose(1, 2, 0),
            shared_down.reshape(groups, hidden, own_cols),
        ],
        axis=1,
    )
    small = jnp.concatenate(
        [
            router_weight.T,
            norm1_gain[None, :],
            norm2_gain[None, :],
            widen(kv_gain[None, :], own_cols),
        ],
        axis=0,
    )
    small = jnp.pad(small, [(0, -small.shape[0] % 16), (0, 0)])
    at_kv = DQK
    at_o = at_kv + kv_block
    at_gate = at_o + DV
    planes, all_planes = heads // 4, groups // 4
    small_swap = Swap(jnp.broadcast_to(small[None], (groups,) + small.shape), True)
    (small_all,), (latent_w,), (got,), (normed1_all,) = exchange(
        [
            small_swap,
            Gather([kva_weight], all_planes),
            Swap(jnp.tile(head_parts, (copies, 1, 1))),
            NormGather(layer_in, small_swap, groups, planes),
        ],
        1,
    )
    query_wt = from_blocks(got[:, :at_kv])
    kvup_w = (
        got[:, at_kv:at_o]
        .reshape(groups, kv_halves, lat_rows, own_cols)
        .transpose(0, 2, 1, 3)
        .reshape(lat_width, DN + DV)
    )
    route_wt = from_blocks(small_all[:, :groups])
    gain_one = small_all[:, groups].reshape(width).astype(jnp.float32)
    gain_two = small_all[:, groups + 1].reshape(width).astype(jnp.float32)
    gain_kv = small_all[:, groups + 2, :lat_rows].reshape(lat_width).astype(jnp.float32)
    latent_w = latent_w.reshape(width, kva_weight.shape[1])
    stat_one = rms_scale(layer_in)
    unit_one = layer_in * stat_one

    cosine, sine_part = rope_tables(seq_len, DR)
    turn_cos = jnp.concatenate([cosine, cosine], axis=-1)
    turn_sin = jnp.concatenate([-sine_part, sine_part], axis=-1)
    by_seq = (heads, seq_len, -1)
    fold = 2

    def attend_forward(refs):
        rows_in, parts, lat_w, kv_gain_ref, cos_ref, sin_ref = refs[:6]
        query_out, key_out, value_out, prob_out, lat_out, latent_out, mixed_out, out_w = refs[6:14]
        query_w, kv_w = refs[14:]

        def assemble():
            for j in range(groups):
                at = slice(j * own_cols, (j + 1) * own_cols)
                query_w[:, at] = parts[j, :at_kv]
                out_w[:, at] = parts[j, at_o:at_gate]
                down = slice(j * lat_rows, (j + 1) * lat_rows)
                for half in range(kv_halves):
                    start = at_kv + half * lat_rows
                    across = slice(half * own_cols, (half + 1) * own_cols)
                    kv_w[down, across] = parts[j, start : start + lat_rows]

        def rotated(block):
            flipped = jnp.concatenate([block[:, DR // 2 :], block[:, : DR // 2]], axis=-1)
            cos_rows = jnp.concatenate([cos_ref[...]] * fold, axis=0)
            sin_rows = jnp.concatenate([sin_ref[...]] * fold, axis=0)
            return (block * cos_rows + flipped * sin_rows).astype(bf16)

        def some(first):
            rows = rows_in[first : first + fold].reshape(fold * seq_len, width)
            query = dot_nt(rows, query_w[...])
            query_plain, query_turn = query[:, :DN].astype(bf16), rotated(query[:, DN:])
            full = fdot(rows, lat_w[...])
            plain = full[:, :lat_width]
            latent = (plain * rms_scale(plain) * kv_gain_ref[...]).astype(bf16)
            key_turn = rotated(full[:, lat_width:])
            key_value = fdot(latent, kv_w[...]).astype(bf16)
            latent_out[first : first + fold] = latent.reshape(fold, seq_len, lat_width)
            lat_out[first : first + fold] = plain.reshape(fold, seq_len, lat_width)
            ahead = lax.broadcasted_iota(jnp.int32, (seq_len, seq_len), 1) > lax.broadcasted_iota(
                jnp.int32, (seq_len, seq_len), 0
            )
            for k in range(fold):
                at, seq = slice(k * seq_len, (k + 1) * seq_len), first + k
                scores = dot_nt(query_plain[at], key_value[at, :DN])
                scores += dot_nt(query_turn[at], key_turn[at])
                scores = jnp.where(ahead, -1e30, scores * DQK ** (-0.5))
                row_max = jnp.max(scores, axis=-1, keepdims=True)
                total = jnp.sum(jnp.exp(scores - row_max), axis=-1, keepdims=True)
                probs = jnp.exp(scores - (row_max + jnp.log(total)))
                values = key_value[at, DN:]
                prob_out[seq] = probs
                mixed_out[seq] = fdot(probs.astype(bf16), values).astype(bf16)
                query_out[seq, :, :DN], query_out[seq, :, DN:] = query_plain[at], query_turn[at]
                key_out[seq, :, :DN], key_out[seq, :, DN:] = key_value[at, :DN], key_turn[at]
                value_out[seq] = values

        steps = [functools.partial(some, first) for first in range(0, heads, fold)]
        return [assemble] + steps

    out_rows = out_grad.astype(bf16)

    def attn_part(part, slot, refs):
        for col in range(0, width, 512):
            product = fdot(refs[12][slot], refs[13][:, col : col + 512])
            part[slot, :, col : col + 512] = product.astype(bf16)

    def shaped(last, kind):
        return jax.ShapeDtypeStruct((heads, seq_len, last), kind)

    (out_all,), (shared_got,), attended = exchange(
        [
            Gather([out_rows], all_planes),
            Swap(shared_parts),
            Reduce(
                [normed1_all, got, latent_w, gain_kv[None, :], turn_cos, turn_sin],
                attn_part,
                heads,
                seq_len,
                width,
                [pltpu.VMEM((DQK, width), bf16), pltpu.VMEM((lat_width, DN + DV), bf16)],
                extra=[
                    shaped(DQK, bf16),
                    shaped(DQK, bf16),
                    shaped(DV, bf16),
                    shaped(seq_len, jnp.float32),
                    shaped(lat_width, jnp.float32),
                    shaped(lat_width, bf16),
                    shaped(DV, bf16),
                    jax.ShapeDtypeStruct((DV, width), bf16),
                ],
                prelude=attend_forward,
            ),
        ],
        2,
    )
    attn_sum, query_rows, key_rows, value_rows, att_probs, lat_plain, latent, mixed, output_w = (
        attended
    )
    att_weights = att_probs.astype(bf16)
    mixed_flat = mixed.reshape(heads * seq_len, DV)
    normed1_all = normed1_all.reshape(heads * seq_len, width)
    latent = latent.reshape(heads * seq_len, lat_width)

    gate_sht = from_blocks(shared_got[:, :hidden])
    up_sht = from_blocks(shared_got[:, hidden : 2 * hidden])
    down_sh = from_blocks(shared_got[:, 2 * hidden :])
    out_flat = out_all.reshape(groups * seq_len, width)
    hidden_state = layer_in + attn_sum

    stat_two = rms_scale(hidden_state)
    unit_two = hidden_state * stat_two
    normed2 = (unit_two * gain_two).astype(bf16)
    router_probs = jax.nn.softmax(fsum("td,ed->te", normed2, route_wt), axis=-1)
    experts = jnp.arange(groups, dtype=jnp.int32)
    chosen = jnp.any(routes[:, :, None] == experts[None, None, :], axis=1)
    marked = widen(jnp.where(chosen, router_probs, -1.0), -(-groups // LANES) * LANES)
    ((normed2_all, marked_all),) = exchange([Gather([normed2, marked], all_planes)], 3)
    here = lax.dynamic_index_in_dim(marked_all, chip, 2, keepdims=False)
    normed2_flat = normed2_all.reshape(groups * seq_len, width)

    routed = here >= 0.0
    order = jnp.cumsum(routed.astype(jnp.int32), axis=1) - 1
    slots = jnp.arange(capacity, dtype=jnp.int32)
    picks = (routed[:, None, :] & (order[:, None, :] == slots[None, :, None])).astype(bf16)
    weight_rows = jnp.sum(picks.astype(jnp.float32) * here[:, None, :], axis=-1).reshape(-1, 1)
    rows_in = fsum("skt,std->skd", picks, normed2_all).astype(bf16).reshape(-1, width)
    grad_rows = fsum("skt,std->skd", picks, out_all).reshape(-1, width)
    cot_in = (weight_rows * grad_rows).astype(bf16)
    gate_w, up_w, down_w = expert_gate[0], expert_up[0], expert_down[0]
    pre_gate = fdot(rows_in, gate_w)
    pre_up = fdot(rows_in, up_w)
    expert_act = (jax.nn.silu(pre_gate) * pre_up).astype(bf16)
    block_out = fdot(expert_act, down_w).astype(bf16).astype(jnp.float32)
    hidden_grad_ex = fsum("md,fd->mf", cot_in, down_w)
    gate_delta = (hidden_grad_ex * pre_up * silu_grad(pre_gate)).astype(bf16)
    up_delta = (hidden_grad_ex * jax.nn.silu(pre_gate)).astype(bf16)
    expert_down_grad = fsum("mf,md->fd", expert_act, cot_in)[None]
    expert_gate_grad = fsum("md,mf->df", rows_in, gate_delta)[None]
    expert_up_grad = fsum("md,mf->df", rows_in, up_delta)[None]
    row_block = (
        fsum("mf,df->md", gate_delta, gate_w) + fsum("mf,df->md", up_delta, up_w)
    ).astype(bf16)
    route_grad_rows = jnp.sum(grad_rows * block_out, axis=-1).reshape(groups, capacity)
    by_slot = (groups, capacity, width)
    out_block = (weight_rows * block_out).astype(bf16).reshape(by_slot)
    route_grad = jnp.sum(picks.astype(jnp.float32) * route_grad_rows[:, :, None], axis=1)
    route_part = (route_grad[:, :, None] * (experts == chip)).astype(bf16)
    route_part = widen(route_part, marked.shape[1])

    shared_pre_gate = fsum("fd,td->ft", gate_sht, normed2_flat)
    shared_pre_up = fsum("fd,td->ft", up_sht, normed2_flat)
    shared_act = (jax.nn.silu(shared_pre_gate) * shared_pre_up).astype(bf16)
    shared_hidden_grad = fsum("fd,td->ft", down_sh, out_flat)
    shared_gate_delta = (shared_hidden_grad * shared_pre_up * silu_grad(shared_pre_gate)).astype(bf16)
    shared_up_delta = (shared_hidden_grad * jax.nn.silu(shared_pre_gate)).astype(bf16)
    shared_grads = jnp.concatenate(
        [
            to_blocks(fdot(shared_gate_delta, normed2_flat), groups),
            to_blocks(fdot(shared_up_delta, normed2_flat), groups),
            to_blocks(fdot(shared_act, out_flat), groups),
        ],
        axis=1,
    )
    room = -(-hidden // 16) * 16

    def stacked(pieces):
        return jnp.concatenate(
            [jnp.pad(x, [(0, room - hidden)] + [(0, 0)] * (x.ndim - 1)) for x in pieces], axis=0
        )

    def left_side(pieces):
        rows = stacked(pieces).reshape(-1, groups, seq_len).transpose(1, 0, 2)
        return jnp.concatenate([picks, rows], axis=1)

    def expert_parts(part, slot, refs):
        for k, start in ((0, 0), (1, width)):
            left, own, held = refs[k], refs[2 + k], refs[7 + k]
            held[:capacity] = own[slot]
            for col in range(0, width, 512):
                product = lax.dot_general(
                    left[slot],
                    held[:, col : col + 512],
                    (((0,), (0,)), ((), ())),
                    preferred_element_type=jnp.float32,
                )
                part[slot, :, start + col : start + col + 512] = product.astype(bf16)
        part[slot, :, 2 * width :] = refs[6][slot]

    def hold_shared(refs):
        refs[7][capacity:] = refs[4][...]
        refs[8][capacity:] = refs[5][...]

    ((summed,),) = exchange(
        [
            Reduce(
                [
                    left_side([shared_act]),
                    left_side([shared_gate_delta, shared_up_delta]),
                    out_block,
                    row_block.reshape(by_slot),
                    stacked([down_sh]),
                    stacked([gate_sht, up_sht]),
                    route_part,
                ],
                expert_parts,
                groups,
                seq_len,
                2 * width + marked.shape[1],
                [
                    pltpu.VMEM((capacity + room, width), bf16),
                    pltpu.VMEM((capacity + 2 * room, width), bf16),
                ],
                hold_shared,
            )
        ],
        4,
    )
    layer_out = hidden_state + summed[:, :width]
    prob_grad = summed[:, 2 * width : 2 * width + groups]
    logit_delta = (
        router_probs * (prob_grad - jnp.sum(router_probs * prob_grad, axis=-1, keepdims=True))
    ).astype(bf16)
    normed2_grad = summed[:, width : 2 * width] + fdot(logit_delta, route_wt)
    router_gradt = fsum("te,td->ed", logit_delta, normed2)
    norm2_gain_grad = jnp.sum(normed2_grad * unit_two, axis=0)
    scaled_two = normed2_grad * gain_two
    hidden_grad = out_grad + stat_two * (
        scaled_two - unit_two * jnp.mean(scaled_two * unit_two, axis=-1, keepdims=True)
    )

    hidden_rows = hidden_grad.astype(bf16)
    ((hidden_all,),) = exchange([Gather([hidden_rows], planes)], 5)
    hidden_all = hidden_all.reshape(heads * seq_len, width)
    o_grad = fdot(lax.optimization_barrier(mixed_flat.T), hidden_all)
    mixed_grad = fsum("td,vd->tv", hidden_all, output_w).astype(bf16).reshape(by_seq)
    value_grad = fsum("sqk,sqd->skd", att_weights, mixed_grad)
    dprob = fsum("sqd,skd->sqk", mixed_grad, value_rows)
    row_delta = jnp.sum(att_probs * dprob, axis=-1, keepdims=True)
    score_delta = (att_probs * (dprob - row_delta) * DQK ** (-0.5)).astype(bf16)
    query_grad = fsum("sqk,skd->sqd", score_delta, key_rows)
    key_grad = fsum("sqk,sqd->skd", score_delta, query_rows)
    query_delta = (
        jnp.concatenate(
            [query_grad[..., :DN], rotate_back(query_grad[..., DN:], cosine, sine_part)], axis=-1
        )
        .astype(bf16)
    )
    kv_delta = (
        jnp.concatenate([key_grad[..., :DN], value_grad], axis=-1)
        .astype(bf16)
    )

    def back_part(part, slot, refs):
        for col in range(0, width, 512):
            product = fdot(refs[0][slot], refs[1][:, col : col + 512])
            part[slot, :, col : col + 512] = product.astype(bf16)
        product = fdot(refs[2][slot], refs[3][...])
        part[slot, :, width : width + lat_width] = product.astype(bf16)
        part[slot, :, width + lat_width :] = refs[4][slot]

    (back,), (owned_early,) = exchange(
        [
            Reduce(
                [
                    query_delta,
                    query_wt,
                    kv_delta,
                    kvup_w.T,
                    widen(key_grad[..., DN:], LANES).astype(bf16),
                ],
                back_part,
                heads,
                seq_len,
                width + lat_width + LANES,
            ),
            Swap(jnp.concatenate([shared_grads, to_blocks(o_grad, groups)], axis=1), pace=3),
        ],
        6,
    )
    normed1_query = back[:, :width]
    latent_grad = back[:, width : width + lat_width]
    rot_sum = back[:, width + lat_width : width + lat_width + DR]

    own_plain = lax.dynamic_index_in_dim(lat_plain, head, 0, keepdims=False)
    own_stat = rms_scale(own_plain)
    own_unit = own_plain * own_stat
    kv_gain_grad = jnp.sum(latent_grad * own_unit, axis=0)
    scaled_lat = latent_grad * gain_kv
    latent_back = own_stat * (
        scaled_lat - own_unit * jnp.mean(scaled_lat * own_unit, axis=-1, keepdims=True)
    )
    latent_delta = jnp.concatenate(
        [latent_back, rotate_back(rot_sum, cosine, sine_part)], axis=-1
    ).astype(bf16)
    query_delta_t = lax.optimization_barrier(query_delta.reshape(heads * seq_len, DQK).T)
    kv_flat = kv_delta.reshape(heads * seq_len, DN + DV)
    latent_t = lax.optimization_barrier(latent.T)
    kvb_blocks = (
        lax.optimization_barrier(fdot(latent_t, kv_flat).astype(bf16))
        .reshape(groups, lat_rows, kv_halves, own_cols)
        .transpose(0, 2, 1, 3)
        .reshape(groups, kv_block, own_cols)
    )
    head_grads = jnp.concatenate([to_blocks(fdot(query_delta_t, normed1_all), groups), kvb_blocks], 1)
    (latent_delta_all,), (owned_heads,) = exchange(
        [Gather([latent_delta], planes), Swap(head_grads, pace=4)], 7
    )
    latent_delta_all = latent_delta_all.reshape(heads * seq_len, -1)
    normed1_grad = normed1_query + fsum("tl,dl->td", latent_delta, latent_w)
    norm1_gain_grad = jnp.sum(normed1_grad * unit_one, axis=0)
    scaled_one = normed1_grad * gain_one
    x_grad = hidden_grad + stat_one * (
        scaled_one - unit_one * jnp.mean(scaled_one * unit_one, axis=-1, keepdims=True)
    )

    share = latent_delta_all.shape[1] // heads
    latent_share = lax.dynamic_slice_in_dim(latent_delta_all, head * share, share, 1)
    kva_blocks = to_blocks(fdot(lax.optimization_barrier(latent_share.T), normed1_all), groups)

    def by_owner(row):
        return widen(row.reshape(groups, 1, -1), own_cols)

    small_grads = jnp.concatenate(
        [
            router_gradt.reshape(groups, groups, own_cols).transpose(1, 0, 2),
            by_owner(norm1_gain_grad),
            by_owner(norm2_gain_grad),
            by_owner(kv_gain_grad),
        ],
        axis=1,
    )
    small_grads = jnp.pad(small_grads, [(0, 0), (0, -small_grads.shape[1] % 8), (0, 0)])
    kva_blocks = jnp.pad(kva_blocks, [(0, 0), (0, -share % 16), (0, 0)])
    (owned_share,), (owned_small,) = exchange([Swap(kva_blocks), Swap(small_grads)], 8)
    small_sums = jnp.sum(owned_small, axis=0)

    def over_copies(blocks):
        blocks = blocks.astype(jnp.float32).reshape((copies, heads) + blocks.shape[1:])
        return jnp.sum(blocks, axis=0)

    of_heads = over_copies(owned_heads)
    q_grad = of_heads[:, :at_kv].transpose(2, 0, 1).reshape(own_cols, heads * DQK)
    kvb_grad = (
        of_heads[:, at_kv:]
        .reshape(heads, kv_halves, lat_rows, own_cols)
        .transpose(2, 0, 1, 3)
        .reshape(lat_rows, heads * (DN + DV))
    )
    own_o_grad = over_copies(owned_early[:, 3 * hidden :]).reshape(heads * DV, own_cols)
    kva_grad = over_copies(owned_share)[:, :share].reshape(heads * share, own_cols).T
    of_shared = owned_early[:, : 3 * hidden].astype(jnp.float32)

    def columns(blocks):
        return blocks.reshape(groups * hidden, own_cols)

    shared_gate_grad = columns(of_shared[:, :hidden]).T
    shared_up_grad = columns(of_shared[:, hidden : 2 * hidden]).T
    shared_down_grad = columns(of_shared[:, 2 * hidden :])
    router_grad = small_sums[:groups].T
    return (
        layer_out,
        x_grad,
        small_sums[groups],
        q_grad,
        kva_grad,
        small_sums[groups + 2, :lat_rows],
        kvb_grad,
        own_o_grad,
        small_sums[groups + 1],
        router_grad,
        shared_gate_grad,
        shared_up_grad,
        shared_down_grad,
        expert_gate_grad,
        expert_up_grad,
        expert_down_grad,
    )


def on_device(layer_in, *rest):
    groups, heads = lax.axis_size(EXPERT), rest[1].shape[1] // DQK
    one_each = rest[11].shape[0] == 1
    if one_each and fits(groups, heads, *layer_in.shape):
        return by_heads(layer_in, *rest)
    return general(layer_in, *rest)


def solution(mesh):
    in_specs = (
        P(EXPERT, None),
        P(EXPERT),
        P(EXPERT, TENSOR),
        P(EXPERT, None),
        P(EXPERT),
        P(EXPERT, TENSOR),
        P(TENSOR, EXPERT),
        P(EXPERT),
        P(EXPERT, None),
        P(EXPERT, TENSOR),
        P(EXPERT, TENSOR),
        P(TENSOR, EXPERT),
        P(EXPERT, None, TENSOR),
        P(EXPERT, None, TENSOR),
        P(EXPERT, TENSOR, None),
        P(EXPERT, None),
        P(EXPERT, None),
    )
    out_specs = (
        P(EXPERT, None),
        P(EXPERT, None),
        P(EXPERT),
        P(EXPERT, TENSOR),
        P(EXPERT, None),
        P(EXPERT),
        P(EXPERT, TENSOR),
        P(TENSOR, EXPERT),
        P(EXPERT),
        P(EXPERT, None),
        P(EXPERT, TENSOR),
        P(EXPERT, TENSOR),
        P(TENSOR, EXPERT),
        P(EXPERT, None, TENSOR),
        P(EXPERT, None, TENSOR),
        P(EXPERT, TENSOR, None),
    )
    return jax.shard_map(
        on_device, mesh=mesh, in_specs=in_specs, out_specs=out_specs, check_vma=False
    )
```

```python
import functools

import jax
import jax.numpy as jnp
from jax import lax
from jax.experimental import pallas as pl
from jax.experimental.pallas import tpu as pltpu
from jax.sharding import PartitionSpec as P

DN = 128
DR = 64
DQK = 192
DV = 128
TOPK = 6
LANES = 128


norm_eps = 1e-06


def rms_scale(inputs):
    return lax.rsqrt(jnp.mean(inputs * inputs, axis=-1, keepdims=True) + norm_eps)


def rope_tables(length, rot_width):
    half_width = rot_width // 2
    frequency = 10000.0 ** (-jnp.arange(half_width).astype(jnp.float32) / half_width)
    angles = jnp.arange(length).astype(jnp.float32)[:, None] * frequency[None, :]
    return (jnp.cos(angles), jnp.sin(angles))


def rotate(inputs, cosine, sine_part):
    half_width = inputs.shape[-1] // 2
    first_half = inputs[..., :half_width]
    second_half = inputs[..., half_width:]
    return jnp.concatenate(
        [
            first_half * cosine - second_half * sine_part,
            second_half * cosine + first_half * sine_part,
        ],
        axis=-1,
    )


def rotate_back(inputs, cosine, sine_part):
    return rotate(inputs, cosine, -sine_part)


def silu_grad(pre_act):
    sigmoid_val = jax.nn.sigmoid(pre_act)
    return sigmoid_val * (1.0 + pre_act * (1.0 - sigmoid_val))


def fdot(left, right):
    return jnp.dot(left, right, preferred_element_type=jnp.float32)


def dot_nt(left, right):
    return lax.dot_general(
        left, right, (((1,), (1,)), ((), ())), preferred_element_type=jnp.float32
    )


def dot_tn(left, right):
    return lax.dot_general(
        left, right, (((0,), (0,)), ((), ())), preferred_element_type=jnp.float32
    )


def fsum(spec, left, right):
    return jnp.einsum(spec, left, right, preferred_element_type=jnp.float32)


EXPERT, TENSOR = "expert", "tensor"
MESH = pl.DeviceIdType.MESH
DMA = pltpu.SemaphoreType.DMA


def remote(src, dst, send, recv, target):
    return pltpu.make_async_remote_copy(
        src_ref=src, dst_ref=dst, send_sem=send, recv_sem=recv, device_id=target, device_id_type=MESH
    )


def part_rows(start, size):
    return pl.ds(pl.multiple_of(start, size), size)


class Place:
    def __init__(self):
        self.groups = lax.axis_size(EXPERT)
        self.chip = lax.axis_index(EXPERT)
        self.core = lax.axis_index(TENSOR)
        self.here = lax.rem(self.chip, 4)
        self.there_x = self.here + 1 - 2 * lax.rem(self.here, 2)
        self.there_y = self.here + 2 - 4 * (self.here // 2)
        self.across = 3 - self.here
        base = self.chip - self.here
        self.by_x = {EXPERT: base + self.there_x}
        self.by_y = {EXPERT: base + self.there_y}
        self.above = {EXPERT: self.chip + 4}
        self.below = {EXPERT: self.chip - 4}
        self.mate = {TENSOR: 1 - self.core}

    def partner(self, j):
        return lax.rem(self.chip + j, self.groups)


def level_at(level, planes, t):
    if planes < 4:
        return lax.rem(level + t, planes)
    flip = level // 2
    near = lax.rem(level + flip, 2)
    order = t + near * (1 - 2 * t) if t < 2 else t
    return order * (1 - 2 * flip) + 3 * flip


class Swap:
    reach = 0

    def __init__(self, blocks, vmem_result=False, pace=2):
        groups = blocks.shape[0]
        self.pace = groups if vmem_result else pace
        self.ins = [(blocks, pltpu.VMEM)]
        self.outs = [
            (
                jax.ShapeDtypeStruct(blocks.shape, blocks.dtype),
                pltpu.VMEM if vmem_result else pl.ANY,
            )
        ]
        self.scratch = [DMA, DMA((groups,)), DMA((groups,))]

    def bind(self, place, ins, outs, scratch):
        self.place, self.groups = place, place.groups
        self.source, self.result = ins[0], outs[0]
        self.own_sem, self.send_sem, self.recv_sem = scratch

    def copy(self, j, src, dst):
        return remote(
            self.source.at[src],
            self.result.at[dst],
            self.send_sem.at[j],
            self.recv_sem.at[j],
            {EXPERT: self.place.partner(j)},
        )

    def own(self):
        chip = self.place.chip
        return pltpu.make_async_copy(self.source.at[chip], self.result.at[chip], self.own_sem)

    def send(self, first):
        for j in range(first, min(first + self.pace, self.groups)):
            self.copy(j, self.place.partner(j), self.place.chip).start()

    def begin(self):
        self.own().start()
        self.send(1)

    def middle(self):
        firsts = range(1 + self.pace, self.groups, self.pace)
        return [functools.partial(self.send, first) for first in firsts]

    def end(self):
        self.own().wait()
        for j in range(1, self.groups):
            self.copy(j, self.place.chip, self.place.partner(self.groups - j)).wait_recv()
            self.copy(j, self.place.partner(j), self.place.chip).wait_send()


class Gather:
    def __init__(self, arrays, planes, vmem_result=False):
        count, slots = len(arrays), planes * 4
        self.planes, self.count, self.reach = planes, count, planes
        self.ins = [(a, pltpu.VMEM) for a in arrays]
        space = pltpu.VMEM if vmem_result else pl.ANY
        self.outs = [(jax.ShapeDtypeStruct((slots,) + a.shape, a.dtype), space) for a in arrays]
        by_level, by_slot = DMA((count, planes)), DMA((count, slots))
        self.scratch = [DMA((count,))] + [by_level] * 5 + [by_slot] + [by_level] * 6 + [by_slot]

    def bind(self, place, ins, outs, scratch):
        self.place, self.sources, self.results = place, ins, outs
        self.level = lax.rem(place.chip // 4, self.planes)
        self.has_up, self.has_down = self.level < self.planes - 1, self.level > 0
        self.own_sem = scratch[0]
        self.in_z, self.in_x, self.in_y, self.in_a, self.in_b, self.in_p = scratch[1:7]
        self.out_up, self.out_down, self.out_x, self.out_y = scratch[7:11]
        self.out_a, self.out_b, self.out_p = scratch[11:14]
        self.landed = False

    def move(self, a, slot, part, send, recv, target, own=False, whose=None):
        half = self.sources[a].shape[0] // 2
        whose = self.place.core if whose is None else whose
        if part is None:
            rows = part_rows(whose * half, half)
        else:
            rows = part_rows(whose * half + part * (half // 2), half // 2)
        dst = self.results[a].at[slot, rows]
        return remote(self.sources[a].at[rows] if own else dst, dst, send, recv, target)

    def along_z(self, a, lev, own, up):
        sems = self.out_up if up else self.out_down
        target = self.place.above if up else self.place.below
        slot = lev * 4 + self.place.here
        return self.move(a, slot, None, sems.at[a, lev], self.in_z.at[a, lev], target, own)

    def along_x(self, a, lev, slot, own=False):
        return self.move(
            a, slot, None, self.out_x.at[a, lev], self.in_x.at[a, lev], self.place.by_x, own
        )

    def along_y(self, a, lev, slot, own=False):
        return self.move(
            a, slot, None, self.out_y.at[a, lev], self.in_y.at[a, lev], self.place.by_y, own
        )

    def corner_x(self, a, lev, slot):
        return self.move(
            a, slot, 0, self.out_a.at[a, lev], self.in_a.at[a, lev], self.place.by_x
        )

    def corner_y(self, a, lev, slot):
        return self.move(
            a, slot, 1, self.out_b.at[a, lev], self.in_b.at[a, lev], self.place.by_y
        )

    def share(self, a, slot, whose=None):
        return self.move(
            a, slot, None, self.out_p.at[a, slot], self.in_p.at[a, slot], self.place.mate, whose=whose
        )

    def own(self, a):
        slot = self.level * 4 + self.place.here
        return pltpu.make_async_copy(self.sources[a], self.results[a].at[slot], self.own_sem.at[a])

    def begin(self):
        for a in range(self.count):
            self.own(a).start()
        self.first(0)

    def relays(self, a, t, act):
        lev = level_at(self.level, self.planes, t)
        up, down = self.has_up, self.has_down
        if t > 0:
            up, down = up & (lev < self.level), down & (lev > self.level)
        pl.when(up)(lambda: act(self.along_z(a, lev, t == 0, True)))
        pl.when(down)(lambda: act(self.along_z(a, lev, t == 0, False)))

    def first(self, t):
        lev = level_at(self.level, self.planes, t)
        for a in range(self.count):
            own, slot = t == 0, lev * 4 + self.place.here
            if not own:
                self.along_z(a, lev, own, True).wait_recv()
            self.relays(a, t, lambda copy: copy.start())
            self.along_x(a, lev, slot, own).start()
            self.along_y(a, lev, slot, own).start()
            if not own:
                self.share(a, slot).start()

    def second(self, t):
        lev = level_at(self.level, self.planes, t)
        for a in range(self.count):
            slot = lev * 4 + self.place.there_y
            self.along_y(a, lev, slot).wait_recv()
            self.corner_x(a, lev, slot).start()
            self.share(a, slot).start()
            slot = lev * 4 + self.place.there_x
            self.along_x(a, lev, slot).wait_recv()
            self.corner_y(a, lev, slot).start()
            self.share(a, slot).start()

    def third(self, t):
        lev = level_at(self.level, self.planes, t)
        for a in range(self.count):
            slot = lev * 4 + self.place.across
            self.corner_x(a, lev, slot).wait_recv()
            self.corner_y(a, lev, slot).wait_recv()
            self.share(a, slot).start()

    def advance(self, i):
        if i < self.planes:
            self.first(i)
        if 0 <= i - 1 < self.planes:
            self.second(i - 1)
        if 0 <= i - 2 < self.planes:
            self.third(i - 2)

    def middle(self):
        return [functools.partial(self.advance, i) for i in range(1, self.planes + 2)]

    def end(self):
        place = self.place
        if not self.landed:
            for t in range(self.planes):
                self.receive(t)
        for t in range(self.planes):
            lev = level_at(self.level, self.planes, t)
            for a in range(self.count):
                own, slot = t == 0, lev * 4 + place.here
                self.relays(a, t, lambda copy: copy.wait_send())
                self.along_x(a, lev, slot, own).wait_send()
                self.along_y(a, lev, slot, own).wait_send()
                self.corner_x(a, lev, lev * 4 + place.there_y).wait_send()
                self.corner_y(a, lev, lev * 4 + place.there_x).wait_send()
                for other in [place.there_y, place.there_x, place.across]:
                    self.share(a, lev * 4 + other).wait_send()
                if not own:
                    self.share(a, slot).wait_send()

    def ready(self, slot, other):
        for a in range(self.count):
            if other:
                self.share(a, slot, 1 - self.place.core).wait_recv()
            else:
                self.own(a).wait()

    def receive(self, t):
        place, lev = self.place, level_at(self.level, self.planes, t)
        self.ready(lev * 4 + place.here, t > 0)
        for spot in (place.there_y, place.there_x, place.across):
            self.ready(lev * 4 + spot, True)


class NormGather(Gather):
    def __init__(self, rows, gains, gain_row, planes):
        super().__init__([jax.ShapeDtypeStruct(rows.shape, jnp.bfloat16)], planes)
        self.ins = [(rows, pltpu.VMEM)]
        self.scratch = self.scratch + [pltpu.VMEM(rows.shape, jnp.bfloat16)]
        self.gains, self.gain_row = gains, gain_row

    def bind(self, place, ins, outs, scratch):
        super().bind(place, [scratch[-1]], outs, scratch[:-1])
        self.rows = ins[0]

    def begin(self):
        self.gains.end()
        rows = self.rows[...]
        stat = lax.rsqrt(jnp.mean(rows * rows, axis=-1, keepdims=True) + norm_eps)
        cols = rows.shape[1] // self.place.groups
        for j in range(self.place.groups):
            at = slice(j * cols, (j + 1) * cols)
            gain = self.gains.result[j, self.gain_row : self.gain_row + 1, :].astype(jnp.float32)
            self.sources[0][:, at] = (rows[:, at] * stat * gain).astype(jnp.bfloat16)
        super().begin()


class Reduce:
    def __init__(
        self, operands, produce, slots, block, width, scratch=(), prepare=None, extra=(), prelude=None, delay=0
    ):
        planes, rows, kind = slots // 4, block // 2, jnp.bfloat16
        self.planes, self.reach = planes, planes
        self.ins = [(a, pltpu.VMEM) for a in operands]
        self.outs = [(jax.ShapeDtypeStruct((block, width), jnp.float32), pltpu.VMEM)]
        self.outs += [(shape, pltpu.VMEM) for shape in extra]
        self.own_scratch, self.produce, self.prepare = len(scratch), produce, prepare
        self.prelude, self.delay = prelude, delay
        by_level = DMA((planes,))
        self.scratch = (
            list(scratch)
            + [pltpu.VMEM((slots, block, width) if produce else (8, LANES), kind)]
            + [pltpu.VMEM((slots, rows, width), kind)]
            + [pltpu.VMEM((planes, rows // 2, width), kind)] * 2
            + [pltpu.VMEM((planes, rows, width), kind)] * 4
            + [DMA((slots,))]
            + [by_level] * 6
            + [DMA, DMA((slots,))]
            + [by_level] * 5
            + [DMA]
        )

    def bind(self, place, ins, outs, scratch):
        self.place, self.out = place, outs[0]
        self.refs = list(ins) + list(outs[1:]) + list(scratch[: self.own_scratch])
        scratch = scratch[self.own_scratch :]
        self.part = scratch[0] if self.produce else ins[0]
        self.mine = scratch[1]
        self.from_a, self.from_b, self.from_x, self.from_y = scratch[2:6]
        self.from_up, self.from_down = scratch[6:8]
        self.in_p, self.in_a, self.in_b, self.in_x, self.in_y = scratch[8:13]
        self.in_up, self.in_down, self.in_m, self.out_p = scratch[13:17]
        self.out_a, self.out_b, self.out_x, self.out_y, self.out_z, self.out_m = scratch[17:]
        self.level = lax.rem(place.chip // 4, self.planes)
        self.has_up, self.has_down = self.level < self.planes - 1, self.level > 0
        self.rows = self.part.shape[1] // 2
        self.half = self.rows // 2

    def swap(self, slot):
        theirs = part_rows((1 - self.place.core) * self.rows, self.rows)
        return remote(
            self.part.at[slot, theirs],
            self.mine.at[slot],
            self.out_p.at[slot],
            self.in_p.at[slot],
            self.place.mate,
        )

    def add_into(self, dst, terms, first, size):
        step = 16

        @pl.loop(0, size // step)
        def _(i):
            at = first + i * step
            total = None
            for term, shift in terms:
                block = term[part_rows(at + shift, step), :].astype(jnp.float32)
                total = block if total is None else total + block
            dst[part_rows(at, step), :] = total.astype(dst.dtype)

    def send_a(self, lev):
        src = self.mine.at[lev * 4 + self.place.across, pl.ds(0, self.half)]
        return remote(
            src, self.from_a.at[lev], self.out_a.at[lev], self.in_a.at[lev], self.place.by_x
        )

    def send_b(self, lev):
        src = self.mine.at[lev * 4 + self.place.across, pl.ds(self.half, self.half)]
        return remote(
            src, self.from_b.at[lev], self.out_b.at[lev], self.in_b.at[lev], self.place.by_y
        )

    def send_y(self, lev):
        src = self.mine.at[lev * 4 + self.place.there_y]
        return remote(
            src, self.from_y.at[lev], self.out_y.at[lev], self.in_y.at[lev], self.place.by_y
        )

    def send_x(self, lev):
        src = self.mine.at[lev * 4 + self.place.there_x]
        return remote(
            src, self.from_x.at[lev], self.out_x.at[lev], self.in_x.at[lev], self.place.by_x
        )

    def send_up(self, lev):
        src = self.mine.at[lev * 4 + self.place.here]
        return remote(
            src, self.from_down.at[lev], self.out_z.at[lev], self.in_down.at[lev], self.place.above
        )

    def send_down(self, lev):
        src = self.mine.at[lev * 4 + self.place.here]
        return remote(
            src, self.from_up.at[lev], self.out_z.at[lev], self.in_up.at[lev], self.place.below
        )

    def plane(self, i):
        return level_at(self.level, self.planes, self.planes - 1 - i)

    def make(self, i):
        for spot in (self.place.across, self.place.there_y, self.place.there_x, self.place.here):
            slot = self.plane(i) * 4 + spot
            if self.produce is not None:
                self.produce(self.part, slot, self.refs)
            self.swap(slot).start()

    def join(self, slot):
        self.swap(slot).wait_recv()
        mine = self.mine.at[slot]
        terms = [(mine, 0), (self.part.at[slot], self.place.core * self.rows)]
        self.add_into(mine, terms, 0, self.rows)

    def first(self, i):
        lev = self.plane(i)
        self.join(lev * 4 + self.place.across)
        self.send_a(lev).start()
        self.send_b(lev).start()
        self.join(lev * 4 + self.place.there_y)
        self.join(lev * 4 + self.place.there_x)

    def second(self, i):
        lev = self.plane(i)
        mine = self.mine.at[lev * 4 + self.place.there_y]
        self.send_a(lev).wait_recv()
        self.add_into(mine, [(mine, 0), (self.from_a.at[lev], 0)], 0, self.half)
        self.send_y(lev).start()
        mine = self.mine.at[lev * 4 + self.place.there_x]
        self.send_b(lev).wait_recv()
        self.add_into(mine, [(mine, 0), (self.from_b.at[lev], -self.half)], self.half, self.half)
        self.send_x(lev).start()
        self.join(lev * 4 + self.place.here)

    def third(self, i):
        rows, out, lev = self.rows, self.out, self.plane(i)
        mine = self.mine.at[lev * 4 + self.place.here]
        self.send_y(lev).wait_recv()
        self.send_x(lev).wait_recv()
        terms = [(mine, 0), (self.from_y.at[lev], 0), (self.from_x.at[lev], 0)]
        own = i == self.planes - 1
        total = out.at[part_rows(self.place.core * rows, rows)] if own else mine
        self.add_into(total, terms, 0, rows)

        def more(cond, send, arrived):
            @pl.when(cond)
            def _():
                send(lev).wait_recv()
                self.add_into(total, [(total, 0), (arrived.at[lev], 0)], 0, rows)

        if own:
            more(self.has_up, self.send_down, self.from_up)
            more(self.has_down, self.send_up, self.from_down)
        else:
            more(self.has_up & (lev < self.level), self.send_down, self.from_up)
            more(self.has_down & (lev > self.level), self.send_up, self.from_down)
            pl.when(lev < self.level)(lambda: self.send_down(lev).start())
            pl.when(lev > self.level)(lambda: self.send_up(lev).start())

    def begin(self):
        if self.prepare is not None:
            self.prepare(self.refs)
        if self.prelude is None:
            self.make(0)

    def advance(self, i):
        if i + 1 < self.planes:
            self.make(i + 1)
        if i < self.planes:
            self.first(i)
        if 0 <= i - 1 < self.planes:
            self.second(i - 1)
        if 0 <= i - 2 < self.planes:
            self.third(i - 2)

    def middle(self):
        calls = []
        if self.prelude is not None:
            calls += [lambda: None] * self.delay + self.prelude(self.refs)
            calls.append(functools.partial(self.make, 0))
        return calls + [functools.partial(self.advance, i) for i in range(self.planes + 2)]

    def hand(self, whose):
        spot = part_rows(whose * self.rows, self.rows)
        return remote(self.out.at[spot], self.out.at[spot], self.out_m, self.in_m, self.place.mate)

    def end(self):
        self.hand(self.place.core).start()

        for i in range(self.planes):
            lev = self.plane(i)
            for spot in range(4):
                self.swap(lev * 4 + spot).wait_send()
            for send in (self.send_a, self.send_b, self.send_y, self.send_x):
                send(lev).wait_send()
            if i < self.planes - 1:
                pl.when(lev < self.level)(lambda lev=lev: self.send_down(lev).wait_send())
                pl.when(lev > self.level)(lambda lev=lev: self.send_up(lev).wait_send())
        self.hand(self.place.core).wait_send()
        self.hand(1 - self.place.core).wait_recv()


class Experts:
    def __init__(self, gather, out_all, weights, shared_w, capacity):
        slots, seq, width = out_all.shape
        hidden, room, bf16 = weights[0].shape[1], shared_w.shape[1], jnp.bfloat16
        self.gather, self.capacity, self.room, self.reach = gather, capacity, room, gather.reach
        self.slots, self.seq, self.width, self.hidden = slots, seq, width, hidden
        rows = (slots, capacity)
        turn = (room, slots * seq)

        def shape(dims, kind=bf16):
            return jax.ShapeDtypeStruct(dims, kind)

        self.ins = [(a, pl.ANY) for a in [out_all] + weights] + [(shared_w, pltpu.VMEM)]
        self.outs = [
            (shape((slots, seq, width + LANES)), pltpu.VMEM),
            (shape(rows + (width,)), pltpu.VMEM),
            (shape(rows + (seq,)), pltpu.VMEM),
            (shape(turn), pltpu.VMEM),
            (shape((3, room, width)), pltpu.VMEM),
            (shape(rows + (width,)), pl.ANY),
            (shape(rows + (width,)), pl.ANY),
        ] + [(shape(rows + (hidden,)), pltpu.VMEM)] * 3
        self.scratch = (
            [pltpu.VMEM(out_all.shape, bf16)]
            + [pltpu.VMEM(w.shape, bf16) for w in weights]
            + [pltpu.VMEM((4 * capacity, width), bf16)] * 4
            + [
                pltpu.VMEM((4 * capacity, LANES), jnp.float32),
                pltpu.VMEM((capacity + 2 * room, width), bf16),
                pltpu.VMEM((4, capacity + 2 * room, seq), bf16),
                pltpu.VMEM((3, room, width), jnp.float32),
                DMA((4,)),
                DMA((2,)),
            ]
        )

    def bind(self, place, ins, outs, scratch):
        self.place = place
        self.out_hbm, self.hbm_weights, self.shared_w = ins[0], ins[1:4], ins[4]
        self.part, self.out_block, self.picks, self.act_turn, self.shared_grads = outs[:5]
        self.rows_hbm, self.cot_hbm, self.act, self.gate_delta, self.up_delta = outs[5:]
        self.out_rows, self.gate, self.up, self.down = scratch[:4]
        self.rows, self.cot, self.grads, self.back = scratch[4:8]
        self.weight, self.held, self.left, self.total, self.load_sem, self.save_sem = scratch[8:]
        self.level = lax.rem(place.chip // 4, self.gather.planes)

    def loads(self):
        pairs = zip([self.out_hbm, *self.hbm_weights], [self.out_rows, self.gate, self.up, self.down])
        return [
            pltpu.make_async_copy(src, dst, self.load_sem.at[k]) for k, (src, dst) in enumerate(pairs)
        ]

    def saves(self, lev):
        at = pl.ds(lev * 4 * self.capacity, 4 * self.capacity)
        pairs = [(self.rows, self.rows_hbm), (self.cot, self.cot_hbm)]
        return [
            pltpu.make_async_copy(
                src.reshape(4, self.capacity, self.width), dst.at[pl.ds(lev * 4, 4)], self.save_sem.at[k]
            )
            for k, (src, dst) in enumerate(pairs)
        ]

    def begin(self):
        for load in self.loads():
            load.start()
        self.total[...] = jnp.zeros_like(self.total)
        self.held[self.capacity :] = self.shared_w[:2].reshape(2 * self.room, self.width)

    def choose(self, lev, t):
        marked, seq, cap = self.gather.results[1], self.seq, self.capacity
        below = lax.broadcasted_iota(jnp.int32, (seq, seq), 0)
        upto = (below <= lax.broadcasted_iota(jnp.int32, (seq, seq), 1)).astype(jnp.bfloat16)
        place_in = lax.broadcasted_iota(jnp.int32, (cap, seq), 0).astype(jnp.float32)
        if t > 0:
            for save in self.saves(lev):
                save.wait()
        for j in range(4):
            slot, at = lev * 4 + j, slice(j * cap, (j + 1) * cap)
            turned = marked[slot].T
            here = jnp.sum(jnp.where(below == self.place.chip, turned, 0.0), axis=0, keepdims=True)
            routed = jnp.where(here >= 0.0, 1.0, 0.0)
            order = fdot(jnp.broadcast_to(routed, (8, seq)).astype(jnp.bfloat16), upto)[:1] - 1.0
            hit = jnp.where(order == place_in, routed, 0.0)
            weight = jnp.sum(hit * here, axis=-1, keepdims=True)
            pick = hit.astype(jnp.bfloat16)
            self.picks[slot] = pick
            self.left[j, :cap] = pick
            self.weight[at] = jnp.broadcast_to(weight, (cap, LANES))
            for col in range(0, self.width, 512):
                cols = slice(col, col + 512)
                own = fdot(pick, self.gather.results[0][slot, :, cols])
                self.rows[at, cols] = own.astype(jnp.bfloat16)
                grad = fdot(pick, self.out_rows[slot, :, cols])
                self.grads[at, cols] = grad.astype(jnp.bfloat16)
                self.cot[at, cols] = (weight * grad).astype(jnp.bfloat16)
        for save in self.saves(lev):
            save.start()

    def hidden_units(self, lev):
        slots, chunk = pl.ds(lev * 4, 4), 256
        for start in range(0, self.hidden, chunk):
            cols = slice(start, min(start + chunk, self.hidden))
            shape = (4, self.capacity, cols.stop - cols.start)
            gate = fdot(self.rows[...], self.gate[:, cols])
            up = fdot(self.rows[...], self.up[:, cols])
            grad = dot_nt(self.cot[...], self.down[cols])
            sig = jax.nn.sigmoid(gate)
            gated = gate * sig
            self.act[slots, :, cols] = (gated * up).astype(jnp.bfloat16).reshape(shape)
            slope = sig * (1.0 + gate * (1.0 - sig))
            self.gate_delta[slots, :, cols] = (grad * up * slope).astype(jnp.bfloat16).reshape(shape)
            self.up_delta[slots, :, cols] = (grad * gated).astype(jnp.bfloat16).reshape(shape)

    def shared_units(self, lev):
        seq4, room = 4 * self.seq, self.room
        tokens = self.gather.results[0][pl.ds(lev * 4, 4)].reshape(seq4, self.width)
        grads = self.out_rows[pl.ds(lev * 4, 4)].reshape(seq4, self.width)
        both = dot_nt(self.shared_w[:2].reshape(2 * room, self.width), tokens)
        gate, up = both[:room], both[room:]
        grad = dot_nt(self.shared_w[2], grads)
        sig = jax.nn.sigmoid(gate)
        act = (gate * sig * up).astype(jnp.bfloat16)
        gate_delta = (grad * up * (sig * (1.0 + gate * (1.0 - sig)))).astype(jnp.bfloat16)
        up_delta = (grad * gate * sig).astype(jnp.bfloat16)
        self.act_turn[:, part_rows(lev * seq4, seq4)] = act
        for j in range(4):
            at = slice(j * self.seq, (j + 1) * self.seq)
            self.left[j, self.capacity : self.capacity + room] = gate_delta[:, at]
            self.left[j, self.capacity + room :] = up_delta[:, at]
        for col in range(0, self.width, 512):
            cols = slice(col, col + 512)
            self.total[0, :, cols] += fdot(gate_delta, tokens[:, cols])
            self.total[1, :, cols] += fdot(up_delta, tokens[:, cols])
            self.total[2, :, cols] += fdot(act, grads[:, cols])

    def outward(self, lev):
        slots, cap, count = pl.ds(lev * 4, 4), self.capacity, 4 * self.capacity
        act = self.act[slots].reshape(count, self.hidden)
        gate_delta = self.gate_delta[slots].reshape(count, self.hidden)
        up_delta = self.up_delta[slots].reshape(count, self.hidden)
        weight = self.weight[:, :1]
        route = jnp.zeros((count, 1), jnp.float32)
        for col in range(0, self.width, 512):
            cols = slice(col, col + 512)
            out = fdot(act, self.down[:, cols]).astype(jnp.bfloat16).astype(jnp.float32)
            route += jnp.sum(out * self.grads[:, cols].astype(jnp.float32), axis=-1, keepdims=True)
            out = (weight * out).astype(jnp.bfloat16)
            self.out_block[slots, :, cols] = out.reshape(4, cap, 512)
            back = dot_nt(gate_delta, self.gate[cols]) + dot_nt(up_delta, self.up[cols])
            self.back[:, cols] = back.astype(jnp.bfloat16)
        lane = lax.broadcasted_iota(jnp.int32, (count, LANES), 1)
        routes = jnp.where(lane == self.place.chip, route, 0.0).astype(jnp.bfloat16)
        for j in range(4):
            slot, at = lev * 4 + j, slice(j * cap, (j + 1) * cap)
            self.held[:cap] = self.back[at]
            left = self.left[j]
            for col in range(0, self.width, 512):
                cols = slice(col, col + 512)
                self.part[slot, :, cols] = dot_tn(left, self.held[:, cols]).astype(jnp.bfloat16)
            self.part[slot, :, self.width :] = dot_tn(left[:cap], routes[at]).astype(jnp.bfloat16)

    def advance(self, i):
        if 0 <= i - 2 < self.gather.planes:
            self.outward(level_at(self.level, self.gather.planes, i - 2))
        if 0 <= i - 1 < self.gather.planes:
            t = i - 1
            lev = level_at(self.level, self.gather.planes, t)
            if t == 0:
                self.gather.landed = True
                for load in self.loads():
                    load.wait()
            self.gather.receive(t)
            self.choose(lev, t)
            self.hidden_units(lev)
            self.shared_units(lev)

    def middle(self):
        return [functools.partial(self.advance, i) for i in range(self.gather.planes + 2)]

    def end(self):
        for save in self.saves(level_at(self.level, self.gather.planes, self.gather.planes - 1)):
            save.wait()
        self.shared_grads[...] = self.total[...].astype(jnp.bfloat16)


def greet(place, ops):
    barrier = pltpu.get_barrier_semaphore()
    expected = 1

    def call(target):
        pl.semaphore_signal(barrier, inc=1, device_id=target, device_id_type=MESH)

    call(place.mate)
    if any(op.reach == 0 for op in ops):
        for j in range(1, place.groups):
            call({EXPERT: place.partner(j)})
        expected += place.groups - 1
    else:
        call(place.by_x)
        call(place.by_y)
        planes = max(op.reach for op in ops)
        level = lax.rem(place.chip // 4, planes)
        has_up, has_down = level < planes - 1, level > 0
        pl.when(has_up)(lambda: call(place.above))
        pl.when(has_down)(lambda: call(place.below))
        expected += 2 + has_up.astype(jnp.int32) + has_down.astype(jnp.int32)
    pl.semaphore_wait(barrier, expected)


def chip_kernel(ops, *refs):
    place = Place()
    n_in = sum(len(op.ins) for op in ops)
    n_out = sum(len(op.outs) for op in ops)
    ins, outs, scratch = refs[:n_in], refs[n_in : n_in + n_out], refs[n_in + n_out :]
    for op in ops:
        op.bind(place, ins[: len(op.ins)], outs[: len(op.outs)], scratch[: len(op.scratch)])
        ins, outs = ins[len(op.ins) :], outs[len(op.outs) :]
        scratch = scratch[len(op.scratch) :]
    greet(place, ops)
    for op in ops:
        op.begin()
    queues = [op.middle() for op in ops]
    for i in range(max(len(q) for q in queues)):
        for queue in queues:
            if i < len(queue):
                queue[i]()
    ended = [op.gains for op in ops if isinstance(op, NormGather)]
    for op in ops:
        if op not in ended:
            op.end()


def exchange(ops, ident):
    ins = [pair for op in ops for pair in op.ins]
    outs = [pair for op in ops for pair in op.outs]
    moved = sum(a.size * a.dtype.itemsize for a, _ in ins + outs)
    results = pl.pallas_call(
        functools.partial(chip_kernel, ops),
        out_shape=[shape for shape, _ in outs],
        in_specs=[pl.BlockSpec(memory_space=space) for _, space in ins],
        out_specs=[pl.BlockSpec(memory_space=space) for _, space in outs],
        scratch_shapes=[entry for op in ops for entry in op.scratch],
        compiler_params=pltpu.CompilerParams(
            collective_id=ident, has_side_effects=True, vmem_limit_bytes=60 << 20
        ),
        cost_estimate=pl.CostEstimate(flops=0, bytes_accessed=moved, transcendentals=0),
    )(*[a for a, _ in ins])
    split = []
    for op in ops:
        split.append(results[: len(op.outs)])
        results = results[len(op.outs) :]
    return split


def general_scores(query_blk, key_rows, first_row):
    scores = jnp.einsum(
        "qhd,khd->hqk", query_blk, key_rows, preferred_element_type=jnp.float32
    ) * DQK ** (-0.5)
    row_pos = first_row + jnp.arange(query_blk.shape[0], dtype=jnp.int32)
    col_pos = jnp.arange(key_rows.shape[0], dtype=jnp.int32)
    return jnp.where(col_pos[None, None, :] <= row_pos[None, :, None], scores, -1e30)


def attend(query_rows, key_rows, value_rows):
    seq_len = query_rows.shape[0]
    blk_rows = min(seq_len, 512)

    def one_block(block_index):
        first_row = block_index * blk_rows
        scores = general_scores(query_rows, key_rows, first_row)
        row_max = jnp.max(scores, axis=-1, keepdims=True)
        log_total = row_max + jnp.log(jnp.sum(jnp.exp(scores - row_max), axis=-1, keepdims=True))
        att_weights = jnp.exp(scores - log_total).astype(jnp.bfloat16)
        mixed_blk = jnp.einsum(
            "hqk,khd->qhd", att_weights, value_rows, preferred_element_type=jnp.float32
        ).astype(jnp.bfloat16)
        return (mixed_blk, log_total)

    mixed_heads, log_totals = lax.map(one_block, jnp.arange(seq_len // blk_rows, dtype=jnp.int32))
    return (mixed_heads.reshape(seq_len, query_rows.shape[1], value_rows.shape[2]), log_totals)


def attend_back(query_rows, key_rows, value_rows, log_totals, mixed_grad):
    seq_len, head_count = (query_rows.shape[0], query_rows.shape[1])
    blk_rows = min(seq_len, 512)

    def one_block(running, block_index):
        key_acc, value_acc = running
        first_row = block_index * blk_rows
        scores = general_scores(query_rows, key_rows, first_row)
        att_probs = jnp.exp(scores - log_totals[block_index])
        att_weights = att_probs.astype(jnp.bfloat16)
        value_acc = value_acc + jnp.einsum(
            "hqk,qhd->khd", att_weights, mixed_grad, preferred_element_type=jnp.float32
        )
        prob_grad = jnp.einsum(
            "qhd,khd->hqk", mixed_grad, value_rows, preferred_element_type=jnp.float32
        )
        row_delta = jnp.sum(att_probs * prob_grad, axis=-1, keepdims=True)
        score_delta = (att_probs * (prob_grad - row_delta) * DQK ** (-0.5)).astype(jnp.bfloat16)
        query_grad = jnp.einsum(
            "hqk,khd->qhd", score_delta, key_rows, preferred_element_type=jnp.float32
        )
        key_acc = key_acc + jnp.einsum(
            "hqk,qhd->khd", score_delta, query_rows, preferred_element_type=jnp.float32
        )
        return ((key_acc, value_acc), query_grad)

    zero_start = (
        jnp.zeros((seq_len, head_count, DQK), jnp.float32),
        jnp.zeros((seq_len, head_count, DV), jnp.float32),
    )
    (key_grad, value_grad), query_grad = lax.scan(
        one_block, zero_start, jnp.arange(seq_len // blk_rows, dtype=jnp.int32)
    )
    return (query_grad.reshape(seq_len, head_count, DQK), key_grad, value_grad)


def attention_forward(seq_in, gain_one, query_w, latent_w, gain_kv, kvup_w):
    seq_len = seq_in.shape[0]
    head_count = query_w.shape[1] // DQK
    cosine, sine_part = rope_tables(seq_len, DR)
    stat_one = rms_scale(seq_in)
    unit_one = seq_in * stat_one
    normed1 = (unit_one * gain_one.astype(jnp.float32)).astype(jnp.bfloat16)
    query_full = jnp.dot(normed1, query_w, preferred_element_type=jnp.float32).reshape(
        seq_len, head_count, DQK
    )
    query_rows = jnp.concatenate(
        [
            query_full[..., :DN],
            rotate(query_full[..., DN:], cosine[:, None, :], sine_part[:, None, :]),
        ],
        axis=-1,
    ).astype(jnp.bfloat16)
    latent_full = jnp.dot(normed1, latent_w, preferred_element_type=jnp.float32)
    latent_stat = rms_scale(latent_full[:, : kvup_w.shape[0]])
    latent_unit = latent_full[:, : kvup_w.shape[0]] * latent_stat
    latent = (latent_unit * gain_kv.astype(jnp.float32)).astype(jnp.bfloat16)
    rot_key = rotate(latent_full[:, kvup_w.shape[0] :], cosine, sine_part).astype(jnp.bfloat16)
    key_value = (
        jnp.dot(latent, kvup_w, preferred_element_type=jnp.float32)
        .astype(jnp.bfloat16)
        .reshape(seq_len, head_count, DN + DV)
    )
    key_rows = jnp.concatenate(
        [key_value[..., :DN], jnp.broadcast_to(rot_key[:, None, :], (seq_len, head_count, DR))],
        axis=-1,
    )
    value_rows = key_value[..., DN:]
    mixed_heads, log_totals = attend(query_rows, key_rows, value_rows)
    return (
        stat_one,
        unit_one,
        normed1,
        query_rows,
        latent_stat,
        latent_unit,
        latent,
        key_rows,
        value_rows,
        mixed_heads,
        log_totals,
        cosine,
        sine_part,
    )


def general(
    layer_in,
    norm1_gain,
    q_weight,
    kva_weight,
    kv_gain,
    kvb_weight,
    o_weight,
    norm2_gain,
    router_weight,
    shared_gate,
    shared_up,
    shared_down,
    expert_gate,
    expert_up,
    expert_down,
    routes,
    out_grad,
):
    groups = lax.axis_size(EXPERT)
    seq_len, width = layer_in.shape
    local_experts = expert_gate.shape[0]
    expert_count = local_experts * groups
    capacity = seq_len * TOPK * 4 // (3 * expert_count)
    rows_total = expert_count * capacity
    (
        gain_one,
        query_w,
        latent_w,
        gain_kv,
        kvup_w,
        output_w,
        gain_two,
        route_w,
        gate_sh,
        up_sh,
        down_sh,
    ) = (
        lax.all_gather(norm1_gain, EXPERT, axis=0, tiled=True),
        lax.all_gather(q_weight, EXPERT, axis=0, tiled=True),
        lax.all_gather(kva_weight, EXPERT, axis=0, tiled=True),
        lax.all_gather(kv_gain, EXPERT, axis=0, tiled=True),
        lax.all_gather(kvb_weight, EXPERT, axis=0, tiled=True),
        lax.all_gather(o_weight, EXPERT, axis=1, tiled=True),
        lax.all_gather(norm2_gain, EXPERT, axis=0, tiled=True),
        lax.all_gather(router_weight, EXPERT, axis=0, tiled=True),
        lax.all_gather(shared_gate, EXPERT, axis=0, tiled=True),
        lax.all_gather(shared_up, EXPERT, axis=0, tiled=True),
        lax.all_gather(shared_down, EXPERT, axis=1, tiled=True),
    )
    (
        stat_one,
        unit_one,
        normed1,
        query_rows,
        latent_stat,
        latent_unit,
        latent,
        key_rows,
        value_rows,
        mixed_heads,
        log_totals,
        cosine,
        sine_part,
    ) = attention_forward(layer_in, gain_one, query_w, latent_w, gain_kv, kvup_w)
    head_count = query_rows.shape[1]
    mixed_flat = mixed_heads.reshape(seq_len, head_count * DV)
    attn_part = jnp.dot(mixed_flat, output_w, preferred_element_type=jnp.float32)
    hidden_state = layer_in + lax.psum(attn_part, TENSOR)
    stat_two = rms_scale(hidden_state)
    unit_two = hidden_state * stat_two
    normed2 = (unit_two * gain_two.astype(jnp.float32)).astype(jnp.bfloat16)
    router_probs = jax.nn.softmax(
        jnp.dot(normed2, route_w, preferred_element_type=jnp.float32), axis=-1
    )
    route_onehot = (
        routes[:, :, None] == jnp.arange(expert_count, dtype=jnp.int32)[None, None, :]
    ).astype(jnp.float32)
    route_weight = jnp.einsum("tke,te->tk", route_onehot, router_probs)
    flat_hot = route_onehot.reshape(seq_len * TOPK, expert_count).astype(jnp.int32)
    slot_pos = jnp.sum(jnp.cumsum(flat_hot, axis=0) * flat_hot, axis=-1) - 1
    buffer_pos = routes.reshape(-1) * capacity + slot_pos

    def to_owners(assigned):
        buffer = jnp.zeros((rows_total, width), jnp.bfloat16).at[buffer_pos].set(assigned)
        buffer = buffer.reshape(groups, local_experts * capacity, width)
        arrived = lax.all_to_all(buffer, EXPERT, split_axis=0, concat_axis=0, tiled=True)
        return (
            arrived.reshape(groups, local_experts, capacity, width)
            .transpose(1, 0, 2, 3)
            .reshape(local_experts, groups * capacity, width)
        )

    def to_sources(results):
        arranged = (
            results.reshape(local_experts, groups, capacity, width)
            .transpose(1, 0, 2, 3)
            .reshape(groups, local_experts * capacity, width)
        )
        arrived = lax.all_to_all(arranged, EXPERT, split_axis=0, concat_axis=0, tiled=True)
        return arrived.reshape(rows_total, width)[buffer_pos].reshape(seq_len, TOPK, width)

    rows_in = to_owners(jnp.repeat(normed2, TOPK, axis=0))
    pre_gate = jnp.einsum("emd,edf->emf", rows_in, expert_gate, preferred_element_type=jnp.float32)
    pre_up = jnp.einsum("emd,edf->emf", rows_in, expert_up, preferred_element_type=jnp.float32)
    expert_act = (jax.nn.silu(pre_gate) * pre_up).astype(jnp.bfloat16)
    block_out = jnp.einsum(
        "emf,efd->emd", expert_act, expert_down, preferred_element_type=jnp.float32
    ).astype(jnp.bfloat16)
    expert_out = to_sources(block_out)
    routed_part = jnp.einsum(
        "tk,tkd->td", route_weight, expert_out, preferred_element_type=jnp.float32
    )
    shared_pre_gate = jnp.dot(normed2, gate_sh, preferred_element_type=jnp.float32)
    shared_pre_up = jnp.dot(normed2, up_sh, preferred_element_type=jnp.float32)
    shared_act = (jax.nn.silu(shared_pre_gate) * shared_pre_up).astype(jnp.bfloat16)
    shared_part = jnp.dot(shared_act, down_sh, preferred_element_type=jnp.float32)
    layer_out = hidden_state + lax.psum(
        (routed_part + shared_part).astype(jnp.bfloat16), TENSOR
    ).astype(jnp.float32)
    out_rows = out_grad.astype(jnp.bfloat16)
    routed_cot = (
        (route_weight[:, :, None] * out_grad[:, None, :])
        .astype(jnp.bfloat16)
        .reshape(seq_len * TOPK, width)
    )
    cot_in = to_owners(routed_cot)
    route_grad_part = jnp.einsum(
        "tkd,td->tk", expert_out, out_grad, preferred_element_type=jnp.float32
    )
    hidden_grad_ex = jnp.einsum(
        "emd,efd->emf", cot_in, expert_down, preferred_element_type=jnp.float32
    )
    gate_delta = (hidden_grad_ex * pre_up * silu_grad(pre_gate)).astype(jnp.bfloat16)
    up_delta = (hidden_grad_ex * jax.nn.silu(pre_gate)).astype(jnp.bfloat16)
    expert_down_grad = jnp.einsum(
        "emf,emd->efd", expert_act, cot_in, preferred_element_type=jnp.float32
    )
    expert_gate_grad = jnp.einsum(
        "emd,emf->edf", rows_in, gate_delta, preferred_element_type=jnp.float32
    )
    expert_up_grad = jnp.einsum(
        "emd,emf->edf", rows_in, up_delta, preferred_element_type=jnp.float32
    )
    row_block = (
        jnp.einsum("emf,edf->emd", gate_delta, expert_gate, preferred_element_type=jnp.float32)
        + jnp.einsum("emf,edf->emd", up_delta, expert_up, preferred_element_type=jnp.float32)
    ).astype(jnp.bfloat16)
    row_grad = to_sources(row_block)
    shared_down_grad = jnp.dot(shared_act.T, out_rows, preferred_element_type=jnp.float32)
    shared_hidden_grad = jnp.dot(out_rows, down_sh.T, preferred_element_type=jnp.float32)
    shared_gate_delta = (shared_hidden_grad * shared_pre_up * silu_grad(shared_pre_gate)).astype(
        jnp.bfloat16
    )
    shared_up_delta = (shared_hidden_grad * jax.nn.silu(shared_pre_gate)).astype(jnp.bfloat16)
    shared_gate_grad = jnp.dot(normed2.T, shared_gate_delta, preferred_element_type=jnp.float32)
    shared_up_grad = jnp.dot(normed2.T, shared_up_delta, preferred_element_type=jnp.float32)
    normed2_part = (
        jnp.sum(row_grad, axis=1, dtype=jnp.float32)
        + jnp.dot(shared_gate_delta, gate_sh.T, preferred_element_type=jnp.float32)
        + jnp.dot(shared_up_delta, up_sh.T, preferred_element_type=jnp.float32)
    )
    normed2_grad, route_grad = lax.psum((normed2_part, route_grad_part), TENSOR)
    prob_grad = jnp.einsum("tk,tke->te", route_grad, route_onehot)
    logit_delta = (
        router_probs * (prob_grad - jnp.sum(router_probs * prob_grad, axis=-1, keepdims=True))
    ).astype(jnp.bfloat16)
    router_grad = jnp.dot(normed2.T, logit_delta, preferred_element_type=jnp.float32)
    normed2_grad = normed2_grad + jnp.dot(
        logit_delta, route_w.T, preferred_element_type=jnp.float32
    )
    norm2_gain_grad = jnp.sum(normed2_grad * unit_two, axis=0)
    scaled_two = normed2_grad * gain_two.astype(jnp.float32)
    hidden_grad = out_grad + stat_two * (
        scaled_two - unit_two * jnp.mean(scaled_two * unit_two, axis=-1, keepdims=True)
    )
    hidden_rows = hidden_grad.astype(jnp.bfloat16)
    o_grad = jnp.dot(mixed_flat.T, hidden_rows, preferred_element_type=jnp.float32)
    mixed_grad = (
        jnp.dot(hidden_rows, output_w.T, preferred_element_type=jnp.float32)
        .astype(jnp.bfloat16)
        .reshape(seq_len, head_count, DV)
    )
    query_grad, key_grad, value_grad = attend_back(
        query_rows, key_rows, value_rows, log_totals, mixed_grad
    )
    query_delta = (
        jnp.concatenate(
            [
                query_grad[..., :DN],
                rotate_back(query_grad[..., DN:], cosine[:, None, :], sine_part[:, None, :]),
            ],
            axis=-1,
        )
        .astype(jnp.bfloat16)
        .reshape(seq_len, head_count * DQK)
    )
    kv_delta = (
        jnp.concatenate([key_grad[..., :DN], value_grad], axis=-1)
        .astype(jnp.bfloat16)
        .reshape(seq_len, head_count * (DN + DV))
    )
    q_grad = jnp.dot(normed1.T, query_delta, preferred_element_type=jnp.float32)
    kvb_grad = jnp.dot(latent.T, kv_delta, preferred_element_type=jnp.float32)
    latent_part = jnp.dot(kv_delta, kvup_w.T, preferred_element_type=jnp.float32)
    rot_part = jnp.sum(key_grad[..., DN:], axis=1)
    normed1_part = jnp.dot(query_delta, query_w.T, preferred_element_type=jnp.float32)
    latent_grad, rot_sum, normed1_query = (
        lax.psum(latent_part.astype(jnp.bfloat16), TENSOR).astype(jnp.float32),
        lax.psum(rot_part.astype(jnp.bfloat16), TENSOR).astype(jnp.float32),
        lax.psum(normed1_part.astype(jnp.bfloat16), TENSOR).astype(jnp.float32),
    )
    kv_gain_grad = jnp.sum(latent_grad * latent_unit, axis=0)
    scaled_lat = latent_grad * gain_kv.astype(jnp.float32)
    latent_back = latent_stat * (
        scaled_lat - latent_unit * jnp.mean(scaled_lat * latent_unit, axis=-1, keepdims=True)
    )
    latent_delta = jnp.concatenate(
        [latent_back, rotate_back(rot_sum, cosine, sine_part)], axis=-1
    ).astype(jnp.bfloat16)
    kva_grad = jnp.dot(normed1.T, latent_delta, preferred_element_type=jnp.float32)
    normed1_grad = normed1_query + jnp.dot(
        latent_delta, latent_w.T, preferred_element_type=jnp.float32
    )
    norm1_gain_grad = jnp.sum(normed1_grad * unit_one, axis=0)
    scaled_one = normed1_grad * gain_one.astype(jnp.float32)
    x_grad = hidden_grad + stat_one * (
        scaled_one - unit_one * jnp.mean(scaled_one * unit_one, axis=-1, keepdims=True)
    )
    (
        norm1_gain_grad,
        q_grad,
        kva_grad,
        kv_gain_grad,
        kvb_grad,
        o_grad,
        norm2_gain_grad,
        router_grad,
        shared_gate_grad,
        shared_up_grad,
        shared_down_grad,
    ) = (
        lax.psum_scatter(norm1_gain_grad, EXPERT, scatter_dimension=0, tiled=True),
        lax.psum_scatter(q_grad, EXPERT, scatter_dimension=0, tiled=True),
        lax.psum_scatter(kva_grad, EXPERT, scatter_dimension=0, tiled=True),
        lax.psum_scatter(kv_gain_grad, EXPERT, scatter_dimension=0, tiled=True),
        lax.psum_scatter(kvb_grad, EXPERT, scatter_dimension=0, tiled=True),
        lax.psum_scatter(o_grad, EXPERT, scatter_dimension=1, tiled=True),
        lax.psum_scatter(norm2_gain_grad, EXPERT, scatter_dimension=0, tiled=True),
        lax.psum_scatter(router_grad, EXPERT, scatter_dimension=0, tiled=True),
        lax.psum_scatter(shared_gate_grad, EXPERT, scatter_dimension=0, tiled=True),
        lax.psum_scatter(shared_up_grad, EXPERT, scatter_dimension=0, tiled=True),
        lax.psum_scatter(shared_down_grad, EXPERT, scatter_dimension=1, tiled=True),
    )
    return (
        layer_out,
        x_grad,
        norm1_gain_grad,
        q_grad,
        kva_grad,
        kv_gain_grad,
        kvb_grad,
        o_grad,
        norm2_gain_grad,
        router_grad,
        shared_gate_grad,
        shared_up_grad,
        shared_down_grad,
        expert_gate_grad,
        expert_up_grad,
        expert_down_grad,
    )


def fits(groups, heads, block, width):
    whole = groups in (4, 8, 16) and heads in (4, 8, 16) and groups % heads == 0
    return whole and block % 64 == 0 and width == groups * LANES


def masked_scores(query_rows, key_rows):
    scores = fsum("sqd,skd->sqk", query_rows, key_rows) * DQK ** (-0.5)
    places = jnp.arange(query_rows.shape[1], dtype=jnp.int32)
    return jnp.where(places[None, None, :] <= places[None, :, None], scores, -1e30)


def to_blocks(grad_rows, groups):
    rows, width = grad_rows.shape
    kept = lax.optimization_barrier(grad_rows.astype(jnp.bfloat16))
    return kept.reshape(rows, groups, width // groups).transpose(1, 0, 2)


def from_blocks(blocks):
    groups, rows, width = blocks.shape
    return blocks.transpose(1, 0, 2).reshape(rows, groups * width)


def widen(rows, width):
    return jnp.pad(rows, [(0, 0)] * (rows.ndim - 1) + [(0, width - rows.shape[-1])])


def by_heads(
    layer_in,
    norm1_gain,
    q_weight,
    kva_weight,
    kv_gain,
    kvb_weight,
    o_weight,
    norm2_gain,
    router_weight,
    shared_gate,
    shared_up,
    shared_down,
    expert_gate,
    expert_up,
    expert_down,
    routes,
    out_grad,
):
    groups = lax.axis_size(EXPERT)
    chip = lax.axis_index(EXPERT)
    seq_len, width = layer_in.shape
    capacity = seq_len * TOPK * 4 // (3 * groups)
    heads = q_weight.shape[1] // DQK
    copies = groups // heads
    head = lax.rem(chip, heads)
    own_cols = kva_weight.shape[0]
    lat_rows, lat_width = kvb_weight.shape[0], kvb_weight.shape[0] * groups
    hidden = shared_gate.shape[1] // groups
    bf16 = jnp.bfloat16

    kv_halves = (DN + DV) // own_cols
    kv_block = lat_rows * kv_halves
    head_parts = jnp.concatenate(
        [
            q_weight.reshape(own_cols, heads, DQK).transpose(1, 2, 0),
            kvb_weight.reshape(lat_rows, heads, kv_halves, own_cols)
            .transpose(1, 2, 0, 3)
            .reshape(heads, kv_block, own_cols),
            o_weight.reshape(heads, DV, own_cols),
        ],
        axis=1,
    )
    shared_parts = jnp.concatenate(
        [
            shared_gate.reshape(own_cols, groups, hidden).transpose(1, 2, 0),
            shared_up.reshape(own_cols, groups, hidden).transpose(1, 2, 0),
            shared_down.reshape(groups, hidden, own_cols),
        ],
        axis=1,
    )
    small = jnp.concatenate(
        [
            router_weight.T,
            norm1_gain[None, :],
            norm2_gain[None, :],
            widen(kv_gain[None, :], own_cols),
        ],
        axis=0,
    )
    small = jnp.pad(small, [(0, -small.shape[0] % 16), (0, 0)])
    at_kv = DQK
    at_o = at_kv + kv_block
    at_gate = at_o + DV
    planes, all_planes = heads // 4, groups // 4
    small_swap = Swap(jnp.broadcast_to(small[None], (groups,) + small.shape), True)
    (small_all,), (latent_w,), (got,), (normed1_all,) = exchange(
        [
            small_swap,
            Gather([kva_weight], all_planes),
            Swap(jnp.tile(head_parts, (copies, 1, 1))),
            NormGather(layer_in, small_swap, groups, planes),
        ],
        1,
    )
    route_wt = from_blocks(small_all[:, :groups])
    gain_one = small_all[:, groups].reshape(width).astype(jnp.float32)
    gain_two = small_all[:, groups + 1].reshape(width).astype(jnp.float32)
    gain_kv = small_all[:, groups + 2, :lat_rows].reshape(lat_width).astype(jnp.float32)
    latent_w = latent_w.reshape(width, kva_weight.shape[1])
    stat_one = rms_scale(layer_in)
    unit_one = layer_in * stat_one

    cosine, sine_part = rope_tables(seq_len, DR)
    turn_cos = jnp.concatenate([cosine, cosine], axis=-1)
    turn_sin = jnp.concatenate([-sine_part, sine_part], axis=-1)
    by_seq = (heads, seq_len, -1)
    fold = 2

    def rotated(block, cos_ref, sin_ref, sign):
        flipped = jnp.concatenate([block[:, DR // 2 :], block[:, : DR // 2]], axis=-1)
        reps = block.shape[0] // seq_len
        cos_rows = jnp.concatenate([cos_ref[...]] * reps, axis=0)
        sin_rows = jnp.concatenate([sin_ref[...]] * reps, axis=0)
        return (block * cos_rows + sign * flipped * sin_rows).astype(bf16)

    def attend_forward(refs):
        rows_in, parts, lat_w, kv_gain_ref, cos_ref, sin_ref = refs[:6]
        query_out, key_out, value_out, prob_out, lat_out, latent_out, mixed_out = refs[6:13]
        out_w, query_w, kv_w = refs[13:]

        def assemble():
            for j in range(groups):
                at = slice(j * own_cols, (j + 1) * own_cols)
                query_w[:, at] = parts[j, :at_kv]
                out_w[:, at] = parts[j, at_o:at_gate]
                down = slice(j * lat_rows, (j + 1) * lat_rows)
                for half in range(kv_halves):
                    start = at_kv + half * lat_rows
                    across = slice(half * own_cols, (half + 1) * own_cols)
                    kv_w[down, across] = parts[j, start : start + lat_rows]

        def some(first):
            rows = rows_in[first : first + fold].reshape(fold * seq_len, width)
            query = dot_nt(rows, query_w[...])
            query_plain, query_turn = query[:, :DN].astype(bf16), rotated(query[:, DN:], cos_ref, sin_ref, 1.0)
            full = fdot(rows, lat_w[...])
            plain = full[:, :lat_width]
            latent = (plain * rms_scale(plain) * kv_gain_ref[...]).astype(bf16)
            key_turn = rotated(full[:, lat_width:], cos_ref, sin_ref, 1.0)
            key_value = fdot(latent, kv_w[...]).astype(bf16)
            latent_out[first : first + fold] = latent.reshape(fold, seq_len, lat_width)
            lat_out[first : first + fold] = plain.reshape(fold, seq_len, lat_width)
            ahead = lax.broadcasted_iota(jnp.int32, (seq_len, seq_len), 1) > lax.broadcasted_iota(
                jnp.int32, (seq_len, seq_len), 0
            )
            for k in range(fold):
                at, seq = slice(k * seq_len, (k + 1) * seq_len), first + k
                scores = dot_nt(query_plain[at], key_value[at, :DN])
                scores += dot_nt(query_turn[at], key_turn[at])
                scores = jnp.where(ahead, -1e30, scores * DQK ** (-0.5))
                row_max = jnp.max(scores, axis=-1, keepdims=True)
                total = jnp.sum(jnp.exp(scores - row_max), axis=-1, keepdims=True)
                probs = jnp.exp(scores - (row_max + jnp.log(total)))
                values = key_value[at, DN:]
                prob_out[seq] = probs
                mixed_out[seq] = fdot(probs.astype(bf16), values).astype(bf16)
                query_out[seq, :, :DN], query_out[seq, :, DN:] = query_plain[at], query_turn[at]
                key_out[seq, :, :DN], key_out[seq, :, DN:] = key_value[at, :DN], key_turn[at]
                value_out[seq] = values

        steps = [functools.partial(some, first) for first in range(0, heads, fold)]
        return [assemble] + steps

    out_rows = out_grad.astype(bf16)

    def attn_part(part, slot, refs):
        for col in range(0, width, 512):
            product = fdot(refs[12][slot], refs[13][:, col : col + 512])
            part[slot, :, col : col + 512] = product.astype(bf16)

    def shaped(last, kind):
        return jax.ShapeDtypeStruct((heads, seq_len, last), kind)

    (out_all,), (shared_got,), attended = exchange(
        [
            Gather([out_rows], all_planes),
            Swap(shared_parts),
            Reduce(
                [normed1_all, got, latent_w, gain_kv[None, :], turn_cos, turn_sin],
                attn_part,
                heads,
                seq_len,
                width,
                extra=[
                    shaped(DQK, bf16),
                    shaped(DQK, bf16),
                    shaped(DV, bf16),
                    shaped(seq_len, jnp.float32),
                    shaped(lat_width, jnp.float32),
                    shaped(lat_width, bf16),
                    shaped(DV, bf16),
                    jax.ShapeDtypeStruct((DV, width), bf16),
                    jax.ShapeDtypeStruct((DQK, width), bf16),
                    jax.ShapeDtypeStruct((lat_width, DN + DV), bf16),
                ],
                prelude=attend_forward,
            ),
        ],
        2,
    )
    attn_sum, query_rows, key_rows, value_rows, att_probs, lat_plain, latent, mixed = attended[:8]
    output_w, query_wt, kvup_w = attended[8:]
    mixed_flat = mixed.reshape(heads * seq_len, DV)
    normed1_all = normed1_all.reshape(heads * seq_len, width)
    latent = latent.reshape(heads * seq_len, lat_width)

    gate_sht = from_blocks(shared_got[:, :hidden])
    up_sht = from_blocks(shared_got[:, hidden : 2 * hidden])
    down_sh = from_blocks(shared_got[:, 2 * hidden :])
    hidden_state = layer_in + attn_sum

    stat_two = rms_scale(hidden_state)
    unit_two = hidden_state * stat_two
    normed2 = (unit_two * gain_two).astype(bf16)
    router_probs = jax.nn.softmax(fsum("td,ed->te", normed2, route_wt), axis=-1)
    experts = jnp.arange(groups, dtype=jnp.int32)
    chosen = jnp.any(routes[:, :, None] == experts[None, None, :], axis=1)
    marked = widen(jnp.where(chosen, router_probs, -1.0), -(-groups // LANES) * LANES)
    room = -(-hidden // 16) * 16

    def stacked(blocks):
        return jnp.pad(blocks, [(0, room - hidden), (0, 0)])

    token_gather = Gather([normed2, marked], all_planes, True)
    experts_op = Experts(
        token_gather,
        out_all,
        [expert_gate[0], expert_up[0], expert_down[0]],
        jnp.stack([stacked(gate_sht), stacked(up_sht), stacked(down_sh)]),
        capacity,
    )
    _, expert_results = exchange([token_gather, experts_op], 3)
    grad_parts, out_block, picks, shared_act, shared_sums = expert_results[:5]
    rows_in, cot_in, expert_act, gate_delta, up_delta = (
        x.reshape(groups * capacity, -1) for x in expert_results[5:]
    )
    expert_down_grad = fsum("mf,md->fd", expert_act, cot_in)[None]
    expert_gate_grad = fsum("md,mf->df", rows_in, gate_delta)[None]
    expert_up_grad = fsum("md,mf->df", rows_in, up_delta)[None]
    shared_grads = (
        shared_sums[:, :hidden]
        .reshape(3 * hidden, groups, own_cols)
        .transpose(1, 0, 2)
    )
    out_left = jnp.concatenate(
        [picks, shared_act.reshape(room, groups, seq_len).transpose(1, 0, 2)], axis=1
    )

    def expert_part(part, slot, refs):
        left, own, held = refs[0], refs[1], refs[-1]
        held[:capacity] = own[slot]
        for col in range(0, width, 512):
            product = lax.dot_general(
                left[slot],
                held[:, col : col + 512],
                (((0,), (0,)), ((), ())),
                preferred_element_type=jnp.float32,
            )
            part[slot, :, col : col + 512] = product.astype(bf16)

    def hold_shared(refs):
        refs[-1][capacity:] = refs[2][...]

    ((summed,),) = exchange(
        [Reduce([grad_parts], None, groups, seq_len, width + marked.shape[1])], 4
    )
    normed2_sum = summed[:, :width]
    prob_grad = summed[:, width : width + groups]
    logit_delta = (
        router_probs * (prob_grad - jnp.sum(router_probs * prob_grad, axis=-1, keepdims=True))
    ).astype(bf16)
    normed2_grad = normed2_sum + fdot(logit_delta, route_wt)
    router_gradt = fsum("te,td->ed", logit_delta, normed2)
    norm2_gain_grad = jnp.sum(normed2_grad * unit_two, axis=0)
    scaled_two = normed2_grad * gain_two
    hidden_grad = out_grad + stat_two * (
        scaled_two - unit_two * jnp.mean(scaled_two * unit_two, axis=-1, keepdims=True)
    )

    hidden_rows = hidden_grad.astype(bf16)
    hidden_gather = Gather([hidden_rows], planes, True)

    def attend_backward(refs):
        rows_in, keys, values, probs, out_w, cos_ref, sin_ref = refs[:7]
        query_to, kv_to, turn_to = refs[9:]
        place, hidden_in = hidden_gather.place, hidden_gather.results[0]

        def some(level, first, second, own):
            slots = [level * 4 + first, level * 4 + second]
            hidden_gather.ready(slots[0], not own)
            hidden_gather.ready(slots[1], True)
            rows = jnp.concatenate([hidden_in[slot] for slot in slots], axis=0)
            mixed_grads = dot_nt(rows, out_w[...]).astype(bf16)
            for k in range(2):
                slot = slots[k]
                mixed_grad = mixed_grads[k * seq_len : (k + 1) * seq_len]
                prob = probs[slot]
                value_grad = dot_tn(prob.astype(bf16), mixed_grad)
                dprob = dot_nt(mixed_grad, values[slot])
                row_delta = jnp.sum(prob * dprob, axis=-1, keepdims=True)
                score_delta = (prob * (dprob - row_delta) * DQK ** (-0.5)).astype(bf16)
                query_grad = fdot(score_delta, keys[slot])
                key_grad = dot_tn(score_delta, rows_in[slot])
                query_to[slot, :, :DN] = query_grad[:, :DN].astype(bf16)
                query_to[slot, :, DN:] = rotated(query_grad[:, DN:], cos_ref, sin_ref, -1.0)
                kv_to[slot, :, :DN] = key_grad[:, :DN].astype(bf16)
                kv_to[slot, :, DN:] = value_grad.astype(bf16)
                turn_to[slot, :, :DR] = key_grad[:, DN:].astype(bf16)
                turn_to[slot, :, DR:] = jnp.zeros((seq_len, LANES - DR), bf16)

        level, calls = hidden_gather.level, []
        hidden_gather.landed = True
        for far in range(planes):
            where = lax.rem(level + far, planes)
            calls.append(functools.partial(some, where, place.here, place.there_x, far == 0))
            calls.append(functools.partial(some, where, place.there_y, place.across, False))
        return calls

    def back_part(part, slot, refs):
        for col in range(0, width, 512):
            product = fdot(refs[9][slot], refs[7][:, col : col + 512])
            part[slot, :, col : col + 512] = product.astype(bf16)
        product = dot_nt(refs[10][slot], refs[8][...])
        part[slot, :, width : width + lat_width] = product.astype(bf16)
        part[slot, :, width + lat_width :] = refs[11][slot]

    ((hidden_all,), (out_sum,), (back, query_delta, kv_delta), (owned_early,)) = exchange(
        [
            hidden_gather,
            Reduce(
                [out_left, out_block, stacked(down_sh)],
                expert_part,
                groups,
                seq_len,
                width,
                [pltpu.VMEM((capacity + room, width), bf16)],
                hold_shared,
            ),
            Reduce(
                [
                    query_rows,
                    key_rows,
                    value_rows,
                    att_probs,
                    output_w,
                    turn_cos,
                    turn_sin,
                    query_wt,
                    kvup_w,
                ],
                back_part,
                heads,
                seq_len,
                width + lat_width + LANES,
                [pltpu.VMEM((heads, seq_len, LANES), bf16)],
                extra=[shaped(DQK, bf16), shaped(DN + DV, bf16)],
                prelude=attend_backward,
                delay=2,
            ),
            Swap(shared_grads),
        ],
        5,
    )
    layer_out = hidden_state + out_sum
    hidden_all = hidden_all.reshape(heads * seq_len, width)
    o_grad = fdot(lax.optimization_barrier(mixed_flat.T), hidden_all)
    normed1_query = back[:, :width]
    latent_grad = back[:, width : width + lat_width]
    rot_sum = back[:, width + lat_width : width + lat_width + DR]

    own_plain = lax.dynamic_index_in_dim(lat_plain, head, 0, keepdims=False)
    own_stat = rms_scale(own_plain)
    own_unit = own_plain * own_stat
    kv_gain_grad = jnp.sum(latent_grad * own_unit, axis=0)
    scaled_lat = latent_grad * gain_kv
    latent_back = own_stat * (
        scaled_lat - own_unit * jnp.mean(scaled_lat * own_unit, axis=-1, keepdims=True)
    )
    latent_delta = jnp.concatenate(
        [latent_back, rotate_back(rot_sum, cosine, sine_part)], axis=-1
    ).astype(bf16)
    query_delta_t = lax.optimization_barrier(query_delta.reshape(heads * seq_len, DQK).T)
    kv_flat = kv_delta.reshape(heads * seq_len, DN + DV)
    latent_t = lax.optimization_barrier(latent.T)
    kvb_blocks = (
        lax.optimization_barrier(fdot(latent_t, kv_flat).astype(bf16))
        .reshape(groups, lat_rows, kv_halves, own_cols)
        .transpose(0, 2, 1, 3)
        .reshape(groups, kv_block, own_cols)
    )
    head_grads = jnp.concatenate(
        [
            to_blocks(fdot(query_delta_t, normed1_all), groups),
            kvb_blocks,
            to_blocks(o_grad, groups),
        ],
        axis=1,
    )
    (latent_delta_all,), (owned_heads,) = exchange(
        [Gather([latent_delta], planes), Swap(head_grads, pace=4)], 7
    )
    latent_delta_all = latent_delta_all.reshape(heads * seq_len, -1)
    normed1_grad = normed1_query + fsum("tl,dl->td", latent_delta, latent_w)
    norm1_gain_grad = jnp.sum(normed1_grad * unit_one, axis=0)
    scaled_one = normed1_grad * gain_one
    x_grad = hidden_grad + stat_one * (
        scaled_one - unit_one * jnp.mean(scaled_one * unit_one, axis=-1, keepdims=True)
    )

    share = latent_delta_all.shape[1] // heads
    latent_share = lax.dynamic_slice_in_dim(latent_delta_all, head * share, share, 1)
    kva_blocks = to_blocks(fdot(lax.optimization_barrier(latent_share.T), normed1_all), groups)

    def by_owner(row):
        return widen(row.reshape(groups, 1, -1), own_cols)

    small_grads = jnp.concatenate(
        [
            router_gradt.reshape(groups, groups, own_cols).transpose(1, 0, 2),
            by_owner(norm1_gain_grad),
            by_owner(norm2_gain_grad),
            by_owner(kv_gain_grad),
        ],
        axis=1,
    )
    small_grads = jnp.pad(small_grads, [(0, 0), (0, -small_grads.shape[1] % 8), (0, 0)])
    kva_blocks = jnp.pad(kva_blocks, [(0, 0), (0, -share % 16), (0, 0)])
    (owned_share,), (owned_small,) = exchange([Swap(kva_blocks), Swap(small_grads)], 8)
    small_sums = jnp.sum(owned_small, axis=0)

    def over_copies(blocks):
        blocks = blocks.astype(jnp.float32).reshape((copies, heads) + blocks.shape[1:])
        return jnp.sum(blocks, axis=0)

    of_heads = over_copies(owned_heads)
    q_grad = of_heads[:, :at_kv].transpose(2, 0, 1).reshape(own_cols, heads * DQK)
    kvb_grad = (
        of_heads[:, at_kv:at_o]
        .reshape(heads, kv_halves, lat_rows, own_cols)
        .transpose(2, 0, 1, 3)
        .reshape(lat_rows, heads * (DN + DV))
    )
    own_o_grad = of_heads[:, at_o:].reshape(heads * DV, own_cols)
    kva_grad = over_copies(owned_share)[:, :share].reshape(heads * share, own_cols).T
    of_shared = owned_early[:, : 3 * hidden].astype(jnp.float32)

    def columns(blocks):
        return blocks.reshape(groups * hidden, own_cols)

    shared_gate_grad = columns(of_shared[:, :hidden]).T
    shared_up_grad = columns(of_shared[:, hidden : 2 * hidden]).T
    shared_down_grad = columns(of_shared[:, 2 * hidden :])
    router_grad = small_sums[:groups].T
    return (
        layer_out,
        x_grad,
        small_sums[groups],
        q_grad,
        kva_grad,
        small_sums[groups + 2, :lat_rows],
        kvb_grad,
        own_o_grad,
        small_sums[groups + 1],
        router_grad,
        shared_gate_grad,
        shared_up_grad,
        shared_down_grad,
        expert_gate_grad,
        expert_up_grad,
        expert_down_grad,
    )


def on_device(layer_in, *rest):
    groups, heads = lax.axis_size(EXPERT), rest[1].shape[1] // DQK
    one_each = rest[11].shape[0] == 1
    if one_each and fits(groups, heads, *layer_in.shape):
        return by_heads(layer_in, *rest)
    return general(layer_in, *rest)


def solution(mesh):
    in_specs = (
        P(EXPERT, None),
        P(EXPERT),
        P(EXPERT, TENSOR),
        P(EXPERT, None),
        P(EXPERT),
        P(EXPERT, TENSOR),
        P(TENSOR, EXPERT),
        P(EXPERT),
        P(EXPERT, None),
        P(EXPERT, TENSOR),
        P(EXPERT, TENSOR),
        P(TENSOR, EXPERT),
        P(EXPERT, None, TENSOR),
        P(EXPERT, None, TENSOR),
        P(EXPERT, TENSOR, None),
        P(EXPERT, None),
        P(EXPERT, None),
    )
    out_specs = (
        P(EXPERT, None),
        P(EXPERT, None),
        P(EXPERT),
        P(EXPERT, TENSOR),
        P(EXPERT, None),
        P(EXPERT),
        P(EXPERT, TENSOR),
        P(TENSOR, EXPERT),
        P(EXPERT),
        P(EXPERT, None),
        P(EXPERT, TENSOR),
        P(EXPERT, TENSOR),
        P(TENSOR, EXPERT),
        P(EXPERT, None, TENSOR),
        P(EXPERT, None, TENSOR),
        P(EXPERT, TENSOR, None),
    )
    return jax.shard_map(
        on_device, mesh=mesh, in_specs=in_specs, out_specs=out_specs, check_vma=False
    )
```

```python
import functools

import jax
import jax.numpy as jnp
from jax import lax
from jax.experimental import pallas as pl
from jax.experimental.pallas import tpu as pltpu
from jax.sharding import PartitionSpec as P

DN = 128
DR = 64
DQK = 192
DV = 128
TOPK = 6
LANES = 128


norm_eps = 1e-06


def rms_scale(inputs):
    return lax.rsqrt(jnp.mean(inputs * inputs, axis=-1, keepdims=True) + norm_eps)


def rope_tables(length, rot_width):
    half_width = rot_width // 2
    frequency = 10000.0 ** (-jnp.arange(half_width).astype(jnp.float32) / half_width)
    angles = jnp.arange(length).astype(jnp.float32)[:, None] * frequency[None, :]
    return (jnp.cos(angles), jnp.sin(angles))


def rotate(inputs, cosine, sine_part):
    half_width = inputs.shape[-1] // 2
    first_half = inputs[..., :half_width]
    second_half = inputs[..., half_width:]
    return jnp.concatenate(
        [
            first_half * cosine - second_half * sine_part,
            second_half * cosine + first_half * sine_part,
        ],
        axis=-1,
    )


def rotate_back(inputs, cosine, sine_part):
    return rotate(inputs, cosine, -sine_part)


def silu_grad(pre_act):
    sigmoid_val = jax.nn.sigmoid(pre_act)
    return sigmoid_val * (1.0 + pre_act * (1.0 - sigmoid_val))


def fdot(left, right):
    return jnp.dot(left, right, preferred_element_type=jnp.float32)


def dot_nt(left, right):
    return lax.dot_general(
        left, right, (((1,), (1,)), ((), ())), preferred_element_type=jnp.float32
    )


def dot_tn(left, right):
    return lax.dot_general(
        left, right, (((0,), (0,)), ((), ())), preferred_element_type=jnp.float32
    )


def fsum(spec, left, right):
    return jnp.einsum(spec, left, right, preferred_element_type=jnp.float32)


EXPERT, TENSOR = "expert", "tensor"
MESH = pl.DeviceIdType.MESH
DMA = pltpu.SemaphoreType.DMA


def remote(src, dst, send, recv, target):
    return pltpu.make_async_remote_copy(
        src_ref=src, dst_ref=dst, send_sem=send, recv_sem=recv, device_id=target, device_id_type=MESH
    )


def part_rows(start, size):
    return pl.ds(pl.multiple_of(start, size), size)


class Place:
    def __init__(self):
        self.groups = lax.axis_size(EXPERT)
        self.chip = lax.axis_index(EXPERT)
        self.core = lax.axis_index(TENSOR)
        self.here = lax.rem(self.chip, 4)
        self.there_x = self.here + 1 - 2 * lax.rem(self.here, 2)
        self.there_y = self.here + 2 - 4 * (self.here // 2)
        self.across = 3 - self.here
        base = self.chip - self.here
        self.by_x = {EXPERT: base + self.there_x}
        self.by_y = {EXPERT: base + self.there_y}
        self.above = {EXPERT: self.chip + 4}
        self.below = {EXPERT: self.chip - 4}
        self.mate = {TENSOR: 1 - self.core}

    def spot(self, q):
        x = lax.rem(self.here + 1 - lax.rem(q, 2), 2)
        y = lax.rem(self.here // 2 + 1 - q // 2, 2)
        return 2 * y + x

    def partner(self, j):
        return lax.rem(self.chip + j, self.groups)


def level_at(level, planes, t):
    if planes < 4:
        return lax.rem(level + t, planes)
    flip = level // 2
    near = lax.rem(level + flip, 2)
    order = t + near * (1 - 2 * t) * (1 - t // 2)
    return order * (1 - 2 * flip) + 3 * flip


class Swap:
    reach = 0

    def __init__(self, blocks, vmem_result=False, pace=2):
        groups = blocks.shape[0]
        self.pace = groups if vmem_result else pace
        self.ins = [(blocks, pltpu.VMEM)]
        self.outs = [
            (
                jax.ShapeDtypeStruct(blocks.shape, blocks.dtype),
                pltpu.VMEM if vmem_result else pl.ANY,
            )
        ]
        self.scratch = [DMA, DMA((groups,)), DMA((groups,))]

    def bind(self, place, ins, outs, scratch):
        self.place, self.groups = place, place.groups
        self.source, self.result = ins[0], outs[0]
        self.own_sem, self.send_sem, self.recv_sem = scratch

    def copy(self, j, src, dst):
        return remote(
            self.source.at[src],
            self.result.at[dst],
            self.send_sem.at[j],
            self.recv_sem.at[j],
            {EXPERT: self.place.partner(j)},
        )

    def own(self):
        chip = self.place.chip
        return pltpu.make_async_copy(self.source.at[chip], self.result.at[chip], self.own_sem)

    def send(self, i):
        for q in range(min(self.pace, self.groups - 1)):
            j = 1 + i * self.pace + q

            @pl.when(j < self.groups)
            def _(j=j):
                self.copy(j, self.place.partner(j), self.place.chip).start()

    def begin(self):
        self.own().start()
        self.send(0)

    def rest(self, offset):
        count = -(-(self.groups - 1) // self.pace) - 1
        return [(offset, count, lambda i: self.send(i + 1))]

    def segments(self):
        return self.rest(0)

    def end(self):
        self.own().wait()

        @pl.loop(1, self.groups)
        def _(j):
            self.copy(j, self.place.chip, self.place.partner(self.groups - j)).wait_recv()
            self.copy(j, self.place.partner(j), self.place.chip).wait_send()


class MadeSwap(Swap):
    def __init__(self, operands, shape, make, delay, pace, scratch=()):
        self.pace, self.make, self.delay = pace, make, delay
        self.ins = [(a, pltpu.VMEM) for a in operands]
        self.outs = [(jax.ShapeDtypeStruct(shape, jnp.bfloat16), pl.ANY)]
        groups = shape[0]
        self.scratch = [DMA, DMA((groups,)), DMA((groups,)), pltpu.VMEM(shape, jnp.bfloat16)]
        self.scratch += list(scratch)

    def bind(self, place, ins, outs, scratch):
        super().bind(place, [scratch[3]], outs, scratch[:3])
        self.refs, self.extra = ins, scratch[4:]

    def begin(self):
        pass

    def segments(self):
        calls = self.make(self) + [lambda i: super(MadeSwap, self).begin()]
        parts = [(self.delay + k, 1, call) for k, call in enumerate(calls)]
        return parts + self.rest(self.delay + len(calls))


class Gather:
    def __init__(self, arrays, planes, vmem_result=False):
        count, slots = len(arrays), planes * 4
        self.planes, self.count, self.reach = planes, count, planes
        self.ins = [(a, pltpu.VMEM) for a in arrays]
        space = pltpu.VMEM if vmem_result else pl.ANY
        self.outs = [(jax.ShapeDtypeStruct((slots,) + a.shape, a.dtype), space) for a in arrays]
        by_level, by_slot = DMA((count, planes)), DMA((count, slots))
        self.scratch = [DMA((count,))] + [by_level] * 5 + [by_slot] + [by_level] * 6 + [by_slot]

    def bind(self, place, ins, outs, scratch):
        self.place, self.sources, self.results = place, ins, outs
        self.level = lax.rem(place.chip // 4, self.planes)
        self.has_up, self.has_down = self.level < self.planes - 1, self.level > 0
        self.own_sem = scratch[0]
        self.in_z, self.in_x, self.in_y, self.in_a, self.in_b, self.in_p = scratch[1:7]
        self.out_up, self.out_down, self.out_x, self.out_y = scratch[7:11]
        self.out_a, self.out_b, self.out_p = scratch[11:14]
        self.landed = False

    def move(self, a, slot, part, send, recv, target, own=False, whose=None):
        half = self.sources[a].shape[0] // 2
        whose = self.place.core if whose is None else whose
        if part is None:
            rows = part_rows(whose * half, half)
        else:
            rows = part_rows(whose * half + part * (half // 2), half // 2)
        dst = self.results[a].at[slot, rows]
        return remote(self.sources[a].at[rows] if own else dst, dst, send, recv, target)

    def along_z(self, a, lev, own, up):
        sems = self.out_up if up else self.out_down
        target = self.place.above if up else self.place.below
        slot = lev * 4 + self.place.here
        return self.move(a, slot, None, sems.at[a, lev], self.in_z.at[a, lev], target, own)

    def along_x(self, a, lev, slot, own=False):
        return self.move(
            a, slot, None, self.out_x.at[a, lev], self.in_x.at[a, lev], self.place.by_x, own
        )

    def along_y(self, a, lev, slot, own=False):
        return self.move(
            a, slot, None, self.out_y.at[a, lev], self.in_y.at[a, lev], self.place.by_y, own
        )

    def corner_x(self, a, lev, slot):
        return self.move(
            a, slot, 0, self.out_a.at[a, lev], self.in_a.at[a, lev], self.place.by_x
        )

    def corner_y(self, a, lev, slot):
        return self.move(
            a, slot, 1, self.out_b.at[a, lev], self.in_b.at[a, lev], self.place.by_y
        )

    def share(self, a, slot, whose=None):
        return self.move(
            a, slot, None, self.out_p.at[a, slot], self.in_p.at[a, slot], self.place.mate, whose=whose
        )

    def own(self, a):
        slot = self.level * 4 + self.place.here
        return pltpu.make_async_copy(self.sources[a], self.results[a].at[slot], self.own_sem.at[a])

    def begin(self):
        for a in range(self.count):
            self.own(a).start()
        self.first(0, True)

    def relays(self, a, t, own, act):
        lev = level_at(self.level, self.planes, t)
        up, down = self.has_up, self.has_down
        if not own:
            up, down = up & (lev < self.level), down & (lev > self.level)
        pl.when(up)(lambda: act(self.along_z(a, lev, own, True)))
        pl.when(down)(lambda: act(self.along_z(a, lev, own, False)))

    def first(self, t, own=False):
        lev = level_at(self.level, self.planes, t)
        for a in range(self.count):
            slot = lev * 4 + self.place.here
            if not own:
                self.along_z(a, lev, own, True).wait_recv()
            self.relays(a, t, own, lambda copy: copy.start())
            self.along_x(a, lev, slot, own).start()
            self.along_y(a, lev, slot, own).start()
            if not own:
                self.share(a, slot).start()

    def second(self, t):
        lev = level_at(self.level, self.planes, t)
        for a in range(self.count):
            slot = lev * 4 + self.place.there_y
            self.along_y(a, lev, slot).wait_recv()
            self.corner_x(a, lev, slot).start()
            self.share(a, slot).start()
            slot = lev * 4 + self.place.there_x
            self.along_x(a, lev, slot).wait_recv()
            self.corner_y(a, lev, slot).start()
            self.share(a, slot).start()

    def third(self, t):
        lev = level_at(self.level, self.planes, t)
        for a in range(self.count):
            slot = lev * 4 + self.place.across
            self.corner_x(a, lev, slot).wait_recv()
            self.corner_y(a, lev, slot).wait_recv()
            self.share(a, slot).start()

    def advance(self, i):
        pl.when(i < self.planes)(lambda: self.first(i))
        pl.when(i < self.planes + 1)(lambda: self.second(i - 1))
        pl.when(i > 1)(lambda: self.third(i - 2))

    def segments(self):
        return [(0, self.planes + 1, lambda i: self.advance(i + 1))]

    def sent(self, t, own):
        place, lev = self.place, level_at(self.level, self.planes, t)
        for a in range(self.count):
            slot = lev * 4 + place.here
            self.relays(a, t, own, lambda copy: copy.wait_send())
            self.along_x(a, lev, slot, own).wait_send()
            self.along_y(a, lev, slot, own).wait_send()
            self.corner_x(a, lev, lev * 4 + place.there_y).wait_send()
            self.corner_y(a, lev, lev * 4 + place.there_x).wait_send()
            for other in [place.there_y, place.there_x, place.across]:
                self.share(a, lev * 4 + other).wait_send()
            if not own:
                self.share(a, slot).wait_send()

    def end(self):
        if not self.landed:
            self.receive_all()
        self.sent(0, True)
        pl.loop(1, self.planes)(lambda t: self.sent(t, False))

    def ready(self, slot, other):
        for a in range(self.count):
            if other:
                self.share(a, slot, 1 - self.place.core).wait_recv()
            else:
                self.own(a).wait()

    def receive(self, t):
        place, lev = self.place, level_at(self.level, self.planes, t)
        pl.when(t == 0)(lambda: self.ready(lev * 4 + place.here, False))
        pl.when(t > 0)(lambda: self.ready(lev * 4 + place.here, True))
        for spot in (place.there_y, place.there_x, place.across):
            self.ready(lev * 4 + spot, True)

    def receive_all(self):
        self.landed = True
        pl.loop(0, self.planes)(self.receive)


class NormGather(Gather):
    def __init__(self, rows, gains, gain_row, planes):
        super().__init__([jax.ShapeDtypeStruct(rows.shape, jnp.bfloat16)], planes)
        self.ins = [(rows, pltpu.VMEM)]
        self.scratch = self.scratch + [pltpu.VMEM(rows.shape, jnp.bfloat16)]
        self.gains, self.gain_row = gains, gain_row

    def bind(self, place, ins, outs, scratch):
        super().bind(place, [scratch[-1]], outs, scratch[:-1])
        self.rows = ins[0]

    def begin(self):
        self.gains.end()
        rows = self.rows[...]
        stat = lax.rsqrt(jnp.mean(rows * rows, axis=-1, keepdims=True) + norm_eps)
        cols = rows.shape[1] // self.place.groups
        for j in range(self.place.groups):
            at = slice(j * cols, (j + 1) * cols)
            gain = self.gains.result[j, self.gain_row : self.gain_row + 1, :].astype(jnp.float32)
            self.sources[0][:, at] = (rows[:, at] * stat * gain).astype(jnp.bfloat16)
        super().begin()


class Reduce:
    def __init__(
        self, operands, produce, slots, block, width, scratch=(), prepare=None, extra=(), prelude=None, delay=0
    ):
        planes, rows, kind = slots // 4, block // 2, jnp.bfloat16
        self.planes, self.reach = planes, planes
        self.ins = [(a, pltpu.VMEM) for a in operands]
        self.outs = [(jax.ShapeDtypeStruct((block, width), jnp.float32), pltpu.VMEM)]
        self.outs += [(shape, pltpu.VMEM) for shape in extra]
        self.own_scratch, self.produce, self.prepare = len(scratch), produce, prepare
        self.prelude, self.delay = prelude, delay
        by_level = DMA((planes,))
        self.scratch = (
            list(scratch)
            + [pltpu.VMEM((slots, block, width) if produce else (8, LANES), kind)]
            + [pltpu.VMEM((slots, rows, width), kind)]
            + [pltpu.VMEM((planes, rows // 2, width), kind)] * 2
            + [pltpu.VMEM((planes, rows, width), kind)] * 4
            + [DMA((slots,))]
            + [by_level] * 6
            + [DMA, DMA((slots,))]
            + [by_level] * 5
            + [DMA]
        )

    def bind(self, place, ins, outs, scratch):
        self.place, self.out = place, outs[0]
        self.refs = list(ins) + list(outs[1:]) + list(scratch[: self.own_scratch])
        scratch = scratch[self.own_scratch :]
        self.part = scratch[0] if self.produce else ins[0]
        self.mine = scratch[1]
        self.from_a, self.from_b, self.from_x, self.from_y = scratch[2:6]
        self.from_up, self.from_down = scratch[6:8]
        self.in_p, self.in_a, self.in_b, self.in_x, self.in_y = scratch[8:13]
        self.in_up, self.in_down, self.in_m, self.out_p = scratch[13:17]
        self.out_a, self.out_b, self.out_x, self.out_y, self.out_z, self.out_m = scratch[17:]
        self.level = lax.rem(place.chip // 4, self.planes)
        self.has_up, self.has_down = self.level < self.planes - 1, self.level > 0
        self.rows = self.part.shape[1] // 2
        self.half = self.rows // 2

    def swap(self, slot):
        theirs = part_rows((1 - self.place.core) * self.rows, self.rows)
        return remote(
            self.part.at[slot, theirs],
            self.mine.at[slot],
            self.out_p.at[slot],
            self.in_p.at[slot],
            self.place.mate,
        )

    def add_into(self, dst, terms, first, size):
        step = 16

        @pl.loop(0, size // step)
        def _(i):
            at = first + i * step
            total = None
            for term, shift in terms:
                block = term[part_rows(at + shift, step), :].astype(jnp.float32)
                total = block if total is None else total + block
            dst[part_rows(at, step), :] = total.astype(dst.dtype)

    def send_a(self, lev):
        src = self.mine.at[lev * 4 + self.place.across, pl.ds(0, self.half)]
        return remote(
            src, self.from_a.at[lev], self.out_a.at[lev], self.in_a.at[lev], self.place.by_x
        )

    def send_b(self, lev):
        src = self.mine.at[lev * 4 + self.place.across, pl.ds(self.half, self.half)]
        return remote(
            src, self.from_b.at[lev], self.out_b.at[lev], self.in_b.at[lev], self.place.by_y
        )

    def send_y(self, lev):
        src = self.mine.at[lev * 4 + self.place.there_y]
        return remote(
            src, self.from_y.at[lev], self.out_y.at[lev], self.in_y.at[lev], self.place.by_y
        )

    def send_x(self, lev):
        src = self.mine.at[lev * 4 + self.place.there_x]
        return remote(
            src, self.from_x.at[lev], self.out_x.at[lev], self.in_x.at[lev], self.place.by_x
        )

    def send_up(self, lev):
        src = self.mine.at[lev * 4 + self.place.here]
        return remote(
            src, self.from_down.at[lev], self.out_z.at[lev], self.in_down.at[lev], self.place.above
        )

    def send_down(self, lev):
        src = self.mine.at[lev * 4 + self.place.here]
        return remote(
            src, self.from_up.at[lev], self.out_z.at[lev], self.in_up.at[lev], self.place.below
        )

    def plane(self, i):
        return level_at(self.level, self.planes, self.planes - 1 - i)

    def make(self, i):
        @pl.loop(0, 4)
        def _(q):
            slot = self.plane(i) * 4 + self.place.spot(q)
            if self.produce is not None:
                self.produce(self.part, slot, self.refs)
            self.swap(slot).start()

    def join(self, slot):
        self.swap(slot).wait_recv()
        mine = self.mine.at[slot]
        terms = [(mine, 0), (self.part.at[slot], self.place.core * self.rows)]
        self.add_into(mine, terms, 0, self.rows)

    def first(self, i):
        lev = self.plane(i)
        self.join(lev * 4 + self.place.across)
        self.send_a(lev).start()
        self.send_b(lev).start()
        self.join(lev * 4 + self.place.there_y)
        self.join(lev * 4 + self.place.there_x)

    def second(self, i):
        lev = self.plane(i)
        mine = self.mine.at[lev * 4 + self.place.there_y]
        self.send_a(lev).wait_recv()
        self.add_into(mine, [(mine, 0), (self.from_a.at[lev], 0)], 0, self.half)
        self.send_y(lev).start()
        mine = self.mine.at[lev * 4 + self.place.there_x]
        self.send_b(lev).wait_recv()
        self.add_into(mine, [(mine, 0), (self.from_b.at[lev], -self.half)], self.half, self.half)
        self.send_x(lev).start()
        self.join(lev * 4 + self.place.here)

    def third(self, i):
        rows, out, lev = self.rows, self.out, self.plane(i)
        mine = self.mine.at[lev * 4 + self.place.here]
        self.send_y(lev).wait_recv()
        self.send_x(lev).wait_recv()
        terms = [(mine, 0), (self.from_y.at[lev], 0), (self.from_x.at[lev], 0)]

        def more(total, cond, send, arrived):
            @pl.when(cond)
            def _():
                send(lev).wait_recv()
                self.add_into(total, [(total, 0), (arrived.at[lev], 0)], 0, rows)

        @pl.when(lev == self.level)
        def _():
            total = out.at[part_rows(self.place.core * rows, rows)]
            self.add_into(total, terms, 0, rows)
            more(total, self.has_up, self.send_down, self.from_up)
            more(total, self.has_down, self.send_up, self.from_down)

        @pl.when(lev < self.level)
        def _():
            self.add_into(mine, terms, 0, rows)
            more(mine, self.has_up, self.send_down, self.from_up)
            self.send_down(lev).start()

        @pl.when(lev > self.level)
        def _():
            self.add_into(mine, terms, 0, rows)
            more(mine, self.has_down, self.send_up, self.from_down)
            self.send_up(lev).start()

    def begin(self):
        if self.prepare is not None:
            self.prepare(self.refs)
        if self.prelude is None:
            self.make(0)

    def advance(self, i):
        pl.when(i + 1 < self.planes)(lambda: self.make(i + 1))
        pl.when(i < self.planes)(lambda: self.first(i))
        pl.when((i > 0) & (i < self.planes + 1))(lambda: self.second(i - 1))
        pl.when(i > 1)(lambda: self.third(i - 2))

    def segments(self):
        parts, start = [], 0
        if self.prelude is not None:
            count, call = self.prelude(self.refs)
            parts = [(self.delay, count, call), (self.delay + count, 1, self.make)]
            start = self.delay + count + 1
        return parts + [(start, self.planes + 2, self.advance)]

    def hand(self, whose):
        spot = part_rows(whose * self.rows, self.rows)
        return remote(self.out.at[spot], self.out.at[spot], self.out_m, self.in_m, self.place.mate)

    def end(self):
        self.hand(self.place.core).start()


        @pl.loop(0, self.planes)
        def _(lev):
            for spot in range(4):
                self.swap(lev * 4 + spot).wait_send()
            for send in (self.send_a, self.send_b, self.send_y, self.send_x):
                send(lev).wait_send()
            pl.when(lev < self.level)(lambda: self.send_down(lev).wait_send())
            pl.when(lev > self.level)(lambda: self.send_up(lev).wait_send())

        self.hand(self.place.core).wait_send()
        self.hand(1 - self.place.core).wait_recv()


class Experts:
    def __init__(self, gather, weights, shared_w, capacity):
        slots, seq, width = gather.outs[0][0].shape
        hidden, room, bf16 = weights[0].shape[0], shared_w.shape[1], jnp.bfloat16
        self.gather, self.capacity, self.room, self.reach = gather, capacity, room, gather.reach
        self.slots, self.seq, self.width, self.hidden = slots, seq, width, hidden
        rows = (slots, capacity)
        turn = (room, slots * seq)

        def shape(dims, kind=bf16):
            return jax.ShapeDtypeStruct(dims, kind)

        self.ins = [(a, pl.ANY) for a in weights] + [(shared_w, pltpu.VMEM)]
        self.outs = [
            (shape((slots, seq, width + LANES)), pltpu.VMEM),
            (shape(rows + (width,)), pltpu.VMEM),
            (shape(rows + (seq,)), pltpu.VMEM),
            (shape(turn), pltpu.VMEM),
            (shape((3, room, width)), pltpu.VMEM),
            (shape(rows + (width,)), pl.ANY),
            (shape(rows + (width,)), pl.ANY),
        ] + [(shape(rows + (hidden,)), pltpu.VMEM)] * 3
        self.scratch = (
            [pltpu.VMEM(w.shape, bf16) for w in weights]
            + [pltpu.VMEM((4 * capacity, width), bf16)] * 3
            + [
                pltpu.VMEM((4 * capacity, LANES), jnp.float32),
                pltpu.VMEM((4 * capacity + 2 * room, width), bf16),
                pltpu.VMEM((4 * capacity + 2 * room, 4 * seq), bf16),
                pltpu.VMEM((3, room, width), jnp.float32),
                DMA((3,)),
                DMA((2,)),
            ]
        )

    def bind(self, place, ins, outs, scratch):
        self.place = place
        self.hbm_weights, self.shared_w = ins[:3], ins[3]
        self.tokens, self.out_rows, self.marked = self.gather.results
        self.part, self.out_block, self.picks, self.act_turn, self.shared_grads = outs[:5]
        self.rows_hbm, self.cot_hbm, self.act, self.gate_delta, self.up_delta = outs[5:]
        self.gate, self.up, self.down = scratch[:3]
        self.rows, self.cot, self.grads = scratch[3:6]
        self.weight, self.held, self.left, self.total, self.load_sem, self.save_sem = scratch[6:]
        self.level = lax.rem(place.chip // 4, self.gather.planes)

    def loads(self):
        pairs = zip(self.hbm_weights, [self.gate, self.up, self.down])
        return [
            pltpu.make_async_copy(src, dst, self.load_sem.at[k]) for k, (src, dst) in enumerate(pairs)
        ]

    def saves(self, lev):
        at = pl.ds(lev * 4 * self.capacity, 4 * self.capacity)
        pairs = [(self.rows, self.rows_hbm), (self.cot, self.cot_hbm)]
        return [
            pltpu.make_async_copy(
                src.reshape(4, self.capacity, self.width), dst.at[pl.ds(lev * 4, 4)], self.save_sem.at[k]
            )
            for k, (src, dst) in enumerate(pairs)
        ]

    def begin(self):
        for load in self.loads():
            load.start()
        self.total[...] = jnp.zeros_like(self.total)
        self.held[4 * self.capacity :] = self.shared_w[:2].reshape(2 * self.room, self.width)
        self.left[: 4 * self.capacity] = jnp.zeros((4 * self.capacity, 4 * self.seq), jnp.bfloat16)

    def choose(self, lev, t):
        seq, cap = self.seq, self.capacity
        below = lax.broadcasted_iota(jnp.int32, (seq, seq), 0)
        upto = (below <= lax.broadcasted_iota(jnp.int32, (seq, seq), 1)).astype(jnp.bfloat16)
        place_in = lax.broadcasted_iota(jnp.int32, (cap, seq), 0).astype(jnp.float32)

        @pl.when(t > 0)
        def _():
            for save in self.saves(lev):
                save.wait()

        for j in range(4):
            slot, at = lev * 4 + j, slice(j * cap, (j + 1) * cap)
            turned = self.marked[slot].T
            here = jnp.sum(jnp.where(below == self.place.chip, turned, 0.0), axis=0, keepdims=True)
            routed = jnp.where(here >= 0.0, 1.0, 0.0)
            order = fdot(jnp.broadcast_to(routed, (8, seq)).astype(jnp.bfloat16), upto)[:1] - 1.0
            hit = jnp.where(order == place_in, routed, 0.0)
            weight = jnp.sum(hit * here, axis=-1, keepdims=True)
            pick = hit.astype(jnp.bfloat16)
            self.picks[slot] = pick
            self.left[at, j * seq : (j + 1) * seq] = pick
            self.weight[at] = jnp.broadcast_to(weight, (cap, LANES))
        chosen, weight = self.left[: 4 * cap], self.weight[:, :1]

        @pl.loop(0, self.width // 512, unroll=True)
        def _(k):
            cols, four = part_rows(k * 512, 512), pl.ds(lev * 4, 4)
            own = fdot(chosen, self.tokens[four, :, cols].reshape(4 * seq, 512))
            self.rows[:, cols] = own.astype(jnp.bfloat16)
            grad = fdot(chosen, self.out_rows[four, :, cols].reshape(4 * seq, 512))
            self.grads[:, cols] = grad.astype(jnp.bfloat16)
            self.cot[:, cols] = (weight * grad).astype(jnp.bfloat16)

        for save in self.saves(lev):
            save.start()

    def hidden_units(self, lev):
        slots, chunk = pl.ds(lev * 4, 4), 256
        for start in range(0, self.hidden, chunk):
            cols = slice(start, min(start + chunk, self.hidden))
            shape = (4, self.capacity, cols.stop - cols.start)
            gate = dot_nt(self.rows[...], self.gate[cols])
            up = dot_nt(self.rows[...], self.up[cols])
            grad = dot_nt(self.cot[...], self.down[cols])
            sig = jax.nn.sigmoid(gate)
            gated = gate * sig
            self.act[slots, :, cols] = (gated * up).astype(jnp.bfloat16).reshape(shape)
            slope = sig * (1.0 + gate * (1.0 - sig))
            self.gate_delta[slots, :, cols] = (grad * up * slope).astype(jnp.bfloat16).reshape(shape)
            self.up_delta[slots, :, cols] = (grad * gated).astype(jnp.bfloat16).reshape(shape)

    def shared_units(self, lev):
        seq4, room = 4 * self.seq, self.room
        tokens = self.tokens[pl.ds(lev * 4, 4)].reshape(seq4, self.width)
        grads = self.out_rows[pl.ds(lev * 4, 4)].reshape(seq4, self.width)
        both = dot_nt(self.shared_w[:2].reshape(2 * room, self.width), tokens)
        gate, up = both[:room], both[room:]
        grad = dot_nt(self.shared_w[2], grads)
        sig = jax.nn.sigmoid(gate)
        act = (gate * sig * up).astype(jnp.bfloat16)
        gate_delta = (grad * up * (sig * (1.0 + gate * (1.0 - sig)))).astype(jnp.bfloat16)
        up_delta = (grad * gate * sig).astype(jnp.bfloat16)
        self.act_turn[:, part_rows(lev * seq4, seq4)] = act
        self.left[4 * self.capacity : 4 * self.capacity + room] = gate_delta
        self.left[4 * self.capacity + room :] = up_delta

        @pl.loop(0, self.width // 512, unroll=True)
        def _(k):
            cols, four = part_rows(k * 512, 512), pl.ds(lev * 4, 4)
            some = self.tokens[four, :, cols].reshape(seq4, 512)
            self.total[0, :, cols] += fdot(gate_delta, some)
            self.total[1, :, cols] += fdot(up_delta, some)
            some = self.out_rows[four, :, cols].reshape(seq4, 512)
            self.total[2, :, cols] += fdot(act, some)

    def outward(self, lev):
        slots, cap, count = pl.ds(lev * 4, 4), self.capacity, 4 * self.capacity
        act = self.act[slots].reshape(count, self.hidden)
        gate_delta = self.gate_delta[slots].reshape(count, self.hidden)
        up_delta = self.up_delta[slots].reshape(count, self.hidden)
        weight = self.weight[:, :1]

        def some(k, route):
            cols = part_rows(k * 512, 512)
            out = fdot(act, self.down[:, cols]).astype(jnp.bfloat16).astype(jnp.float32)
            route += jnp.sum(out * self.grads[:, cols].astype(jnp.float32), axis=-1, keepdims=True)
            out = (weight * out).astype(jnp.bfloat16)
            self.out_block[slots, :, cols] = out.reshape(4, cap, 512)
            back = fdot(gate_delta, self.gate[:, cols]) + fdot(up_delta, self.up[:, cols])
            self.held[:count, cols] = back.astype(jnp.bfloat16)
            return route

        route = lax.fori_loop(
            0, self.width // 512, some, jnp.zeros((count, 1), jnp.float32), unroll=True
        )
        lane = lax.broadcasted_iota(jnp.int32, (count, LANES), 1)
        routes = jnp.where(lane == self.place.chip, route, 0.0).astype(jnp.bfloat16)
        shape = (4, self.seq, LANES)
        turned = dot_tn(self.left[:count], routes).astype(jnp.bfloat16)
        self.part[slots, :, self.width :] = turned.reshape(shape)
        left = self.left[...]

        @pl.loop(0, self.width // 512, unroll=True)
        def _(k):
            cols = part_rows(k * 512, 512)
            sums = dot_tn(left, self.held[:, cols]).astype(jnp.bfloat16)
            self.part[slots, :, cols] = sums.reshape(4, self.seq, 512)

    def compute(self, t):
        lev = level_at(self.level, self.gather.planes, t)

        @pl.when(t == 0)
        def _():
            for load in self.loads():
                load.wait()

        self.gather.receive(t)
        self.choose(lev, t)
        self.hidden_units(lev)
        self.shared_units(lev)

    def advance(self, i):
        planes = self.gather.planes
        pl.when(i > 1)(lambda: self.outward(level_at(self.level, planes, i - 2)))
        pl.when((i > 0) & (i < planes + 1))(lambda: self.compute(i - 1))

    def segments(self):
        self.gather.landed = True
        return [(0, self.gather.planes + 2, self.advance)]

    def end(self):
        for save in self.saves(level_at(self.level, self.gather.planes, self.gather.planes - 1)):
            save.wait()
        self.shared_grads[...] = self.total[...].astype(jnp.bfloat16)


def greet(place, ops):
    barrier = pltpu.get_barrier_semaphore()
    expected = 1

    def call(target):
        pl.semaphore_signal(barrier, inc=1, device_id=target, device_id_type=MESH)

    call(place.mate)
    if any(op.reach == 0 for op in ops):
        for j in range(1, place.groups):
            call({EXPERT: place.partner(j)})
        expected += place.groups - 1
    else:
        call(place.by_x)
        call(place.by_y)
        planes = max(op.reach for op in ops)
        level = lax.rem(place.chip // 4, planes)
        has_up, has_down = level < planes - 1, level > 0
        pl.when(has_up)(lambda: call(place.above))
        pl.when(has_down)(lambda: call(place.below))
        expected += 2 + has_up.astype(jnp.int32) + has_down.astype(jnp.int32)
    pl.semaphore_wait(barrier, expected)


def chip_kernel(ops, *refs):
    place = Place()
    n_in = sum(len(op.ins) for op in ops)
    n_out = sum(len(op.outs) for op in ops)
    ins, outs, scratch = refs[:n_in], refs[n_in : n_in + n_out], refs[n_in + n_out :]
    for op in ops:
        op.bind(place, ins[: len(op.ins)], outs[: len(op.outs)], scratch[: len(op.scratch)])
        ins, outs = ins[len(op.ins) :], outs[len(op.outs) :]
        scratch = scratch[len(op.scratch) :]
    greet(place, ops)
    for op in ops:
        op.begin()
    parts = [part for op in ops for part in op.segments() if part[1] > 0]
    if parts:

        @pl.loop(0, max(start + count for start, count, _ in parts))
        def _(r):
            for start, count, call in parts:
                inside = (r >= start) & (r < start + count)
                pl.when(inside)(functools.partial(call, r - start))

    ended = [op.gains for op in ops if isinstance(op, NormGather)]
    for op in ops:
        if op not in ended:
            op.end()


def exchange(ops, ident):
    ins = [pair for op in ops for pair in op.ins]
    outs = [pair for op in ops for pair in op.outs]
    moved = sum(a.size * a.dtype.itemsize for a, _ in ins + outs)
    results = pl.pallas_call(
        functools.partial(chip_kernel, ops),
        out_shape=[shape for shape, _ in outs],
        in_specs=[pl.BlockSpec(memory_space=space) for _, space in ins],
        out_specs=[pl.BlockSpec(memory_space=space) for _, space in outs],
        scratch_shapes=[entry for op in ops for entry in op.scratch],
        compiler_params=pltpu.CompilerParams(
            collective_id=ident, has_side_effects=True, vmem_limit_bytes=60 << 20
        ),
        cost_estimate=pl.CostEstimate(flops=0, bytes_accessed=moved, transcendentals=0),
    )(*[a for a, _ in ins])
    split = []
    for op in ops:
        split.append(results[: len(op.outs)])
        results = results[len(op.outs) :]
    return split


def general_scores(query_blk, key_rows, first_row):
    scores = jnp.einsum(
        "qhd,khd->hqk", query_blk, key_rows, preferred_element_type=jnp.float32
    ) * DQK ** (-0.5)
    row_pos = first_row + jnp.arange(query_blk.shape[0], dtype=jnp.int32)
    col_pos = jnp.arange(key_rows.shape[0], dtype=jnp.int32)
    return jnp.where(col_pos[None, None, :] <= row_pos[None, :, None], scores, -1e30)


def attend(query_rows, key_rows, value_rows):
    seq_len = query_rows.shape[0]
    blk_rows = min(seq_len, 512)

    def one_block(block_index):
        first_row = block_index * blk_rows
        scores = general_scores(query_rows, key_rows, first_row)
        row_max = jnp.max(scores, axis=-1, keepdims=True)
        log_total = row_max + jnp.log(jnp.sum(jnp.exp(scores - row_max), axis=-1, keepdims=True))
        att_weights = jnp.exp(scores - log_total).astype(jnp.bfloat16)
        mixed_blk = jnp.einsum(
            "hqk,khd->qhd", att_weights, value_rows, preferred_element_type=jnp.float32
        ).astype(jnp.bfloat16)
        return (mixed_blk, log_total)

    mixed_heads, log_totals = lax.map(one_block, jnp.arange(seq_len // blk_rows, dtype=jnp.int32))
    return (mixed_heads.reshape(seq_len, query_rows.shape[1], value_rows.shape[2]), log_totals)


def attend_back(query_rows, key_rows, value_rows, log_totals, mixed_grad):
    seq_len, head_count = (query_rows.shape[0], query_rows.shape[1])
    blk_rows = min(seq_len, 512)

    def one_block(running, block_index):
        key_acc, value_acc = running
        first_row = block_index * blk_rows
        scores = general_scores(query_rows, key_rows, first_row)
        att_probs = jnp.exp(scores - log_totals[block_index])
        att_weights = att_probs.astype(jnp.bfloat16)
        value_acc = value_acc + jnp.einsum(
            "hqk,qhd->khd", att_weights, mixed_grad, preferred_element_type=jnp.float32
        )
        prob_grad = jnp.einsum(
            "qhd,khd->hqk", mixed_grad, value_rows, preferred_element_type=jnp.float32
        )
        row_delta = jnp.sum(att_probs * prob_grad, axis=-1, keepdims=True)
        score_delta = (att_probs * (prob_grad - row_delta) * DQK ** (-0.5)).astype(jnp.bfloat16)
        query_grad = jnp.einsum(
            "hqk,khd->qhd", score_delta, key_rows, preferred_element_type=jnp.float32
        )
        key_acc = key_acc + jnp.einsum(
            "hqk,qhd->khd", score_delta, query_rows, preferred_element_type=jnp.float32
        )
        return ((key_acc, value_acc), query_grad)

    zero_start = (
        jnp.zeros((seq_len, head_count, DQK), jnp.float32),
        jnp.zeros((seq_len, head_count, DV), jnp.float32),
    )
    (key_grad, value_grad), query_grad = lax.scan(
        one_block, zero_start, jnp.arange(seq_len // blk_rows, dtype=jnp.int32)
    )
    return (query_grad.reshape(seq_len, head_count, DQK), key_grad, value_grad)


def attention_forward(seq_in, gain_one, query_w, latent_w, gain_kv, kvup_w):
    seq_len = seq_in.shape[0]
    head_count = query_w.shape[1] // DQK
    cosine, sine_part = rope_tables(seq_len, DR)
    stat_one = rms_scale(seq_in)
    unit_one = seq_in * stat_one
    normed1 = (unit_one * gain_one.astype(jnp.float32)).astype(jnp.bfloat16)
    query_full = jnp.dot(normed1, query_w, preferred_element_type=jnp.float32).reshape(
        seq_len, head_count, DQK
    )
    query_rows = jnp.concatenate(
        [
            query_full[..., :DN],
            rotate(query_full[..., DN:], cosine[:, None, :], sine_part[:, None, :]),
        ],
        axis=-1,
    ).astype(jnp.bfloat16)
    latent_full = jnp.dot(normed1, latent_w, preferred_element_type=jnp.float32)
    latent_stat = rms_scale(latent_full[:, : kvup_w.shape[0]])
    latent_unit = latent_full[:, : kvup_w.shape[0]] * latent_stat
    latent = (latent_unit * gain_kv.astype(jnp.float32)).astype(jnp.bfloat16)
    rot_key = rotate(latent_full[:, kvup_w.shape[0] :], cosine, sine_part).astype(jnp.bfloat16)
    key_value = (
        jnp.dot(latent, kvup_w, preferred_element_type=jnp.float32)
        .astype(jnp.bfloat16)
        .reshape(seq_len, head_count, DN + DV)
    )
    key_rows = jnp.concatenate(
        [key_value[..., :DN], jnp.broadcast_to(rot_key[:, None, :], (seq_len, head_count, DR))],
        axis=-1,
    )
    value_rows = key_value[..., DN:]
    mixed_heads, log_totals = attend(query_rows, key_rows, value_rows)
    return (
        stat_one,
        unit_one,
        normed1,
        query_rows,
        latent_stat,
        latent_unit,
        latent,
        key_rows,
        value_rows,
        mixed_heads,
        log_totals,
        cosine,
        sine_part,
    )


def general(
    layer_in,
    norm1_gain,
    q_weight,
    kva_weight,
    kv_gain,
    kvb_weight,
    o_weight,
    norm2_gain,
    router_weight,
    shared_gate,
    shared_up,
    shared_down,
    expert_gate,
    expert_up,
    expert_down,
    routes,
    out_grad,
):
    groups = lax.axis_size(EXPERT)
    seq_len, width = layer_in.shape
    local_experts = expert_gate.shape[0]
    expert_count = local_experts * groups
    capacity = seq_len * TOPK * 4 // (3 * expert_count)
    rows_total = expert_count * capacity
    (
        gain_one,
        query_w,
        latent_w,
        gain_kv,
        kvup_w,
        output_w,
        gain_two,
        route_w,
        gate_sh,
        up_sh,
        down_sh,
    ) = (
        lax.all_gather(norm1_gain, EXPERT, axis=0, tiled=True),
        lax.all_gather(q_weight, EXPERT, axis=0, tiled=True),
        lax.all_gather(kva_weight, EXPERT, axis=0, tiled=True),
        lax.all_gather(kv_gain, EXPERT, axis=0, tiled=True),
        lax.all_gather(kvb_weight, EXPERT, axis=0, tiled=True),
        lax.all_gather(o_weight, EXPERT, axis=1, tiled=True),
        lax.all_gather(norm2_gain, EXPERT, axis=0, tiled=True),
        lax.all_gather(router_weight, EXPERT, axis=0, tiled=True),
        lax.all_gather(shared_gate, EXPERT, axis=0, tiled=True),
        lax.all_gather(shared_up, EXPERT, axis=0, tiled=True),
        lax.all_gather(shared_down, EXPERT, axis=1, tiled=True),
    )
    (
        stat_one,
        unit_one,
        normed1,
        query_rows,
        latent_stat,
        latent_unit,
        latent,
        key_rows,
        value_rows,
        mixed_heads,
        log_totals,
        cosine,
        sine_part,
    ) = attention_forward(layer_in, gain_one, query_w, latent_w, gain_kv, kvup_w)
    head_count = query_rows.shape[1]
    mixed_flat = mixed_heads.reshape(seq_len, head_count * DV)
    attn_part = jnp.dot(mixed_flat, output_w, preferred_element_type=jnp.float32)
    hidden_state = layer_in + lax.psum(attn_part, TENSOR)
    stat_two = rms_scale(hidden_state)
    unit_two = hidden_state * stat_two
    normed2 = (unit_two * gain_two.astype(jnp.float32)).astype(jnp.bfloat16)
    router_probs = jax.nn.softmax(
        jnp.dot(normed2, route_w, preferred_element_type=jnp.float32), axis=-1
    )
    route_onehot = (
        routes[:, :, None] == jnp.arange(expert_count, dtype=jnp.int32)[None, None, :]
    ).astype(jnp.float32)
    route_weight = jnp.einsum("tke,te->tk", route_onehot, router_probs)
    flat_hot = route_onehot.reshape(seq_len * TOPK, expert_count).astype(jnp.int32)
    slot_pos = jnp.sum(jnp.cumsum(flat_hot, axis=0) * flat_hot, axis=-1) - 1
    buffer_pos = routes.reshape(-1) * capacity + slot_pos

    def to_owners(assigned):
        buffer = jnp.zeros((rows_total, width), jnp.bfloat16).at[buffer_pos].set(assigned)
        buffer = buffer.reshape(groups, local_experts * capacity, width)
        arrived = lax.all_to_all(buffer, EXPERT, split_axis=0, concat_axis=0, tiled=True)
        return (
            arrived.reshape(groups, local_experts, capacity, width)
            .transpose(1, 0, 2, 3)
            .reshape(local_experts, groups * capacity, width)
        )

    def to_sources(results):
        arranged = (
            results.reshape(local_experts, groups, capacity, width)
            .transpose(1, 0, 2, 3)
            .reshape(groups, local_experts * capacity, width)
        )
        arrived = lax.all_to_all(arranged, EXPERT, split_axis=0, concat_axis=0, tiled=True)
        return arrived.reshape(rows_total, width)[buffer_pos].reshape(seq_len, TOPK, width)

    rows_in = to_owners(jnp.repeat(normed2, TOPK, axis=0))
    pre_gate = jnp.einsum("emd,edf->emf", rows_in, expert_gate, preferred_element_type=jnp.float32)
    pre_up = jnp.einsum("emd,edf->emf", rows_in, expert_up, preferred_element_type=jnp.float32)
    expert_act = (jax.nn.silu(pre_gate) * pre_up).astype(jnp.bfloat16)
    block_out = jnp.einsum(
        "emf,efd->emd", expert_act, expert_down, preferred_element_type=jnp.float32
    ).astype(jnp.bfloat16)
    expert_out = to_sources(block_out)
    routed_part = jnp.einsum(
        "tk,tkd->td", route_weight, expert_out, preferred_element_type=jnp.float32
    )
    shared_pre_gate = jnp.dot(normed2, gate_sh, preferred_element_type=jnp.float32)
    shared_pre_up = jnp.dot(normed2, up_sh, preferred_element_type=jnp.float32)
    shared_act = (jax.nn.silu(shared_pre_gate) * shared_pre_up).astype(jnp.bfloat16)
    shared_part = jnp.dot(shared_act, down_sh, preferred_element_type=jnp.float32)
    layer_out = hidden_state + lax.psum(
        (routed_part + shared_part).astype(jnp.bfloat16), TENSOR
    ).astype(jnp.float32)
    out_rows = out_grad.astype(jnp.bfloat16)
    routed_cot = (
        (route_weight[:, :, None] * out_grad[:, None, :])
        .astype(jnp.bfloat16)
        .reshape(seq_len * TOPK, width)
    )
    cot_in = to_owners(routed_cot)
    route_grad_part = jnp.einsum(
        "tkd,td->tk", expert_out, out_grad, preferred_element_type=jnp.float32
    )
    hidden_grad_ex = jnp.einsum(
        "emd,efd->emf", cot_in, expert_down, preferred_element_type=jnp.float32
    )
    gate_delta = (hidden_grad_ex * pre_up * silu_grad(pre_gate)).astype(jnp.bfloat16)
    up_delta = (hidden_grad_ex * jax.nn.silu(pre_gate)).astype(jnp.bfloat16)
    expert_down_grad = jnp.einsum(
        "emf,emd->efd", expert_act, cot_in, preferred_element_type=jnp.float32
    )
    expert_gate_grad = jnp.einsum(
        "emd,emf->edf", rows_in, gate_delta, preferred_element_type=jnp.float32
    )
    expert_up_grad = jnp.einsum(
        "emd,emf->edf", rows_in, up_delta, preferred_element_type=jnp.float32
    )
    row_block = (
        jnp.einsum("emf,edf->emd", gate_delta, expert_gate, preferred_element_type=jnp.float32)
        + jnp.einsum("emf,edf->emd", up_delta, expert_up, preferred_element_type=jnp.float32)
    ).astype(jnp.bfloat16)
    row_grad = to_sources(row_block)
    shared_down_grad = jnp.dot(shared_act.T, out_rows, preferred_element_type=jnp.float32)
    shared_hidden_grad = jnp.dot(out_rows, down_sh.T, preferred_element_type=jnp.float32)
    shared_gate_delta = (shared_hidden_grad * shared_pre_up * silu_grad(shared_pre_gate)).astype(
        jnp.bfloat16
    )
    shared_up_delta = (shared_hidden_grad * jax.nn.silu(shared_pre_gate)).astype(jnp.bfloat16)
    shared_gate_grad = jnp.dot(normed2.T, shared_gate_delta, preferred_element_type=jnp.float32)
    shared_up_grad = jnp.dot(normed2.T, shared_up_delta, preferred_element_type=jnp.float32)
    normed2_part = (
        jnp.sum(row_grad, axis=1, dtype=jnp.float32)
        + jnp.dot(shared_gate_delta, gate_sh.T, preferred_element_type=jnp.float32)
        + jnp.dot(shared_up_delta, up_sh.T, preferred_element_type=jnp.float32)
    )
    normed2_grad, route_grad = lax.psum((normed2_part, route_grad_part), TENSOR)
    prob_grad = jnp.einsum("tk,tke->te", route_grad, route_onehot)
    logit_delta = (
        router_probs * (prob_grad - jnp.sum(router_probs * prob_grad, axis=-1, keepdims=True))
    ).astype(jnp.bfloat16)
    router_grad = jnp.dot(normed2.T, logit_delta, preferred_element_type=jnp.float32)
    normed2_grad = normed2_grad + jnp.dot(
        logit_delta, route_w.T, preferred_element_type=jnp.float32
    )
    norm2_gain_grad = jnp.sum(normed2_grad * unit_two, axis=0)
    scaled_two = normed2_grad * gain_two.astype(jnp.float32)
    hidden_grad = out_grad + stat_two * (
        scaled_two - unit_two * jnp.mean(scaled_two * unit_two, axis=-1, keepdims=True)
    )
    hidden_rows = hidden_grad.astype(jnp.bfloat16)
    o_grad = jnp.dot(mixed_flat.T, hidden_rows, preferred_element_type=jnp.float32)
    mixed_grad = (
        jnp.dot(hidden_rows, output_w.T, preferred_element_type=jnp.float32)
        .astype(jnp.bfloat16)
        .reshape(seq_len, head_count, DV)
    )
    query_grad, key_grad, value_grad = attend_back(
        query_rows, key_rows, value_rows, log_totals, mixed_grad
    )
    query_delta = (
        jnp.concatenate(
            [
                query_grad[..., :DN],
                rotate_back(query_grad[..., DN:], cosine[:, None, :], sine_part[:, None, :]),
            ],
            axis=-1,
        )
        .astype(jnp.bfloat16)
        .reshape(seq_len, head_count * DQK)
    )
    kv_delta = (
        jnp.concatenate([key_grad[..., :DN], value_grad], axis=-1)
        .astype(jnp.bfloat16)
        .reshape(seq_len, head_count * (DN + DV))
    )
    q_grad = jnp.dot(normed1.T, query_delta, preferred_element_type=jnp.float32)
    kvb_grad = jnp.dot(latent.T, kv_delta, preferred_element_type=jnp.float32)
    latent_part = jnp.dot(kv_delta, kvup_w.T, preferred_element_type=jnp.float32)
    rot_part = jnp.sum(key_grad[..., DN:], axis=1)
    normed1_part = jnp.dot(query_delta, query_w.T, preferred_element_type=jnp.float32)
    latent_grad, rot_sum, normed1_query = (
        lax.psum(latent_part.astype(jnp.bfloat16), TENSOR).astype(jnp.float32),
        lax.psum(rot_part.astype(jnp.bfloat16), TENSOR).astype(jnp.float32),
        lax.psum(normed1_part.astype(jnp.bfloat16), TENSOR).astype(jnp.float32),
    )
    kv_gain_grad = jnp.sum(latent_grad * latent_unit, axis=0)
    scaled_lat = latent_grad * gain_kv.astype(jnp.float32)
    latent_back = latent_stat * (
        scaled_lat - latent_unit * jnp.mean(scaled_lat * latent_unit, axis=-1, keepdims=True)
    )
    latent_delta = jnp.concatenate(
        [latent_back, rotate_back(rot_sum, cosine, sine_part)], axis=-1
    ).astype(jnp.bfloat16)
    kva_grad = jnp.dot(normed1.T, latent_delta, preferred_element_type=jnp.float32)
    normed1_grad = normed1_query + jnp.dot(
        latent_delta, latent_w.T, preferred_element_type=jnp.float32
    )
    norm1_gain_grad = jnp.sum(normed1_grad * unit_one, axis=0)
    scaled_one = normed1_grad * gain_one.astype(jnp.float32)
    x_grad = hidden_grad + stat_one * (
        scaled_one - unit_one * jnp.mean(scaled_one * unit_one, axis=-1, keepdims=True)
    )
    (
        norm1_gain_grad,
        q_grad,
        kva_grad,
        kv_gain_grad,
        kvb_grad,
        o_grad,
        norm2_gain_grad,
        router_grad,
        shared_gate_grad,
        shared_up_grad,
        shared_down_grad,
    ) = (
        lax.psum_scatter(norm1_gain_grad, EXPERT, scatter_dimension=0, tiled=True),
        lax.psum_scatter(q_grad, EXPERT, scatter_dimension=0, tiled=True),
        lax.psum_scatter(kva_grad, EXPERT, scatter_dimension=0, tiled=True),
        lax.psum_scatter(kv_gain_grad, EXPERT, scatter_dimension=0, tiled=True),
        lax.psum_scatter(kvb_grad, EXPERT, scatter_dimension=0, tiled=True),
        lax.psum_scatter(o_grad, EXPERT, scatter_dimension=1, tiled=True),
        lax.psum_scatter(norm2_gain_grad, EXPERT, scatter_dimension=0, tiled=True),
        lax.psum_scatter(router_grad, EXPERT, scatter_dimension=0, tiled=True),
        lax.psum_scatter(shared_gate_grad, EXPERT, scatter_dimension=0, tiled=True),
        lax.psum_scatter(shared_up_grad, EXPERT, scatter_dimension=0, tiled=True),
        lax.psum_scatter(shared_down_grad, EXPERT, scatter_dimension=1, tiled=True),
    )
    return (
        layer_out,
        x_grad,
        norm1_gain_grad,
        q_grad,
        kva_grad,
        kv_gain_grad,
        kvb_grad,
        o_grad,
        norm2_gain_grad,
        router_grad,
        shared_gate_grad,
        shared_up_grad,
        shared_down_grad,
        expert_gate_grad,
        expert_up_grad,
        expert_down_grad,
    )


def fits(groups, heads, block, width):
    whole = groups in (4, 8, 16) and heads in (4, 8, 16) and groups % heads == 0
    return whole and block % 64 == 0 and width == groups * LANES


def to_blocks(grad_rows, groups):
    rows, width = grad_rows.shape
    kept = lax.optimization_barrier(grad_rows.astype(jnp.bfloat16))
    return kept.reshape(rows, groups, width // groups).transpose(1, 0, 2)


def from_blocks(blocks):
    groups, rows, width = blocks.shape
    return blocks.transpose(1, 0, 2).reshape(rows, groups * width)


def widen(rows, width):
    return jnp.pad(rows, [(0, 0)] * (rows.ndim - 1) + [(0, width - rows.shape[-1])])


def by_heads(
    layer_in,
    norm1_gain,
    q_weight,
    kva_weight,
    kv_gain,
    kvb_weight,
    o_weight,
    norm2_gain,
    router_weight,
    shared_gate,
    shared_up,
    shared_down,
    expert_gate,
    expert_up,
    expert_down,
    routes,
    out_grad,
):
    groups = lax.axis_size(EXPERT)
    chip = lax.axis_index(EXPERT)
    seq_len, width = layer_in.shape
    capacity = seq_len * TOPK * 4 // (3 * groups)
    heads = q_weight.shape[1] // DQK
    copies = groups // heads
    head = lax.rem(chip, heads)
    own_cols = kva_weight.shape[0]
    lat_rows, lat_width = kvb_weight.shape[0], kvb_weight.shape[0] * groups
    hidden = shared_gate.shape[1] // groups
    bf16 = jnp.bfloat16

    kv_halves = (DN + DV) // own_cols
    kv_block = lat_rows * kv_halves
    head_parts = jnp.concatenate(
        [
            q_weight.reshape(own_cols, heads, DQK).transpose(1, 2, 0),
            kvb_weight.reshape(lat_rows, heads, kv_halves, own_cols)
            .transpose(1, 2, 0, 3)
            .reshape(heads, kv_block, own_cols),
            o_weight.reshape(heads, DV, own_cols),
        ],
        axis=1,
    )
    shared_parts = jnp.concatenate(
        [
            shared_gate.reshape(own_cols, groups, hidden).transpose(1, 2, 0),
            shared_up.reshape(own_cols, groups, hidden).transpose(1, 2, 0),
            shared_down.reshape(groups, hidden, own_cols),
        ],
        axis=1,
    )
    small = jnp.concatenate(
        [
            router_weight.T,
            norm1_gain[None, :],
            norm2_gain[None, :],
            widen(kv_gain[None, :], own_cols),
        ],
        axis=0,
    )
    small = jnp.pad(small, [(0, -small.shape[0] % 16), (0, 0)])
    at_kv = DQK
    at_o = at_kv + kv_block
    at_gate = at_o + DV
    planes, all_planes = heads // 4, groups // 4
    small_swap = Swap(jnp.broadcast_to(small[None], (groups,) + small.shape), True)
    (small_all,), (latent_w,), (got,), (normed1_all,) = exchange(
        [
            small_swap,
            Gather([kva_weight], all_planes),
            Swap(jnp.tile(head_parts, (copies, 1, 1))),
            NormGather(layer_in, small_swap, groups, planes),
        ],
        1,
    )
    route_wt = from_blocks(small_all[:, :groups])
    gain_one = small_all[:, groups].reshape(width).astype(jnp.float32)
    gain_two = small_all[:, groups + 1].reshape(width).astype(jnp.float32)
    gain_kv = small_all[:, groups + 2, :lat_rows].reshape(lat_width).astype(jnp.float32)
    latent_w = latent_w.reshape(width, kva_weight.shape[1])
    stat_one = rms_scale(layer_in)
    unit_one = layer_in * stat_one

    cosine, sine_part = rope_tables(seq_len, DR)
    turn_cos = jnp.concatenate([cosine, cosine], axis=-1)
    turn_sin = jnp.concatenate([-sine_part, sine_part], axis=-1)
    by_seq = (heads, seq_len, -1)
    fold = 2

    def rotated(block, cos_ref, sin_ref, sign):
        flipped = jnp.concatenate([block[:, DR // 2 :], block[:, : DR // 2]], axis=-1)
        reps = block.shape[0] // seq_len
        cos_rows = jnp.concatenate([cos_ref[...]] * reps, axis=0)
        sin_rows = jnp.concatenate([sin_ref[...]] * reps, axis=0)
        return (block * cos_rows + sign * flipped * sin_rows).astype(bf16)

    def attend_forward(refs):
        rows_in, parts, lat_w, kv_gain_ref, cos_ref, sin_ref = refs[:6]
        query_out, key_out, value_out, prob_out, lat_out, latent_out, mixed_out = refs[6:13]
        out_w, query_w, kv_w = refs[13:]

        def assemble():
            for j in range(groups):
                at = slice(j * own_cols, (j + 1) * own_cols)
                query_w[:, at] = parts[j, :at_kv]
                out_w[:, at] = parts[j, at_o:at_gate]
                down = slice(j * lat_rows, (j + 1) * lat_rows)
                for half in range(kv_halves):
                    start = at_kv + half * lat_rows
                    across = slice(half * own_cols, (half + 1) * own_cols)
                    kv_w[down, across] = parts[j, start : start + lat_rows]

        def some(first):
            rows = rows_in[pl.ds(first, fold)].reshape(fold * seq_len, width)
            query = dot_nt(rows, query_w[...])
            query_plain, query_turn = query[:, :DN].astype(bf16), rotated(query[:, DN:], cos_ref, sin_ref, 1.0)
            full = fdot(rows, lat_w[...])
            plain = full[:, :lat_width]
            latent = (plain * rms_scale(plain) * kv_gain_ref[...]).astype(bf16)
            key_turn = rotated(full[:, lat_width:], cos_ref, sin_ref, 1.0)
            key_value = fdot(latent, kv_w[...]).astype(bf16)
            latent_out[pl.ds(first, fold)] = latent.reshape(fold, seq_len, lat_width)
            lat_out[pl.ds(first, fold)] = plain.reshape(fold, seq_len, lat_width)
            ahead = lax.broadcasted_iota(jnp.int32, (seq_len, seq_len), 1) > lax.broadcasted_iota(
                jnp.int32, (seq_len, seq_len), 0
            )
            for k in range(fold):
                at, seq = slice(k * seq_len, (k + 1) * seq_len), first + k
                scores = dot_nt(query_plain[at], key_value[at, :DN])
                scores += dot_nt(query_turn[at], key_turn[at])
                scores = jnp.where(ahead, -1e30, scores * DQK ** (-0.5))
                row_max = jnp.max(scores, axis=-1, keepdims=True)
                total = jnp.sum(jnp.exp(scores - row_max), axis=-1, keepdims=True)
                probs = jnp.exp(scores - (row_max + jnp.log(total)))
                values = key_value[at, DN:]
                prob_out[seq] = probs
                mixed_out[seq] = fdot(probs.astype(bf16), values).astype(bf16)
                query_out[seq, :, :DN], query_out[seq, :, DN:] = query_plain[at], query_turn[at]
                key_out[seq, :, :DN], key_out[seq, :, DN:] = key_value[at, :DN], key_turn[at]
                value_out[seq] = values

        def two(r):
            pl.when(r == 0)(assemble)
            pl.loop(0, 2)(lambda q: some((2 * r + q) * fold))

        return heads // (2 * fold), two

    out_rows = out_grad.astype(bf16)

    def attn_part(part, slot, refs):
        @pl.loop(0, width // 512)
        def _(k):
            cols = part_rows(k * 512, 512)
            part[slot, :, cols] = fdot(refs[12][slot], refs[13][:, cols]).astype(bf16)

    def shaped(last, kind):
        return jax.ShapeDtypeStruct((heads, seq_len, last), kind)

    attended, (shared_got,) = exchange(
        [
            Reduce(
                [normed1_all, got, latent_w, gain_kv[None, :], turn_cos, turn_sin],
                attn_part,
                heads,
                seq_len,
                width,
                extra=[
                    shaped(DQK, bf16),
                    shaped(DQK, bf16),
                    shaped(DV, bf16),
                    shaped(seq_len, jnp.float32),
                    shaped(lat_width, jnp.float32),
                    shaped(lat_width, bf16),
                    shaped(DV, bf16),
                    jax.ShapeDtypeStruct((DV, width), bf16),
                    jax.ShapeDtypeStruct((DQK, width), bf16),
                    jax.ShapeDtypeStruct((lat_width, DN + DV), bf16),
                ],
                prelude=attend_forward,
            ),
            Swap(shared_parts, pace=3),
        ],
        2,
    )
    attn_sum, query_rows, key_rows, value_rows, att_probs, lat_plain, latent, mixed = attended[:8]
    output_w, query_wt, kvup_w = attended[8:]

    gate_sht = from_blocks(shared_got[:, :hidden])
    up_sht = from_blocks(shared_got[:, hidden : 2 * hidden])
    down_sh = from_blocks(shared_got[:, 2 * hidden :])
    hidden_state = layer_in + attn_sum

    stat_two = rms_scale(hidden_state)
    unit_two = hidden_state * stat_two
    normed2 = (unit_two * gain_two).astype(bf16)
    router_probs = jax.nn.softmax(fsum("td,ed->te", normed2, route_wt), axis=-1)
    experts = jnp.arange(groups, dtype=jnp.int32)
    chosen = jnp.any(routes[:, :, None] == experts[None, None, :], axis=1)
    marked = widen(jnp.where(chosen, router_probs, -1.0), -(-groups // LANES) * LANES)
    room = -(-hidden // 16) * 16

    def stacked(blocks):
        return jnp.pad(blocks, [(0, room - hidden), (0, 0)])

    token_gather = Gather([normed2, out_rows, marked], all_planes, True)
    experts_op = Experts(
        token_gather,
        [expert_gate[0].T, expert_up[0].T, expert_down[0]],
        jnp.stack([stacked(gate_sht), stacked(up_sht), stacked(down_sh)]),
        capacity,
    )
    _, expert_results = exchange([token_gather, experts_op], 3)
    grad_parts, out_block, picks, shared_act, shared_sums = expert_results[:5]
    rows_in, cot_in, expert_act, gate_delta, up_delta = (
        x.reshape(groups * capacity, -1) for x in expert_results[5:]
    )
    expert_down_grad = fsum("mf,md->fd", expert_act, cot_in)[None]
    expert_gate_grad = fsum("md,mf->df", rows_in, gate_delta)[None]
    expert_up_grad = fsum("md,mf->df", rows_in, up_delta)[None]
    shared_grads = (
        shared_sums[:, :hidden]
        .reshape(3 * hidden, groups, own_cols)
        .transpose(1, 0, 2)
    )
    out_left = jnp.concatenate(
        [picks, shared_act.reshape(room, groups, seq_len).transpose(1, 0, 2)], axis=1
    )

    def expert_part(part, slot, refs):
        left, own, held = refs[0], refs[1], refs[-1]
        held[:capacity] = own[slot]

        @pl.loop(0, width // 512)
        def _(k):
            cols = part_rows(k * 512, 512)
            part[slot, :, cols] = dot_tn(left[slot], held[:, cols]).astype(bf16)

    def hold_shared(refs):
        refs[-1][capacity:] = refs[2][...]

    ((summed,),) = exchange(
        [Reduce([grad_parts], None, groups, seq_len, width + marked.shape[1])], 4
    )
    normed2_sum = summed[:, :width]
    prob_grad = summed[:, width : width + groups]
    logit_delta = (
        router_probs * (prob_grad - jnp.sum(router_probs * prob_grad, axis=-1, keepdims=True))
    ).astype(bf16)
    normed2_grad = normed2_sum + fdot(logit_delta, route_wt)
    router_gradt = fsum("te,td->ed", logit_delta, normed2)
    norm2_gain_grad = jnp.sum(normed2_grad * unit_two, axis=0)
    scaled_two = normed2_grad * gain_two
    hidden_grad = out_grad + stat_two * (
        scaled_two - unit_two * jnp.mean(scaled_two * unit_two, axis=-1, keepdims=True)
    )

    hidden_rows = hidden_grad.astype(bf16)
    hidden_gather = Gather([hidden_rows], planes, True)

    def attend_backward(refs):
        rows_in, keys, values, probs, out_w, cos_ref, sin_ref = refs[:7]
        query_to, kv_to, turn_to = refs[9:]
        place, hidden_in = hidden_gather.place, hidden_gather.results[0]

        def some(r):
            level = lax.rem(hidden_gather.level + r // 2, planes)
            first = level * 4 + place.spot(3 - 2 * lax.rem(r, 2))
            second = level * 4 + place.spot(2 - 2 * lax.rem(r, 2))
            slots = [first, second]
            pl.when(r == 0)(lambda: hidden_gather.ready(first, False))
            pl.when(r > 0)(lambda: hidden_gather.ready(first, True))
            hidden_gather.ready(second, True)
            rows = jnp.concatenate([hidden_in[slot] for slot in slots], axis=0)
            mixed_grads = dot_nt(rows, out_w[...]).astype(bf16)
            for k in range(2):
                slot = slots[k]
                mixed_grad = mixed_grads[k * seq_len : (k + 1) * seq_len]
                prob = probs[slot]
                value_grad = dot_tn(prob.astype(bf16), mixed_grad)
                dprob = dot_nt(mixed_grad, values[slot])
                row_delta = jnp.sum(prob * dprob, axis=-1, keepdims=True)
                score_delta = (prob * (dprob - row_delta) * DQK ** (-0.5)).astype(bf16)
                query_grad = fdot(score_delta, keys[slot])
                key_grad = dot_tn(score_delta, rows_in[slot])
                query_to[slot, :, :DN] = query_grad[:, :DN].astype(bf16)
                query_to[slot, :, DN:] = rotated(query_grad[:, DN:], cos_ref, sin_ref, -1.0)
                kv_to[slot, :, :DN] = key_grad[:, :DN].astype(bf16)
                kv_to[slot, :, DN:] = value_grad.astype(bf16)
                turn_to[slot, :, :DR] = key_grad[:, DN:].astype(bf16)
                turn_to[slot, :, DR:] = jnp.zeros((seq_len, LANES - DR), bf16)

        hidden_gather.landed = True
        return 2 * planes, some

    def back_part(part, slot, refs):
        @pl.loop(0, width // 512)
        def _(k):
            cols = part_rows(k * 512, 512)
            part[slot, :, cols] = fdot(refs[9][slot], refs[7][:, cols]).astype(bf16)

        product = dot_nt(refs[10][slot], refs[8][...])
        part[slot, :, width : width + lat_width] = product.astype(bf16)
        part[slot, :, width + lat_width :] = refs[11][slot]

    (hidden_all,), (back, query_delta, kv_delta), (owned_early,) = exchange(
        [
            hidden_gather,
            Reduce(
                [
                    query_rows,
                    key_rows,
                    value_rows,
                    att_probs,
                    output_w,
                    turn_cos,
                    turn_sin,
                    query_wt,
                    kvup_w,
                ],
                back_part,
                heads,
                seq_len,
                width + lat_width + LANES,
                [pltpu.VMEM((heads, seq_len, LANES), bf16)],
                extra=[shaped(DQK, bf16), shaped(DN + DV, bf16)],
                prelude=attend_backward,
                delay=2,
            ),
            Swap(shared_grads),
        ],
        5,
    )
    normed1_query = back[:, :width]
    latent_grad = back[:, width : width + lat_width]
    rot_sum = back[:, width + lat_width : width + lat_width + DR]

    own_plain = lax.dynamic_index_in_dim(lat_plain, head, 0, keepdims=False)
    own_stat = rms_scale(own_plain)
    own_unit = own_plain * own_stat
    kv_gain_grad = jnp.sum(latent_grad * own_unit, axis=0)
    scaled_lat = latent_grad * gain_kv
    latent_back = own_stat * (
        scaled_lat - own_unit * jnp.mean(scaled_lat * own_unit, axis=-1, keepdims=True)
    )
    latent_delta = jnp.concatenate(
        [latent_back, rotate_back(rot_sum, cosine, sine_part)], axis=-1
    ).astype(bf16)
    normed1_grad = normed1_query + fsum("tl,dl->td", latent_delta, latent_w)
    norm1_gain_grad = jnp.sum(normed1_grad * unit_one, axis=0)
    scaled_one = normed1_grad * gain_one
    x_grad = hidden_grad + stat_one * (
        scaled_one - unit_one * jnp.mean(scaled_one * unit_one, axis=-1, keepdims=True)
    )

    share = (lat_width + DR) // heads

    def by_owner(row):
        return widen(row.reshape(groups, 1, -1), own_cols)

    small_grads = jnp.concatenate(
        [
            router_gradt.reshape(groups, groups, own_cols).transpose(1, 0, 2),
            by_owner(norm1_gain_grad),
            by_owner(norm2_gain_grad),
            by_owner(kv_gain_grad),
        ],
        axis=1,
    )
    small_grads = jnp.pad(small_grads, [(0, 0), (0, -small_grads.shape[1] % 8), (0, 0)])

    def make_head_grads(op):
        query_ref, rows_ref, mixed_ref, hidden_ref, latent_ref, kv_ref = op.refs
        tokens = heads * seq_len

        def projections(_):
            queries = query_ref[...].reshape(tokens, DQK)
            mixed_rows = mixed_ref[...].reshape(tokens, DV)

            @pl.loop(0, width // 512)
            def _(part):
                cols, first = part_rows(part * 512, 512), part * (512 // own_cols)
                rows = rows_ref[:, :, cols].reshape(tokens, 512)
                hidden_part = hidden_ref[:, :, cols].reshape(tokens, 512)
                of_query = dot_tn(queries, rows).astype(bf16)
                of_out = dot_tn(mixed_rows, hidden_part).astype(bf16)
                for k in range(512 // own_cols):
                    at = slice(k * own_cols, (k + 1) * own_cols)
                    op.source[first + k, :at_kv] = of_query[:, at]
                    op.source[first + k, at_o:at_gate] = of_out[:, at]

        def latents(_):
            lat = latent_ref[...].reshape(tokens, lat_width)
            of_kv = dot_tn(lat, kv_ref[...].reshape(tokens, DN + DV)).astype(bf16)
            for j in range(groups):
                for half in range(kv_halves):
                    start = at_kv + half * lat_rows
                    block = of_kv[
                        j * lat_rows : (j + 1) * lat_rows, half * own_cols : (half + 1) * own_cols
                    ]
                    op.source[j, start : start + lat_rows] = block

        return [projections, latents]

    latent_gather = Gather([latent_delta], planes, True)
    head_swap = MadeSwap(
        [query_delta, normed1_all, mixed, hidden_all, latent, kv_delta],
        (groups, at_gate, own_cols),
        make_head_grads,
        0,
        4,
    )

    def make_latent_grads(op):
        def product(_):
            pl.loop(0, planes)(latent_gather.receive)
            deltas = latent_gather.results[0][...].reshape(heads * seq_len, lat_width + DR)

            @pl.loop(0, width // 512)
            def _(part):
                cols = part_rows(part * 512, 512)
                rows = head_swap.refs[1][:, :, cols].reshape(heads * seq_len, 512)
                op.extra[0][:, cols] = dot_tn(deltas, rows)

            first = lax.rem(op.place.chip, heads) * share
            mine = op.extra[0][pl.ds(pl.multiple_of(first, 8), share), :].astype(bf16)
            for j in range(groups):
                op.source[j] = mine[:, j * own_cols : (j + 1) * own_cols]

        latent_gather.landed = True
        return [product]

    (latent_delta_all,), (out_sum,), (owned_heads,), (owned_small,), (owned_share,) = exchange(
        [
            latent_gather,
            Reduce(
                [out_left, out_block, stacked(down_sh)],
                expert_part,
                groups,
                seq_len,
                width,
                [pltpu.VMEM((capacity + room, width), bf16)],
                hold_shared,
            ),
            head_swap,
            Swap(small_grads, pace=5),
            MadeSwap(
                [],
                (groups, share, own_cols),
                make_latent_grads,
                planes + 1,
                groups,
                [pltpu.VMEM((lat_width + DR, width), jnp.float32)],
            ),
        ],
        6,
    )
    layer_out = hidden_state + out_sum
    small_sums = jnp.sum(owned_small, axis=0)

    def over_copies(blocks):
        blocks = blocks.astype(jnp.float32).reshape((copies, heads) + blocks.shape[1:])
        return jnp.sum(blocks, axis=0)

    of_heads = over_copies(owned_heads)
    q_grad = of_heads[:, :at_kv].transpose(2, 0, 1).reshape(own_cols, heads * DQK)
    kvb_grad = (
        of_heads[:, at_kv:at_o]
        .reshape(heads, kv_halves, lat_rows, own_cols)
        .transpose(2, 0, 1, 3)
        .reshape(lat_rows, heads * (DN + DV))
    )
    own_o_grad = of_heads[:, at_o:].reshape(heads * DV, own_cols)
    kva_grad = over_copies(owned_share)[:, :share].reshape(heads * share, own_cols).T
    of_shared = owned_early[:, : 3 * hidden].astype(jnp.float32)

    def columns(blocks):
        return blocks.reshape(groups * hidden, own_cols)

    shared_gate_grad = columns(of_shared[:, :hidden]).T
    shared_up_grad = columns(of_shared[:, hidden : 2 * hidden]).T
    shared_down_grad = columns(of_shared[:, 2 * hidden :])
    router_grad = small_sums[:groups].T
    return (
        layer_out,
        x_grad,
        small_sums[groups],
        q_grad,
        kva_grad,
        small_sums[groups + 2, :lat_rows],
        kvb_grad,
        own_o_grad,
        small_sums[groups + 1],
        router_grad,
        shared_gate_grad,
        shared_up_grad,
        shared_down_grad,
        expert_gate_grad,
        expert_up_grad,
        expert_down_grad,
    )


def on_device(layer_in, *rest):
    groups, heads = lax.axis_size(EXPERT), rest[1].shape[1] // DQK
    one_each = rest[11].shape[0] == 1
    if one_each and fits(groups, heads, *layer_in.shape):
        return by_heads(layer_in, *rest)
    return general(layer_in, *rest)


def solution(mesh):
    in_specs = (
        P(EXPERT, None),
        P(EXPERT),
        P(EXPERT, TENSOR),
        P(EXPERT, None),
        P(EXPERT),
        P(EXPERT, TENSOR),
        P(TENSOR, EXPERT),
        P(EXPERT),
        P(EXPERT, None),
        P(EXPERT, TENSOR),
        P(EXPERT, TENSOR),
        P(TENSOR, EXPERT),
        P(EXPERT, None, TENSOR),
        P(EXPERT, None, TENSOR),
        P(EXPERT, TENSOR, None),
        P(EXPERT, None),
        P(EXPERT, None),
    )
    out_specs = (
        P(EXPERT, None),
        P(EXPERT, None),
        P(EXPERT),
        P(EXPERT, TENSOR),
        P(EXPERT, None),
        P(EXPERT),
        P(EXPERT, TENSOR),
        P(TENSOR, EXPERT),
        P(EXPERT),
        P(EXPERT, None),
        P(EXPERT, TENSOR),
        P(EXPERT, TENSOR),
        P(TENSOR, EXPERT),
        P(EXPERT, None, TENSOR),
        P(EXPERT, None, TENSOR),
        P(EXPERT, TENSOR, None),
    )
    return jax.shard_map(
        on_device, mesh=mesh, in_specs=in_specs, out_specs=out_specs, check_vma=False
    )
```

```python
import functools

import jax
import jax.numpy as jnp
from jax import lax
from jax.experimental import pallas as pl
from jax.experimental.pallas import tpu as pltpu
from jax.sharding import PartitionSpec as P

DN = 128
DR = 64
DQK = 192
DV = 128
TOPK = 6
LANES = 128


norm_eps = 1e-06


def rms_scale(inputs):
    return lax.rsqrt(jnp.mean(inputs * inputs, axis=-1, keepdims=True) + norm_eps)


def rope_tables(length, rot_width):
    half_width = rot_width // 2
    frequency = 10000.0 ** (-jnp.arange(half_width).astype(jnp.float32) / half_width)
    angles = jnp.arange(length).astype(jnp.float32)[:, None] * frequency[None, :]
    return (jnp.cos(angles), jnp.sin(angles))


def rotate(inputs, cosine, sine_part):
    half_width = inputs.shape[-1] // 2
    first_half = inputs[..., :half_width]
    second_half = inputs[..., half_width:]
    return jnp.concatenate(
        [
            first_half * cosine - second_half * sine_part,
            second_half * cosine + first_half * sine_part,
        ],
        axis=-1,
    )


def rotate_back(inputs, cosine, sine_part):
    return rotate(inputs, cosine, -sine_part)


def silu_grad(pre_act):
    sigmoid_val = jax.nn.sigmoid(pre_act)
    return sigmoid_val * (1.0 + pre_act * (1.0 - sigmoid_val))


def fdot(left, right):
    return jnp.dot(left, right, preferred_element_type=jnp.float32)


def dot_nt(left, right):
    return lax.dot_general(
        left, right, (((1,), (1,)), ((), ())), preferred_element_type=jnp.float32
    )


def dot_tn(left, right):
    return lax.dot_general(
        left, right, (((0,), (0,)), ((), ())), preferred_element_type=jnp.float32
    )


def fsum(spec, left, right):
    return jnp.einsum(spec, left, right, preferred_element_type=jnp.float32)


EXPERT, TENSOR = "expert", "tensor"
MESH = pl.DeviceIdType.MESH
DMA = pltpu.SemaphoreType.DMA


def remote(src, dst, send, recv, target):
    return pltpu.make_async_remote_copy(
        src_ref=src, dst_ref=dst, send_sem=send, recv_sem=recv, device_id=target, device_id_type=MESH
    )


def part_rows(start, size):
    return pl.ds(pl.multiple_of(start, size), size)


class Place:
    def __init__(self):
        self.groups = lax.axis_size(EXPERT)
        self.chip = lax.axis_index(EXPERT)
        self.core = lax.axis_index(TENSOR)
        self.here = lax.rem(self.chip, 4)
        self.there_x = self.here + 1 - 2 * lax.rem(self.here, 2)
        self.there_y = self.here + 2 - 4 * (self.here // 2)
        self.across = 3 - self.here
        base = self.chip - self.here
        self.by_x = {EXPERT: base + self.there_x}
        self.by_y = {EXPERT: base + self.there_y}
        self.above = {EXPERT: self.chip + 4}
        self.below = {EXPERT: self.chip - 4}
        self.mate = {TENSOR: 1 - self.core}

    def spot(self, q):
        x = lax.rem(self.here + 1 - lax.rem(q, 2), 2)
        y = lax.rem(self.here // 2 + 1 - q // 2, 2)
        return 2 * y + x

    def partner(self, j):
        return lax.rem(self.chip + j, self.groups)


def level_at(level, planes, t):
    if planes < 4:
        return lax.rem(level + t, planes)
    flip = level // 2
    near = lax.rem(level + flip, 2)
    order = t + near * (1 - 2 * t) * (1 - t // 2)
    return order * (1 - 2 * flip) + 3 * flip


class Swap:
    reach, lazy = 0, False

    def __init__(self, blocks, vmem_result=False, pace=2):
        groups = blocks.shape[0]
        self.pace = groups if vmem_result else pace
        self.ins = [(blocks, pltpu.VMEM)]
        self.outs = [
            (
                jax.ShapeDtypeStruct(blocks.shape, blocks.dtype),
                pltpu.VMEM if vmem_result else pl.ANY,
            )
        ]
        self.scratch = [DMA, DMA((groups,)), DMA((groups,))]

    def bind(self, place, ins, outs, scratch):
        self.place, self.groups = place, place.groups
        self.source, self.result = ins[0], outs[0]
        self.own_sem, self.send_sem, self.recv_sem = scratch

    def copy(self, j, src, dst):
        return remote(
            self.source.at[src],
            self.result.at[dst],
            self.send_sem.at[j],
            self.recv_sem.at[j],
            {EXPERT: self.place.partner(j)},
        )

    def own(self):
        chip = self.place.chip
        return pltpu.make_async_copy(self.source.at[chip], self.result.at[chip], self.own_sem)

    def send(self, i):
        for q in range(min(self.pace, self.groups - 1)):
            j = 1 + i * self.pace + q

            @pl.when(j < self.groups)
            def _(j=j):
                self.copy(j, self.place.partner(j), self.place.chip).start()

    def begin(self):
        self.own().start()
        self.send(0)

    def rest(self, offset):
        count = -(-(self.groups - 1) // self.pace) - 1
        return [(offset, count, lambda i: self.send(i + 1))]

    def segments(self):
        return self.rest(0)

    def end(self):
        self.own().wait()

        @pl.loop(1, self.groups)
        def _(j):
            self.copy(j, self.place.chip, self.place.partner(self.groups - j)).wait_recv()
            self.copy(j, self.place.partner(j), self.place.chip).wait_send()


class MadeSwap(Swap):
    def __init__(self, operands, shape, make, delay, pace, scratch=()):
        self.pace, self.make, self.delay = pace, make, delay
        self.ins = [(a, pltpu.VMEM) for a in operands]
        self.outs = [(jax.ShapeDtypeStruct(shape, jnp.bfloat16), pl.ANY)]
        groups = shape[0]
        self.scratch = [DMA, DMA((groups,)), DMA((groups,)), pltpu.VMEM(shape, jnp.bfloat16)]
        self.scratch += list(scratch)

    def bind(self, place, ins, outs, scratch):
        super().bind(place, [scratch[3]], outs, scratch[:3])
        self.refs, self.extra = ins, scratch[4:]

    def begin(self):
        if self.delay is None:
            for call in self.make(self):
                call(0)
            super().begin()

    def segments(self):
        if self.delay is None:
            return self.rest(0)
        calls = self.make(self) + [lambda i: super(MadeSwap, self).begin()]
        parts = [(self.delay + k, 1, call) for k, call in enumerate(calls)]
        return parts + self.rest(self.delay + len(calls))


class Gather:
    lazy = False

    def __init__(self, arrays, planes, vmem_result=False):
        count, slots = len(arrays), planes * 4
        self.planes, self.count, self.reach = planes, count, planes
        self.ins = [(a, pltpu.VMEM) for a in arrays]
        space = pltpu.VMEM if vmem_result else pl.ANY
        self.outs = [(jax.ShapeDtypeStruct((slots,) + a.shape, a.dtype), space) for a in arrays]
        by_level, by_slot = DMA((count, planes)), DMA((count, slots))
        self.scratch = [DMA((count,))] + [by_level] * 5 + [by_slot] + [by_level] * 6 + [by_slot]

    def bind(self, place, ins, outs, scratch):
        self.place, self.sources, self.results = place, ins, outs
        self.level = lax.rem(place.chip // 4, self.planes)
        self.has_up, self.has_down = self.level < self.planes - 1, self.level > 0
        self.own_sem = scratch[0]
        self.in_z, self.in_x, self.in_y, self.in_a, self.in_b, self.in_p = scratch[1:7]
        self.out_up, self.out_down, self.out_x, self.out_y = scratch[7:11]
        self.out_a, self.out_b, self.out_p = scratch[11:14]
        self.landed = False

    def move(self, a, slot, part, send, recv, target, own=False, whose=None):
        half = self.sources[a].shape[0] // 2
        whose = self.place.core if whose is None else whose
        if part is None:
            rows = part_rows(whose * half, half)
        else:
            rows = part_rows(whose * half + part * (half // 2), half // 2)
        dst = self.results[a].at[slot, rows]
        return remote(self.sources[a].at[rows] if own else dst, dst, send, recv, target)

    def along_z(self, a, lev, own, up):
        sems = self.out_up if up else self.out_down
        target = self.place.above if up else self.place.below
        slot = lev * 4 + self.place.here
        return self.move(a, slot, None, sems.at[a, lev], self.in_z.at[a, lev], target, own)

    def along_x(self, a, lev, slot, own=False):
        return self.move(
            a, slot, None, self.out_x.at[a, lev], self.in_x.at[a, lev], self.place.by_x, own
        )

    def along_y(self, a, lev, slot, own=False):
        return self.move(
            a, slot, None, self.out_y.at[a, lev], self.in_y.at[a, lev], self.place.by_y, own
        )

    def corner_x(self, a, lev, slot):
        return self.move(
            a, slot, 0, self.out_a.at[a, lev], self.in_a.at[a, lev], self.place.by_x
        )

    def corner_y(self, a, lev, slot):
        return self.move(
            a, slot, 1, self.out_b.at[a, lev], self.in_b.at[a, lev], self.place.by_y
        )

    def share(self, a, slot, whose=None):
        return self.move(
            a, slot, None, self.out_p.at[a, slot], self.in_p.at[a, slot], self.place.mate, whose=whose
        )

    def own(self, a):
        slot = self.level * 4 + self.place.here
        return pltpu.make_async_copy(self.sources[a], self.results[a].at[slot], self.own_sem.at[a])

    def begin(self):
        for a in range(self.count):
            self.own(a).start()
        self.first(0, True)

    def relays(self, a, t, own, act):
        lev = level_at(self.level, self.planes, t)
        up, down = self.has_up, self.has_down
        if not own:
            up, down = up & (lev < self.level), down & (lev > self.level)
        pl.when(up)(lambda: act(self.along_z(a, lev, own, True)))
        pl.when(down)(lambda: act(self.along_z(a, lev, own, False)))

    def first(self, t, own=False):
        lev = level_at(self.level, self.planes, t)
        for a in range(self.count):
            slot = lev * 4 + self.place.here
            if not own:
                self.along_z(a, lev, own, True).wait_recv()
            self.relays(a, t, own, lambda copy: copy.start())
            self.along_x(a, lev, slot, own).start()
            self.along_y(a, lev, slot, own).start()
            if not own:
                self.share(a, slot).start()

    def second(self, t):
        lev = level_at(self.level, self.planes, t)
        for a in range(self.count):
            slot = lev * 4 + self.place.there_y
            self.along_y(a, lev, slot).wait_recv()
            self.corner_x(a, lev, slot).start()
            self.share(a, slot).start()
            slot = lev * 4 + self.place.there_x
            self.along_x(a, lev, slot).wait_recv()
            self.corner_y(a, lev, slot).start()
            self.share(a, slot).start()

    def third(self, t):
        lev = level_at(self.level, self.planes, t)
        for a in range(self.count):
            slot = lev * 4 + self.place.across
            self.corner_x(a, lev, slot).wait_recv()
            self.corner_y(a, lev, slot).wait_recv()
            self.share(a, slot).start()

    def advance(self, i):
        pl.when(i < self.planes)(lambda: self.first(i))
        pl.when(i < self.planes + 1)(lambda: self.second(i - 1))
        pl.when(i > 1)(lambda: self.third(i - 2))

    def segments(self):
        return [(0, self.planes + 1, lambda i: self.advance(i + 1))]

    def sent(self, t, own):
        place, lev = self.place, level_at(self.level, self.planes, t)
        for a in range(self.count):
            slot = lev * 4 + place.here
            self.relays(a, t, own, lambda copy: copy.wait_send())
            self.along_x(a, lev, slot, own).wait_send()
            self.along_y(a, lev, slot, own).wait_send()
            self.corner_x(a, lev, lev * 4 + place.there_y).wait_send()
            self.corner_y(a, lev, lev * 4 + place.there_x).wait_send()
            for other in [place.there_y, place.there_x, place.across]:
                self.share(a, lev * 4 + other).wait_send()
            if not own:
                self.share(a, slot).wait_send()

    def end(self):
        if not self.landed:
            self.receive_all()
        self.sent(0, True)
        pl.loop(1, self.planes)(lambda t: self.sent(t, False))

    def ready(self, slot, other):
        for a in range(self.count):
            if other:
                self.share(a, slot, 1 - self.place.core).wait_recv()
            else:
                self.own(a).wait()

    def receive(self, t):
        place, lev = self.place, level_at(self.level, self.planes, t)
        pl.when(t == 0)(lambda: self.ready(lev * 4 + place.here, False))
        pl.when(t > 0)(lambda: self.ready(lev * 4 + place.here, True))
        for spot in (place.there_y, place.there_x, place.across):
            self.ready(lev * 4 + spot, True)

    def receive_all(self):
        self.landed = True
        pl.loop(0, self.planes)(self.receive)


class NormGather(Gather):
    def __init__(self, rows, gains, gain_row, planes):
        super().__init__([jax.ShapeDtypeStruct(rows.shape, jnp.bfloat16)], planes)
        self.ins = [(rows, pltpu.VMEM)]
        self.scratch = self.scratch + [pltpu.VMEM(rows.shape, jnp.bfloat16)]
        self.gains, self.gain_row = gains, gain_row

    def bind(self, place, ins, outs, scratch):
        super().bind(place, [scratch[-1]], outs, scratch[:-1])
        self.rows = ins[0]

    def begin(self):
        self.gains.end()
        rows = self.rows[...]
        stat = lax.rsqrt(jnp.mean(rows * rows, axis=-1, keepdims=True) + norm_eps)
        cols = rows.shape[1] // self.place.groups
        for j in range(self.place.groups):
            at = slice(j * cols, (j + 1) * cols)
            gain = self.gains.result[j, self.gain_row : self.gain_row + 1, :].astype(jnp.float32)
            self.sources[0][:, at] = (rows[:, at] * stat * gain).astype(jnp.bfloat16)
        super().begin()


class Reduce:
    def __init__(
        self, operands, produce, slots, block, width, scratch=(), prepare=None, extra=(), prelude=None, delay=0
    ):
        planes, rows, kind = slots // 4, block // 2, jnp.bfloat16
        self.planes, self.reach = planes, planes
        self.ins = [(a, pltpu.VMEM) for a in operands]
        self.outs = [(jax.ShapeDtypeStruct((block, width), jnp.float32), pltpu.VMEM)]
        self.outs += [(shape, pltpu.VMEM) for shape in extra]
        self.own_scratch, self.produce, self.prepare = len(scratch), produce, prepare
        self.prelude, self.delay, self.lazy = prelude, delay, prelude is not None
        by_level = DMA((planes,))
        self.scratch = (
            list(scratch)
            + [pltpu.VMEM((slots, block, width) if produce else (8, LANES), kind)]
            + [pltpu.VMEM((slots, rows, width), kind)]
            + [pltpu.VMEM((planes, rows // 2, width), kind)] * 2
            + [pltpu.VMEM((planes, rows, width), kind)] * 4
            + [DMA((slots,))]
            + [by_level] * 6
            + [DMA, DMA((slots,))]
            + [by_level] * 5
            + [DMA]
        )

    def bind(self, place, ins, outs, scratch):
        self.place, self.out = place, outs[0]
        self.refs = list(ins) + list(outs[1:]) + list(scratch[: self.own_scratch])
        scratch = scratch[self.own_scratch :]
        self.part = scratch[0] if self.produce else ins[0]
        self.mine = scratch[1]
        self.from_a, self.from_b, self.from_x, self.from_y = scratch[2:6]
        self.from_up, self.from_down = scratch[6:8]
        self.in_p, self.in_a, self.in_b, self.in_x, self.in_y = scratch[8:13]
        self.in_up, self.in_down, self.in_m, self.out_p = scratch[13:17]
        self.out_a, self.out_b, self.out_x, self.out_y, self.out_z, self.out_m = scratch[17:]
        self.level = lax.rem(place.chip // 4, self.planes)
        self.has_up, self.has_down = self.level < self.planes - 1, self.level > 0
        self.rows = self.part.shape[1] // 2
        self.half = self.rows // 2

    def swap(self, slot):
        theirs = part_rows((1 - self.place.core) * self.rows, self.rows)
        return remote(
            self.part.at[slot, theirs],
            self.mine.at[slot],
            self.out_p.at[slot],
            self.in_p.at[slot],
            self.place.mate,
        )

    def add_into(self, dst, terms, first, size):
        step = 16

        @pl.loop(0, size // step)
        def _(i):
            at = first + i * step
            total = None
            for term, shift in terms:
                block = term[part_rows(at + shift, step), :].astype(jnp.float32)
                total = block if total is None else total + block
            dst[part_rows(at, step), :] = total.astype(dst.dtype)

    def send_a(self, lev):
        src = self.mine.at[lev * 4 + self.place.across, pl.ds(0, self.half)]
        return remote(
            src, self.from_a.at[lev], self.out_a.at[lev], self.in_a.at[lev], self.place.by_x
        )

    def send_b(self, lev):
        src = self.mine.at[lev * 4 + self.place.across, pl.ds(self.half, self.half)]
        return remote(
            src, self.from_b.at[lev], self.out_b.at[lev], self.in_b.at[lev], self.place.by_y
        )

    def send_y(self, lev):
        src = self.mine.at[lev * 4 + self.place.there_y]
        return remote(
            src, self.from_y.at[lev], self.out_y.at[lev], self.in_y.at[lev], self.place.by_y
        )

    def send_x(self, lev):
        src = self.mine.at[lev * 4 + self.place.there_x]
        return remote(
            src, self.from_x.at[lev], self.out_x.at[lev], self.in_x.at[lev], self.place.by_x
        )

    def send_up(self, lev):
        src = self.mine.at[lev * 4 + self.place.here]
        return remote(
            src, self.from_down.at[lev], self.out_z.at[lev], self.in_down.at[lev], self.place.above
        )

    def send_down(self, lev):
        src = self.mine.at[lev * 4 + self.place.here]
        return remote(
            src, self.from_up.at[lev], self.out_z.at[lev], self.in_up.at[lev], self.place.below
        )

    def plane(self, i):
        return level_at(self.level, self.planes, self.planes - 1 - i)

    def make(self, i):
        @pl.loop(0, 4)
        def _(q):
            slot = self.plane(i) * 4 + self.place.spot(q)
            if self.produce is not None:
                self.produce(self.part, slot, self.refs)
            self.swap(slot).start()

    def join(self, slot):
        self.swap(slot).wait_recv()
        mine = self.mine.at[slot]
        terms = [(mine, 0), (self.part.at[slot], self.place.core * self.rows)]
        self.add_into(mine, terms, 0, self.rows)

    def first(self, i):
        lev = self.plane(i)
        self.join(lev * 4 + self.place.across)
        self.send_a(lev).start()
        self.send_b(lev).start()
        self.join(lev * 4 + self.place.there_y)
        self.join(lev * 4 + self.place.there_x)

    def second(self, i):
        lev = self.plane(i)
        mine = self.mine.at[lev * 4 + self.place.there_y]
        self.send_a(lev).wait_recv()
        self.add_into(mine, [(mine, 0), (self.from_a.at[lev], 0)], 0, self.half)
        self.send_y(lev).start()
        mine = self.mine.at[lev * 4 + self.place.there_x]
        self.send_b(lev).wait_recv()
        self.add_into(mine, [(mine, 0), (self.from_b.at[lev], -self.half)], self.half, self.half)
        self.send_x(lev).start()
        self.join(lev * 4 + self.place.here)

    def third(self, i):
        rows, out, lev = self.rows, self.out, self.plane(i)
        mine = self.mine.at[lev * 4 + self.place.here]
        self.send_y(lev).wait_recv()
        self.send_x(lev).wait_recv()
        terms = [(mine, 0), (self.from_y.at[lev], 0), (self.from_x.at[lev], 0)]

        def more(total, cond, send, arrived):
            @pl.when(cond)
            def _():
                send(lev).wait_recv()
                self.add_into(total, [(total, 0), (arrived.at[lev], 0)], 0, rows)

        @pl.when(lev == self.level)
        def _():
            total = out.at[part_rows(self.place.core * rows, rows)]
            self.add_into(total, terms, 0, rows)
            more(total, self.has_up, self.send_down, self.from_up)
            more(total, self.has_down, self.send_up, self.from_down)

        @pl.when(lev < self.level)
        def _():
            self.add_into(mine, terms, 0, rows)
            more(mine, self.has_up, self.send_down, self.from_up)
            self.send_down(lev).start()

        @pl.when(lev > self.level)
        def _():
            self.add_into(mine, terms, 0, rows)
            more(mine, self.has_down, self.send_up, self.from_down)
            self.send_up(lev).start()

    def begin(self):
        if self.prepare is not None:
            self.prepare(self.refs)
        if self.prelude is None:
            self.make(0)

    def advance(self, i):
        pl.when(i + 1 < self.planes)(lambda: self.make(i + 1))
        pl.when(i < self.planes)(lambda: self.first(i))
        pl.when((i > 0) & (i < self.planes + 1))(lambda: self.second(i - 1))
        pl.when(i > 1)(lambda: self.third(i - 2))

    def segments(self):
        parts, start = [], 0
        if self.prelude is not None:
            count, call = self.prelude(self.refs)
            parts = [(self.delay, count, call), (self.delay + count, 1, self.make)]
            start = self.delay + count + 1
        return parts + [(start, self.planes + 2, self.advance)]

    def hand(self, whose):
        spot = part_rows(whose * self.rows, self.rows)
        return remote(self.out.at[spot], self.out.at[spot], self.out_m, self.in_m, self.place.mate)

    def end(self):
        self.hand(self.place.core).start()


        @pl.loop(0, self.planes)
        def _(lev):
            for spot in range(4):
                self.swap(lev * 4 + spot).wait_send()
            for send in (self.send_a, self.send_b, self.send_y, self.send_x):
                send(lev).wait_send()
            pl.when(lev < self.level)(lambda: self.send_down(lev).wait_send())
            pl.when(lev > self.level)(lambda: self.send_up(lev).wait_send())

        self.hand(self.place.core).wait_send()
        self.hand(1 - self.place.core).wait_recv()


class Experts:
    lazy = False

    def __init__(self, gather, weights, shared_w, capacity):
        slots, seq, width = gather.outs[0][0].shape
        hidden, room, bf16 = weights[0].shape[0], shared_w.shape[1], jnp.bfloat16
        self.gather, self.capacity, self.room, self.reach = gather, capacity, room, gather.reach
        self.slots, self.seq, self.width, self.hidden = slots, seq, width, hidden
        rows = (slots, capacity)
        turn = (room, slots * seq)

        def shape(dims, kind=bf16):
            return jax.ShapeDtypeStruct(dims, kind)

        self.ins = [(a, pl.ANY) for a in weights] + [(shared_w, pltpu.VMEM)]
        self.outs = [
            (shape((slots, seq, width + LANES)), pl.ANY),
            (shape(rows + (width,)), pl.ANY),
            (shape(rows + (seq,)), pltpu.VMEM),
            (shape(turn), pltpu.VMEM),
            (shape((3, room, width)), pltpu.VMEM),
            (shape(rows + (width,)), pl.ANY),
            (shape(rows + (width,)), pl.ANY),
        ] + [(shape(rows + (hidden,)), pl.ANY)] * 3
        staged = [self.outs[k][0] for k in (0, 1, 7, 8, 9)]
        self.scratch = [pltpu.VMEM(x.shape, bf16) for x in staged]
        self.scratch += [DMA((len(staged), gather.planes))]
        self.scratch += (
            [pltpu.VMEM(w.shape, bf16) for w in weights]
            + [pltpu.VMEM((4 * capacity, width), bf16)] * 3
            + [
                pltpu.VMEM((4 * capacity, LANES), jnp.float32),
                pltpu.VMEM((4 * capacity + 2 * room, width), bf16),
                pltpu.VMEM((4 * capacity + 2 * room, 4 * seq), bf16),
                pltpu.VMEM((3, room, width), jnp.float32),
                DMA((3,)),
                DMA((2,)),
            ]
        )

    def bind(self, place, ins, outs, scratch):
        self.place = place
        self.hbm_weights, self.shared_w = ins[:3], ins[3]
        self.tokens, self.out_rows, self.marked = self.gather.results
        self.picks, self.act_turn, self.shared_grads, self.rows_hbm, self.cot_hbm = outs[2:7]
        self.staged, self.leave_sem, scratch = scratch[:5], scratch[5], scratch[6:]
        self.part, self.out_block, self.act, self.gate_delta, self.up_delta = self.staged
        self.final = list(outs[:2]) + list(outs[7:])
        self.gate, self.up, self.down = scratch[:3]
        self.rows, self.cot, self.grads = scratch[3:6]
        self.weight, self.held, self.left, self.total, self.load_sem, self.save_sem = scratch[6:]
        self.level = lax.rem(place.chip // 4, self.gather.planes)

    def loads(self):
        pairs = zip(self.hbm_weights, [self.gate, self.up, self.down])
        return [
            pltpu.make_async_copy(src, dst, self.load_sem.at[k]) for k, (src, dst) in enumerate(pairs)
        ]

    def saves(self, lev):
        at = pl.ds(lev * 4 * self.capacity, 4 * self.capacity)
        pairs = [(self.rows, self.rows_hbm), (self.cot, self.cot_hbm)]
        return [
            pltpu.make_async_copy(
                src.reshape(4, self.capacity, self.width), dst.at[pl.ds(lev * 4, 4)], self.save_sem.at[k]
            )
            for k, (src, dst) in enumerate(pairs)
        ]

    def begin(self):
        for load in self.loads():
            load.start()
        self.total[...] = jnp.zeros_like(self.total)
        self.held[4 * self.capacity :] = self.shared_w[:2].reshape(2 * self.room, self.width)
        self.left[: 4 * self.capacity] = jnp.zeros((4 * self.capacity, 4 * self.seq), jnp.bfloat16)

    def choose(self, lev, t):
        seq, cap = self.seq, self.capacity
        below = lax.broadcasted_iota(jnp.int32, (seq, seq), 0)
        upto = (below <= lax.broadcasted_iota(jnp.int32, (seq, seq), 1)).astype(jnp.bfloat16)
        place_in = lax.broadcasted_iota(jnp.int32, (cap, seq), 0).astype(jnp.float32)

        @pl.when(t > 0)
        def _():
            for save in self.saves(lev):
                save.wait()

        for j in range(4):
            slot, at = lev * 4 + j, slice(j * cap, (j + 1) * cap)
            turned = self.marked[slot].T
            here = jnp.sum(jnp.where(below == self.place.chip, turned, 0.0), axis=0, keepdims=True)
            routed = jnp.where(here >= 0.0, 1.0, 0.0)
            order = fdot(jnp.broadcast_to(routed, (8, seq)).astype(jnp.bfloat16), upto)[:1] - 1.0
            hit = jnp.where(order == place_in, routed, 0.0)
            weight = jnp.sum(hit * here, axis=-1, keepdims=True)
            pick = hit.astype(jnp.bfloat16)
            self.picks[slot] = pick
            self.left[at, j * seq : (j + 1) * seq] = pick
            self.weight[at] = jnp.broadcast_to(weight, (cap, LANES))
        chosen, weight = self.left[: 4 * cap], self.weight[:, :1]

        @pl.loop(0, self.width // 512, unroll=True)
        def _(k):
            cols, four = part_rows(k * 512, 512), pl.ds(lev * 4, 4)
            own = fdot(chosen, self.tokens[four, :, cols].reshape(4 * seq, 512))
            self.rows[:, cols] = own.astype(jnp.bfloat16)
            grad = fdot(chosen, self.out_rows[four, :, cols].reshape(4 * seq, 512))
            self.grads[:, cols] = grad.astype(jnp.bfloat16)
            self.cot[:, cols] = (weight * grad).astype(jnp.bfloat16)

        for save in self.saves(lev):
            save.start()

    def hidden_units(self, lev):
        slots, chunk = pl.ds(lev * 4, 4), 256
        for start in range(0, self.hidden, chunk):
            cols = slice(start, min(start + chunk, self.hidden))
            shape = (4, self.capacity, cols.stop - cols.start)
            gate = dot_nt(self.rows[...], self.gate[cols])
            up = dot_nt(self.rows[...], self.up[cols])
            grad = dot_nt(self.cot[...], self.down[cols])
            sig = jax.nn.sigmoid(gate)
            gated = gate * sig
            self.act[slots, :, cols] = (gated * up).astype(jnp.bfloat16).reshape(shape)
            slope = sig * (1.0 + gate * (1.0 - sig))
            self.gate_delta[slots, :, cols] = (grad * up * slope).astype(jnp.bfloat16).reshape(shape)
            self.up_delta[slots, :, cols] = (grad * gated).astype(jnp.bfloat16).reshape(shape)

    def shared_units(self, lev):
        seq4, room = 4 * self.seq, self.room
        tokens = self.tokens[pl.ds(lev * 4, 4)].reshape(seq4, self.width)
        grads = self.out_rows[pl.ds(lev * 4, 4)].reshape(seq4, self.width)
        both = dot_nt(self.shared_w[:2].reshape(2 * room, self.width), tokens)
        gate, up = both[:room], both[room:]
        grad = dot_nt(self.shared_w[2], grads)
        sig = jax.nn.sigmoid(gate)
        act = (gate * sig * up).astype(jnp.bfloat16)
        gate_delta = (grad * up * (sig * (1.0 + gate * (1.0 - sig)))).astype(jnp.bfloat16)
        up_delta = (grad * gate * sig).astype(jnp.bfloat16)
        self.act_turn[:, part_rows(lev * seq4, seq4)] = act
        self.left[4 * self.capacity : 4 * self.capacity + room] = gate_delta
        self.left[4 * self.capacity + room :] = up_delta

        @pl.loop(0, self.width // 512, unroll=True)
        def _(k):
            cols, four = part_rows(k * 512, 512), pl.ds(lev * 4, 4)
            some = self.tokens[four, :, cols].reshape(seq4, 512)
            self.total[0, :, cols] += fdot(gate_delta, some)
            self.total[1, :, cols] += fdot(up_delta, some)
            some = self.out_rows[four, :, cols].reshape(seq4, 512)
            self.total[2, :, cols] += fdot(act, some)

    def outward(self, lev):
        slots, cap, count = pl.ds(lev * 4, 4), self.capacity, 4 * self.capacity
        act = self.act[slots].reshape(count, self.hidden)
        gate_delta = self.gate_delta[slots].reshape(count, self.hidden)
        up_delta = self.up_delta[slots].reshape(count, self.hidden)
        weight = self.weight[:, :1]

        def some(k, route):
            cols = part_rows(k * 512, 512)
            out = fdot(act, self.down[:, cols]).astype(jnp.bfloat16).astype(jnp.float32)
            route += jnp.sum(out * self.grads[:, cols].astype(jnp.float32), axis=-1, keepdims=True)
            out = (weight * out).astype(jnp.bfloat16)
            self.out_block[slots, :, cols] = out.reshape(4, cap, 512)
            back = fdot(gate_delta, self.gate[:, cols]) + fdot(up_delta, self.up[:, cols])
            self.held[:count, cols] = back.astype(jnp.bfloat16)
            return route

        route = lax.fori_loop(
            0, self.width // 512, some, jnp.zeros((count, 1), jnp.float32), unroll=True
        )
        lane = lax.broadcasted_iota(jnp.int32, (count, LANES), 1)
        routes = jnp.where(lane == self.place.chip, route, 0.0).astype(jnp.bfloat16)
        shape = (4, self.seq, LANES)
        turned = dot_tn(self.left[:count], routes).astype(jnp.bfloat16)
        self.part[slots, :, self.width :] = turned.reshape(shape)
        left = self.left[...]

        @pl.loop(0, self.width // 512, unroll=True)
        def _(k):
            cols = part_rows(k * 512, 512)
            sums = dot_tn(left, self.held[:, cols]).astype(jnp.bfloat16)
            self.part[slots, :, cols] = sums.reshape(4, self.seq, 512)

        for copy in self.leaving(lev):
            copy.start()

    def leaving(self, lev):
        four = pl.ds(lev * 4, 4)
        return [
            pltpu.make_async_copy(src.at[four], dst.at[four], self.leave_sem.at[k, lev])
            for k, (src, dst) in enumerate(zip(self.staged, self.final))
        ]

    def compute(self, t):
        lev = level_at(self.level, self.gather.planes, t)

        @pl.when(t == 0)
        def _():
            for load in self.loads():
                load.wait()

        self.gather.receive(t)
        self.choose(lev, t)
        self.hidden_units(lev)
        self.shared_units(lev)

    def advance(self, i):
        planes = self.gather.planes
        pl.when(i > 1)(lambda: self.outward(level_at(self.level, planes, i - 2)))
        pl.when((i > 0) & (i < planes + 1))(lambda: self.compute(i - 1))

    def segments(self):
        self.gather.landed = True
        return [(0, self.gather.planes + 2, self.advance)]

    def end(self):
        for save in self.saves(level_at(self.level, self.gather.planes, self.gather.planes - 1)):
            save.wait()
        self.shared_grads[...] = self.total[...].astype(jnp.bfloat16)

        @pl.loop(0, self.gather.planes)
        def _(lev):
            for copy in self.leaving(lev):
                copy.wait()


def greet(place, ops):
    barrier = pltpu.get_barrier_semaphore()
    expected = 1

    def call(target):
        pl.semaphore_signal(barrier, inc=1, device_id=target, device_id_type=MESH)

    call(place.mate)
    if any(op.reach == 0 for op in ops):
        for j in range(1, place.groups):
            call({EXPERT: place.partner(j)})
        expected += place.groups - 1
    else:
        call(place.by_x)
        call(place.by_y)
        planes = max(op.reach for op in ops)
        level = lax.rem(place.chip // 4, planes)
        has_up, has_down = level < planes - 1, level > 0
        pl.when(has_up)(lambda: call(place.above))
        pl.when(has_down)(lambda: call(place.below))
        expected += 2 + has_up.astype(jnp.int32) + has_down.astype(jnp.int32)
    pl.semaphore_wait(barrier, expected)


def is_large(pair):
    array, space = pair
    return space == pltpu.VMEM and array.size * array.dtype.itemsize >= 1 << 17


def chip_kernel(ops, *refs):
    place = Place()
    pairs = [pair for op in ops for pair in op.ins]
    n_in, large = len(pairs), [k for k, pair in enumerate(pairs) if is_large(pair)]
    n_out = sum(len(op.outs) for op in ops)
    ins, outs, scratch = list(refs[:n_in]), refs[n_in : n_in + n_out], refs[n_in + n_out :]
    loads = {}
    for n, k in enumerate(large):
        loads[k] = pltpu.make_async_copy(ins[k], scratch[n], scratch[len(large)].at[n])
        loads[k].start()
        ins[k] = scratch[n]
    scratch = scratch[len(large) + 1 :]
    first = 0
    for op in ops:
        op.fetches = [loads[k] for k in range(first, first + len(op.ins)) if k in loads]
        first += len(op.ins)
        op.bind(place, ins[: len(op.ins)], outs[: len(op.outs)], scratch[: len(op.scratch)])
        ins, outs = ins[len(op.ins) :], outs[len(op.outs) :]
        scratch = scratch[len(op.scratch) :]
    greet(place, ops)


    def load(op):
        for copy in op.fetches:
            copy.wait()

    parts = []
    for op in ops:
        segments = [part for part in op.segments() if part[1] > 0]
        if op.lazy:
            parts.append((min(start for start, _, _ in segments), 1, lambda _, op=op: load(op)))
        else:
            load(op)
        op.begin()
        parts += segments
    if parts:

        @pl.loop(0, max(start + count for start, count, _ in parts))
        def _(r):
            for start, count, call in parts:
                inside = (r >= start) & (r < start + count)
                pl.when(inside)(functools.partial(call, r - start))

    ended = [op.gains for op in ops if isinstance(op, NormGather)]
    for op in ops:
        if op not in ended:
            op.end()


def exchange(ops, ident):
    ins = [pair for op in ops for pair in op.ins]
    outs = [pair for op in ops for pair in op.outs]
    moved = sum(a.size * a.dtype.itemsize for a, _ in ins + outs)
    large = [pair[0] for pair in ins if is_large(pair)]
    spaces = [pl.ANY if is_large(pair) else pair[1] for pair in ins]
    held = [pltpu.VMEM(a.shape, a.dtype) for a in large] + [DMA((max(1, len(large)),))]
    results = pl.pallas_call(
        functools.partial(chip_kernel, ops),
        out_shape=[shape for shape, _ in outs],
        in_specs=[pl.BlockSpec(memory_space=space) for space in spaces],
        out_specs=[pl.BlockSpec(memory_space=space) for _, space in outs],
        scratch_shapes=held + [entry for op in ops for entry in op.scratch],
        compiler_params=pltpu.CompilerParams(
            collective_id=ident, has_side_effects=True, vmem_limit_bytes=60 << 20
        ),
        cost_estimate=pl.CostEstimate(flops=0, bytes_accessed=moved, transcendentals=0),
    )(*[a for a, _ in ins])
    split = []
    for op in ops:
        split.append(results[: len(op.outs)])
        results = results[len(op.outs) :]
    return split


def grads_kernel(act, gate_delta, up_delta, rows, cot, gate_out, up_out, down_out):
    gate_out[...] = dot_tn(gate_delta[...], rows[...])
    up_out[...] = dot_tn(up_delta[...], rows[...])
    down_out[...] = dot_tn(act[...], cot[...])


def expert_weight_grads(act, gate_delta, up_delta, rows, cot):
    count, hidden = act.shape
    width, tile = rows.shape[1], 256
    left = pl.BlockSpec((count, hidden), lambda i: (0, 0), pipeline_mode=pl.Buffered(1))
    right = pl.BlockSpec((count, tile), lambda i: (0, i))
    return pl.pallas_call(
        grads_kernel,
        grid=(width // tile,),
        out_shape=[jax.ShapeDtypeStruct((hidden, width), jnp.float32)] * 3,
        in_specs=[left] * 3 + [right] * 2,
        out_specs=[pl.BlockSpec((hidden, tile), lambda i: (0, i))] * 3,
        compiler_params=pltpu.CompilerParams(vmem_limit_bytes=48 << 20),
        cost_estimate=pl.CostEstimate(
            flops=6 * count * hidden * width,
            bytes_accessed=12 * hidden * width + 4 * count * width,
            transcendentals=0,
        ),
    )(act, gate_delta, up_delta, rows, cot)


def finish_kernel(sizes, heads_in, shared_in, share_in, small_in, state, added, *refs):
    heads, at_kv, at_o, lat_rows, hidden, share = sizes
    layer_out, q_out, kvb_out, o_out, gate_out, up_out, down_out, kva_out, small_out = refs[:9]
    q_turn, gate_turn, up_turn = refs[9:]
    groups, own_cols = heads_in.shape[0], heads_in.shape[2]
    copies = range(0, groups, heads)

    def over_copies(ref, k):
        return sum(ref[first + k].astype(jnp.float32) for first in copies)

    layer_out[...] = state[...] + added[...]
    small_out[...] = sum(small_in[j] for j in range(groups))
    for k in range(heads):
        block = over_copies(heads_in, k)
        q_turn[k * at_kv : (k + 1) * at_kv] = block[:at_kv]
        halves = (at_o - at_kv) // lat_rows
        for half in range(halves):
            start, col = at_kv + half * lat_rows, (k * halves + half) * own_cols
            kvb_out[:, col : col + own_cols] = block[start : start + lat_rows]
        wide = block.shape[0] - at_o
        o_out[k * wide : (k + 1) * wide] = block[at_o:]
        kva_out[k * share : (k + 1) * share] = over_copies(share_in, k)
    for j in range(groups):
        block, at = shared_in[j].astype(jnp.float32), slice(j * hidden, (j + 1) * hidden)
        gate_turn[at] = block[:hidden]
        up_turn[at] = block[hidden : 2 * hidden]
        down_out[at] = block[2 * hidden :]
    q_out[...] = q_turn[...].T
    gate_out[...] = gate_turn[...].T
    up_out[...] = up_turn[...].T


def finish(sizes, heads_in, shared_in, share_in, small_in, state, added):
    heads, at_kv, at_o, lat_rows, hidden, share = sizes
    groups, rows, own_cols = heads_in.shape
    many = groups * hidden

    def shape(*dims):
        return jax.ShapeDtypeStruct(dims, jnp.float32)

    outs = [
        shape(*state.shape),
        shape(own_cols, heads * at_kv),
        shape(lat_rows, heads * (at_o - at_kv) // lat_rows * own_cols),
        shape(heads * (rows - at_o), own_cols),
        shape(own_cols, many),
        shape(own_cols, many),
        shape(many, own_cols),
        shape(heads * share, own_cols),
        shape(*small_in.shape[1:]),
    ]
    turned = [(heads * at_kv, own_cols), (many, own_cols), (many, own_cols)]
    return pl.pallas_call(
        functools.partial(finish_kernel, sizes),
        out_shape=outs,
        in_specs=[pl.BlockSpec(memory_space=pltpu.VMEM)] * 6,
        out_specs=[pl.BlockSpec(memory_space=pltpu.VMEM)] * len(outs),
        scratch_shapes=[pltpu.VMEM(dims, jnp.float32) for dims in turned],
        compiler_params=pltpu.CompilerParams(vmem_limit_bytes=32 << 20),
    )(heads_in, shared_in, share_in, small_in, state, added)


def general_scores(query_blk, key_rows, first_row):
    scores = jnp.einsum(
        "qhd,khd->hqk", query_blk, key_rows, preferred_element_type=jnp.float32
    ) * DQK ** (-0.5)
    row_pos = first_row + jnp.arange(query_blk.shape[0], dtype=jnp.int32)
    col_pos = jnp.arange(key_rows.shape[0], dtype=jnp.int32)
    return jnp.where(col_pos[None, None, :] <= row_pos[None, :, None], scores, -1e30)


def attend(query_rows, key_rows, value_rows):
    seq_len = query_rows.shape[0]
    blk_rows = min(seq_len, 512)

    def one_block(block_index):
        first_row = block_index * blk_rows
        scores = general_scores(query_rows, key_rows, first_row)
        row_max = jnp.max(scores, axis=-1, keepdims=True)
        log_total = row_max + jnp.log(jnp.sum(jnp.exp(scores - row_max), axis=-1, keepdims=True))
        att_weights = jnp.exp(scores - log_total).astype(jnp.bfloat16)
        mixed_blk = jnp.einsum(
            "hqk,khd->qhd", att_weights, value_rows, preferred_element_type=jnp.float32
        ).astype(jnp.bfloat16)
        return (mixed_blk, log_total)

    mixed_heads, log_totals = lax.map(one_block, jnp.arange(seq_len // blk_rows, dtype=jnp.int32))
    return (mixed_heads.reshape(seq_len, query_rows.shape[1], value_rows.shape[2]), log_totals)


def attend_back(query_rows, key_rows, value_rows, log_totals, mixed_grad):
    seq_len, head_count = (query_rows.shape[0], query_rows.shape[1])
    blk_rows = min(seq_len, 512)

    def one_block(running, block_index):
        key_acc, value_acc = running
        first_row = block_index * blk_rows
        scores = general_scores(query_rows, key_rows, first_row)
        att_probs = jnp.exp(scores - log_totals[block_index])
        att_weights = att_probs.astype(jnp.bfloat16)
        value_acc = value_acc + jnp.einsum(
            "hqk,qhd->khd", att_weights, mixed_grad, preferred_element_type=jnp.float32
        )
        prob_grad = jnp.einsum(
            "qhd,khd->hqk", mixed_grad, value_rows, preferred_element_type=jnp.float32
        )
        row_delta = jnp.sum(att_probs * prob_grad, axis=-1, keepdims=True)
        score_delta = (att_probs * (prob_grad - row_delta) * DQK ** (-0.5)).astype(jnp.bfloat16)
        query_grad = jnp.einsum(
            "hqk,khd->qhd", score_delta, key_rows, preferred_element_type=jnp.float32
        )
        key_acc = key_acc + jnp.einsum(
            "hqk,qhd->khd", score_delta, query_rows, preferred_element_type=jnp.float32
        )
        return ((key_acc, value_acc), query_grad)

    zero_start = (
        jnp.zeros((seq_len, head_count, DQK), jnp.float32),
        jnp.zeros((seq_len, head_count, DV), jnp.float32),
    )
    (key_grad, value_grad), query_grad = lax.scan(
        one_block, zero_start, jnp.arange(seq_len // blk_rows, dtype=jnp.int32)
    )
    return (query_grad.reshape(seq_len, head_count, DQK), key_grad, value_grad)


def attention_forward(seq_in, gain_one, query_w, latent_w, gain_kv, kvup_w):
    seq_len = seq_in.shape[0]
    head_count = query_w.shape[1] // DQK
    cosine, sine_part = rope_tables(seq_len, DR)
    stat_one = rms_scale(seq_in)
    unit_one = seq_in * stat_one
    normed1 = (unit_one * gain_one.astype(jnp.float32)).astype(jnp.bfloat16)
    query_full = jnp.dot(normed1, query_w, preferred_element_type=jnp.float32).reshape(
        seq_len, head_count, DQK
    )
    query_rows = jnp.concatenate(
        [
            query_full[..., :DN],
            rotate(query_full[..., DN:], cosine[:, None, :], sine_part[:, None, :]),
        ],
        axis=-1,
    ).astype(jnp.bfloat16)
    latent_full = jnp.dot(normed1, latent_w, preferred_element_type=jnp.float32)
    latent_stat = rms_scale(latent_full[:, : kvup_w.shape[0]])
    latent_unit = latent_full[:, : kvup_w.shape[0]] * latent_stat
    latent = (latent_unit * gain_kv.astype(jnp.float32)).astype(jnp.bfloat16)
    rot_key = rotate(latent_full[:, kvup_w.shape[0] :], cosine, sine_part).astype(jnp.bfloat16)
    key_value = (
        jnp.dot(latent, kvup_w, preferred_element_type=jnp.float32)
        .astype(jnp.bfloat16)
        .reshape(seq_len, head_count, DN + DV)
    )
    key_rows = jnp.concatenate(
        [key_value[..., :DN], jnp.broadcast_to(rot_key[:, None, :], (seq_len, head_count, DR))],
        axis=-1,
    )
    value_rows = key_value[..., DN:]
    mixed_heads, log_totals = attend(query_rows, key_rows, value_rows)
    return (
        stat_one,
        unit_one,
        normed1,
        query_rows,
        latent_stat,
        latent_unit,
        latent,
        key_rows,
        value_rows,
        mixed_heads,
        log_totals,
        cosine,
        sine_part,
    )


def general(
    layer_in,
    norm1_gain,
    q_weight,
    kva_weight,
    kv_gain,
    kvb_weight,
    o_weight,
    norm2_gain,
    router_weight,
    shared_gate,
    shared_up,
    shared_down,
    expert_gate,
    expert_up,
    expert_down,
    routes,
    out_grad,
):
    groups = lax.axis_size(EXPERT)
    seq_len, width = layer_in.shape
    local_experts = expert_gate.shape[0]
    expert_count = local_experts * groups
    capacity = seq_len * TOPK * 4 // (3 * expert_count)
    rows_total = expert_count * capacity
    (
        gain_one,
        query_w,
        latent_w,
        gain_kv,
        kvup_w,
        output_w,
        gain_two,
        route_w,
        gate_sh,
        up_sh,
        down_sh,
    ) = (
        lax.all_gather(norm1_gain, EXPERT, axis=0, tiled=True),
        lax.all_gather(q_weight, EXPERT, axis=0, tiled=True),
        lax.all_gather(kva_weight, EXPERT, axis=0, tiled=True),
        lax.all_gather(kv_gain, EXPERT, axis=0, tiled=True),
        lax.all_gather(kvb_weight, EXPERT, axis=0, tiled=True),
        lax.all_gather(o_weight, EXPERT, axis=1, tiled=True),
        lax.all_gather(norm2_gain, EXPERT, axis=0, tiled=True),
        lax.all_gather(router_weight, EXPERT, axis=0, tiled=True),
        lax.all_gather(shared_gate, EXPERT, axis=0, tiled=True),
        lax.all_gather(shared_up, EXPERT, axis=0, tiled=True),
        lax.all_gather(shared_down, EXPERT, axis=1, tiled=True),
    )
    (
        stat_one,
        unit_one,
        normed1,
        query_rows,
        latent_stat,
        latent_unit,
        latent,
        key_rows,
        value_rows,
        mixed_heads,
        log_totals,
        cosine,
        sine_part,
    ) = attention_forward(layer_in, gain_one, query_w, latent_w, gain_kv, kvup_w)
    head_count = query_rows.shape[1]
    mixed_flat = mixed_heads.reshape(seq_len, head_count * DV)
    attn_part = jnp.dot(mixed_flat, output_w, preferred_element_type=jnp.float32)
    hidden_state = layer_in + lax.psum(attn_part, TENSOR)
    stat_two = rms_scale(hidden_state)
    unit_two = hidden_state * stat_two
    normed2 = (unit_two * gain_two.astype(jnp.float32)).astype(jnp.bfloat16)
    router_probs = jax.nn.softmax(
        jnp.dot(normed2, route_w, preferred_element_type=jnp.float32), axis=-1
    )
    route_onehot = (
        routes[:, :, None] == jnp.arange(expert_count, dtype=jnp.int32)[None, None, :]
    ).astype(jnp.float32)
    route_weight = jnp.einsum("tke,te->tk", route_onehot, router_probs)
    flat_hot = route_onehot.reshape(seq_len * TOPK, expert_count).astype(jnp.int32)
    slot_pos = jnp.sum(jnp.cumsum(flat_hot, axis=0) * flat_hot, axis=-1) - 1
    buffer_pos = routes.reshape(-1) * capacity + slot_pos

    def to_owners(assigned):
        buffer = jnp.zeros((rows_total, width), jnp.bfloat16).at[buffer_pos].set(assigned)
        buffer = buffer.reshape(groups, local_experts * capacity, width)
        arrived = lax.all_to_all(buffer, EXPERT, split_axis=0, concat_axis=0, tiled=True)
        return (
            arrived.reshape(groups, local_experts, capacity, width)
            .transpose(1, 0, 2, 3)
            .reshape(local_experts, groups * capacity, width)
        )

    def to_sources(results):
        arranged = (
            results.reshape(local_experts, groups, capacity, width)
            .transpose(1, 0, 2, 3)
            .reshape(groups, local_experts * capacity, width)
        )
        arrived = lax.all_to_all(arranged, EXPERT, split_axis=0, concat_axis=0, tiled=True)
        return arrived.reshape(rows_total, width)[buffer_pos].reshape(seq_len, TOPK, width)

    rows_in = to_owners(jnp.repeat(normed2, TOPK, axis=0))
    pre_gate = jnp.einsum("emd,edf->emf", rows_in, expert_gate, preferred_element_type=jnp.float32)
    pre_up = jnp.einsum("emd,edf->emf", rows_in, expert_up, preferred_element_type=jnp.float32)
    expert_act = (jax.nn.silu(pre_gate) * pre_up).astype(jnp.bfloat16)
    block_out = jnp.einsum(
        "emf,efd->emd", expert_act, expert_down, preferred_element_type=jnp.float32
    ).astype(jnp.bfloat16)
    expert_out = to_sources(block_out)
    routed_part = jnp.einsum(
        "tk,tkd->td", route_weight, expert_out, preferred_element_type=jnp.float32
    )
    shared_pre_gate = jnp.dot(normed2, gate_sh, preferred_element_type=jnp.float32)
    shared_pre_up = jnp.dot(normed2, up_sh, preferred_element_type=jnp.float32)
    shared_act = (jax.nn.silu(shared_pre_gate) * shared_pre_up).astype(jnp.bfloat16)
    shared_part = jnp.dot(shared_act, down_sh, preferred_element_type=jnp.float32)
    layer_out = hidden_state + lax.psum(
        (routed_part + shared_part).astype(jnp.bfloat16), TENSOR
    ).astype(jnp.float32)
    out_rows = out_grad.astype(jnp.bfloat16)
    routed_cot = (
        (route_weight[:, :, None] * out_grad[:, None, :])
        .astype(jnp.bfloat16)
        .reshape(seq_len * TOPK, width)
    )
    cot_in = to_owners(routed_cot)
    route_grad_part = jnp.einsum(
        "tkd,td->tk", expert_out, out_grad, preferred_element_type=jnp.float32
    )
    hidden_grad_ex = jnp.einsum(
        "emd,efd->emf", cot_in, expert_down, preferred_element_type=jnp.float32
    )
    gate_delta = (hidden_grad_ex * pre_up * silu_grad(pre_gate)).astype(jnp.bfloat16)
    up_delta = (hidden_grad_ex * jax.nn.silu(pre_gate)).astype(jnp.bfloat16)
    expert_down_grad = jnp.einsum(
        "emf,emd->efd", expert_act, cot_in, preferred_element_type=jnp.float32
    )
    expert_gate_grad = jnp.einsum(
        "emd,emf->edf", rows_in, gate_delta, preferred_element_type=jnp.float32
    )
    expert_up_grad = jnp.einsum(
        "emd,emf->edf", rows_in, up_delta, preferred_element_type=jnp.float32
    )
    row_block = (
        jnp.einsum("emf,edf->emd", gate_delta, expert_gate, preferred_element_type=jnp.float32)
        + jnp.einsum("emf,edf->emd", up_delta, expert_up, preferred_element_type=jnp.float32)
    ).astype(jnp.bfloat16)
    row_grad = to_sources(row_block)
    shared_down_grad = jnp.dot(shared_act.T, out_rows, preferred_element_type=jnp.float32)
    shared_hidden_grad = jnp.dot(out_rows, down_sh.T, preferred_element_type=jnp.float32)
    shared_gate_delta = (shared_hidden_grad * shared_pre_up * silu_grad(shared_pre_gate)).astype(
        jnp.bfloat16
    )
    shared_up_delta = (shared_hidden_grad * jax.nn.silu(shared_pre_gate)).astype(jnp.bfloat16)
    shared_gate_grad = jnp.dot(normed2.T, shared_gate_delta, preferred_element_type=jnp.float32)
    shared_up_grad = jnp.dot(normed2.T, shared_up_delta, preferred_element_type=jnp.float32)
    normed2_part = (
        jnp.sum(row_grad, axis=1, dtype=jnp.float32)
        + jnp.dot(shared_gate_delta, gate_sh.T, preferred_element_type=jnp.float32)
        + jnp.dot(shared_up_delta, up_sh.T, preferred_element_type=jnp.float32)
    )
    normed2_grad, route_grad = lax.psum((normed2_part, route_grad_part), TENSOR)
    prob_grad = jnp.einsum("tk,tke->te", route_grad, route_onehot)
    logit_delta = (
        router_probs * (prob_grad - jnp.sum(router_probs * prob_grad, axis=-1, keepdims=True))
    ).astype(jnp.bfloat16)
    router_grad = jnp.dot(normed2.T, logit_delta, preferred_element_type=jnp.float32)
    normed2_grad = normed2_grad + jnp.dot(
        logit_delta, route_w.T, preferred_element_type=jnp.float32
    )
    norm2_gain_grad = jnp.sum(normed2_grad * unit_two, axis=0)
    scaled_two = normed2_grad * gain_two.astype(jnp.float32)
    hidden_grad = out_grad + stat_two * (
        scaled_two - unit_two * jnp.mean(scaled_two * unit_two, axis=-1, keepdims=True)
    )
    hidden_rows = hidden_grad.astype(jnp.bfloat16)
    o_grad = jnp.dot(mixed_flat.T, hidden_rows, preferred_element_type=jnp.float32)
    mixed_grad = (
        jnp.dot(hidden_rows, output_w.T, preferred_element_type=jnp.float32)
        .astype(jnp.bfloat16)
        .reshape(seq_len, head_count, DV)
    )
    query_grad, key_grad, value_grad = attend_back(
        query_rows, key_rows, value_rows, log_totals, mixed_grad
    )
    query_delta = (
        jnp.concatenate(
            [
                query_grad[..., :DN],
                rotate_back(query_grad[..., DN:], cosine[:, None, :], sine_part[:, None, :]),
            ],
            axis=-1,
        )
        .astype(jnp.bfloat16)
        .reshape(seq_len, head_count * DQK)
    )
    kv_delta = (
        jnp.concatenate([key_grad[..., :DN], value_grad], axis=-1)
        .astype(jnp.bfloat16)
        .reshape(seq_len, head_count * (DN + DV))
    )
    q_grad = jnp.dot(normed1.T, query_delta, preferred_element_type=jnp.float32)
    kvb_grad = jnp.dot(latent.T, kv_delta, preferred_element_type=jnp.float32)
    latent_part = jnp.dot(kv_delta, kvup_w.T, preferred_element_type=jnp.float32)
    rot_part = jnp.sum(key_grad[..., DN:], axis=1)
    normed1_part = jnp.dot(query_delta, query_w.T, preferred_element_type=jnp.float32)
    latent_grad, rot_sum, normed1_query = (
        lax.psum(latent_part.astype(jnp.bfloat16), TENSOR).astype(jnp.float32),
        lax.psum(rot_part.astype(jnp.bfloat16), TENSOR).astype(jnp.float32),
        lax.psum(normed1_part.astype(jnp.bfloat16), TENSOR).astype(jnp.float32),
    )
    kv_gain_grad = jnp.sum(latent_grad * latent_unit, axis=0)
    scaled_lat = latent_grad * gain_kv.astype(jnp.float32)
    latent_back = latent_stat * (
        scaled_lat - latent_unit * jnp.mean(scaled_lat * latent_unit, axis=-1, keepdims=True)
    )
    latent_delta = jnp.concatenate(
        [latent_back, rotate_back(rot_sum, cosine, sine_part)], axis=-1
    ).astype(jnp.bfloat16)
    kva_grad = jnp.dot(normed1.T, latent_delta, preferred_element_type=jnp.float32)
    normed1_grad = normed1_query + jnp.dot(
        latent_delta, latent_w.T, preferred_element_type=jnp.float32
    )
    norm1_gain_grad = jnp.sum(normed1_grad * unit_one, axis=0)
    scaled_one = normed1_grad * gain_one.astype(jnp.float32)
    x_grad = hidden_grad + stat_one * (
        scaled_one - unit_one * jnp.mean(scaled_one * unit_one, axis=-1, keepdims=True)
    )
    (
        norm1_gain_grad,
        q_grad,
        kva_grad,
        kv_gain_grad,
        kvb_grad,
        o_grad,
        norm2_gain_grad,
        router_grad,
        shared_gate_grad,
        shared_up_grad,
        shared_down_grad,
    ) = (
        lax.psum_scatter(norm1_gain_grad, EXPERT, scatter_dimension=0, tiled=True),
        lax.psum_scatter(q_grad, EXPERT, scatter_dimension=0, tiled=True),
        lax.psum_scatter(kva_grad, EXPERT, scatter_dimension=0, tiled=True),
        lax.psum_scatter(kv_gain_grad, EXPERT, scatter_dimension=0, tiled=True),
        lax.psum_scatter(kvb_grad, EXPERT, scatter_dimension=0, tiled=True),
        lax.psum_scatter(o_grad, EXPERT, scatter_dimension=1, tiled=True),
        lax.psum_scatter(norm2_gain_grad, EXPERT, scatter_dimension=0, tiled=True),
        lax.psum_scatter(router_grad, EXPERT, scatter_dimension=0, tiled=True),
        lax.psum_scatter(shared_gate_grad, EXPERT, scatter_dimension=0, tiled=True),
        lax.psum_scatter(shared_up_grad, EXPERT, scatter_dimension=0, tiled=True),
        lax.psum_scatter(shared_down_grad, EXPERT, scatter_dimension=1, tiled=True),
    )
    return (
        layer_out,
        x_grad,
        norm1_gain_grad,
        q_grad,
        kva_grad,
        kv_gain_grad,
        kvb_grad,
        o_grad,
        norm2_gain_grad,
        router_grad,
        shared_gate_grad,
        shared_up_grad,
        shared_down_grad,
        expert_gate_grad,
        expert_up_grad,
        expert_down_grad,
    )


def fits(groups, heads, block, width):
    whole = groups in (4, 8, 16) and heads in (4, 8, 16) and groups % heads == 0
    return whole and block % 64 == 0 and width == groups * LANES


def to_blocks(grad_rows, groups):
    rows, width = grad_rows.shape
    kept = lax.optimization_barrier(grad_rows.astype(jnp.bfloat16))
    return kept.reshape(rows, groups, width // groups).transpose(1, 0, 2)


def from_blocks(blocks):
    groups, rows, width = blocks.shape
    return blocks.transpose(1, 0, 2).reshape(rows, groups * width)


def widen(rows, width):
    return jnp.pad(rows, [(0, 0)] * (rows.ndim - 1) + [(0, width - rows.shape[-1])])


def by_heads(
    layer_in,
    norm1_gain,
    q_weight,
    kva_weight,
    kv_gain,
    kvb_weight,
    o_weight,
    norm2_gain,
    router_weight,
    shared_gate,
    shared_up,
    shared_down,
    expert_gate,
    expert_up,
    expert_down,
    routes,
    out_grad,
):
    groups = lax.axis_size(EXPERT)
    chip = lax.axis_index(EXPERT)
    seq_len, width = layer_in.shape
    capacity = seq_len * TOPK * 4 // (3 * groups)
    heads = q_weight.shape[1] // DQK
    copies = groups // heads
    head = lax.rem(chip, heads)
    own_cols = kva_weight.shape[0]
    lat_rows, lat_width = kvb_weight.shape[0], kvb_weight.shape[0] * groups
    hidden = shared_gate.shape[1] // groups
    bf16 = jnp.bfloat16

    kv_halves = (DN + DV) // own_cols
    kv_block = lat_rows * kv_halves
    head_parts = jnp.concatenate(
        [
            q_weight.reshape(own_cols, heads, DQK).transpose(1, 2, 0),
            kvb_weight.reshape(lat_rows, heads, kv_halves, own_cols)
            .transpose(1, 2, 0, 3)
            .reshape(heads, kv_block, own_cols),
            o_weight.reshape(heads, DV, own_cols),
        ],
        axis=1,
    )
    shared_parts = jnp.concatenate(
        [
            shared_gate.reshape(own_cols, groups, hidden).transpose(1, 2, 0),
            shared_up.reshape(own_cols, groups, hidden).transpose(1, 2, 0),
            shared_down.reshape(groups, hidden, own_cols),
        ],
        axis=1,
    )
    small = jnp.concatenate(
        [
            router_weight.T,
            norm1_gain[None, :],
            norm2_gain[None, :],
            widen(kv_gain[None, :], own_cols),
        ],
        axis=0,
    )
    small = jnp.pad(small, [(0, -small.shape[0] % 16), (0, 0)])
    at_kv = DQK
    at_o = at_kv + kv_block
    at_gate = at_o + DV
    planes, all_planes = heads // 4, groups // 4
    small_swap = Swap(jnp.broadcast_to(small[None], (groups,) + small.shape), True)
    (small_all,), (latent_w,), (got,), (normed1_all,) = exchange(
        [
            small_swap,
            Gather([kva_weight], all_planes),
            Swap(jnp.tile(head_parts, (copies, 1, 1))),
            NormGather(layer_in, small_swap, groups, planes),
        ],
        1,
    )
    route_wt = from_blocks(small_all[:, :groups])
    gain_one = small_all[:, groups].reshape(width).astype(jnp.float32)
    gain_two = small_all[:, groups + 1].reshape(width).astype(jnp.float32)
    gain_kv = small_all[:, groups + 2, :lat_rows].reshape(lat_width).astype(jnp.float32)
    latent_w = latent_w.reshape(width, kva_weight.shape[1])
    stat_one = rms_scale(layer_in)
    unit_one = layer_in * stat_one

    cosine, sine_part = rope_tables(seq_len, DR)
    turn_cos = jnp.concatenate([cosine, cosine], axis=-1)
    turn_sin = jnp.concatenate([-sine_part, sine_part], axis=-1)
    by_seq = (heads, seq_len, -1)
    fold = 2

    def rotated(block, cos_ref, sin_ref, sign):
        flipped = jnp.concatenate([block[:, DR // 2 :], block[:, : DR // 2]], axis=-1)
        reps = block.shape[0] // seq_len
        cos_rows = jnp.concatenate([cos_ref[...]] * reps, axis=0)
        sin_rows = jnp.concatenate([sin_ref[...]] * reps, axis=0)
        return (block * cos_rows + sign * flipped * sin_rows).astype(bf16)

    def attend_forward(refs):
        rows_in, parts, lat_w, kv_gain_ref, cos_ref, sin_ref = refs[:6]
        query_out, key_out, value_out, prob_out, lat_out, latent_out, mixed_out = refs[6:13]
        out_w, query_w, kv_w = refs[13:]

        def assemble():
            for j in range(groups):
                at = slice(j * own_cols, (j + 1) * own_cols)
                query_w[:, at] = parts[j, :at_kv]
                out_w[:, at] = parts[j, at_o:at_gate]
                down = slice(j * lat_rows, (j + 1) * lat_rows)
                for half in range(kv_halves):
                    start = at_kv + half * lat_rows
                    across = slice(half * own_cols, (half + 1) * own_cols)
                    kv_w[down, across] = parts[j, start : start + lat_rows]

        def some(first):
            rows = rows_in[pl.ds(first, fold)].reshape(fold * seq_len, width)
            query = dot_nt(rows, query_w[...])
            query_plain, query_turn = query[:, :DN].astype(bf16), rotated(query[:, DN:], cos_ref, sin_ref, 1.0)
            full = fdot(rows, lat_w[...])
            plain = full[:, :lat_width]
            latent = (plain * rms_scale(plain) * kv_gain_ref[...]).astype(bf16)
            key_turn = rotated(full[:, lat_width:], cos_ref, sin_ref, 1.0)
            key_value = fdot(latent, kv_w[...]).astype(bf16)
            latent_out[pl.ds(first, fold)] = latent.reshape(fold, seq_len, lat_width)
            lat_out[pl.ds(first, fold)] = plain.reshape(fold, seq_len, lat_width)
            ahead = lax.broadcasted_iota(jnp.int32, (seq_len, seq_len), 1) > lax.broadcasted_iota(
                jnp.int32, (seq_len, seq_len), 0
            )
            for k in range(fold):
                at, seq = slice(k * seq_len, (k + 1) * seq_len), first + k
                scores = dot_nt(query_plain[at], key_value[at, :DN])
                scores += dot_nt(query_turn[at], key_turn[at])
                scores = jnp.where(ahead, -1e30, scores * DQK ** (-0.5))
                row_max = jnp.max(scores, axis=-1, keepdims=True)
                total = jnp.sum(jnp.exp(scores - row_max), axis=-1, keepdims=True)
                probs = jnp.exp(scores - (row_max + jnp.log(total)))
                values = key_value[at, DN:]
                prob_out[seq] = probs
                mixed_out[seq] = fdot(probs.astype(bf16), values).astype(bf16)
                query_out[seq, :, :DN], query_out[seq, :, DN:] = query_plain[at], query_turn[at]
                key_out[seq, :, :DN], key_out[seq, :, DN:] = key_value[at, :DN], key_turn[at]
                value_out[seq] = values

        def two(r):
            pl.when(r == 0)(assemble)
            pl.loop(0, 2)(lambda q: some((2 * r + q) * fold))

        return heads // (2 * fold), two

    out_rows = out_grad.astype(bf16)

    def attn_part(part, slot, refs):
        @pl.loop(0, width // 512)
        def _(k):
            cols = part_rows(k * 512, 512)
            part[slot, :, cols] = fdot(refs[12][slot], refs[13][:, cols]).astype(bf16)

    def shaped(last, kind):
        return jax.ShapeDtypeStruct((heads, seq_len, last), kind)

    attended, (shared_got,) = exchange(
        [
            Reduce(
                [normed1_all, got, latent_w, gain_kv[None, :], turn_cos, turn_sin],
                attn_part,
                heads,
                seq_len,
                width,
                extra=[
                    shaped(DQK, bf16),
                    shaped(DQK, bf16),
                    shaped(DV, bf16),
                    shaped(seq_len, jnp.float32),
                    shaped(lat_width, jnp.float32),
                    shaped(lat_width, bf16),
                    shaped(DV, bf16),
                    jax.ShapeDtypeStruct((DV, width), bf16),
                    jax.ShapeDtypeStruct((DQK, width), bf16),
                    jax.ShapeDtypeStruct((lat_width, DN + DV), bf16),
                ],
                prelude=attend_forward,
            ),
            Swap(shared_parts, pace=3),
        ],
        2,
    )
    attn_sum, query_rows, key_rows, value_rows, att_probs, lat_plain, latent, mixed = attended[:8]
    output_w, query_wt, kvup_w = attended[8:]

    gate_sht = from_blocks(shared_got[:, :hidden])
    up_sht = from_blocks(shared_got[:, hidden : 2 * hidden])
    down_sh = from_blocks(shared_got[:, 2 * hidden :])
    hidden_state = layer_in + attn_sum

    stat_two = rms_scale(hidden_state)
    unit_two = hidden_state * stat_two
    normed2 = (unit_two * gain_two).astype(bf16)
    router_probs = jax.nn.softmax(fsum("td,ed->te", normed2, route_wt), axis=-1)
    experts = jnp.arange(groups, dtype=jnp.int32)
    chosen = jnp.any(routes[:, :, None] == experts[None, None, :], axis=1)
    marked = widen(jnp.where(chosen, router_probs, -1.0), -(-groups // LANES) * LANES)
    room = -(-hidden // 16) * 16

    def stacked(blocks):
        return jnp.pad(blocks, [(0, room - hidden), (0, 0)])

    token_gather = Gather([normed2, out_rows, marked], all_planes, True)
    experts_op = Experts(
        token_gather,
        [expert_gate[0].T, expert_up[0].T, expert_down[0]],
        jnp.stack([stacked(gate_sht), stacked(up_sht), stacked(down_sh)]),
        capacity,
    )
    _, expert_results = exchange([token_gather, experts_op], 3)
    grad_parts, out_block, picks, shared_act, shared_sums = expert_results[:5]
    rows_in, cot_in, expert_act, gate_delta, up_delta = (
        x.reshape(groups * capacity, -1) for x in expert_results[5:]
    )
    gate_grad_turn, up_grad_turn, down_grad = expert_weight_grads(
        expert_act, gate_delta, up_delta, rows_in, cot_in
    )
    expert_gate_grad, expert_up_grad = gate_grad_turn.T[None], up_grad_turn.T[None]
    expert_down_grad = down_grad[None]
    shared_grads = (
        shared_sums[:, :hidden]
        .reshape(3 * hidden, groups, own_cols)
        .transpose(1, 0, 2)
    )
    out_left = jnp.concatenate(
        [picks, shared_act.reshape(room, groups, seq_len).transpose(1, 0, 2)], axis=1
    )

    def expert_part(part, slot, refs):
        left, own, held = refs[0], refs[1], refs[-1]
        held[:capacity] = own[slot]

        @pl.loop(0, width // 512)
        def _(k):
            cols = part_rows(k * 512, 512)
            part[slot, :, cols] = dot_tn(left[slot], held[:, cols]).astype(bf16)

    def hold_shared(refs):
        refs[-1][capacity:] = refs[2][...]

    ((summed,),) = exchange(
        [Reduce([grad_parts], None, groups, seq_len, width + marked.shape[1])], 4
    )
    normed2_sum = summed[:, :width]
    prob_grad = summed[:, width : width + groups]
    logit_delta = (
        router_probs * (prob_grad - jnp.sum(router_probs * prob_grad, axis=-1, keepdims=True))
    ).astype(bf16)
    normed2_grad = normed2_sum + fdot(logit_delta, route_wt)
    router_gradt = fsum("te,td->ed", logit_delta, normed2)
    norm2_gain_grad = jnp.sum(normed2_grad * unit_two, axis=0)
    scaled_two = normed2_grad * gain_two
    hidden_grad = out_grad + stat_two * (
        scaled_two - unit_two * jnp.mean(scaled_two * unit_two, axis=-1, keepdims=True)
    )

    hidden_rows = hidden_grad.astype(bf16)
    hidden_gather = Gather([hidden_rows], planes, True)

    def attend_backward(refs):
        rows_in, keys, values, probs, out_w, cos_ref, sin_ref = refs[:7]
        query_to, kv_to, turn_to = refs[9:]
        place, hidden_in = hidden_gather.place, hidden_gather.results[0]

        def some(r):
            level = lax.rem(hidden_gather.level + r // 2, planes)
            first = level * 4 + place.spot(3 - 2 * lax.rem(r, 2))
            second = level * 4 + place.spot(2 - 2 * lax.rem(r, 2))
            slots = [first, second]
            pl.when(r == 0)(lambda: hidden_gather.ready(first, False))
            pl.when(r > 0)(lambda: hidden_gather.ready(first, True))
            hidden_gather.ready(second, True)
            rows = jnp.concatenate([hidden_in[slot] for slot in slots], axis=0)
            mixed_grads = dot_nt(rows, out_w[...]).astype(bf16)
            for k in range(2):
                slot = slots[k]
                mixed_grad = mixed_grads[k * seq_len : (k + 1) * seq_len]
                prob = probs[slot]
                value_grad = dot_tn(prob.astype(bf16), mixed_grad)
                dprob = dot_nt(mixed_grad, values[slot])
                row_delta = jnp.sum(prob * dprob, axis=-1, keepdims=True)
                score_delta = (prob * (dprob - row_delta) * DQK ** (-0.5)).astype(bf16)
                query_grad = fdot(score_delta, keys[slot])
                key_grad = dot_tn(score_delta, rows_in[slot])
                query_to[slot, :, :DN] = query_grad[:, :DN].astype(bf16)
                query_to[slot, :, DN:] = rotated(query_grad[:, DN:], cos_ref, sin_ref, -1.0)
                kv_to[slot, :, :DN] = key_grad[:, :DN].astype(bf16)
                kv_to[slot, :, DN:] = value_grad.astype(bf16)
                turn_to[slot, :, :DR] = key_grad[:, DN:].astype(bf16)
                turn_to[slot, :, DR:] = jnp.zeros((seq_len, LANES - DR), bf16)

        hidden_gather.landed = True
        return 2 * planes, some

    def back_part(part, slot, refs):
        @pl.loop(0, width // 512)
        def _(k):
            cols = part_rows(k * 512, 512)
            part[slot, :, cols] = fdot(refs[9][slot], refs[7][:, cols]).astype(bf16)

        product = dot_nt(refs[10][slot], refs[8][...])
        part[slot, :, width : width + lat_width] = product.astype(bf16)
        part[slot, :, width + lat_width :] = refs[11][slot]

    (hidden_all,), (back, query_delta, kv_delta), (owned_early,) = exchange(
        [
            hidden_gather,
            Reduce(
                [
                    query_rows,
                    key_rows,
                    value_rows,
                    att_probs,
                    output_w,
                    turn_cos,
                    turn_sin,
                    query_wt,
                    kvup_w,
                ],
                back_part,
                heads,
                seq_len,
                width + lat_width + LANES,
                [pltpu.VMEM((heads, seq_len, LANES), bf16)],
                extra=[shaped(DQK, bf16), shaped(DN + DV, bf16)],
                prelude=attend_backward,
                delay=2,
            ),
            Swap(shared_grads),
        ],
        5,
    )
    normed1_query = back[:, :width]
    latent_grad = back[:, width : width + lat_width]
    rot_sum = back[:, width + lat_width : width + lat_width + DR]

    own_plain = lax.dynamic_index_in_dim(lat_plain, head, 0, keepdims=False)
    own_stat = rms_scale(own_plain)
    own_unit = own_plain * own_stat
    kv_gain_grad = jnp.sum(latent_grad * own_unit, axis=0)
    scaled_lat = latent_grad * gain_kv
    latent_back = own_stat * (
        scaled_lat - own_unit * jnp.mean(scaled_lat * own_unit, axis=-1, keepdims=True)
    )
    latent_delta = jnp.concatenate(
        [latent_back, rotate_back(rot_sum, cosine, sine_part)], axis=-1
    ).astype(bf16)
    normed1_grad = normed1_query + fsum("tl,dl->td", latent_delta, latent_w)
    norm1_gain_grad = jnp.sum(normed1_grad * unit_one, axis=0)
    scaled_one = normed1_grad * gain_one
    x_grad = hidden_grad + stat_one * (
        scaled_one - unit_one * jnp.mean(scaled_one * unit_one, axis=-1, keepdims=True)
    )

    share = (lat_width + DR) // heads

    def by_owner(row):
        return widen(row.reshape(groups, 1, -1), own_cols)

    small_grads = jnp.concatenate(
        [
            router_gradt.reshape(groups, groups, own_cols).transpose(1, 0, 2),
            by_owner(norm1_gain_grad),
            by_owner(norm2_gain_grad),
            by_owner(kv_gain_grad),
        ],
        axis=1,
    )
    small_grads = jnp.pad(small_grads, [(0, 0), (0, -small_grads.shape[1] % 8), (0, 0)])

    def make_head_grads(op):
        query_ref, rows_ref, mixed_ref, hidden_ref, latent_ref, kv_ref = op.refs
        tokens = heads * seq_len

        def projections(_):
            queries = query_ref[...].reshape(tokens, DQK)
            mixed_rows = mixed_ref[...].reshape(tokens, DV)

            @pl.loop(0, width // 512)
            def _(part):
                cols, first = part_rows(part * 512, 512), part * (512 // own_cols)
                rows = rows_ref[:, :, cols].reshape(tokens, 512)
                hidden_part = hidden_ref[:, :, cols].reshape(tokens, 512)
                of_query = dot_tn(queries, rows).astype(bf16)
                of_out = dot_tn(mixed_rows, hidden_part).astype(bf16)
                for k in range(512 // own_cols):
                    at = slice(k * own_cols, (k + 1) * own_cols)
                    op.source[first + k, :at_kv] = of_query[:, at]
                    op.source[first + k, at_o:at_gate] = of_out[:, at]

        def latents(_):
            lat = latent_ref[...].reshape(tokens, lat_width)
            of_kv = dot_tn(lat, kv_ref[...].reshape(tokens, DN + DV)).astype(bf16)
            for j in range(groups):
                for half in range(kv_halves):
                    start = at_kv + half * lat_rows
                    block = of_kv[
                        j * lat_rows : (j + 1) * lat_rows, half * own_cols : (half + 1) * own_cols
                    ]
                    op.source[j, start : start + lat_rows] = block

        return [projections, latents]

    latent_gather = Gather([latent_delta], planes, True)
    head_swap = MadeSwap(
        [query_delta, normed1_all, mixed, hidden_all, latent, kv_delta],
        (groups, at_gate, own_cols),
        make_head_grads,
        None,
        5,
    )

    def make_latent_grads(op):
        def product(_):
            pl.loop(0, planes)(latent_gather.receive)
            deltas = latent_gather.results[0][...].reshape(heads * seq_len, lat_width + DR)

            @pl.loop(0, width // 512)
            def _(part):
                cols = part_rows(part * 512, 512)
                rows = head_swap.refs[1][:, :, cols].reshape(heads * seq_len, 512)
                op.extra[0][:, cols] = dot_tn(deltas, rows)

            first = lax.rem(op.place.chip, heads) * share
            mine = op.extra[0][pl.ds(pl.multiple_of(first, 8), share), :].astype(bf16)
            for j in range(groups):
                op.source[j] = mine[:, j * own_cols : (j + 1) * own_cols]

        latent_gather.landed = True
        return [product]

    (latent_delta_all,), (out_sum,), (owned_heads,), (owned_small,), (owned_share,) = exchange(
        [
            latent_gather,
            Reduce(
                [out_left, out_block, stacked(down_sh)],
                expert_part,
                groups,
                seq_len,
                width,
                [pltpu.VMEM((capacity + room, width), bf16)],
                hold_shared,
            ),
            head_swap,
            Swap(small_grads, pace=5),
            MadeSwap(
                [],
                (groups, share, own_cols),
                make_latent_grads,
                planes + 1,
                groups,
                [pltpu.VMEM((lat_width + DR, width), jnp.float32)],
            ),
        ],
        6,
    )
    (
        layer_out,
        q_grad,
        kvb_grad,
        own_o_grad,
        shared_gate_grad,
        shared_up_grad,
        shared_down_grad,
        kva_turn,
        small_sums,
    ) = finish(
        (heads, at_kv, at_o, lat_rows, hidden, share),
        owned_heads,
        owned_early,
        owned_share,
        owned_small,
        hidden_state,
        out_sum,
    )
    kva_grad, router_grad = kva_turn.T, small_sums[:groups].T
    return (
        layer_out,
        x_grad,
        small_sums[groups],
        q_grad,
        kva_grad,
        small_sums[groups + 2, :lat_rows],
        kvb_grad,
        own_o_grad,
        small_sums[groups + 1],
        router_grad,
        shared_gate_grad,
        shared_up_grad,
        shared_down_grad,
        expert_gate_grad,
        expert_up_grad,
        expert_down_grad,
    )


def on_device(layer_in, *rest):
    groups, heads = lax.axis_size(EXPERT), rest[1].shape[1] // DQK
    one_each = rest[11].shape[0] == 1
    if one_each and fits(groups, heads, *layer_in.shape):
        return by_heads(layer_in, *rest)
    return general(layer_in, *rest)


def solution(mesh):
    in_specs = (
        P(EXPERT, None),
        P(EXPERT),
        P(EXPERT, TENSOR),
        P(EXPERT, None),
        P(EXPERT),
        P(EXPERT, TENSOR),
        P(TENSOR, EXPERT),
        P(EXPERT),
        P(EXPERT, None),
        P(EXPERT, TENSOR),
        P(EXPERT, TENSOR),
        P(TENSOR, EXPERT),
        P(EXPERT, None, TENSOR),
        P(EXPERT, None, TENSOR),
        P(EXPERT, TENSOR, None),
        P(EXPERT, None),
        P(EXPERT, None),
    )
    out_specs = (
        P(EXPERT, None),
        P(EXPERT, None),
        P(EXPERT),
        P(EXPERT, TENSOR),
        P(EXPERT, None),
        P(EXPERT),
        P(EXPERT, TENSOR),
        P(TENSOR, EXPERT),
        P(EXPERT),
        P(EXPERT, None),
        P(EXPERT, TENSOR),
        P(EXPERT, TENSOR),
        P(TENSOR, EXPERT),
        P(EXPERT, None, TENSOR),
        P(EXPERT, None, TENSOR),
        P(EXPERT, TENSOR, None),
    )
    return jax.shard_map(
        on_device, mesh=mesh, in_specs=in_specs, out_specs=out_specs, check_vma=False
    )
```

```python
import functools

import jax
import jax.numpy as jnp
from jax import lax
from jax.experimental import pallas as pl
from jax.experimental.pallas import tpu as pltpu
from jax.sharding import PartitionSpec as P

DN = 128
DR = 64
DQK = 192
DV = 128
TOPK = 6
LANES = 128


norm_eps = 1e-06


def rms_scale(inputs):
    return lax.rsqrt(jnp.mean(inputs * inputs, axis=-1, keepdims=True) + norm_eps)


def rope_tables(length, rot_width):
    half_width = rot_width // 2
    frequency = 10000.0 ** (-jnp.arange(half_width).astype(jnp.float32) / half_width)
    angles = jnp.arange(length).astype(jnp.float32)[:, None] * frequency[None, :]
    return (jnp.cos(angles), jnp.sin(angles))


def rotate(inputs, cosine, sine_part):
    half_width = inputs.shape[-1] // 2
    first_half = inputs[..., :half_width]
    second_half = inputs[..., half_width:]
    return jnp.concatenate(
        [
            first_half * cosine - second_half * sine_part,
            second_half * cosine + first_half * sine_part,
        ],
        axis=-1,
    )


def rotate_back(inputs, cosine, sine_part):
    return rotate(inputs, cosine, -sine_part)


def silu_grad(pre_act):
    sigmoid_val = jax.nn.sigmoid(pre_act)
    return sigmoid_val * (1.0 + pre_act * (1.0 - sigmoid_val))


def fdot(left, right):
    return jnp.dot(left, right, preferred_element_type=jnp.float32)


def dot_nt(left, right):
    return lax.dot_general(
        left, right, (((1,), (1,)), ((), ())), preferred_element_type=jnp.float32
    )


def dot_tn(left, right):
    return lax.dot_general(
        left, right, (((0,), (0,)), ((), ())), preferred_element_type=jnp.float32
    )


def fsum(spec, left, right):
    return jnp.einsum(spec, left, right, preferred_element_type=jnp.float32)


EXPERT, TENSOR = "expert", "tensor"
MESH = pl.DeviceIdType.MESH
DMA = pltpu.SemaphoreType.DMA


def remote(src, dst, send, recv, target):
    return pltpu.make_async_remote_copy(
        src_ref=src, dst_ref=dst, send_sem=send, recv_sem=recv, device_id=target, device_id_type=MESH
    )


def part_rows(start, size):
    return pl.ds(pl.multiple_of(start, size), size)


class Place:
    def __init__(self):
        self.groups = lax.axis_size(EXPERT)
        self.chip = lax.axis_index(EXPERT)
        self.core = lax.axis_index(TENSOR)
        self.here = lax.rem(self.chip, 4)
        self.there_x = self.here + 1 - 2 * lax.rem(self.here, 2)
        self.there_y = self.here + 2 - 4 * (self.here // 2)
        self.across = 3 - self.here
        base = self.chip - self.here
        self.by_x = {EXPERT: base + self.there_x}
        self.by_y = {EXPERT: base + self.there_y}
        self.above = {EXPERT: self.chip + 4}
        self.below = {EXPERT: self.chip - 4}
        self.mate = {TENSOR: 1 - self.core}

    def spot(self, q):
        x = lax.rem(self.here + 1 - lax.rem(q, 2), 2)
        y = lax.rem(self.here // 2 + 1 - q // 2, 2)
        return 2 * y + x

    def partner(self, j):
        return lax.rem(self.chip + j, self.groups)


def level_at(level, planes, t):
    if planes < 4:
        return lax.rem(level + t, planes)
    flip = level // 2
    near = lax.rem(level + flip, 2)
    order = t + near * (1 - 2 * t) * (1 - t // 2)
    return order * (1 - 2 * flip) + 3 * flip


class Swap:
    reach, lazy = 0, False

    def __init__(self, blocks, vmem_result=False, pace=2):
        groups = blocks.shape[0]
        self.pace = groups if vmem_result else pace
        self.ins = [(blocks, pltpu.VMEM)]
        self.outs = [
            (
                jax.ShapeDtypeStruct(blocks.shape, blocks.dtype),
                pltpu.VMEM if vmem_result else pl.ANY,
            )
        ]
        self.scratch = [DMA, DMA((groups,)), DMA((groups,))]

    def bind(self, place, ins, outs, scratch):
        self.place, self.groups = place, place.groups
        self.source, self.result = ins[0], outs[0]
        self.own_sem, self.send_sem, self.recv_sem = scratch

    def copy(self, j, src, dst):
        return remote(
            self.source.at[src],
            self.result.at[dst],
            self.send_sem.at[j],
            self.recv_sem.at[j],
            {EXPERT: self.place.partner(j)},
        )

    def own(self):
        chip = self.place.chip
        return pltpu.make_async_copy(self.source.at[chip], self.result.at[chip], self.own_sem)

    def send(self, i):
        for q in range(min(self.pace, self.groups - 1)):
            j = 1 + i * self.pace + q

            @pl.when(j < self.groups)
            def _(j=j):
                self.copy(j, self.place.partner(j), self.place.chip).start()

    def begin(self):
        self.own().start()
        self.send(0)

    def rest(self, offset):
        count = -(-(self.groups - 1) // self.pace) - 1
        return [(offset, count, lambda i: self.send(i + 1))]

    def segments(self):
        return self.rest(0)

    def end(self):
        self.own().wait()

        @pl.loop(1, self.groups)
        def _(j):
            self.copy(j, self.place.chip, self.place.partner(self.groups - j)).wait_recv()
            self.copy(j, self.place.partner(j), self.place.chip).wait_send()


class MadeSwap(Swap):
    def __init__(self, operands, shape, make, delay, pace, scratch=()):
        self.pace, self.make, self.delay = pace, make, delay
        self.ins = [(a, pltpu.VMEM) for a in operands]
        self.outs = [(jax.ShapeDtypeStruct(shape, jnp.bfloat16), pl.ANY)]
        groups = shape[0]
        self.scratch = [DMA, DMA((groups,)), DMA((groups,)), pltpu.VMEM(shape, jnp.bfloat16)]
        self.scratch += list(scratch)

    def bind(self, place, ins, outs, scratch):
        super().bind(place, [scratch[3]], outs, scratch[:3])
        self.refs, self.extra = ins, scratch[4:]

    def begin(self):
        if self.delay is None:
            for call in self.make(self):
                call(0)
            super().begin()

    def segments(self):
        if self.delay is None:
            return self.rest(0)
        calls = self.make(self) + [lambda i: super(MadeSwap, self).begin()]
        parts = [(self.delay + k, 1, call) for k, call in enumerate(calls)]
        return parts + self.rest(self.delay + len(calls))


class Gather:
    lazy = False

    def __init__(self, arrays, planes, vmem_result=False):
        count, slots = len(arrays), planes * 4
        self.planes, self.count, self.reach = planes, count, planes
        self.ins = [(a, pltpu.VMEM) for a in arrays]
        space = pltpu.VMEM if vmem_result else pl.ANY
        self.outs = [(jax.ShapeDtypeStruct((slots,) + a.shape, a.dtype), space) for a in arrays]
        by_level, by_slot = DMA((count, planes)), DMA((count, slots))
        self.scratch = [DMA((count,))] + [by_level] * 5 + [by_slot] + [by_level] * 6 + [by_slot]

    def bind(self, place, ins, outs, scratch):
        self.place, self.sources, self.results = place, ins, outs
        self.level = lax.rem(place.chip // 4, self.planes)
        self.has_up, self.has_down = self.level < self.planes - 1, self.level > 0
        self.own_sem = scratch[0]
        self.in_z, self.in_x, self.in_y, self.in_a, self.in_b, self.in_p = scratch[1:7]
        self.out_up, self.out_down, self.out_x, self.out_y = scratch[7:11]
        self.out_a, self.out_b, self.out_p = scratch[11:14]
        self.landed = False

    def move(self, a, slot, part, send, recv, target, own=False, whose=None):
        half = self.sources[a].shape[0] // 2
        whose = self.place.core if whose is None else whose
        if part is None:
            rows = part_rows(whose * half, half)
        else:
            rows = part_rows(whose * half + part * (half // 2), half // 2)
        dst = self.results[a].at[slot, rows]
        return remote(self.sources[a].at[rows] if own else dst, dst, send, recv, target)

    def along_z(self, a, lev, own, up):
        sems = self.out_up if up else self.out_down
        target = self.place.above if up else self.place.below
        slot = lev * 4 + self.place.here
        return self.move(a, slot, None, sems.at[a, lev], self.in_z.at[a, lev], target, own)

    def along_x(self, a, lev, slot, own=False):
        return self.move(
            a, slot, None, self.out_x.at[a, lev], self.in_x.at[a, lev], self.place.by_x, own
        )

    def along_y(self, a, lev, slot, own=False):
        return self.move(
            a, slot, None, self.out_y.at[a, lev], self.in_y.at[a, lev], self.place.by_y, own
        )

    def corner_x(self, a, lev, slot):
        return self.move(
            a, slot, 0, self.out_a.at[a, lev], self.in_a.at[a, lev], self.place.by_x
        )

    def corner_y(self, a, lev, slot):
        return self.move(
            a, slot, 1, self.out_b.at[a, lev], self.in_b.at[a, lev], self.place.by_y
        )

    def share(self, a, slot, whose=None):
        return self.move(
            a, slot, None, self.out_p.at[a, slot], self.in_p.at[a, slot], self.place.mate, whose=whose
        )

    def own(self, a):
        slot = self.level * 4 + self.place.here
        return pltpu.make_async_copy(self.sources[a], self.results[a].at[slot], self.own_sem.at[a])

    def begin(self):
        for a in range(self.count):
            self.own(a).start()
        self.first(0, True)

    def relays(self, a, t, own, act):
        lev = level_at(self.level, self.planes, t)
        up, down = self.has_up, self.has_down
        if not own:
            up, down = up & (lev < self.level), down & (lev > self.level)
        pl.when(up)(lambda: act(self.along_z(a, lev, own, True)))
        pl.when(down)(lambda: act(self.along_z(a, lev, own, False)))

    def first(self, t, own=False):
        lev = level_at(self.level, self.planes, t)
        for a in range(self.count):
            slot = lev * 4 + self.place.here
            if not own:
                self.along_z(a, lev, own, True).wait_recv()
            self.relays(a, t, own, lambda copy: copy.start())
            self.along_x(a, lev, slot, own).start()
            self.along_y(a, lev, slot, own).start()
            if not own:
                self.share(a, slot).start()

    def second(self, t):
        lev = level_at(self.level, self.planes, t)
        for a in range(self.count):
            slot = lev * 4 + self.place.there_y
            self.along_y(a, lev, slot).wait_recv()
            self.corner_x(a, lev, slot).start()
            self.share(a, slot).start()
            slot = lev * 4 + self.place.there_x
            self.along_x(a, lev, slot).wait_recv()
            self.corner_y(a, lev, slot).start()
            self.share(a, slot).start()

    def third(self, t):
        lev = level_at(self.level, self.planes, t)
        for a in range(self.count):
            slot = lev * 4 + self.place.across
            self.corner_x(a, lev, slot).wait_recv()
            self.corner_y(a, lev, slot).wait_recv()
            self.share(a, slot).start()

    def advance(self, i):
        pl.when(i < self.planes)(lambda: self.first(i))
        pl.when(i < self.planes + 1)(lambda: self.second(i - 1))
        pl.when(i > 1)(lambda: self.third(i - 2))

    def segments(self):
        return [(0, self.planes + 1, lambda i: self.advance(i + 1))]

    def sent(self, t, own):
        place, lev = self.place, level_at(self.level, self.planes, t)
        for a in range(self.count):
            slot = lev * 4 + place.here
            self.relays(a, t, own, lambda copy: copy.wait_send())
            self.along_x(a, lev, slot, own).wait_send()
            self.along_y(a, lev, slot, own).wait_send()
            self.corner_x(a, lev, lev * 4 + place.there_y).wait_send()
            self.corner_y(a, lev, lev * 4 + place.there_x).wait_send()
            for other in [place.there_y, place.there_x, place.across]:
                self.share(a, lev * 4 + other).wait_send()
            if not own:
                self.share(a, slot).wait_send()

    def end(self):
        if not self.landed:
            self.receive_all()
        self.sent(0, True)
        pl.loop(1, self.planes)(lambda t: self.sent(t, False))

    def ready(self, slot, other):
        for a in range(self.count):
            if other:
                self.share(a, slot, 1 - self.place.core).wait_recv()
            else:
                self.own(a).wait()

    def receive(self, t):
        place, lev = self.place, level_at(self.level, self.planes, t)
        pl.when(t == 0)(lambda: self.ready(lev * 4 + place.here, False))
        pl.when(t > 0)(lambda: self.ready(lev * 4 + place.here, True))
        for spot in (place.there_y, place.there_x, place.across):
            self.ready(lev * 4 + spot, True)

    def receive_all(self):
        self.landed = True
        pl.loop(0, self.planes)(self.receive)


class NormGather(Gather):
    def __init__(self, rows, gains, gain_row, planes):
        super().__init__([jax.ShapeDtypeStruct(rows.shape, jnp.bfloat16)], planes)
        self.ins = [(rows, pltpu.VMEM)]
        self.scratch = self.scratch + [pltpu.VMEM(rows.shape, jnp.bfloat16)]
        self.gains, self.gain_row = gains, gain_row

    def bind(self, place, ins, outs, scratch):
        super().bind(place, [scratch[-1]], outs, scratch[:-1])
        self.rows = ins[0]

    def begin(self):
        self.gains.end()
        rows = self.rows[...]
        stat = lax.rsqrt(jnp.mean(rows * rows, axis=-1, keepdims=True) + norm_eps)
        cols = rows.shape[1] // self.place.groups
        for j in range(self.place.groups):
            at = slice(j * cols, (j + 1) * cols)
            gain = self.gains.result[j, self.gain_row : self.gain_row + 1, :].astype(jnp.float32)
            self.sources[0][:, at] = (rows[:, at] * stat * gain).astype(jnp.bfloat16)
        super().begin()


class Reduce:
    def __init__(
        self, operands, produce, slots, block, width, scratch=(), prepare=None, extra=(), prelude=None, delay=0, maker=None
    ):
        planes, rows, kind = slots // 4, block // 2, jnp.bfloat16
        self.planes, self.reach = planes, planes
        self.ins = [(a, pltpu.VMEM) for a in operands]
        self.outs = [(jax.ShapeDtypeStruct((block, width), jnp.float32), pltpu.VMEM)]
        self.outs += [(shape, pltpu.VMEM) for shape in extra]
        self.own_scratch, self.produce, self.prepare = len(scratch), produce, prepare
        self.prelude, self.delay, self.maker = prelude, delay, maker
        self.lazy = prelude is not None
        by_level = DMA((planes,))
        self.scratch = (
            list(scratch)
            + [pltpu.VMEM((slots, block, width) if produce else (8, LANES), kind)]
            + [pltpu.VMEM((slots, rows, width), kind)]
            + [pltpu.VMEM((planes, rows // 2, width), kind)] * 2
            + [pltpu.VMEM((planes, rows, width), kind)] * 4
            + [DMA((slots,))]
            + [by_level] * 6
            + [DMA, DMA((slots,))]
            + [by_level] * 5
            + [DMA]
        )

    def bind(self, place, ins, outs, scratch):
        self.place, self.out = place, outs[0]
        self.refs = list(ins) + list(outs[1:]) + list(scratch[: self.own_scratch])
        scratch = scratch[self.own_scratch :]
        self.part = scratch[0] if self.produce else self.maker.part
        self.mine = scratch[1]
        self.from_a, self.from_b, self.from_x, self.from_y = scratch[2:6]
        self.from_up, self.from_down = scratch[6:8]
        self.in_p, self.in_a, self.in_b, self.in_x, self.in_y = scratch[8:13]
        self.in_up, self.in_down, self.in_m, self.out_p = scratch[13:17]
        self.out_a, self.out_b, self.out_x, self.out_y, self.out_z, self.out_m = scratch[17:]
        self.level = lax.rem(place.chip // 4, self.planes)
        self.has_up, self.has_down = self.level < self.planes - 1, self.level > 0
        self.rows = self.part.shape[1] // 2
        self.half = self.rows // 2

    def swap(self, slot):
        theirs = part_rows((1 - self.place.core) * self.rows, self.rows)
        return remote(
            self.part.at[slot, theirs],
            self.mine.at[slot],
            self.out_p.at[slot],
            self.in_p.at[slot],
            self.place.mate,
        )

    def add_into(self, dst, terms, first, size):
        step = 16

        @pl.loop(0, size // step)
        def _(i):
            at = first + i * step
            total = None
            for term, shift in terms:
                block = term[part_rows(at + shift, step), :].astype(jnp.float32)
                total = block if total is None else total + block
            dst[part_rows(at, step), :] = total.astype(dst.dtype)

    def send_a(self, lev):
        src = self.mine.at[lev * 4 + self.place.across, pl.ds(0, self.half)]
        return remote(
            src, self.from_a.at[lev], self.out_a.at[lev], self.in_a.at[lev], self.place.by_x
        )

    def send_b(self, lev):
        src = self.mine.at[lev * 4 + self.place.across, pl.ds(self.half, self.half)]
        return remote(
            src, self.from_b.at[lev], self.out_b.at[lev], self.in_b.at[lev], self.place.by_y
        )

    def send_y(self, lev):
        src = self.mine.at[lev * 4 + self.place.there_y]
        return remote(
            src, self.from_y.at[lev], self.out_y.at[lev], self.in_y.at[lev], self.place.by_y
        )

    def send_x(self, lev):
        src = self.mine.at[lev * 4 + self.place.there_x]
        return remote(
            src, self.from_x.at[lev], self.out_x.at[lev], self.in_x.at[lev], self.place.by_x
        )

    def send_up(self, lev):
        src = self.mine.at[lev * 4 + self.place.here]
        return remote(
            src, self.from_down.at[lev], self.out_z.at[lev], self.in_down.at[lev], self.place.above
        )

    def send_down(self, lev):
        src = self.mine.at[lev * 4 + self.place.here]
        return remote(
            src, self.from_up.at[lev], self.out_z.at[lev], self.in_up.at[lev], self.place.below
        )

    def plane(self, i):
        return level_at(self.level, self.planes, self.planes - 1 - i)

    def make(self, i):
        @pl.loop(0, 4)
        def _(q):
            slot = self.plane(i) * 4 + self.place.spot(q)
            if self.produce is not None:
                self.produce(self.part, slot, self.refs)
            self.swap(slot).start()

    def join(self, slot):
        self.swap(slot).wait_recv()
        mine = self.mine.at[slot]
        terms = [(mine, 0), (self.part.at[slot], self.place.core * self.rows)]
        self.add_into(mine, terms, 0, self.rows)

    def first(self, i):
        lev = self.plane(i)
        self.join(lev * 4 + self.place.across)
        self.send_a(lev).start()
        self.send_b(lev).start()
        self.join(lev * 4 + self.place.there_y)
        self.join(lev * 4 + self.place.there_x)

    def second(self, i):
        lev = self.plane(i)
        mine = self.mine.at[lev * 4 + self.place.there_y]
        self.send_a(lev).wait_recv()
        self.add_into(mine, [(mine, 0), (self.from_a.at[lev], 0)], 0, self.half)
        self.send_y(lev).start()
        mine = self.mine.at[lev * 4 + self.place.there_x]
        self.send_b(lev).wait_recv()
        self.add_into(mine, [(mine, 0), (self.from_b.at[lev], -self.half)], self.half, self.half)
        self.send_x(lev).start()
        self.join(lev * 4 + self.place.here)

    def third(self, i):
        rows, out, lev = self.rows, self.out, self.plane(i)
        mine = self.mine.at[lev * 4 + self.place.here]
        self.send_y(lev).wait_recv()
        self.send_x(lev).wait_recv()
        terms = [(mine, 0), (self.from_y.at[lev], 0), (self.from_x.at[lev], 0)]

        def more(total, cond, send, arrived):
            @pl.when(cond)
            def _():
                send(lev).wait_recv()
                self.add_into(total, [(total, 0), (arrived.at[lev], 0)], 0, rows)

        @pl.when(lev == self.level)
        def _():
            total = out.at[part_rows(self.place.core * rows, rows)]
            self.add_into(total, terms, 0, rows)
            more(total, self.has_up, self.send_down, self.from_up)
            more(total, self.has_down, self.send_up, self.from_down)

        @pl.when(lev < self.level)
        def _():
            self.add_into(mine, terms, 0, rows)
            more(mine, self.has_up, self.send_down, self.from_up)
            self.send_down(lev).start()

        @pl.when(lev > self.level)
        def _():
            self.add_into(mine, terms, 0, rows)
            more(mine, self.has_down, self.send_up, self.from_down)
            self.send_up(lev).start()

    def begin(self):
        if self.prepare is not None:
            self.prepare(self.refs)
        if self.prelude is None and self.maker is None:
            self.make(0)

    def advance(self, i):
        pl.when(i + 1 < self.planes)(lambda: self.make(i + 1))
        pl.when(i < self.planes)(lambda: self.first(i))
        pl.when((i > 0) & (i < self.planes + 1))(lambda: self.second(i - 1))
        pl.when(i > 1)(lambda: self.third(i - 2))

    def segments(self):
        parts, start = [], 0
        if self.prelude is not None:
            count, call = self.prelude(self.refs)
            parts = [(self.delay, count, call), (self.delay + count, 1, self.make)]
            start = self.delay + count + 1
        if self.maker is not None:
            parts, start = [(self.delay, 1, self.make)], self.delay + 1
        return parts + [(start, self.planes + 2, self.advance)]

    def hand(self, whose):
        spot = part_rows(whose * self.rows, self.rows)
        return remote(self.out.at[spot], self.out.at[spot], self.out_m, self.in_m, self.place.mate)

    def end(self):
        self.hand(self.place.core).start()


        @pl.loop(0, self.planes)
        def _(lev):
            for spot in range(4):
                self.swap(lev * 4 + spot).wait_send()
            for send in (self.send_a, self.send_b, self.send_y, self.send_x):
                send(lev).wait_send()
            pl.when(lev < self.level)(lambda: self.send_down(lev).wait_send())
            pl.when(lev > self.level)(lambda: self.send_up(lev).wait_send())

        self.hand(self.place.core).wait_send()
        self.hand(1 - self.place.core).wait_recv()


class Experts:
    lazy = False

    def __init__(self, gather, weights, shared_w, capacity):
        slots, seq, width = gather.outs[0][0].shape
        hidden, room, bf16 = weights[0].shape[0], shared_w.shape[1], jnp.bfloat16
        self.gather, self.capacity, self.room, self.reach = gather, capacity, room, gather.reach
        self.slots, self.seq, self.width, self.hidden = slots, seq, width, hidden
        rows = (slots, capacity)
        turn = (room, slots * seq)

        def shape(dims, kind=bf16):
            return jax.ShapeDtypeStruct(dims, kind)

        self.ins = [(a, pl.ANY) for a in weights] + [(shared_w, pltpu.VMEM)]
        self.outs = [
            (shape(rows + (width,)), pl.ANY),
            (shape(rows + (seq,)), pltpu.VMEM),
            (shape(turn), pltpu.VMEM),
            (shape((3, room, width)), pltpu.VMEM),
            (shape(rows + (width,)), pl.ANY),
            (shape(rows + (width,)), pl.ANY),
        ] + [(shape(rows + (hidden,)), pl.ANY)] * 3
        staged = [self.outs[k][0] for k in (0, 6, 7, 8)]
        self.scratch = [pltpu.VMEM((slots, seq, width + LANES), bf16)]
        self.scratch += [pltpu.VMEM(x.shape, bf16) for x in staged]
        self.scratch += [DMA((len(staged), gather.planes))]
        self.scratch += (
            [pltpu.VMEM((4, seq, width), bf16)] * 2
            + [pltpu.VMEM((4, seq, LANES), jnp.float32), DMA((3,))]
            + [pltpu.VMEM(w.shape, bf16) for w in weights]
            + [pltpu.VMEM((4 * capacity, width), bf16)] * 3
            + [
                pltpu.VMEM((4 * capacity, LANES), jnp.float32),
                pltpu.VMEM((4 * capacity + 2 * room, width), bf16),
                pltpu.VMEM((4 * capacity + 2 * room, 4 * seq), bf16),
                pltpu.VMEM((3, room, width), jnp.float32),
                DMA((3,)),
                DMA((2,)),
            ]
        )

    def bind(self, place, ins, outs, scratch):
        self.place = place
        self.hbm_weights, self.shared_w = ins[:3], ins[3]
        self.picks, self.act_turn, self.shared_grads, self.rows_hbm, self.cot_hbm = outs[1:6]
        self.part, self.staged, self.leave_sem = scratch[0], scratch[1:5], scratch[5]
        scratch = scratch[6:]
        self.out_block, self.act, self.gate_delta, self.up_delta = self.staged
        self.final = [outs[0]] + list(outs[6:])
        self.tokens, self.out_rows, self.marked, self.plane_sem = scratch[:4]
        scratch = scratch[4:]
        self.gate, self.up, self.down = scratch[:3]
        self.rows, self.cot, self.grads = scratch[3:6]
        self.weight, self.held, self.left, self.total, self.load_sem, self.save_sem = scratch[6:]
        self.level = lax.rem(place.chip // 4, self.gather.planes)

    def loads(self):
        pairs = zip(self.hbm_weights, [self.gate, self.up, self.down])
        return [
            pltpu.make_async_copy(src, dst, self.load_sem.at[k]) for k, (src, dst) in enumerate(pairs)
        ]

    def saves(self, lev):
        at = pl.ds(lev * 4 * self.capacity, 4 * self.capacity)
        pairs = [(self.rows, self.rows_hbm), (self.cot, self.cot_hbm)]
        return [
            pltpu.make_async_copy(
                src.reshape(4, self.capacity, self.width), dst.at[pl.ds(lev * 4, 4)], self.save_sem.at[k]
            )
            for k, (src, dst) in enumerate(pairs)
        ]

    def begin(self):
        for load in self.loads():
            load.start()
        self.total[...] = jnp.zeros_like(self.total)
        self.held[4 * self.capacity :] = self.shared_w[:2].reshape(2 * self.room, self.width)
        self.left[: 4 * self.capacity] = jnp.zeros((4 * self.capacity, 4 * self.seq), jnp.bfloat16)

    def choose(self, lev, t):
        seq, cap = self.seq, self.capacity
        below = lax.broadcasted_iota(jnp.int32, (seq, seq), 0)
        upto = (below <= lax.broadcasted_iota(jnp.int32, (seq, seq), 1)).astype(jnp.bfloat16)
        place_in = lax.broadcasted_iota(jnp.int32, (cap, seq), 0).astype(jnp.float32)

        @pl.when(t > 0)
        def _():
            for save in self.saves(lev):
                save.wait()

        for j in range(4):
            slot, at = lev * 4 + j, slice(j * cap, (j + 1) * cap)
            turned = self.marked[j].T
            here = jnp.sum(jnp.where(below == self.place.chip, turned, 0.0), axis=0, keepdims=True)
            routed = jnp.where(here >= 0.0, 1.0, 0.0)
            order = fdot(jnp.broadcast_to(routed, (8, seq)).astype(jnp.bfloat16), upto)[:1] - 1.0
            hit = jnp.where(order == place_in, routed, 0.0)
            weight = jnp.sum(hit * here, axis=-1, keepdims=True)
            pick = hit.astype(jnp.bfloat16)
            self.picks[slot] = pick
            self.left[at, j * seq : (j + 1) * seq] = pick
            self.weight[at] = jnp.broadcast_to(weight, (cap, LANES))
        chosen, weight = self.left[: 4 * cap], self.weight[:, :1]

        @pl.loop(0, self.width // 512, unroll=True)
        def _(k):
            cols = part_rows(k * 512, 512)
            own = fdot(chosen, self.tokens[:, :, cols].reshape(4 * seq, 512))
            self.rows[:, cols] = own.astype(jnp.bfloat16)
            grad = fdot(chosen, self.out_rows[:, :, cols].reshape(4 * seq, 512))
            self.grads[:, cols] = grad.astype(jnp.bfloat16)
            self.cot[:, cols] = (weight * grad).astype(jnp.bfloat16)

        for save in self.saves(lev):
            save.start()

    def hidden_units(self, lev):
        slots, chunk = pl.ds(lev * 4, 4), 256
        for start in range(0, self.hidden, chunk):
            cols = slice(start, min(start + chunk, self.hidden))
            shape = (4, self.capacity, cols.stop - cols.start)
            gate = dot_nt(self.rows[...], self.gate[cols])
            up = dot_nt(self.rows[...], self.up[cols])
            grad = dot_nt(self.cot[...], self.down[cols])
            sig = jax.nn.sigmoid(gate)
            gated = gate * sig
            self.act[slots, :, cols] = (gated * up).astype(jnp.bfloat16).reshape(shape)
            slope = sig * (1.0 + gate * (1.0 - sig))
            self.gate_delta[slots, :, cols] = (grad * up * slope).astype(jnp.bfloat16).reshape(shape)
            self.up_delta[slots, :, cols] = (grad * gated).astype(jnp.bfloat16).reshape(shape)

    def shared_units(self, lev):
        seq4, room = 4 * self.seq, self.room
        tokens = self.tokens[...].reshape(seq4, self.width)
        grads = self.out_rows[...].reshape(seq4, self.width)
        both = dot_nt(self.shared_w[:2].reshape(2 * room, self.width), tokens)
        gate, up = both[:room], both[room:]
        grad = dot_nt(self.shared_w[2], grads)
        sig = jax.nn.sigmoid(gate)
        act = (gate * sig * up).astype(jnp.bfloat16)
        gate_delta = (grad * up * (sig * (1.0 + gate * (1.0 - sig)))).astype(jnp.bfloat16)
        up_delta = (grad * gate * sig).astype(jnp.bfloat16)
        self.act_turn[:, part_rows(lev * seq4, seq4)] = act
        self.left[4 * self.capacity : 4 * self.capacity + room] = gate_delta
        self.left[4 * self.capacity + room :] = up_delta

        @pl.loop(0, self.width // 512, unroll=True)
        def _(k):
            cols = part_rows(k * 512, 512)
            some = self.tokens[:, :, cols].reshape(seq4, 512)
            self.total[0, :, cols] += fdot(gate_delta, some)
            self.total[1, :, cols] += fdot(up_delta, some)
            some = self.out_rows[:, :, cols].reshape(seq4, 512)
            self.total[2, :, cols] += fdot(act, some)

    def outward(self, lev):
        slots, cap, count = pl.ds(lev * 4, 4), self.capacity, 4 * self.capacity
        act = self.act[slots].reshape(count, self.hidden)
        gate_delta = self.gate_delta[slots].reshape(count, self.hidden)
        up_delta = self.up_delta[slots].reshape(count, self.hidden)
        weight = self.weight[:, :1]

        def some(k, route):
            cols = part_rows(k * 512, 512)
            out = fdot(act, self.down[:, cols]).astype(jnp.bfloat16).astype(jnp.float32)
            route += jnp.sum(out * self.grads[:, cols].astype(jnp.float32), axis=-1, keepdims=True)
            out = (weight * out).astype(jnp.bfloat16)
            self.out_block[slots, :, cols] = out.reshape(4, cap, 512)
            back = fdot(gate_delta, self.gate[:, cols]) + fdot(up_delta, self.up[:, cols])
            self.held[:count, cols] = back.astype(jnp.bfloat16)
            return route

        route = lax.fori_loop(
            0, self.width // 512, some, jnp.zeros((count, 1), jnp.float32), unroll=True
        )
        lane = lax.broadcasted_iota(jnp.int32, (count, LANES), 1)
        routes = jnp.where(lane == self.place.chip, route, 0.0).astype(jnp.bfloat16)
        shape = (4, self.seq, LANES)
        turned = dot_tn(self.left[:count], routes).astype(jnp.bfloat16)
        self.part[slots, :, self.width :] = turned.reshape(shape)
        left = self.left[...]

        @pl.loop(0, self.width // 512, unroll=True)
        def _(k):
            cols = part_rows(k * 512, 512)
            sums = dot_tn(left, self.held[:, cols]).astype(jnp.bfloat16)
            self.part[slots, :, cols] = sums.reshape(4, self.seq, 512)

        for copy in self.leaving(lev):
            copy.start()

    def leaving(self, lev):
        four = pl.ds(lev * 4, 4)
        return [
            pltpu.make_async_copy(src.at[four], dst.at[four], self.leave_sem.at[k, lev])
            for k, (src, dst) in enumerate(zip(self.staged, self.final))
        ]

    def compute(self, t):
        lev = level_at(self.level, self.gather.planes, t)

        @pl.when(t == 0)
        def _():
            for load in self.loads():
                load.wait()

        self.gather.receive(t)
        held = [self.tokens, self.out_rows, self.marked]
        copies = [
            pltpu.make_async_copy(src.at[pl.ds(lev * 4, 4)], dst, self.plane_sem.at[k])
            for k, (src, dst) in enumerate(zip(self.gather.results, held))
        ]
        for copy in copies:
            copy.start()
        for copy in copies:
            copy.wait()
        self.choose(lev, t)
        self.hidden_units(lev)
        self.shared_units(lev)

    def advance(self, i):
        planes = self.gather.planes
        pl.when(i > 1)(lambda: self.outward(level_at(self.level, planes, i - 2)))
        pl.when((i > 0) & (i < planes + 1))(lambda: self.compute(i - 1))

    def segments(self):
        self.gather.landed = True
        return [(0, self.gather.planes + 2, self.advance)]

    def end(self):
        for save in self.saves(level_at(self.level, self.gather.planes, self.gather.planes - 1)):
            save.wait()
        self.shared_grads[...] = self.total[...].astype(jnp.bfloat16)

        @pl.loop(0, self.gather.planes)
        def _(lev):
            for copy in self.leaving(lev):
                copy.wait()


def greet(place, ops):
    barrier = pltpu.get_barrier_semaphore()
    expected = 1

    def call(target):
        pl.semaphore_signal(barrier, inc=1, device_id=target, device_id_type=MESH)

    call(place.mate)
    if any(op.reach == 0 for op in ops):
        for j in range(1, place.groups):
            call({EXPERT: place.partner(j)})
        expected += place.groups - 1
    else:
        call(place.by_x)
        call(place.by_y)
        planes = max(op.reach for op in ops)
        level = lax.rem(place.chip // 4, planes)
        has_up, has_down = level < planes - 1, level > 0
        pl.when(has_up)(lambda: call(place.above))
        pl.when(has_down)(lambda: call(place.below))
        expected += 2 + has_up.astype(jnp.int32) + has_down.astype(jnp.int32)
    pl.semaphore_wait(barrier, expected)


def is_large(pair):
    array, space = pair
    return space == pltpu.VMEM and array.size * array.dtype.itemsize >= 1 << 17


def chip_kernel(ops, *refs):
    place = Place()
    pairs = [pair for op in ops for pair in op.ins]
    n_in, large = len(pairs), [k for k, pair in enumerate(pairs) if is_large(pair)]
    n_out = sum(len(op.outs) for op in ops)
    ins, outs, scratch = list(refs[:n_in]), refs[n_in : n_in + n_out], refs[n_in + n_out :]
    loads = {}
    for n, k in enumerate(large):
        loads[k] = pltpu.make_async_copy(ins[k], scratch[n], scratch[len(large)].at[n])
        loads[k].start()
        ins[k] = scratch[n]
    scratch = scratch[len(large) + 1 :]
    first = 0
    for op in ops:
        op.fetches = [loads[k] for k in range(first, first + len(op.ins)) if k in loads]
        first += len(op.ins)
        op.bind(place, ins[: len(op.ins)], outs[: len(op.outs)], scratch[: len(op.scratch)])
        ins, outs = ins[len(op.ins) :], outs[len(op.outs) :]
        scratch = scratch[len(op.scratch) :]
    greet(place, ops)


    def load(op):
        for copy in op.fetches:
            copy.wait()

    parts = []
    for op in ops:
        segments = [part for part in op.segments() if part[1] > 0]
        if op.lazy:
            parts.append((min(start for start, _, _ in segments), 1, lambda _, op=op: load(op)))
        else:
            load(op)
        op.begin()
        parts += segments
    if parts:

        @pl.loop(0, max(start + count for start, count, _ in parts))
        def _(r):
            for start, count, call in parts:
                inside = (r >= start) & (r < start + count)
                pl.when(inside)(functools.partial(call, r - start))

    ended = [op.gains for op in ops if isinstance(op, NormGather)]
    for op in ops:
        if op not in ended:
            op.end()


def exchange(ops, ident):
    ins = [pair for op in ops for pair in op.ins]
    outs = [pair for op in ops for pair in op.outs]
    moved = sum(a.size * a.dtype.itemsize for a, _ in ins + outs)
    large = [pair[0] for pair in ins if is_large(pair)]
    spaces = [pl.ANY if is_large(pair) else pair[1] for pair in ins]
    held = [pltpu.VMEM(a.shape, a.dtype) for a in large] + [DMA((max(1, len(large)),))]
    results = pl.pallas_call(
        functools.partial(chip_kernel, ops),
        out_shape=[shape for shape, _ in outs],
        in_specs=[pl.BlockSpec(memory_space=space) for space in spaces],
        out_specs=[pl.BlockSpec(memory_space=space) for _, space in outs],
        scratch_shapes=held + [entry for op in ops for entry in op.scratch],
        compiler_params=pltpu.CompilerParams(
            collective_id=ident, has_side_effects=True, vmem_limit_bytes=60 << 20
        ),
        cost_estimate=pl.CostEstimate(flops=0, bytes_accessed=moved, transcendentals=0),
    )(*[a for a, _ in ins])
    split = []
    for op in ops:
        split.append(results[: len(op.outs)])
        results = results[len(op.outs) :]
    return split


def grads_kernel(act, gate_delta, up_delta, rows, cot, gate_out, up_out, down_out):
    gate_out[...] = dot_tn(gate_delta[...], rows[...])
    up_out[...] = dot_tn(up_delta[...], rows[...])
    down_out[...] = dot_tn(act[...], cot[...])


def expert_weight_grads(act, gate_delta, up_delta, rows, cot):
    count, hidden = act.shape
    width, tile = rows.shape[1], 256
    left = pl.BlockSpec((count, hidden), lambda i: (0, 0), pipeline_mode=pl.Buffered(1))
    right = pl.BlockSpec((count, tile), lambda i: (0, i))
    return pl.pallas_call(
        grads_kernel,
        grid=(width // tile,),
        out_shape=[jax.ShapeDtypeStruct((hidden, width), jnp.float32)] * 3,
        in_specs=[left] * 3 + [right] * 2,
        out_specs=[pl.BlockSpec((hidden, tile), lambda i: (0, i))] * 3,
        compiler_params=pltpu.CompilerParams(vmem_limit_bytes=48 << 20),
        cost_estimate=pl.CostEstimate(
            flops=6 * count * hidden * width,
            bytes_accessed=12 * hidden * width + 4 * count * width,
            transcendentals=0,
        ),
    )(act, gate_delta, up_delta, rows, cot)


def finish_kernel(sizes, heads_in, shared_in, share_in, small_in, state, added, *refs):
    heads, at_kv, at_o, lat_rows, hidden, share = sizes
    layer_out, q_out, kvb_out, o_out, gate_out, up_out, down_out, kva_out, small_out = refs[:9]
    q_turn, gate_turn, up_turn = refs[9:]
    groups, own_cols = heads_in.shape[0], heads_in.shape[2]
    copies = range(0, groups, heads)

    def over_copies(ref, k):
        return sum(ref[first + k].astype(jnp.float32) for first in copies)

    layer_out[...] = state[...] + added[...]
    small_out[...] = sum(small_in[j] for j in range(groups))
    for k in range(heads):
        block = over_copies(heads_in, k)
        q_turn[k * at_kv : (k + 1) * at_kv] = block[:at_kv]
        halves = (at_o - at_kv) // lat_rows
        for half in range(halves):
            start, col = at_kv + half * lat_rows, (k * halves + half) * own_cols
            kvb_out[:, col : col + own_cols] = block[start : start + lat_rows]
        wide = block.shape[0] - at_o
        o_out[k * wide : (k + 1) * wide] = block[at_o:]
        kva_out[k * share : (k + 1) * share] = over_copies(share_in, k)
    for j in range(groups):
        block, at = shared_in[j].astype(jnp.float32), slice(j * hidden, (j + 1) * hidden)
        gate_turn[at] = block[:hidden]
        up_turn[at] = block[hidden : 2 * hidden]
        down_out[at] = block[2 * hidden :]
    q_out[...] = q_turn[...].T
    gate_out[...] = gate_turn[...].T
    up_out[...] = up_turn[...].T


def finish(sizes, heads_in, shared_in, share_in, small_in, state, added):
    heads, at_kv, at_o, lat_rows, hidden, share = sizes
    groups, rows, own_cols = heads_in.shape
    many = groups * hidden

    def shape(*dims):
        return jax.ShapeDtypeStruct(dims, jnp.float32)

    outs = [
        shape(*state.shape),
        shape(own_cols, heads * at_kv),
        shape(lat_rows, heads * (at_o - at_kv) // lat_rows * own_cols),
        shape(heads * (rows - at_o), own_cols),
        shape(own_cols, many),
        shape(own_cols, many),
        shape(many, own_cols),
        shape(heads * share, own_cols),
        shape(*small_in.shape[1:]),
    ]
    turned = [(heads * at_kv, own_cols), (many, own_cols), (many, own_cols)]
    return pl.pallas_call(
        functools.partial(finish_kernel, sizes),
        out_shape=outs,
        in_specs=[pl.BlockSpec(memory_space=pltpu.VMEM)] * 6,
        out_specs=[pl.BlockSpec(memory_space=pltpu.VMEM)] * len(outs),
        scratch_shapes=[pltpu.VMEM(dims, jnp.float32) for dims in turned],
        compiler_params=pltpu.CompilerParams(vmem_limit_bytes=32 << 20),
    )(heads_in, shared_in, share_in, small_in, state, added)


def general_scores(query_blk, key_rows, first_row):
    scores = jnp.einsum(
        "qhd,khd->hqk", query_blk, key_rows, preferred_element_type=jnp.float32
    ) * DQK ** (-0.5)
    row_pos = first_row + jnp.arange(query_blk.shape[0], dtype=jnp.int32)
    col_pos = jnp.arange(key_rows.shape[0], dtype=jnp.int32)
    return jnp.where(col_pos[None, None, :] <= row_pos[None, :, None], scores, -1e30)


def attend(query_rows, key_rows, value_rows):
    seq_len = query_rows.shape[0]
    blk_rows = min(seq_len, 512)

    def one_block(block_index):
        first_row = block_index * blk_rows
        scores = general_scores(query_rows, key_rows, first_row)
        row_max = jnp.max(scores, axis=-1, keepdims=True)
        log_total = row_max + jnp.log(jnp.sum(jnp.exp(scores - row_max), axis=-1, keepdims=True))
        att_weights = jnp.exp(scores - log_total).astype(jnp.bfloat16)
        mixed_blk = jnp.einsum(
            "hqk,khd->qhd", att_weights, value_rows, preferred_element_type=jnp.float32
        ).astype(jnp.bfloat16)
        return (mixed_blk, log_total)

    mixed_heads, log_totals = lax.map(one_block, jnp.arange(seq_len // blk_rows, dtype=jnp.int32))
    return (mixed_heads.reshape(seq_len, query_rows.shape[1], value_rows.shape[2]), log_totals)


def attend_back(query_rows, key_rows, value_rows, log_totals, mixed_grad):
    seq_len, head_count = (query_rows.shape[0], query_rows.shape[1])
    blk_rows = min(seq_len, 512)

    def one_block(running, block_index):
        key_acc, value_acc = running
        first_row = block_index * blk_rows
        scores = general_scores(query_rows, key_rows, first_row)
        att_probs = jnp.exp(scores - log_totals[block_index])
        att_weights = att_probs.astype(jnp.bfloat16)
        value_acc = value_acc + jnp.einsum(
            "hqk,qhd->khd", att_weights, mixed_grad, preferred_element_type=jnp.float32
        )
        prob_grad = jnp.einsum(
            "qhd,khd->hqk", mixed_grad, value_rows, preferred_element_type=jnp.float32
        )
        row_delta = jnp.sum(att_probs * prob_grad, axis=-1, keepdims=True)
        score_delta = (att_probs * (prob_grad - row_delta) * DQK ** (-0.5)).astype(jnp.bfloat16)
        query_grad = jnp.einsum(
            "hqk,khd->qhd", score_delta, key_rows, preferred_element_type=jnp.float32
        )
        key_acc = key_acc + jnp.einsum(
            "hqk,qhd->khd", score_delta, query_rows, preferred_element_type=jnp.float32
        )
        return ((key_acc, value_acc), query_grad)

    zero_start = (
        jnp.zeros((seq_len, head_count, DQK), jnp.float32),
        jnp.zeros((seq_len, head_count, DV), jnp.float32),
    )
    (key_grad, value_grad), query_grad = lax.scan(
        one_block, zero_start, jnp.arange(seq_len // blk_rows, dtype=jnp.int32)
    )
    return (query_grad.reshape(seq_len, head_count, DQK), key_grad, value_grad)


def attention_forward(seq_in, gain_one, query_w, latent_w, gain_kv, kvup_w):
    seq_len = seq_in.shape[0]
    head_count = query_w.shape[1] // DQK
    cosine, sine_part = rope_tables(seq_len, DR)
    stat_one = rms_scale(seq_in)
    unit_one = seq_in * stat_one
    normed1 = (unit_one * gain_one.astype(jnp.float32)).astype(jnp.bfloat16)
    query_full = jnp.dot(normed1, query_w, preferred_element_type=jnp.float32).reshape(
        seq_len, head_count, DQK
    )
    query_rows = jnp.concatenate(
        [
            query_full[..., :DN],
            rotate(query_full[..., DN:], cosine[:, None, :], sine_part[:, None, :]),
        ],
        axis=-1,
    ).astype(jnp.bfloat16)
    latent_full = jnp.dot(normed1, latent_w, preferred_element_type=jnp.float32)
    latent_stat = rms_scale(latent_full[:, : kvup_w.shape[0]])
    latent_unit = latent_full[:, : kvup_w.shape[0]] * latent_stat
    latent = (latent_unit * gain_kv.astype(jnp.float32)).astype(jnp.bfloat16)
    rot_key = rotate(latent_full[:, kvup_w.shape[0] :], cosine, sine_part).astype(jnp.bfloat16)
    key_value = (
        jnp.dot(latent, kvup_w, preferred_element_type=jnp.float32)
        .astype(jnp.bfloat16)
        .reshape(seq_len, head_count, DN + DV)
    )
    key_rows = jnp.concatenate(
        [key_value[..., :DN], jnp.broadcast_to(rot_key[:, None, :], (seq_len, head_count, DR))],
        axis=-1,
    )
    value_rows = key_value[..., DN:]
    mixed_heads, log_totals = attend(query_rows, key_rows, value_rows)
    return (
        stat_one,
        unit_one,
        normed1,
        query_rows,
        latent_stat,
        latent_unit,
        latent,
        key_rows,
        value_rows,
        mixed_heads,
        log_totals,
        cosine,
        sine_part,
    )


def general(
    layer_in,
    norm1_gain,
    q_weight,
    kva_weight,
    kv_gain,
    kvb_weight,
    o_weight,
    norm2_gain,
    router_weight,
    shared_gate,
    shared_up,
    shared_down,
    expert_gate,
    expert_up,
    expert_down,
    routes,
    out_grad,
):
    groups = lax.axis_size(EXPERT)
    seq_len, width = layer_in.shape
    local_experts = expert_gate.shape[0]
    expert_count = local_experts * groups
    capacity = seq_len * TOPK * 4 // (3 * expert_count)
    rows_total = expert_count * capacity
    (
        gain_one,
        query_w,
        latent_w,
        gain_kv,
        kvup_w,
        output_w,
        gain_two,
        route_w,
        gate_sh,
        up_sh,
        down_sh,
    ) = (
        lax.all_gather(norm1_gain, EXPERT, axis=0, tiled=True),
        lax.all_gather(q_weight, EXPERT, axis=0, tiled=True),
        lax.all_gather(kva_weight, EXPERT, axis=0, tiled=True),
        lax.all_gather(kv_gain, EXPERT, axis=0, tiled=True),
        lax.all_gather(kvb_weight, EXPERT, axis=0, tiled=True),
        lax.all_gather(o_weight, EXPERT, axis=1, tiled=True),
        lax.all_gather(norm2_gain, EXPERT, axis=0, tiled=True),
        lax.all_gather(router_weight, EXPERT, axis=0, tiled=True),
        lax.all_gather(shared_gate, EXPERT, axis=0, tiled=True),
        lax.all_gather(shared_up, EXPERT, axis=0, tiled=True),
        lax.all_gather(shared_down, EXPERT, axis=1, tiled=True),
    )
    (
        stat_one,
        unit_one,
        normed1,
        query_rows,
        latent_stat,
        latent_unit,
        latent,
        key_rows,
        value_rows,
        mixed_heads,
        log_totals,
        cosine,
        sine_part,
    ) = attention_forward(layer_in, gain_one, query_w, latent_w, gain_kv, kvup_w)
    head_count = query_rows.shape[1]
    mixed_flat = mixed_heads.reshape(seq_len, head_count * DV)
    attn_part = jnp.dot(mixed_flat, output_w, preferred_element_type=jnp.float32)
    hidden_state = layer_in + lax.psum(attn_part, TENSOR)
    stat_two = rms_scale(hidden_state)
    unit_two = hidden_state * stat_two
    normed2 = (unit_two * gain_two.astype(jnp.float32)).astype(jnp.bfloat16)
    router_probs = jax.nn.softmax(
        jnp.dot(normed2, route_w, preferred_element_type=jnp.float32), axis=-1
    )
    route_onehot = (
        routes[:, :, None] == jnp.arange(expert_count, dtype=jnp.int32)[None, None, :]
    ).astype(jnp.float32)
    route_weight = jnp.einsum("tke,te->tk", route_onehot, router_probs)
    flat_hot = route_onehot.reshape(seq_len * TOPK, expert_count).astype(jnp.int32)
    slot_pos = jnp.sum(jnp.cumsum(flat_hot, axis=0) * flat_hot, axis=-1) - 1
    buffer_pos = routes.reshape(-1) * capacity + slot_pos

    def to_owners(assigned):
        buffer = jnp.zeros((rows_total, width), jnp.bfloat16).at[buffer_pos].set(assigned)
        buffer = buffer.reshape(groups, local_experts * capacity, width)
        arrived = lax.all_to_all(buffer, EXPERT, split_axis=0, concat_axis=0, tiled=True)
        return (
            arrived.reshape(groups, local_experts, capacity, width)
            .transpose(1, 0, 2, 3)
            .reshape(local_experts, groups * capacity, width)
        )

    def to_sources(results):
        arranged = (
            results.reshape(local_experts, groups, capacity, width)
            .transpose(1, 0, 2, 3)
            .reshape(groups, local_experts * capacity, width)
        )
        arrived = lax.all_to_all(arranged, EXPERT, split_axis=0, concat_axis=0, tiled=True)
        return arrived.reshape(rows_total, width)[buffer_pos].reshape(seq_len, TOPK, width)

    rows_in = to_owners(jnp.repeat(normed2, TOPK, axis=0))
    pre_gate = jnp.einsum("emd,edf->emf", rows_in, expert_gate, preferred_element_type=jnp.float32)
    pre_up = jnp.einsum("emd,edf->emf", rows_in, expert_up, preferred_element_type=jnp.float32)
    expert_act = (jax.nn.silu(pre_gate) * pre_up).astype(jnp.bfloat16)
    block_out = jnp.einsum(
        "emf,efd->emd", expert_act, expert_down, preferred_element_type=jnp.float32
    ).astype(jnp.bfloat16)
    expert_out = to_sources(block_out)
    routed_part = jnp.einsum(
        "tk,tkd->td", route_weight, expert_out, preferred_element_type=jnp.float32
    )
    shared_pre_gate = jnp.dot(normed2, gate_sh, preferred_element_type=jnp.float32)
    shared_pre_up = jnp.dot(normed2, up_sh, preferred_element_type=jnp.float32)
    shared_act = (jax.nn.silu(shared_pre_gate) * shared_pre_up).astype(jnp.bfloat16)
    shared_part = jnp.dot(shared_act, down_sh, preferred_element_type=jnp.float32)
    layer_out = hidden_state + lax.psum(
        (routed_part + shared_part).astype(jnp.bfloat16), TENSOR
    ).astype(jnp.float32)
    out_rows = out_grad.astype(jnp.bfloat16)
    routed_cot = (
        (route_weight[:, :, None] * out_grad[:, None, :])
        .astype(jnp.bfloat16)
        .reshape(seq_len * TOPK, width)
    )
    cot_in = to_owners(routed_cot)
    route_grad_part = jnp.einsum(
        "tkd,td->tk", expert_out, out_grad, preferred_element_type=jnp.float32
    )
    hidden_grad_ex = jnp.einsum(
        "emd,efd->emf", cot_in, expert_down, preferred_element_type=jnp.float32
    )
    gate_delta = (hidden_grad_ex * pre_up * silu_grad(pre_gate)).astype(jnp.bfloat16)
    up_delta = (hidden_grad_ex * jax.nn.silu(pre_gate)).astype(jnp.bfloat16)
    expert_down_grad = jnp.einsum(
        "emf,emd->efd", expert_act, cot_in, preferred_element_type=jnp.float32
    )
    expert_gate_grad = jnp.einsum(
        "emd,emf->edf", rows_in, gate_delta, preferred_element_type=jnp.float32
    )
    expert_up_grad = jnp.einsum(
        "emd,emf->edf", rows_in, up_delta, preferred_element_type=jnp.float32
    )
    row_block = (
        jnp.einsum("emf,edf->emd", gate_delta, expert_gate, preferred_element_type=jnp.float32)
        + jnp.einsum("emf,edf->emd", up_delta, expert_up, preferred_element_type=jnp.float32)
    ).astype(jnp.bfloat16)
    row_grad = to_sources(row_block)
    shared_down_grad = jnp.dot(shared_act.T, out_rows, preferred_element_type=jnp.float32)
    shared_hidden_grad = jnp.dot(out_rows, down_sh.T, preferred_element_type=jnp.float32)
    shared_gate_delta = (shared_hidden_grad * shared_pre_up * silu_grad(shared_pre_gate)).astype(
        jnp.bfloat16
    )
    shared_up_delta = (shared_hidden_grad * jax.nn.silu(shared_pre_gate)).astype(jnp.bfloat16)
    shared_gate_grad = jnp.dot(normed2.T, shared_gate_delta, preferred_element_type=jnp.float32)
    shared_up_grad = jnp.dot(normed2.T, shared_up_delta, preferred_element_type=jnp.float32)
    normed2_part = (
        jnp.sum(row_grad, axis=1, dtype=jnp.float32)
        + jnp.dot(shared_gate_delta, gate_sh.T, preferred_element_type=jnp.float32)
        + jnp.dot(shared_up_delta, up_sh.T, preferred_element_type=jnp.float32)
    )
    normed2_grad, route_grad = lax.psum((normed2_part, route_grad_part), TENSOR)
    prob_grad = jnp.einsum("tk,tke->te", route_grad, route_onehot)
    logit_delta = (
        router_probs * (prob_grad - jnp.sum(router_probs * prob_grad, axis=-1, keepdims=True))
    ).astype(jnp.bfloat16)
    router_grad = jnp.dot(normed2.T, logit_delta, preferred_element_type=jnp.float32)
    normed2_grad = normed2_grad + jnp.dot(
        logit_delta, route_w.T, preferred_element_type=jnp.float32
    )
    norm2_gain_grad = jnp.sum(normed2_grad * unit_two, axis=0)
    scaled_two = normed2_grad * gain_two.astype(jnp.float32)
    hidden_grad = out_grad + stat_two * (
        scaled_two - unit_two * jnp.mean(scaled_two * unit_two, axis=-1, keepdims=True)
    )
    hidden_rows = hidden_grad.astype(jnp.bfloat16)
    o_grad = jnp.dot(mixed_flat.T, hidden_rows, preferred_element_type=jnp.float32)
    mixed_grad = (
        jnp.dot(hidden_rows, output_w.T, preferred_element_type=jnp.float32)
        .astype(jnp.bfloat16)
        .reshape(seq_len, head_count, DV)
    )
    query_grad, key_grad, value_grad = attend_back(
        query_rows, key_rows, value_rows, log_totals, mixed_grad
    )
    query_delta = (
        jnp.concatenate(
            [
                query_grad[..., :DN],
                rotate_back(query_grad[..., DN:], cosine[:, None, :], sine_part[:, None, :]),
            ],
            axis=-1,
        )
        .astype(jnp.bfloat16)
        .reshape(seq_len, head_count * DQK)
    )
    kv_delta = (
        jnp.concatenate([key_grad[..., :DN], value_grad], axis=-1)
        .astype(jnp.bfloat16)
        .reshape(seq_len, head_count * (DN + DV))
    )
    q_grad = jnp.dot(normed1.T, query_delta, preferred_element_type=jnp.float32)
    kvb_grad = jnp.dot(latent.T, kv_delta, preferred_element_type=jnp.float32)
    latent_part = jnp.dot(kv_delta, kvup_w.T, preferred_element_type=jnp.float32)
    rot_part = jnp.sum(key_grad[..., DN:], axis=1)
    normed1_part = jnp.dot(query_delta, query_w.T, preferred_element_type=jnp.float32)
    latent_grad, rot_sum, normed1_query = (
        lax.psum(latent_part.astype(jnp.bfloat16), TENSOR).astype(jnp.float32),
        lax.psum(rot_part.astype(jnp.bfloat16), TENSOR).astype(jnp.float32),
        lax.psum(normed1_part.astype(jnp.bfloat16), TENSOR).astype(jnp.float32),
    )
    kv_gain_grad = jnp.sum(latent_grad * latent_unit, axis=0)
    scaled_lat = latent_grad * gain_kv.astype(jnp.float32)
    latent_back = latent_stat * (
        scaled_lat - latent_unit * jnp.mean(scaled_lat * latent_unit, axis=-1, keepdims=True)
    )
    latent_delta = jnp.concatenate(
        [latent_back, rotate_back(rot_sum, cosine, sine_part)], axis=-1
    ).astype(jnp.bfloat16)
    kva_grad = jnp.dot(normed1.T, latent_delta, preferred_element_type=jnp.float32)
    normed1_grad = normed1_query + jnp.dot(
        latent_delta, latent_w.T, preferred_element_type=jnp.float32
    )
    norm1_gain_grad = jnp.sum(normed1_grad * unit_one, axis=0)
    scaled_one = normed1_grad * gain_one.astype(jnp.float32)
    x_grad = hidden_grad + stat_one * (
        scaled_one - unit_one * jnp.mean(scaled_one * unit_one, axis=-1, keepdims=True)
    )
    (
        norm1_gain_grad,
        q_grad,
        kva_grad,
        kv_gain_grad,
        kvb_grad,
        o_grad,
        norm2_gain_grad,
        router_grad,
        shared_gate_grad,
        shared_up_grad,
        shared_down_grad,
    ) = (
        lax.psum_scatter(norm1_gain_grad, EXPERT, scatter_dimension=0, tiled=True),
        lax.psum_scatter(q_grad, EXPERT, scatter_dimension=0, tiled=True),
        lax.psum_scatter(kva_grad, EXPERT, scatter_dimension=0, tiled=True),
        lax.psum_scatter(kv_gain_grad, EXPERT, scatter_dimension=0, tiled=True),
        lax.psum_scatter(kvb_grad, EXPERT, scatter_dimension=0, tiled=True),
        lax.psum_scatter(o_grad, EXPERT, scatter_dimension=1, tiled=True),
        lax.psum_scatter(norm2_gain_grad, EXPERT, scatter_dimension=0, tiled=True),
        lax.psum_scatter(router_grad, EXPERT, scatter_dimension=0, tiled=True),
        lax.psum_scatter(shared_gate_grad, EXPERT, scatter_dimension=0, tiled=True),
        lax.psum_scatter(shared_up_grad, EXPERT, scatter_dimension=0, tiled=True),
        lax.psum_scatter(shared_down_grad, EXPERT, scatter_dimension=1, tiled=True),
    )
    return (
        layer_out,
        x_grad,
        norm1_gain_grad,
        q_grad,
        kva_grad,
        kv_gain_grad,
        kvb_grad,
        o_grad,
        norm2_gain_grad,
        router_grad,
        shared_gate_grad,
        shared_up_grad,
        shared_down_grad,
        expert_gate_grad,
        expert_up_grad,
        expert_down_grad,
    )


def fits(groups, heads, block, width):
    whole = groups in (4, 8, 16) and heads in (4, 8, 16) and groups % heads == 0
    return whole and block % 64 == 0 and width == groups * LANES


def to_blocks(grad_rows, groups):
    rows, width = grad_rows.shape
    kept = lax.optimization_barrier(grad_rows.astype(jnp.bfloat16))
    return kept.reshape(rows, groups, width // groups).transpose(1, 0, 2)


def from_blocks(blocks):
    groups, rows, width = blocks.shape
    return blocks.transpose(1, 0, 2).reshape(rows, groups * width)


def widen(rows, width):
    return jnp.pad(rows, [(0, 0)] * (rows.ndim - 1) + [(0, width - rows.shape[-1])])


def by_heads(
    layer_in,
    norm1_gain,
    q_weight,
    kva_weight,
    kv_gain,
    kvb_weight,
    o_weight,
    norm2_gain,
    router_weight,
    shared_gate,
    shared_up,
    shared_down,
    expert_gate,
    expert_up,
    expert_down,
    routes,
    out_grad,
):
    groups = lax.axis_size(EXPERT)
    chip = lax.axis_index(EXPERT)
    seq_len, width = layer_in.shape
    capacity = seq_len * TOPK * 4 // (3 * groups)
    heads = q_weight.shape[1] // DQK
    copies = groups // heads
    head = lax.rem(chip, heads)
    own_cols = kva_weight.shape[0]
    lat_rows, lat_width = kvb_weight.shape[0], kvb_weight.shape[0] * groups
    hidden = shared_gate.shape[1] // groups
    bf16 = jnp.bfloat16

    kv_halves = (DN + DV) // own_cols
    kv_block = lat_rows * kv_halves
    head_parts = jnp.concatenate(
        [
            q_weight.reshape(own_cols, heads, DQK).transpose(1, 2, 0),
            kvb_weight.reshape(lat_rows, heads, kv_halves, own_cols)
            .transpose(1, 2, 0, 3)
            .reshape(heads, kv_block, own_cols),
            o_weight.reshape(heads, DV, own_cols),
        ],
        axis=1,
    )
    shared_parts = jnp.concatenate(
        [
            shared_gate.reshape(own_cols, groups, hidden).transpose(1, 2, 0),
            shared_up.reshape(own_cols, groups, hidden).transpose(1, 2, 0),
            shared_down.reshape(groups, hidden, own_cols),
        ],
        axis=1,
    )
    small = jnp.concatenate(
        [
            router_weight.T,
            norm1_gain[None, :],
            norm2_gain[None, :],
            widen(kv_gain[None, :], own_cols),
        ],
        axis=0,
    )
    small = jnp.pad(small, [(0, -small.shape[0] % 16), (0, 0)])
    at_kv = DQK
    at_o = at_kv + kv_block
    at_gate = at_o + DV
    planes, all_planes = heads // 4, groups // 4
    small_swap = Swap(jnp.broadcast_to(small[None], (groups,) + small.shape), True)
    (small_all,), (latent_w,), (got,), (normed1_all,) = exchange(
        [
            small_swap,
            Gather([kva_weight], all_planes),
            Swap(jnp.tile(head_parts, (copies, 1, 1)), pace=4),
            NormGather(layer_in, small_swap, groups, planes),
        ],
        1,
    )
    route_wt = from_blocks(small_all[:, :groups])
    gain_one = small_all[:, groups].reshape(width).astype(jnp.float32)
    gain_two = small_all[:, groups + 1].reshape(width).astype(jnp.float32)
    gain_kv = small_all[:, groups + 2, :lat_rows].reshape(lat_width).astype(jnp.float32)
    latent_w = latent_w.reshape(width, kva_weight.shape[1])
    stat_one = rms_scale(layer_in)
    unit_one = layer_in * stat_one

    cosine, sine_part = rope_tables(seq_len, DR)
    turn_cos = jnp.concatenate([cosine, cosine], axis=-1)
    turn_sin = jnp.concatenate([-sine_part, sine_part], axis=-1)
    by_seq = (heads, seq_len, -1)
    fold = 2

    def rotated(block, cos_ref, sin_ref, sign):
        flipped = jnp.concatenate([block[:, DR // 2 :], block[:, : DR // 2]], axis=-1)
        reps = block.shape[0] // seq_len
        cos_rows = jnp.concatenate([cos_ref[...]] * reps, axis=0)
        sin_rows = jnp.concatenate([sin_ref[...]] * reps, axis=0)
        return (block * cos_rows + sign * flipped * sin_rows).astype(bf16)

    def attend_forward(refs):
        rows_in, parts, lat_w, kv_gain_ref, cos_ref, sin_ref = refs[:6]
        query_out, key_out, value_out, prob_out, lat_out, latent_out, mixed_out = refs[6:13]
        out_w, query_w, kv_w = refs[13:]

        def assemble():
            for j in range(groups):
                at = slice(j * own_cols, (j + 1) * own_cols)
                query_w[:, at] = parts[j, :at_kv]
                out_w[:, at] = parts[j, at_o:at_gate]
                down = slice(j * lat_rows, (j + 1) * lat_rows)
                for half in range(kv_halves):
                    start = at_kv + half * lat_rows
                    across = slice(half * own_cols, (half + 1) * own_cols)
                    kv_w[down, across] = parts[j, start : start + lat_rows]

        def some(first):
            rows = rows_in[pl.ds(first, fold)].reshape(fold * seq_len, width)
            query = dot_nt(rows, query_w[...])
            query_plain, query_turn = query[:, :DN].astype(bf16), rotated(query[:, DN:], cos_ref, sin_ref, 1.0)
            full = fdot(rows, lat_w[...])
            plain = full[:, :lat_width]
            latent = (plain * rms_scale(plain) * kv_gain_ref[...]).astype(bf16)
            key_turn = rotated(full[:, lat_width:], cos_ref, sin_ref, 1.0)
            key_value = fdot(latent, kv_w[...]).astype(bf16)
            latent_out[pl.ds(first, fold)] = latent.reshape(fold, seq_len, lat_width)
            lat_out[pl.ds(first, fold)] = plain.reshape(fold, seq_len, lat_width)
            ahead = lax.broadcasted_iota(jnp.int32, (seq_len, seq_len), 1) > lax.broadcasted_iota(
                jnp.int32, (seq_len, seq_len), 0
            )
            for k in range(fold):
                at, seq = slice(k * seq_len, (k + 1) * seq_len), first + k
                scores = dot_nt(query_plain[at], key_value[at, :DN])
                scores += dot_nt(query_turn[at], key_turn[at])
                scores = jnp.where(ahead, -1e30, scores * DQK ** (-0.5))
                row_max = jnp.max(scores, axis=-1, keepdims=True)
                total = jnp.sum(jnp.exp(scores - row_max), axis=-1, keepdims=True)
                probs = jnp.exp(scores - (row_max + jnp.log(total)))
                values = key_value[at, DN:]
                prob_out[seq] = probs
                mixed_out[seq] = fdot(probs.astype(bf16), values).astype(bf16)
                query_out[seq, :, :DN], query_out[seq, :, DN:] = query_plain[at], query_turn[at]
                key_out[seq, :, :DN], key_out[seq, :, DN:] = key_value[at, :DN], key_turn[at]
                value_out[seq] = values

        def two(r):
            pl.when(r == 0)(assemble)
            pl.loop(0, 2)(lambda q: some((2 * r + q) * fold))

        return heads // (2 * fold), two

    out_rows = out_grad.astype(bf16)

    def attn_part(part, slot, refs):
        @pl.loop(0, width // 512)
        def _(k):
            cols = part_rows(k * 512, 512)
            part[slot, :, cols] = fdot(refs[12][slot], refs[13][:, cols]).astype(bf16)

    def shaped(last, kind):
        return jax.ShapeDtypeStruct((heads, seq_len, last), kind)

    attended, (shared_got,) = exchange(
        [
            Reduce(
                [normed1_all, got, latent_w, gain_kv[None, :], turn_cos, turn_sin],
                attn_part,
                heads,
                seq_len,
                width,
                extra=[
                    shaped(DQK, bf16),
                    shaped(DQK, bf16),
                    shaped(DV, bf16),
                    shaped(seq_len, jnp.float32),
                    shaped(lat_width, jnp.float32),
                    shaped(lat_width, bf16),
                    shaped(DV, bf16),
                    jax.ShapeDtypeStruct((DV, width), bf16),
                    jax.ShapeDtypeStruct((DQK, width), bf16),
                    jax.ShapeDtypeStruct((lat_width, DN + DV), bf16),
                ],
                prelude=attend_forward,
            ),
            Swap(shared_parts, pace=groups),
        ],
        2,
    )
    attn_sum, query_rows, key_rows, value_rows, att_probs, lat_plain, latent, mixed = attended[:8]
    output_w, query_wt, kvup_w = attended[8:]

    gate_sht = from_blocks(shared_got[:, :hidden])
    up_sht = from_blocks(shared_got[:, hidden : 2 * hidden])
    down_sh = from_blocks(shared_got[:, 2 * hidden :])
    hidden_state = layer_in + attn_sum

    stat_two = rms_scale(hidden_state)
    unit_two = hidden_state * stat_two
    normed2 = (unit_two * gain_two).astype(bf16)
    router_probs = jax.nn.softmax(fsum("td,ed->te", normed2, route_wt), axis=-1)
    experts = jnp.arange(groups, dtype=jnp.int32)
    chosen = jnp.any(routes[:, :, None] == experts[None, None, :], axis=1)
    marked = widen(jnp.where(chosen, router_probs, -1.0), -(-groups // LANES) * LANES)
    room = -(-hidden // 16) * 16

    def stacked(blocks):
        return jnp.pad(blocks, [(0, room - hidden), (0, 0)])

    token_gather = Gather([normed2, out_rows, marked], all_planes)
    experts_op = Experts(
        token_gather,
        [expert_gate[0].T, expert_up[0].T, expert_down[0]],
        jnp.stack([stacked(gate_sht), stacked(up_sht), stacked(down_sh)]),
        capacity,
    )
    grad_reduce = Reduce(
        [],
        None,
        groups,
        seq_len,
        width + marked.shape[1],
        delay=all_planes + 2,
        maker=experts_op,
    )
    _, expert_results, (summed,) = exchange([token_gather, experts_op, grad_reduce], 3)
    out_block, picks, shared_act, shared_sums = expert_results[:4]
    rows_in, cot_in, expert_act, gate_delta, up_delta = (
        x.reshape(groups * capacity, -1) for x in expert_results[4:]
    )
    gate_grad_turn, up_grad_turn, down_grad = expert_weight_grads(
        expert_act, gate_delta, up_delta, rows_in, cot_in
    )
    expert_gate_grad, expert_up_grad = gate_grad_turn.T[None], up_grad_turn.T[None]
    expert_down_grad = down_grad[None]
    shared_grads = (
        shared_sums[:, :hidden]
        .reshape(3 * hidden, groups, own_cols)
        .transpose(1, 0, 2)
    )
    out_left = jnp.concatenate(
        [picks, shared_act.reshape(room, groups, seq_len).transpose(1, 0, 2)], axis=1
    )

    def expert_part(part, slot, refs):
        left, own, held = refs[0], refs[1], refs[-1]
        held[:capacity] = own[slot]

        @pl.loop(0, width // 512)
        def _(k):
            cols = part_rows(k * 512, 512)
            part[slot, :, cols] = dot_tn(left[slot], held[:, cols]).astype(bf16)

    def hold_shared(refs):
        refs[-1][capacity:] = refs[2][...]

    normed2_sum = summed[:, :width]
    prob_grad = summed[:, width : width + groups]
    logit_delta = (
        router_probs * (prob_grad - jnp.sum(router_probs * prob_grad, axis=-1, keepdims=True))
    ).astype(bf16)
    normed2_grad = normed2_sum + fdot(logit_delta, route_wt)
    router_gradt = fsum("te,td->ed", logit_delta, normed2)
    norm2_gain_grad = jnp.sum(normed2_grad * unit_two, axis=0)
    scaled_two = normed2_grad * gain_two
    hidden_grad = out_grad + stat_two * (
        scaled_two - unit_two * jnp.mean(scaled_two * unit_two, axis=-1, keepdims=True)
    )

    hidden_rows = hidden_grad.astype(bf16)
    hidden_gather = Gather([hidden_rows], planes, True)

    def attend_backward(refs):
        rows_in, keys, values, probs, out_w, cos_ref, sin_ref = refs[:7]
        query_to, kv_to, turn_to = refs[9:]
        place, hidden_in = hidden_gather.place, hidden_gather.results[0]

        def some(r):
            level = lax.rem(hidden_gather.level + r // 2, planes)
            first = level * 4 + place.spot(3 - 2 * lax.rem(r, 2))
            second = level * 4 + place.spot(2 - 2 * lax.rem(r, 2))
            slots = [first, second]
            pl.when(r == 0)(lambda: hidden_gather.ready(first, False))
            pl.when(r > 0)(lambda: hidden_gather.ready(first, True))
            hidden_gather.ready(second, True)
            rows = jnp.concatenate([hidden_in[slot] for slot in slots], axis=0)
            mixed_grads = dot_nt(rows, out_w[...]).astype(bf16)
            for k in range(2):
                slot = slots[k]
                mixed_grad = mixed_grads[k * seq_len : (k + 1) * seq_len]
                prob = probs[slot]
                value_grad = dot_tn(prob.astype(bf16), mixed_grad)
                dprob = dot_nt(mixed_grad, values[slot])
                row_delta = jnp.sum(prob * dprob, axis=-1, keepdims=True)
                score_delta = (prob * (dprob - row_delta) * DQK ** (-0.5)).astype(bf16)
                query_grad = fdot(score_delta, keys[slot])
                key_grad = dot_tn(score_delta, rows_in[slot])
                query_to[slot, :, :DN] = query_grad[:, :DN].astype(bf16)
                query_to[slot, :, DN:] = rotated(query_grad[:, DN:], cos_ref, sin_ref, -1.0)
                kv_to[slot, :, :DN] = key_grad[:, :DN].astype(bf16)
                kv_to[slot, :, DN:] = value_grad.astype(bf16)
                turn_to[slot, :, :DR] = key_grad[:, DN:].astype(bf16)
                turn_to[slot, :, DR:] = jnp.zeros((seq_len, LANES - DR), bf16)

        hidden_gather.landed = True
        return 2 * planes, some

    def back_part(part, slot, refs):
        @pl.loop(0, width // 512)
        def _(k):
            cols = part_rows(k * 512, 512)
            part[slot, :, cols] = fdot(refs[9][slot], refs[7][:, cols]).astype(bf16)

        product = dot_nt(refs[10][slot], refs[8][...])
        part[slot, :, width : width + lat_width] = product.astype(bf16)
        part[slot, :, width + lat_width :] = refs[11][slot]

    (hidden_all,), (back, query_delta, kv_delta), (owned_early,) = exchange(
        [
            hidden_gather,
            Reduce(
                [
                    query_rows,
                    key_rows,
                    value_rows,
                    att_probs,
                    output_w,
                    turn_cos,
                    turn_sin,
                    query_wt,
                    kvup_w,
                ],
                back_part,
                heads,
                seq_len,
                width + lat_width + LANES,
                [pltpu.VMEM((heads, seq_len, LANES), bf16)],
                extra=[shaped(DQK, bf16), shaped(DN + DV, bf16)],
                prelude=attend_backward,
                delay=2,
            ),
            Swap(shared_grads, pace=4),
        ],
        5,
    )
    normed1_query = back[:, :width]
    latent_grad = back[:, width : width + lat_width]
    rot_sum = back[:, width + lat_width : width + lat_width + DR]

    own_plain = lax.dynamic_index_in_dim(lat_plain, head, 0, keepdims=False)
    own_stat = rms_scale(own_plain)
    own_unit = own_plain * own_stat
    kv_gain_grad = jnp.sum(latent_grad * own_unit, axis=0)
    scaled_lat = latent_grad * gain_kv
    latent_back = own_stat * (
        scaled_lat - own_unit * jnp.mean(scaled_lat * own_unit, axis=-1, keepdims=True)
    )
    latent_delta = jnp.concatenate(
        [latent_back, rotate_back(rot_sum, cosine, sine_part)], axis=-1
    ).astype(bf16)
    normed1_grad = normed1_query + fsum("tl,dl->td", latent_delta, latent_w)
    norm1_gain_grad = jnp.sum(normed1_grad * unit_one, axis=0)
    scaled_one = normed1_grad * gain_one
    x_grad = hidden_grad + stat_one * (
        scaled_one - unit_one * jnp.mean(scaled_one * unit_one, axis=-1, keepdims=True)
    )

    share = (lat_width + DR) // heads

    def by_owner(row):
        return widen(row.reshape(groups, 1, -1), own_cols)

    small_grads = jnp.concatenate(
        [
            router_gradt.reshape(groups, groups, own_cols).transpose(1, 0, 2),
            by_owner(norm1_gain_grad),
            by_owner(norm2_gain_grad),
            by_owner(kv_gain_grad),
        ],
        axis=1,
    )
    small_grads = jnp.pad(small_grads, [(0, 0), (0, -small_grads.shape[1] % 8), (0, 0)])

    def make_head_grads(op):
        query_ref, rows_ref, mixed_ref, hidden_ref, latent_ref, kv_ref = op.refs
        tokens = heads * seq_len

        def projections(_):
            queries = query_ref[...].reshape(tokens, DQK)
            mixed_rows = mixed_ref[...].reshape(tokens, DV)

            @pl.loop(0, width // 512)
            def _(part):
                cols, first = part_rows(part * 512, 512), part * (512 // own_cols)
                rows = rows_ref[:, :, cols].reshape(tokens, 512)
                hidden_part = hidden_ref[:, :, cols].reshape(tokens, 512)
                of_query = dot_tn(queries, rows).astype(bf16)
                of_out = dot_tn(mixed_rows, hidden_part).astype(bf16)
                for k in range(512 // own_cols):
                    at = slice(k * own_cols, (k + 1) * own_cols)
                    op.source[first + k, :at_kv] = of_query[:, at]
                    op.source[first + k, at_o:at_gate] = of_out[:, at]

        def latents(_):
            lat = latent_ref[...].reshape(tokens, lat_width)
            of_kv = dot_tn(lat, kv_ref[...].reshape(tokens, DN + DV)).astype(bf16)
            for j in range(groups):
                for half in range(kv_halves):
                    start = at_kv + half * lat_rows
                    block = of_kv[
                        j * lat_rows : (j + 1) * lat_rows, half * own_cols : (half + 1) * own_cols
                    ]
                    op.source[j, start : start + lat_rows] = block

        return [projections, latents]

    latent_gather = Gather([latent_delta], planes, True)
    head_swap = MadeSwap(
        [query_delta, normed1_all, mixed, hidden_all, latent, kv_delta],
        (groups, at_gate, own_cols),
        make_head_grads,
        None,
        groups,
    )

    def make_latent_grads(op):
        def product(_):
            pl.loop(0, planes)(latent_gather.receive)
            deltas = latent_gather.results[0][...].reshape(heads * seq_len, lat_width + DR)

            @pl.loop(0, width // 512)
            def _(part):
                cols = part_rows(part * 512, 512)
                rows = head_swap.refs[1][:, :, cols].reshape(heads * seq_len, 512)
                op.extra[0][:, cols] = dot_tn(deltas, rows)

            first = lax.rem(op.place.chip, heads) * share
            mine = op.extra[0][pl.ds(pl.multiple_of(first, 8), share), :].astype(bf16)
            for j in range(groups):
                op.source[j] = mine[:, j * own_cols : (j + 1) * own_cols]

        latent_gather.landed = True
        return [product]

    (latent_delta_all,), (out_sum,), (owned_heads,), (owned_small,), (owned_share,) = exchange(
        [
            latent_gather,
            Reduce(
                [out_left, out_block, stacked(down_sh)],
                expert_part,
                groups,
                seq_len,
                width,
                [pltpu.VMEM((capacity + room, width), bf16)],
                hold_shared,
            ),
            head_swap,
            Swap(small_grads, pace=groups),
            MadeSwap(
                [],
                (groups, share, own_cols),
                make_latent_grads,
                planes + 1,
                groups,
                [pltpu.VMEM((lat_width + DR, width), jnp.float32)],
            ),
        ],
        6,
    )
    (
        layer_out,
        q_grad,
        kvb_grad,
        own_o_grad,
        shared_gate_grad,
        shared_up_grad,
        shared_down_grad,
        kva_turn,
        small_sums,
    ) = finish(
        (heads, at_kv, at_o, lat_rows, hidden, share),
        owned_heads,
        owned_early,
        owned_share,
        owned_small,
        hidden_state,
        out_sum,
    )
    kva_grad, router_grad = kva_turn.T, small_sums[:groups].T
    return (
        layer_out,
        x_grad,
        small_sums[groups],
        q_grad,
        kva_grad,
        small_sums[groups + 2, :lat_rows],
        kvb_grad,
        own_o_grad,
        small_sums[groups + 1],
        router_grad,
        shared_gate_grad,
        shared_up_grad,
        shared_down_grad,
        expert_gate_grad,
        expert_up_grad,
        expert_down_grad,
    )


def on_device(layer_in, *rest):
    groups, heads = lax.axis_size(EXPERT), rest[1].shape[1] // DQK
    one_each = rest[11].shape[0] == 1
    if one_each and fits(groups, heads, *layer_in.shape):
        return by_heads(layer_in, *rest)
    return general(layer_in, *rest)


def solution(mesh):
    in_specs = (
        P(EXPERT, None),
        P(EXPERT),
        P(EXPERT, TENSOR),
        P(EXPERT, None),
        P(EXPERT),
        P(EXPERT, TENSOR),
        P(TENSOR, EXPERT),
        P(EXPERT),
        P(EXPERT, None),
        P(EXPERT, TENSOR),
        P(EXPERT, TENSOR),
        P(TENSOR, EXPERT),
        P(EXPERT, None, TENSOR),
        P(EXPERT, None, TENSOR),
        P(EXPERT, TENSOR, None),
        P(EXPERT, None),
        P(EXPERT, None),
    )
    out_specs = (
        P(EXPERT, None),
        P(EXPERT, None),
        P(EXPERT),
        P(EXPERT, TENSOR),
        P(EXPERT, None),
        P(EXPERT),
        P(EXPERT, TENSOR),
        P(TENSOR, EXPERT),
        P(EXPERT),
        P(EXPERT, None),
        P(EXPERT, TENSOR),
        P(EXPERT, TENSOR),
        P(TENSOR, EXPERT),
        P(EXPERT, None, TENSOR),
        P(EXPERT, None, TENSOR),
        P(EXPERT, TENSOR, None),
    )
    return jax.shard_map(
        on_device, mesh=mesh, in_specs=in_specs, out_specs=out_specs, check_vma=False
    )
```

```python
import functools

import jax
import jax.numpy as jnp
from jax import lax
from jax.experimental import pallas as pl
from jax.experimental.pallas import tpu as pltpu
from jax.sharding import PartitionSpec as P

DN = 128
DR = 64
DQK = 192
DV = 128
TOPK = 6
LANES = 128


norm_eps = 1e-06


def rms_scale(inputs):
    return lax.rsqrt(jnp.mean(inputs * inputs, axis=-1, keepdims=True) + norm_eps)


def rope_tables(length, rot_width):
    half_width = rot_width // 2
    frequency = 10000.0 ** (-jnp.arange(half_width).astype(jnp.float32) / half_width)
    angles = jnp.arange(length).astype(jnp.float32)[:, None] * frequency[None, :]
    return (jnp.cos(angles), jnp.sin(angles))


def rotate(inputs, cosine, sine_part):
    half_width = inputs.shape[-1] // 2
    first_half = inputs[..., :half_width]
    second_half = inputs[..., half_width:]
    return jnp.concatenate(
        [
            first_half * cosine - second_half * sine_part,
            second_half * cosine + first_half * sine_part,
        ],
        axis=-1,
    )


def rotate_back(inputs, cosine, sine_part):
    return rotate(inputs, cosine, -sine_part)


def silu_grad(pre_act):
    sigmoid_val = jax.nn.sigmoid(pre_act)
    return sigmoid_val * (1.0 + pre_act * (1.0 - sigmoid_val))


def fdot(left, right):
    return jnp.dot(left, right, preferred_element_type=jnp.float32)


def dot_nt(left, right):
    return lax.dot_general(
        left, right, (((1,), (1,)), ((), ())), preferred_element_type=jnp.float32
    )


def dot_tn(left, right):
    return lax.dot_general(
        left, right, (((0,), (0,)), ((), ())), preferred_element_type=jnp.float32
    )


def fsum(spec, left, right):
    return jnp.einsum(spec, left, right, preferred_element_type=jnp.float32)


EXPERT, TENSOR = "expert", "tensor"
MESH = pl.DeviceIdType.MESH
DMA = pltpu.SemaphoreType.DMA


def remote(src, dst, send, recv, target):
    return pltpu.make_async_remote_copy(
        src_ref=src, dst_ref=dst, send_sem=send, recv_sem=recv, device_id=target, device_id_type=MESH
    )


def part_rows(start, size):
    return pl.ds(pl.multiple_of(start, size), size)


class Place:
    def __init__(self):
        self.groups = lax.axis_size(EXPERT)
        self.chip = lax.axis_index(EXPERT)
        self.core = lax.axis_index(TENSOR)
        self.here = lax.rem(self.chip, 4)
        self.there_x = self.here + 1 - 2 * lax.rem(self.here, 2)
        self.there_y = self.here + 2 - 4 * (self.here // 2)
        self.across = 3 - self.here
        base = self.chip - self.here
        self.by_x = {EXPERT: base + self.there_x}
        self.by_y = {EXPERT: base + self.there_y}
        self.above = {EXPERT: self.chip + 4}
        self.below = {EXPERT: self.chip - 4}
        self.mate = {TENSOR: 1 - self.core}

    def spot(self, q):
        x = lax.rem(self.here + 1 - lax.rem(q, 2), 2)
        y = lax.rem(self.here // 2 + 1 - q // 2, 2)
        return 2 * y + x

    def partner(self, j):
        return lax.rem(self.chip + j, self.groups)


def level_at(level, planes, t):
    if planes < 4:
        return lax.rem(level + t, planes)
    flip = level // 2
    near = lax.rem(level + flip, 2)
    order = t + near * (1 - 2 * t) * (1 - t // 2)
    return order * (1 - 2 * flip) + 3 * flip


class Swap:
    reach, lazy = 0, False

    def __init__(self, blocks, vmem_result=False, pace=2):
        groups = blocks.shape[0]
        self.pace = groups if vmem_result else pace
        self.ins = [(blocks, pltpu.VMEM)]
        self.outs = [
            (
                jax.ShapeDtypeStruct(blocks.shape, blocks.dtype),
                pltpu.VMEM if vmem_result else pl.ANY,
            )
        ]
        self.scratch = [DMA, DMA((groups,)), DMA((groups,))]

    def bind(self, place, ins, outs, scratch):
        self.place, self.groups = place, place.groups
        self.source, self.result = ins[0], outs[0]
        self.own_sem, self.send_sem, self.recv_sem = scratch

    def copy(self, j, src, dst):
        return remote(
            self.source.at[src],
            self.result.at[dst],
            self.send_sem.at[j],
            self.recv_sem.at[j],
            {EXPERT: self.place.partner(j)},
        )

    def own(self):
        chip = self.place.chip
        return pltpu.make_async_copy(self.source.at[chip], self.result.at[chip], self.own_sem)

    def send(self, i):
        for q in range(min(self.pace, self.groups - 1)):
            j = 1 + i * self.pace + q

            @pl.when(j < self.groups)
            def _(j=j):
                self.copy(j, self.place.partner(j), self.place.chip).start()

    def begin(self):
        self.own().start()
        self.send(0)

    def rest(self, offset):
        count = -(-(self.groups - 1) // self.pace) - 1
        return [(offset, count, lambda i: self.send(i + 1))]

    def segments(self):
        return self.rest(0)

    def end(self):
        self.own().wait()

        @pl.loop(1, self.groups)
        def _(j):
            self.copy(j, self.place.chip, self.place.partner(self.groups - j)).wait_recv()
            self.copy(j, self.place.partner(j), self.place.chip).wait_send()


class MadeSwap(Swap):
    def __init__(self, operands, shape, make, delay, pace, scratch=()):
        self.pace, self.make, self.delay = pace, make, delay
        self.ins = [(a, pltpu.VMEM) for a in operands]
        self.outs = [(jax.ShapeDtypeStruct(shape, jnp.bfloat16), pl.ANY)]
        groups = shape[0]
        self.scratch = [DMA, DMA((groups,)), DMA((groups,)), pltpu.VMEM(shape, jnp.bfloat16)]
        self.scratch += list(scratch)

    def bind(self, place, ins, outs, scratch):
        super().bind(place, [scratch[3]], outs, scratch[:3])
        self.refs, self.extra = ins, scratch[4:]

    def begin(self):
        if self.delay is None:
            for call in self.make(self):
                call(0)
            super().begin()

    def segments(self):
        if self.delay is None:
            return self.rest(0)
        calls = self.make(self) + [lambda i: super(MadeSwap, self).begin()]
        parts = [(self.delay + k, 1, call) for k, call in enumerate(calls)]
        return parts + self.rest(self.delay + len(calls))


class Gather:
    lazy = False

    def __init__(self, arrays, planes, vmem_result=False):
        count, slots = len(arrays), planes * 4
        self.planes, self.count, self.reach = planes, count, planes
        self.ins = [(a, pltpu.VMEM) for a in arrays]
        space = pltpu.VMEM if vmem_result else pl.ANY
        self.outs = [(jax.ShapeDtypeStruct((slots,) + a.shape, a.dtype), space) for a in arrays]
        by_level, by_slot = DMA((count, planes)), DMA((count, slots))
        self.scratch = [DMA((count,))] + [by_level] * 5 + [by_slot] + [by_level] * 6 + [by_slot]

    def bind(self, place, ins, outs, scratch):
        self.place, self.sources, self.results = place, ins, outs
        self.level = lax.rem(place.chip // 4, self.planes)
        self.has_up, self.has_down = self.level < self.planes - 1, self.level > 0
        self.own_sem = scratch[0]
        self.in_z, self.in_x, self.in_y, self.in_a, self.in_b, self.in_p = scratch[1:7]
        self.out_up, self.out_down, self.out_x, self.out_y = scratch[7:11]
        self.out_a, self.out_b, self.out_p = scratch[11:14]
        self.landed = False

    def move(self, a, slot, part, send, recv, target, own=False, whose=None):
        half = self.sources[a].shape[0] // 2
        whose = self.place.core if whose is None else whose
        if part is None:
            rows = part_rows(whose * half, half)
        else:
            rows = part_rows(whose * half + part * (half // 2), half // 2)
        dst = self.results[a].at[slot, rows]
        return remote(self.sources[a].at[rows] if own else dst, dst, send, recv, target)

    def along_z(self, a, lev, own, up):
        sems = self.out_up if up else self.out_down
        target = self.place.above if up else self.place.below
        slot = lev * 4 + self.place.here
        return self.move(a, slot, None, sems.at[a, lev], self.in_z.at[a, lev], target, own)

    def along_x(self, a, lev, slot, own=False):
        return self.move(
            a, slot, None, self.out_x.at[a, lev], self.in_x.at[a, lev], self.place.by_x, own
        )

    def along_y(self, a, lev, slot, own=False):
        return self.move(
            a, slot, None, self.out_y.at[a, lev], self.in_y.at[a, lev], self.place.by_y, own
        )

    def corner_x(self, a, lev, slot):
        return self.move(
            a, slot, 0, self.out_a.at[a, lev], self.in_a.at[a, lev], self.place.by_x
        )

    def corner_y(self, a, lev, slot):
        return self.move(
            a, slot, 1, self.out_b.at[a, lev], self.in_b.at[a, lev], self.place.by_y
        )

    def share(self, a, slot, whose=None):
        return self.move(
            a, slot, None, self.out_p.at[a, slot], self.in_p.at[a, slot], self.place.mate, whose=whose
        )

    def own(self, a):
        slot = self.level * 4 + self.place.here
        return pltpu.make_async_copy(self.sources[a], self.results[a].at[slot], self.own_sem.at[a])

    def begin(self):
        for a in range(self.count):
            self.own(a).start()
        self.first(0, True)

    def relays(self, a, t, own, act):
        lev = level_at(self.level, self.planes, t)
        up, down = self.has_up, self.has_down
        if not own:
            up, down = up & (lev < self.level), down & (lev > self.level)
        pl.when(up)(lambda: act(self.along_z(a, lev, own, True)))
        pl.when(down)(lambda: act(self.along_z(a, lev, own, False)))

    def first(self, t, own=False):
        lev = level_at(self.level, self.planes, t)
        for a in range(self.count):
            slot = lev * 4 + self.place.here
            if not own:
                self.along_z(a, lev, own, True).wait_recv()
            self.relays(a, t, own, lambda copy: copy.start())
            self.along_x(a, lev, slot, own).start()
            self.along_y(a, lev, slot, own).start()
            if not own:
                self.share(a, slot).start()

    def second(self, t):
        lev = level_at(self.level, self.planes, t)
        for a in range(self.count):
            slot = lev * 4 + self.place.there_y
            self.along_y(a, lev, slot).wait_recv()
            self.corner_x(a, lev, slot).start()
            self.share(a, slot).start()
            slot = lev * 4 + self.place.there_x
            self.along_x(a, lev, slot).wait_recv()
            self.corner_y(a, lev, slot).start()
            self.share(a, slot).start()

    def third(self, t):
        lev = level_at(self.level, self.planes, t)
        for a in range(self.count):
            slot = lev * 4 + self.place.across
            self.corner_x(a, lev, slot).wait_recv()
            self.corner_y(a, lev, slot).wait_recv()
            self.share(a, slot).start()

    def advance(self, i):
        pl.when(i < self.planes)(lambda: self.first(i))
        pl.when(i < self.planes + 1)(lambda: self.second(i - 1))
        pl.when(i > 1)(lambda: self.third(i - 2))

    def segments(self):
        return [(0, self.planes + 1, lambda i: self.advance(i + 1))]

    def sent(self, t, own):
        place, lev = self.place, level_at(self.level, self.planes, t)
        for a in range(self.count):
            slot = lev * 4 + place.here
            self.relays(a, t, own, lambda copy: copy.wait_send())
            self.along_x(a, lev, slot, own).wait_send()
            self.along_y(a, lev, slot, own).wait_send()
            self.corner_x(a, lev, lev * 4 + place.there_y).wait_send()
            self.corner_y(a, lev, lev * 4 + place.there_x).wait_send()
            for other in [place.there_y, place.there_x, place.across]:
                self.share(a, lev * 4 + other).wait_send()
            if not own:
                self.share(a, slot).wait_send()

    def end(self):
        if not self.landed:
            self.receive_all()
        self.sent(0, True)
        pl.loop(1, self.planes)(lambda t: self.sent(t, False))

    def ready(self, slot, other):
        for a in range(self.count):
            if other:
                self.share(a, slot, 1 - self.place.core).wait_recv()
            else:
                self.own(a).wait()

    def receive(self, t):
        place, lev = self.place, level_at(self.level, self.planes, t)
        pl.when(t == 0)(lambda: self.ready(lev * 4 + place.here, False))
        pl.when(t > 0)(lambda: self.ready(lev * 4 + place.here, True))
        for spot in (place.there_y, place.there_x, place.across):
            self.ready(lev * 4 + spot, True)

    def receive_all(self):
        self.landed = True
        pl.loop(0, self.planes)(self.receive)


class NormGather(Gather):
    def __init__(self, rows, gains, gain_row, planes):
        super().__init__([jax.ShapeDtypeStruct(rows.shape, jnp.bfloat16)], planes)
        self.ins = [(rows, pltpu.VMEM)]
        self.scratch = self.scratch + [pltpu.VMEM(rows.shape, jnp.bfloat16)]
        self.gains, self.gain_row = gains, gain_row

    def bind(self, place, ins, outs, scratch):
        super().bind(place, [scratch[-1]], outs, scratch[:-1])
        self.rows = ins[0]

    def begin(self):
        self.gains.end()
        rows = self.rows[...]
        stat = lax.rsqrt(jnp.mean(rows * rows, axis=-1, keepdims=True) + norm_eps)
        cols = rows.shape[1] // self.place.groups
        for j in range(self.place.groups):
            at = slice(j * cols, (j + 1) * cols)
            gain = self.gains.result[j, self.gain_row : self.gain_row + 1, :].astype(jnp.float32)
            self.sources[0][:, at] = (rows[:, at] * stat * gain).astype(jnp.bfloat16)
        super().begin()


class Reduce:
    def __init__(
        self, operands, produce, slots, block, width, scratch=(), prepare=None, extra=(), prelude=None, delay=0, maker=None
    ):
        planes, rows, kind = slots // 4, block // 2, jnp.bfloat16
        self.planes, self.reach = planes, planes
        self.ins = [(a, pltpu.VMEM) for a in operands]
        self.outs = [(jax.ShapeDtypeStruct((block, width), jnp.float32), pltpu.VMEM)]
        self.outs += [(shape, pltpu.VMEM) for shape in extra]
        self.own_scratch, self.produce, self.prepare = len(scratch), produce, prepare
        self.prelude, self.delay, self.maker = prelude, delay, maker
        self.lazy = prelude is not None
        by_level = DMA((planes,))
        self.scratch = (
            list(scratch)
            + [pltpu.VMEM((slots, block, width) if produce else (8, LANES), kind)]
            + [pltpu.VMEM((slots, rows, width), kind)]
            + [pltpu.VMEM((planes, rows // 2, width), kind)] * 2
            + [pltpu.VMEM((planes, rows, width), kind)] * 4
            + [DMA((slots,))]
            + [by_level] * 6
            + [DMA, DMA((slots,))]
            + [by_level] * 5
            + [DMA]
        )

    def bind(self, place, ins, outs, scratch):
        self.place, self.out = place, outs[0]
        self.refs = list(ins) + list(outs[1:]) + list(scratch[: self.own_scratch])
        scratch = scratch[self.own_scratch :]
        self.part = scratch[0] if self.produce else self.maker.part
        self.mine = scratch[1]
        self.from_a, self.from_b, self.from_x, self.from_y = scratch[2:6]
        self.from_up, self.from_down = scratch[6:8]
        self.in_p, self.in_a, self.in_b, self.in_x, self.in_y = scratch[8:13]
        self.in_up, self.in_down, self.in_m, self.out_p = scratch[13:17]
        self.out_a, self.out_b, self.out_x, self.out_y, self.out_z, self.out_m = scratch[17:]
        self.level = lax.rem(place.chip // 4, self.planes)
        self.has_up, self.has_down = self.level < self.planes - 1, self.level > 0
        self.rows = self.part.shape[1] // 2
        self.half = self.rows // 2

    def swap(self, slot):
        theirs = part_rows((1 - self.place.core) * self.rows, self.rows)
        return remote(
            self.part.at[slot, theirs],
            self.mine.at[slot],
            self.out_p.at[slot],
            self.in_p.at[slot],
            self.place.mate,
        )

    def add_into(self, dst, terms, first, size):
        step = 16

        @pl.loop(0, size // step)
        def _(i):
            at = first + i * step
            total = None
            for term, shift in terms:
                block = term[part_rows(at + shift, step), :].astype(jnp.float32)
                total = block if total is None else total + block
            dst[part_rows(at, step), :] = total.astype(dst.dtype)

    def send_a(self, lev):
        src = self.mine.at[lev * 4 + self.place.across, pl.ds(0, self.half)]
        return remote(
            src, self.from_a.at[lev], self.out_a.at[lev], self.in_a.at[lev], self.place.by_x
        )

    def send_b(self, lev):
        src = self.mine.at[lev * 4 + self.place.across, pl.ds(self.half, self.half)]
        return remote(
            src, self.from_b.at[lev], self.out_b.at[lev], self.in_b.at[lev], self.place.by_y
        )

    def send_y(self, lev):
        src = self.mine.at[lev * 4 + self.place.there_y]
        return remote(
            src, self.from_y.at[lev], self.out_y.at[lev], self.in_y.at[lev], self.place.by_y
        )

    def send_x(self, lev):
        src = self.mine.at[lev * 4 + self.place.there_x]
        return remote(
            src, self.from_x.at[lev], self.out_x.at[lev], self.in_x.at[lev], self.place.by_x
        )

    def send_up(self, lev):
        src = self.mine.at[lev * 4 + self.place.here]
        return remote(
            src, self.from_down.at[lev], self.out_z.at[lev], self.in_down.at[lev], self.place.above
        )

    def send_down(self, lev):
        src = self.mine.at[lev * 4 + self.place.here]
        return remote(
            src, self.from_up.at[lev], self.out_z.at[lev], self.in_up.at[lev], self.place.below
        )

    def plane(self, i):
        return level_at(self.level, self.planes, self.planes - 1 - i)

    def make(self, i):
        @pl.loop(0, 4)
        def _(q):
            slot = self.plane(i) * 4 + self.place.spot(q)
            if self.produce is not None:
                self.produce(self.part, slot, self.refs)
            self.swap(slot).start()

    def join(self, slot):
        self.swap(slot).wait_recv()
        mine = self.mine.at[slot]
        terms = [(mine, 0), (self.part.at[slot], self.place.core * self.rows)]
        self.add_into(mine, terms, 0, self.rows)

    def first(self, i):
        lev = self.plane(i)
        self.join(lev * 4 + self.place.across)
        self.send_a(lev).start()
        self.send_b(lev).start()
        self.join(lev * 4 + self.place.there_y)
        self.join(lev * 4 + self.place.there_x)

    def second(self, i):
        lev = self.plane(i)
        mine = self.mine.at[lev * 4 + self.place.there_y]
        self.send_a(lev).wait_recv()
        self.add_into(mine, [(mine, 0), (self.from_a.at[lev], 0)], 0, self.half)
        self.send_y(lev).start()
        mine = self.mine.at[lev * 4 + self.place.there_x]
        self.send_b(lev).wait_recv()
        self.add_into(mine, [(mine, 0), (self.from_b.at[lev], -self.half)], self.half, self.half)
        self.send_x(lev).start()
        self.join(lev * 4 + self.place.here)

    def third(self, i):
        rows, out, lev = self.rows, self.out, self.plane(i)
        mine = self.mine.at[lev * 4 + self.place.here]
        self.send_y(lev).wait_recv()
        self.send_x(lev).wait_recv()
        terms = [(mine, 0), (self.from_y.at[lev], 0), (self.from_x.at[lev], 0)]

        def more(total, cond, send, arrived):
            @pl.when(cond)
            def _():
                send(lev).wait_recv()
                self.add_into(total, [(total, 0), (arrived.at[lev], 0)], 0, rows)

        @pl.when(lev == self.level)
        def _():
            total = out.at[part_rows(self.place.core * rows, rows)]
            self.add_into(total, terms, 0, rows)
            more(total, self.has_up, self.send_down, self.from_up)
            more(total, self.has_down, self.send_up, self.from_down)

        @pl.when(lev < self.level)
        def _():
            self.add_into(mine, terms, 0, rows)
            more(mine, self.has_up, self.send_down, self.from_up)
            self.send_down(lev).start()

        @pl.when(lev > self.level)
        def _():
            self.add_into(mine, terms, 0, rows)
            more(mine, self.has_down, self.send_up, self.from_down)
            self.send_up(lev).start()

    def begin(self):
        if self.prepare is not None:
            self.prepare(self.refs)
        if self.prelude is None and self.maker is None:
            self.make(0)

    def advance(self, i):
        pl.when(i + 1 < self.planes)(lambda: self.make(i + 1))
        pl.when(i < self.planes)(lambda: self.first(i))
        pl.when((i > 0) & (i < self.planes + 1))(lambda: self.second(i - 1))
        pl.when(i > 1)(lambda: self.third(i - 2))

    def segments(self):
        parts, start = [], 0
        if self.prelude is not None:
            count, call = self.prelude(self.refs)
            parts = [(self.delay, count, call), (self.delay + count, 1, self.make)]
            start = self.delay + count + 1
        if self.maker is not None:
            parts, start = [(self.delay, 1, self.make)], self.delay + 1
        return parts + [(start, self.planes + 2, self.advance)]

    def hand(self, whose):
        spot = part_rows(whose * self.rows, self.rows)
        return remote(self.out.at[spot], self.out.at[spot], self.out_m, self.in_m, self.place.mate)

    def end(self):
        self.hand(self.place.core).start()


        @pl.loop(0, self.planes)
        def _(lev):
            for spot in range(4):
                self.swap(lev * 4 + spot).wait_send()
            for send in (self.send_a, self.send_b, self.send_y, self.send_x):
                send(lev).wait_send()
            pl.when(lev < self.level)(lambda: self.send_down(lev).wait_send())
            pl.when(lev > self.level)(lambda: self.send_up(lev).wait_send())

        self.hand(self.place.core).wait_send()
        self.hand(1 - self.place.core).wait_recv()


class Experts:
    lazy = False

    def __init__(self, gather, weights, shared_w, capacity):
        slots, seq, width = gather.outs[0][0].shape
        hidden, room, bf16 = weights[0].shape[0], shared_w.shape[1], jnp.bfloat16
        self.gather, self.capacity, self.room, self.reach = gather, capacity, room, gather.reach
        self.slots, self.seq, self.width, self.hidden = slots, seq, width, hidden
        rows = (slots, capacity)
        turn = (room, slots * seq)

        def shape(dims, kind=bf16):
            return jax.ShapeDtypeStruct(dims, kind)

        self.ins = [(a, pl.ANY) for a in weights] + [(shared_w, pltpu.VMEM)]
        self.outs = [
            (shape(rows + (width,)), pl.ANY),
            (shape(rows + (seq,)), pltpu.VMEM),
            (shape(turn), pltpu.VMEM),
            (shape((3, room, width)), pltpu.VMEM),
            (shape(rows + (width,)), pl.ANY),
            (shape(rows + (width,)), pl.ANY),
        ] + [(shape(rows + (hidden,)), pl.ANY)] * 3
        staged = [self.outs[k][0] for k in (0, 6, 7, 8)]
        self.scratch = [pltpu.VMEM((slots, seq, width + LANES), bf16)]
        self.scratch += [pltpu.VMEM(x.shape, bf16) for x in staged]
        self.scratch += [DMA((len(staged), gather.planes))]
        self.scratch += (
            [pltpu.VMEM((4, seq, width), bf16)] * 2
            + [pltpu.VMEM((4, seq, LANES), jnp.float32), DMA((3,))]
            + [pltpu.VMEM(w.shape, bf16) for w in weights]
            + [pltpu.VMEM((4 * capacity, width), bf16)] * 3
            + [
                pltpu.VMEM((4 * capacity, LANES), jnp.float32),
                pltpu.VMEM((4 * capacity + 2 * room, width), bf16),
                pltpu.VMEM((4 * capacity + 2 * room, 4 * seq), bf16),
                pltpu.VMEM((3, room, width), jnp.float32),
                DMA((3,)),
                DMA((2,)),
            ]
        )

    def bind(self, place, ins, outs, scratch):
        self.place = place
        self.hbm_weights, self.shared_w = ins[:3], ins[3]
        self.picks, self.act_turn, self.shared_grads, self.rows_hbm, self.cot_hbm = outs[1:6]
        self.part, self.staged, self.leave_sem = scratch[0], scratch[1:5], scratch[5]
        scratch = scratch[6:]
        self.out_block, self.act, self.gate_delta, self.up_delta = self.staged
        self.final = [outs[0]] + list(outs[6:])
        self.tokens, self.out_rows, self.marked, self.plane_sem = scratch[:4]
        scratch = scratch[4:]
        self.gate, self.up, self.down = scratch[:3]
        self.rows, self.cot, self.grads = scratch[3:6]
        self.weight, self.held, self.left, self.total, self.load_sem, self.save_sem = scratch[6:]
        self.level = lax.rem(place.chip // 4, self.gather.planes)

    def loads(self):
        pairs = zip(self.hbm_weights, [self.gate, self.up, self.down])
        return [
            pltpu.make_async_copy(src, dst, self.load_sem.at[k]) for k, (src, dst) in enumerate(pairs)
        ]

    def saves(self, lev):
        at = pl.ds(lev * 4 * self.capacity, 4 * self.capacity)
        pairs = [(self.rows, self.rows_hbm), (self.cot, self.cot_hbm)]
        return [
            pltpu.make_async_copy(
                src.reshape(4, self.capacity, self.width), dst.at[pl.ds(lev * 4, 4)], self.save_sem.at[k]
            )
            for k, (src, dst) in enumerate(pairs)
        ]

    def begin(self):
        for load in self.loads():
            load.start()
        self.total[...] = jnp.zeros_like(self.total)
        self.held[4 * self.capacity :] = self.shared_w[:2].reshape(2 * self.room, self.width)
        self.left[: 4 * self.capacity] = jnp.zeros((4 * self.capacity, 4 * self.seq), jnp.bfloat16)

    def choose(self, lev, t):
        seq, cap = self.seq, self.capacity
        below = lax.broadcasted_iota(jnp.int32, (seq, seq), 0)
        upto = (below <= lax.broadcasted_iota(jnp.int32, (seq, seq), 1)).astype(jnp.bfloat16)
        place_in = lax.broadcasted_iota(jnp.int32, (cap, seq), 0).astype(jnp.float32)

        @pl.when(t > 0)
        def _():
            for save in self.saves(lev):
                save.wait()

        for j in range(4):
            slot, at = lev * 4 + j, slice(j * cap, (j + 1) * cap)
            turned = self.marked[j].T
            here = jnp.sum(jnp.where(below == self.place.chip, turned, 0.0), axis=0, keepdims=True)
            routed = jnp.where(here >= 0.0, 1.0, 0.0)
            order = fdot(jnp.broadcast_to(routed, (8, seq)).astype(jnp.bfloat16), upto)[:1] - 1.0
            hit = jnp.where(order == place_in, routed, 0.0)
            weight = jnp.sum(hit * here, axis=-1, keepdims=True)
            pick = hit.astype(jnp.bfloat16)
            self.picks[slot] = pick
            self.left[at, j * seq : (j + 1) * seq] = pick
            self.weight[at] = jnp.broadcast_to(weight, (cap, LANES))
        chosen, weight = self.left[: 4 * cap], self.weight[:, :1]

        @pl.loop(0, self.width // 512, unroll=True)
        def _(k):
            cols = part_rows(k * 512, 512)
            own = fdot(chosen, self.tokens[:, :, cols].reshape(4 * seq, 512))
            self.rows[:, cols] = own.astype(jnp.bfloat16)
            grad = fdot(chosen, self.out_rows[:, :, cols].reshape(4 * seq, 512))
            self.grads[:, cols] = grad.astype(jnp.bfloat16)
            self.cot[:, cols] = (weight * grad).astype(jnp.bfloat16)

        for save in self.saves(lev):
            save.start()

    def hidden_units(self, lev):
        slots, chunk = pl.ds(lev * 4, 4), 256
        for start in range(0, self.hidden, chunk):
            cols = slice(start, min(start + chunk, self.hidden))
            shape = (4, self.capacity, cols.stop - cols.start)
            gate = dot_nt(self.rows[...], self.gate[cols])
            up = dot_nt(self.rows[...], self.up[cols])
            grad = dot_nt(self.cot[...], self.down[cols])
            sig = jax.nn.sigmoid(gate)
            gated = gate * sig
            self.act[slots, :, cols] = (gated * up).astype(jnp.bfloat16).reshape(shape)
            slope = sig * (1.0 + gate * (1.0 - sig))
            self.gate_delta[slots, :, cols] = (grad * up * slope).astype(jnp.bfloat16).reshape(shape)
            self.up_delta[slots, :, cols] = (grad * gated).astype(jnp.bfloat16).reshape(shape)

    def shared_units(self, lev):
        seq4, room = 4 * self.seq, self.room
        tokens = self.tokens[...].reshape(seq4, self.width)
        grads = self.out_rows[...].reshape(seq4, self.width)
        both = dot_nt(self.shared_w[:2].reshape(2 * room, self.width), tokens)
        gate, up = both[:room], both[room:]
        grad = dot_nt(self.shared_w[2], grads)
        sig = jax.nn.sigmoid(gate)
        act = (gate * sig * up).astype(jnp.bfloat16)
        gate_delta = (grad * up * (sig * (1.0 + gate * (1.0 - sig)))).astype(jnp.bfloat16)
        up_delta = (grad * gate * sig).astype(jnp.bfloat16)
        self.act_turn[:, part_rows(lev * seq4, seq4)] = act
        self.left[4 * self.capacity : 4 * self.capacity + room] = gate_delta
        self.left[4 * self.capacity + room :] = up_delta

        @pl.loop(0, self.width // 512, unroll=True)
        def _(k):
            cols = part_rows(k * 512, 512)
            some = self.tokens[:, :, cols].reshape(seq4, 512)
            self.total[0, :, cols] += fdot(gate_delta, some)
            self.total[1, :, cols] += fdot(up_delta, some)
            some = self.out_rows[:, :, cols].reshape(seq4, 512)
            self.total[2, :, cols] += fdot(act, some)

    def outward(self, lev):
        slots, cap, count = pl.ds(lev * 4, 4), self.capacity, 4 * self.capacity
        act = self.act[slots].reshape(count, self.hidden)
        gate_delta = self.gate_delta[slots].reshape(count, self.hidden)
        up_delta = self.up_delta[slots].reshape(count, self.hidden)
        weight = self.weight[:, :1]

        def some(k, route):
            cols = part_rows(k * 512, 512)
            out = fdot(act, self.down[:, cols]).astype(jnp.bfloat16).astype(jnp.float32)
            route += jnp.sum(out * self.grads[:, cols].astype(jnp.float32), axis=-1, keepdims=True)
            out = (weight * out).astype(jnp.bfloat16)
            self.out_block[slots, :, cols] = out.reshape(4, cap, 512)
            back = fdot(gate_delta, self.gate[:, cols]) + fdot(up_delta, self.up[:, cols])
            self.held[:count, cols] = back.astype(jnp.bfloat16)
            return route

        route = lax.fori_loop(
            0, self.width // 512, some, jnp.zeros((count, 1), jnp.float32), unroll=True
        )
        lane = lax.broadcasted_iota(jnp.int32, (count, LANES), 1)
        routes = jnp.where(lane == self.place.chip, route, 0.0).astype(jnp.bfloat16)
        shape = (4, self.seq, LANES)
        turned = dot_tn(self.left[:count], routes).astype(jnp.bfloat16)
        self.part[slots, :, self.width :] = turned.reshape(shape)
        left = self.left[...]

        @pl.loop(0, self.width // 512, unroll=True)
        def _(k):
            cols = part_rows(k * 512, 512)
            sums = dot_tn(left, self.held[:, cols]).astype(jnp.bfloat16)
            self.part[slots, :, cols] = sums.reshape(4, self.seq, 512)

        for copy in self.leaving(lev):
            copy.start()

    def leaving(self, lev):
        four = pl.ds(lev * 4, 4)
        return [
            pltpu.make_async_copy(src.at[four], dst.at[four], self.leave_sem.at[k, lev])
            for k, (src, dst) in enumerate(zip(self.staged, self.final))
        ]

    def compute(self, t):
        lev = level_at(self.level, self.gather.planes, t)

        @pl.when(t == 0)
        def _():
            for load in self.loads():
                load.wait()

        self.gather.receive(t)
        held = [self.tokens, self.out_rows, self.marked]
        copies = [
            pltpu.make_async_copy(src.at[pl.ds(lev * 4, 4)], dst, self.plane_sem.at[k])
            for k, (src, dst) in enumerate(zip(self.gather.results, held))
        ]
        for copy in copies:
            copy.start()
        for copy in copies:
            copy.wait()
        self.choose(lev, t)
        self.hidden_units(lev)
        self.shared_units(lev)

    def advance(self, i):
        planes = self.gather.planes
        pl.when(i > 1)(lambda: self.outward(level_at(self.level, planes, i - 2)))
        pl.when((i > 0) & (i < planes + 1))(lambda: self.compute(i - 1))

    def segments(self):
        self.gather.landed = True
        return [(0, self.gather.planes + 2, self.advance)]

    def end(self):
        for save in self.saves(level_at(self.level, self.gather.planes, self.gather.planes - 1)):
            save.wait()
        self.shared_grads[...] = self.total[...].astype(jnp.bfloat16)

        @pl.loop(0, self.gather.planes)
        def _(lev):
            for copy in self.leaving(lev):
                copy.wait()


def greet(place, ops):
    barrier = pltpu.get_barrier_semaphore()
    expected = 1

    def call(target):
        pl.semaphore_signal(barrier, inc=1, device_id=target, device_id_type=MESH)

    call(place.mate)
    if any(op.reach == 0 for op in ops):
        for j in range(1, place.groups):
            call({EXPERT: place.partner(j)})
        expected += place.groups - 1
    else:
        call(place.by_x)
        call(place.by_y)
        planes = max(op.reach for op in ops)
        level = lax.rem(place.chip // 4, planes)
        has_up, has_down = level < planes - 1, level > 0
        pl.when(has_up)(lambda: call(place.above))
        pl.when(has_down)(lambda: call(place.below))
        expected += 2 + has_up.astype(jnp.int32) + has_down.astype(jnp.int32)
    pl.semaphore_wait(barrier, expected)


def is_large(pair):
    array, space = pair
    return space == pltpu.VMEM and array.size * array.dtype.itemsize >= 1 << 17


def chip_kernel(ops, *refs):
    place = Place()
    pairs = [pair for op in ops for pair in op.ins]
    n_in, large = len(pairs), [k for k, pair in enumerate(pairs) if is_large(pair)]
    n_out = sum(len(op.outs) for op in ops)
    ins, outs, scratch = list(refs[:n_in]), refs[n_in : n_in + n_out], refs[n_in + n_out :]
    loads = {}
    for n, k in enumerate(large):
        loads[k] = pltpu.make_async_copy(ins[k], scratch[n], scratch[len(large)].at[n])
        loads[k].start()
        ins[k] = scratch[n]
    scratch = scratch[len(large) + 1 :]
    first = 0
    for op in ops:
        op.fetches = [loads[k] for k in range(first, first + len(op.ins)) if k in loads]
        first += len(op.ins)
        op.bind(place, ins[: len(op.ins)], outs[: len(op.outs)], scratch[: len(op.scratch)])
        ins, outs = ins[len(op.ins) :], outs[len(op.outs) :]
        scratch = scratch[len(op.scratch) :]
    greet(place, ops)


    def load(op):
        for copy in op.fetches:
            copy.wait()

    parts = []
    for op in ops:
        segments = [part for part in op.segments() if part[1] > 0]
        if op.lazy:
            parts.append((min(start for start, _, _ in segments), 1, lambda _, op=op: load(op)))
        else:
            load(op)
        op.begin()
        parts += segments
    if parts:

        @pl.loop(0, max(start + count for start, count, _ in parts))
        def _(r):
            for start, count, call in parts:
                inside = (r >= start) & (r < start + count)
                pl.when(inside)(functools.partial(call, r - start))

    ended = [op.gains for op in ops if isinstance(op, NormGather)]
    for op in ops:
        if op not in ended:
            op.end()


def exchange(ops, ident):
    ins = [pair for op in ops for pair in op.ins]
    outs = [pair for op in ops for pair in op.outs]
    moved = sum(a.size * a.dtype.itemsize for a, _ in ins + outs)
    large = [pair[0] for pair in ins if is_large(pair)]
    spaces = [pl.ANY if is_large(pair) else pair[1] for pair in ins]
    held = [pltpu.VMEM(a.shape, a.dtype) for a in large] + [DMA((max(1, len(large)),))]
    results = pl.pallas_call(
        functools.partial(chip_kernel, ops),
        out_shape=[shape for shape, _ in outs],
        in_specs=[pl.BlockSpec(memory_space=space) for space in spaces],
        out_specs=[pl.BlockSpec(memory_space=space) for _, space in outs],
        scratch_shapes=held + [entry for op in ops for entry in op.scratch],
        compiler_params=pltpu.CompilerParams(
            collective_id=ident, has_side_effects=True, vmem_limit_bytes=60 << 20
        ),
        cost_estimate=pl.CostEstimate(flops=0, bytes_accessed=moved, transcendentals=0),
    )(*[a for a, _ in ins])
    split = []
    for op in ops:
        split.append(results[: len(op.outs)])
        results = results[len(op.outs) :]
    return split


def grads_kernel(act, gate_delta, up_delta, rows, cot, gate_out, up_out, down_out):
    gate_out[...] = dot_tn(gate_delta[...], rows[...])
    up_out[...] = dot_tn(up_delta[...], rows[...])
    down_out[...] = dot_tn(act[...], cot[...])


def expert_weight_grads(act, gate_delta, up_delta, rows, cot):
    count, hidden = act.shape
    width, tile = rows.shape[1], 256
    left = pl.BlockSpec((count, hidden), lambda i: (0, 0), pipeline_mode=pl.Buffered(1))
    right = pl.BlockSpec((count, tile), lambda i: (0, i))
    return pl.pallas_call(
        grads_kernel,
        grid=(width // tile,),
        out_shape=[jax.ShapeDtypeStruct((hidden, width), jnp.float32)] * 3,
        in_specs=[left] * 3 + [right] * 2,
        out_specs=[pl.BlockSpec((hidden, tile), lambda i: (0, i))] * 3,
        compiler_params=pltpu.CompilerParams(vmem_limit_bytes=48 << 20),
        cost_estimate=pl.CostEstimate(
            flops=6 * count * hidden * width,
            bytes_accessed=12 * hidden * width + 4 * count * width,
            transcendentals=0,
        ),
    )(act, gate_delta, up_delta, rows, cot)


def finish_kernel(sizes, heads_in, shared_in, share_in, small_in, state, added, *refs):
    heads, at_kv, at_o, lat_rows, hidden, share = sizes
    layer_out, q_out, kvb_out, o_out, gate_out, up_out, down_out, kva_out, small_out = refs[:9]
    q_turn, gate_turn, up_turn = refs[9:]
    groups, own_cols = heads_in.shape[0], heads_in.shape[2]
    copies = range(0, groups, heads)

    def over_copies(ref, k):
        return sum(ref[first + k].astype(jnp.float32) for first in copies)

    layer_out[...] = state[...] + added[...]
    small_out[...] = sum(small_in[j] for j in range(groups))
    for k in range(heads):
        block = over_copies(heads_in, k)
        q_turn[k * at_kv : (k + 1) * at_kv] = block[:at_kv]
        halves = (at_o - at_kv) // lat_rows
        for half in range(halves):
            start, col = at_kv + half * lat_rows, (k * halves + half) * own_cols
            kvb_out[:, col : col + own_cols] = block[start : start + lat_rows]
        wide = block.shape[0] - at_o
        o_out[k * wide : (k + 1) * wide] = block[at_o:]
        kva_out[k * share : (k + 1) * share] = over_copies(share_in, k)
    for j in range(groups):
        block, at = shared_in[j].astype(jnp.float32), slice(j * hidden, (j + 1) * hidden)
        gate_turn[at] = block[:hidden]
        up_turn[at] = block[hidden : 2 * hidden]
        down_out[at] = block[2 * hidden :]
    q_out[...] = q_turn[...].T
    gate_out[...] = gate_turn[...].T
    up_out[...] = up_turn[...].T


def finish(sizes, heads_in, shared_in, share_in, small_in, state, added):
    heads, at_kv, at_o, lat_rows, hidden, share = sizes
    groups, rows, own_cols = heads_in.shape
    many = groups * hidden

    def shape(*dims):
        return jax.ShapeDtypeStruct(dims, jnp.float32)

    outs = [
        shape(*state.shape),
        shape(own_cols, heads * at_kv),
        shape(lat_rows, heads * (at_o - at_kv) // lat_rows * own_cols),
        shape(heads * (rows - at_o), own_cols),
        shape(own_cols, many),
        shape(own_cols, many),
        shape(many, own_cols),
        shape(heads * share, own_cols),
        shape(*small_in.shape[1:]),
    ]
    turned = [(heads * at_kv, own_cols), (many, own_cols), (many, own_cols)]
    return pl.pallas_call(
        functools.partial(finish_kernel, sizes),
        out_shape=outs,
        in_specs=[pl.BlockSpec(memory_space=pltpu.VMEM)] * 6,
        out_specs=[pl.BlockSpec(memory_space=pltpu.VMEM)] * len(outs),
        scratch_shapes=[pltpu.VMEM(dims, jnp.float32) for dims in turned],
        compiler_params=pltpu.CompilerParams(vmem_limit_bytes=32 << 20),
    )(heads_in, shared_in, share_in, small_in, state, added)


def general_scores(query_blk, key_rows, first_row):
    scores = jnp.einsum(
        "qhd,khd->hqk", query_blk, key_rows, preferred_element_type=jnp.float32
    ) * DQK ** (-0.5)
    row_pos = first_row + jnp.arange(query_blk.shape[0], dtype=jnp.int32)
    col_pos = jnp.arange(key_rows.shape[0], dtype=jnp.int32)
    return jnp.where(col_pos[None, None, :] <= row_pos[None, :, None], scores, -1e30)


def attend(query_rows, key_rows, value_rows):
    seq_len = query_rows.shape[0]
    blk_rows = min(seq_len, 512)

    def one_block(block_index):
        first_row = block_index * blk_rows
        scores = general_scores(query_rows, key_rows, first_row)
        row_max = jnp.max(scores, axis=-1, keepdims=True)
        log_total = row_max + jnp.log(jnp.sum(jnp.exp(scores - row_max), axis=-1, keepdims=True))
        att_weights = jnp.exp(scores - log_total).astype(jnp.bfloat16)
        mixed_blk = jnp.einsum(
            "hqk,khd->qhd", att_weights, value_rows, preferred_element_type=jnp.float32
        ).astype(jnp.bfloat16)
        return (mixed_blk, log_total)

    mixed_heads, log_totals = lax.map(one_block, jnp.arange(seq_len // blk_rows, dtype=jnp.int32))
    return (mixed_heads.reshape(seq_len, query_rows.shape[1], value_rows.shape[2]), log_totals)


def attend_back(query_rows, key_rows, value_rows, log_totals, mixed_grad):
    seq_len, head_count = (query_rows.shape[0], query_rows.shape[1])
    blk_rows = min(seq_len, 512)

    def one_block(running, block_index):
        key_acc, value_acc = running
        first_row = block_index * blk_rows
        scores = general_scores(query_rows, key_rows, first_row)
        att_probs = jnp.exp(scores - log_totals[block_index])
        att_weights = att_probs.astype(jnp.bfloat16)
        value_acc = value_acc + jnp.einsum(
            "hqk,qhd->khd", att_weights, mixed_grad, preferred_element_type=jnp.float32
        )
        prob_grad = jnp.einsum(
            "qhd,khd->hqk", mixed_grad, value_rows, preferred_element_type=jnp.float32
        )
        row_delta = jnp.sum(att_probs * prob_grad, axis=-1, keepdims=True)
        score_delta = (att_probs * (prob_grad - row_delta) * DQK ** (-0.5)).astype(jnp.bfloat16)
        query_grad = jnp.einsum(
            "hqk,khd->qhd", score_delta, key_rows, preferred_element_type=jnp.float32
        )
        key_acc = key_acc + jnp.einsum(
            "hqk,qhd->khd", score_delta, query_rows, preferred_element_type=jnp.float32
        )
        return ((key_acc, value_acc), query_grad)

    zero_start = (
        jnp.zeros((seq_len, head_count, DQK), jnp.float32),
        jnp.zeros((seq_len, head_count, DV), jnp.float32),
    )
    (key_grad, value_grad), query_grad = lax.scan(
        one_block, zero_start, jnp.arange(seq_len // blk_rows, dtype=jnp.int32)
    )
    return (query_grad.reshape(seq_len, head_count, DQK), key_grad, value_grad)


def attention_forward(seq_in, gain_one, query_w, latent_w, gain_kv, kvup_w):
    seq_len = seq_in.shape[0]
    head_count = query_w.shape[1] // DQK
    cosine, sine_part = rope_tables(seq_len, DR)
    stat_one = rms_scale(seq_in)
    unit_one = seq_in * stat_one
    normed1 = (unit_one * gain_one.astype(jnp.float32)).astype(jnp.bfloat16)
    query_full = jnp.dot(normed1, query_w, preferred_element_type=jnp.float32).reshape(
        seq_len, head_count, DQK
    )
    query_rows = jnp.concatenate(
        [
            query_full[..., :DN],
            rotate(query_full[..., DN:], cosine[:, None, :], sine_part[:, None, :]),
        ],
        axis=-1,
    ).astype(jnp.bfloat16)
    latent_full = jnp.dot(normed1, latent_w, preferred_element_type=jnp.float32)
    latent_stat = rms_scale(latent_full[:, : kvup_w.shape[0]])
    latent_unit = latent_full[:, : kvup_w.shape[0]] * latent_stat
    latent = (latent_unit * gain_kv.astype(jnp.float32)).astype(jnp.bfloat16)
    rot_key = rotate(latent_full[:, kvup_w.shape[0] :], cosine, sine_part).astype(jnp.bfloat16)
    key_value = (
        jnp.dot(latent, kvup_w, preferred_element_type=jnp.float32)
        .astype(jnp.bfloat16)
        .reshape(seq_len, head_count, DN + DV)
    )
    key_rows = jnp.concatenate(
        [key_value[..., :DN], jnp.broadcast_to(rot_key[:, None, :], (seq_len, head_count, DR))],
        axis=-1,
    )
    value_rows = key_value[..., DN:]
    mixed_heads, log_totals = attend(query_rows, key_rows, value_rows)
    return (
        stat_one,
        unit_one,
        normed1,
        query_rows,
        latent_stat,
        latent_unit,
        latent,
        key_rows,
        value_rows,
        mixed_heads,
        log_totals,
        cosine,
        sine_part,
    )


def general(
    layer_in,
    norm1_gain,
    q_weight,
    kva_weight,
    kv_gain,
    kvb_weight,
    o_weight,
    norm2_gain,
    router_weight,
    shared_gate,
    shared_up,
    shared_down,
    expert_gate,
    expert_up,
    expert_down,
    routes,
    out_grad,
):
    groups = lax.axis_size(EXPERT)
    seq_len, width = layer_in.shape
    local_experts = expert_gate.shape[0]
    expert_count = local_experts * groups
    capacity = seq_len * TOPK * 4 // (3 * expert_count)
    rows_total = expert_count * capacity
    (
        gain_one,
        query_w,
        latent_w,
        gain_kv,
        kvup_w,
        output_w,
        gain_two,
        route_w,
        gate_sh,
        up_sh,
        down_sh,
    ) = (
        lax.all_gather(norm1_gain, EXPERT, axis=0, tiled=True),
        lax.all_gather(q_weight, EXPERT, axis=0, tiled=True),
        lax.all_gather(kva_weight, EXPERT, axis=0, tiled=True),
        lax.all_gather(kv_gain, EXPERT, axis=0, tiled=True),
        lax.all_gather(kvb_weight, EXPERT, axis=0, tiled=True),
        lax.all_gather(o_weight, EXPERT, axis=1, tiled=True),
        lax.all_gather(norm2_gain, EXPERT, axis=0, tiled=True),
        lax.all_gather(router_weight, EXPERT, axis=0, tiled=True),
        lax.all_gather(shared_gate, EXPERT, axis=0, tiled=True),
        lax.all_gather(shared_up, EXPERT, axis=0, tiled=True),
        lax.all_gather(shared_down, EXPERT, axis=1, tiled=True),
    )
    (
        stat_one,
        unit_one,
        normed1,
        query_rows,
        latent_stat,
        latent_unit,
        latent,
        key_rows,
        value_rows,
        mixed_heads,
        log_totals,
        cosine,
        sine_part,
    ) = attention_forward(layer_in, gain_one, query_w, latent_w, gain_kv, kvup_w)
    head_count = query_rows.shape[1]
    mixed_flat = mixed_heads.reshape(seq_len, head_count * DV)
    attn_part = jnp.dot(mixed_flat, output_w, preferred_element_type=jnp.float32)
    hidden_state = layer_in + lax.psum(attn_part, TENSOR)
    stat_two = rms_scale(hidden_state)
    unit_two = hidden_state * stat_two
    normed2 = (unit_two * gain_two.astype(jnp.float32)).astype(jnp.bfloat16)
    router_probs = jax.nn.softmax(
        jnp.dot(normed2, route_w, preferred_element_type=jnp.float32), axis=-1
    )
    route_onehot = (
        routes[:, :, None] == jnp.arange(expert_count, dtype=jnp.int32)[None, None, :]
    ).astype(jnp.float32)
    route_weight = jnp.einsum("tke,te->tk", route_onehot, router_probs)
    flat_hot = route_onehot.reshape(seq_len * TOPK, expert_count).astype(jnp.int32)
    slot_pos = jnp.sum(jnp.cumsum(flat_hot, axis=0) * flat_hot, axis=-1) - 1
    buffer_pos = routes.reshape(-1) * capacity + slot_pos

    def to_owners(assigned):
        buffer = jnp.zeros((rows_total, width), jnp.bfloat16).at[buffer_pos].set(assigned)
        buffer = buffer.reshape(groups, local_experts * capacity, width)
        arrived = lax.all_to_all(buffer, EXPERT, split_axis=0, concat_axis=0, tiled=True)
        return (
            arrived.reshape(groups, local_experts, capacity, width)
            .transpose(1, 0, 2, 3)
            .reshape(local_experts, groups * capacity, width)
        )

    def to_sources(results):
        arranged = (
            results.reshape(local_experts, groups, capacity, width)
            .transpose(1, 0, 2, 3)
            .reshape(groups, local_experts * capacity, width)
        )
        arrived = lax.all_to_all(arranged, EXPERT, split_axis=0, concat_axis=0, tiled=True)
        return arrived.reshape(rows_total, width)[buffer_pos].reshape(seq_len, TOPK, width)

    rows_in = to_owners(jnp.repeat(normed2, TOPK, axis=0))
    pre_gate = jnp.einsum("emd,edf->emf", rows_in, expert_gate, preferred_element_type=jnp.float32)
    pre_up = jnp.einsum("emd,edf->emf", rows_in, expert_up, preferred_element_type=jnp.float32)
    expert_act = (jax.nn.silu(pre_gate) * pre_up).astype(jnp.bfloat16)
    block_out = jnp.einsum(
        "emf,efd->emd", expert_act, expert_down, preferred_element_type=jnp.float32
    ).astype(jnp.bfloat16)
    expert_out = to_sources(block_out)
    routed_part = jnp.einsum(
        "tk,tkd->td", route_weight, expert_out, preferred_element_type=jnp.float32
    )
    shared_pre_gate = jnp.dot(normed2, gate_sh, preferred_element_type=jnp.float32)
    shared_pre_up = jnp.dot(normed2, up_sh, preferred_element_type=jnp.float32)
    shared_act = (jax.nn.silu(shared_pre_gate) * shared_pre_up).astype(jnp.bfloat16)
    shared_part = jnp.dot(shared_act, down_sh, preferred_element_type=jnp.float32)
    layer_out = hidden_state + lax.psum(
        (routed_part + shared_part).astype(jnp.bfloat16), TENSOR
    ).astype(jnp.float32)
    out_rows = out_grad.astype(jnp.bfloat16)
    routed_cot = (
        (route_weight[:, :, None] * out_grad[:, None, :])
        .astype(jnp.bfloat16)
        .reshape(seq_len * TOPK, width)
    )
    cot_in = to_owners(routed_cot)
    route_grad_part = jnp.einsum(
        "tkd,td->tk", expert_out, out_grad, preferred_element_type=jnp.float32
    )
    hidden_grad_ex = jnp.einsum(
        "emd,efd->emf", cot_in, expert_down, preferred_element_type=jnp.float32
    )
    gate_delta = (hidden_grad_ex * pre_up * silu_grad(pre_gate)).astype(jnp.bfloat16)
    up_delta = (hidden_grad_ex * jax.nn.silu(pre_gate)).astype(jnp.bfloat16)
    expert_down_grad = jnp.einsum(
        "emf,emd->efd", expert_act, cot_in, preferred_element_type=jnp.float32
    )
    expert_gate_grad = jnp.einsum(
        "emd,emf->edf", rows_in, gate_delta, preferred_element_type=jnp.float32
    )
    expert_up_grad = jnp.einsum(
        "emd,emf->edf", rows_in, up_delta, preferred_element_type=jnp.float32
    )
    row_block = (
        jnp.einsum("emf,edf->emd", gate_delta, expert_gate, preferred_element_type=jnp.float32)
        + jnp.einsum("emf,edf->emd", up_delta, expert_up, preferred_element_type=jnp.float32)
    ).astype(jnp.bfloat16)
    row_grad = to_sources(row_block)
    shared_down_grad = jnp.dot(shared_act.T, out_rows, preferred_element_type=jnp.float32)
    shared_hidden_grad = jnp.dot(out_rows, down_sh.T, preferred_element_type=jnp.float32)
    shared_gate_delta = (shared_hidden_grad * shared_pre_up * silu_grad(shared_pre_gate)).astype(
        jnp.bfloat16
    )
    shared_up_delta = (shared_hidden_grad * jax.nn.silu(shared_pre_gate)).astype(jnp.bfloat16)
    shared_gate_grad = jnp.dot(normed2.T, shared_gate_delta, preferred_element_type=jnp.float32)
    shared_up_grad = jnp.dot(normed2.T, shared_up_delta, preferred_element_type=jnp.float32)
    normed2_part = (
        jnp.sum(row_grad, axis=1, dtype=jnp.float32)
        + jnp.dot(shared_gate_delta, gate_sh.T, preferred_element_type=jnp.float32)
        + jnp.dot(shared_up_delta, up_sh.T, preferred_element_type=jnp.float32)
    )
    normed2_grad, route_grad = lax.psum((normed2_part, route_grad_part), TENSOR)
    prob_grad = jnp.einsum("tk,tke->te", route_grad, route_onehot)
    logit_delta = (
        router_probs * (prob_grad - jnp.sum(router_probs * prob_grad, axis=-1, keepdims=True))
    ).astype(jnp.bfloat16)
    router_grad = jnp.dot(normed2.T, logit_delta, preferred_element_type=jnp.float32)
    normed2_grad = normed2_grad + jnp.dot(
        logit_delta, route_w.T, preferred_element_type=jnp.float32
    )
    norm2_gain_grad = jnp.sum(normed2_grad * unit_two, axis=0)
    scaled_two = normed2_grad * gain_two.astype(jnp.float32)
    hidden_grad = out_grad + stat_two * (
        scaled_two - unit_two * jnp.mean(scaled_two * unit_two, axis=-1, keepdims=True)
    )
    hidden_rows = hidden_grad.astype(jnp.bfloat16)
    o_grad = jnp.dot(mixed_flat.T, hidden_rows, preferred_element_type=jnp.float32)
    mixed_grad = (
        jnp.dot(hidden_rows, output_w.T, preferred_element_type=jnp.float32)
        .astype(jnp.bfloat16)
        .reshape(seq_len, head_count, DV)
    )
    query_grad, key_grad, value_grad = attend_back(
        query_rows, key_rows, value_rows, log_totals, mixed_grad
    )
    query_delta = (
        jnp.concatenate(
            [
                query_grad[..., :DN],
                rotate_back(query_grad[..., DN:], cosine[:, None, :], sine_part[:, None, :]),
            ],
            axis=-1,
        )
        .astype(jnp.bfloat16)
        .reshape(seq_len, head_count * DQK)
    )
    kv_delta = (
        jnp.concatenate([key_grad[..., :DN], value_grad], axis=-1)
        .astype(jnp.bfloat16)
        .reshape(seq_len, head_count * (DN + DV))
    )
    q_grad = jnp.dot(normed1.T, query_delta, preferred_element_type=jnp.float32)
    kvb_grad = jnp.dot(latent.T, kv_delta, preferred_element_type=jnp.float32)
    latent_part = jnp.dot(kv_delta, kvup_w.T, preferred_element_type=jnp.float32)
    rot_part = jnp.sum(key_grad[..., DN:], axis=1)
    normed1_part = jnp.dot(query_delta, query_w.T, preferred_element_type=jnp.float32)
    latent_grad, rot_sum, normed1_query = (
        lax.psum(latent_part.astype(jnp.bfloat16), TENSOR).astype(jnp.float32),
        lax.psum(rot_part.astype(jnp.bfloat16), TENSOR).astype(jnp.float32),
        lax.psum(normed1_part.astype(jnp.bfloat16), TENSOR).astype(jnp.float32),
    )
    kv_gain_grad = jnp.sum(latent_grad * latent_unit, axis=0)
    scaled_lat = latent_grad * gain_kv.astype(jnp.float32)
    latent_back = latent_stat * (
        scaled_lat - latent_unit * jnp.mean(scaled_lat * latent_unit, axis=-1, keepdims=True)
    )
    latent_delta = jnp.concatenate(
        [latent_back, rotate_back(rot_sum, cosine, sine_part)], axis=-1
    ).astype(jnp.bfloat16)
    kva_grad = jnp.dot(normed1.T, latent_delta, preferred_element_type=jnp.float32)
    normed1_grad = normed1_query + jnp.dot(
        latent_delta, latent_w.T, preferred_element_type=jnp.float32
    )
    norm1_gain_grad = jnp.sum(normed1_grad * unit_one, axis=0)
    scaled_one = normed1_grad * gain_one.astype(jnp.float32)
    x_grad = hidden_grad + stat_one * (
        scaled_one - unit_one * jnp.mean(scaled_one * unit_one, axis=-1, keepdims=True)
    )
    (
        norm1_gain_grad,
        q_grad,
        kva_grad,
        kv_gain_grad,
        kvb_grad,
        o_grad,
        norm2_gain_grad,
        router_grad,
        shared_gate_grad,
        shared_up_grad,
        shared_down_grad,
    ) = (
        lax.psum_scatter(norm1_gain_grad, EXPERT, scatter_dimension=0, tiled=True),
        lax.psum_scatter(q_grad, EXPERT, scatter_dimension=0, tiled=True),
        lax.psum_scatter(kva_grad, EXPERT, scatter_dimension=0, tiled=True),
        lax.psum_scatter(kv_gain_grad, EXPERT, scatter_dimension=0, tiled=True),
        lax.psum_scatter(kvb_grad, EXPERT, scatter_dimension=0, tiled=True),
        lax.psum_scatter(o_grad, EXPERT, scatter_dimension=1, tiled=True),
        lax.psum_scatter(norm2_gain_grad, EXPERT, scatter_dimension=0, tiled=True),
        lax.psum_scatter(router_grad, EXPERT, scatter_dimension=0, tiled=True),
        lax.psum_scatter(shared_gate_grad, EXPERT, scatter_dimension=0, tiled=True),
        lax.psum_scatter(shared_up_grad, EXPERT, scatter_dimension=0, tiled=True),
        lax.psum_scatter(shared_down_grad, EXPERT, scatter_dimension=1, tiled=True),
    )
    return (
        layer_out,
        x_grad,
        norm1_gain_grad,
        q_grad,
        kva_grad,
        kv_gain_grad,
        kvb_grad,
        o_grad,
        norm2_gain_grad,
        router_grad,
        shared_gate_grad,
        shared_up_grad,
        shared_down_grad,
        expert_gate_grad,
        expert_up_grad,
        expert_down_grad,
    )


def fits(groups, heads, block, width):
    whole = groups in (4, 8, 16) and heads in (4, 8, 16) and groups % heads == 0
    return whole and block % 64 == 0 and width == groups * LANES


def to_blocks(grad_rows, groups):
    rows, width = grad_rows.shape
    kept = lax.optimization_barrier(grad_rows.astype(jnp.bfloat16))
    return kept.reshape(rows, groups, width // groups).transpose(1, 0, 2)


def from_blocks(blocks):
    groups, rows, width = blocks.shape
    return blocks.transpose(1, 0, 2).reshape(rows, groups * width)


def widen(rows, width):
    return jnp.pad(rows, [(0, 0)] * (rows.ndim - 1) + [(0, width - rows.shape[-1])])


def by_heads(
    layer_in,
    norm1_gain,
    q_weight,
    kva_weight,
    kv_gain,
    kvb_weight,
    o_weight,
    norm2_gain,
    router_weight,
    shared_gate,
    shared_up,
    shared_down,
    expert_gate,
    expert_up,
    expert_down,
    routes,
    out_grad,
):
    groups = lax.axis_size(EXPERT)
    chip = lax.axis_index(EXPERT)
    seq_len, width = layer_in.shape
    capacity = seq_len * TOPK * 4 // (3 * groups)
    heads = q_weight.shape[1] // DQK
    copies = groups // heads
    head = lax.rem(chip, heads)
    own_cols = kva_weight.shape[0]
    lat_rows, lat_width = kvb_weight.shape[0], kvb_weight.shape[0] * groups
    hidden = shared_gate.shape[1] // groups
    bf16 = jnp.bfloat16

    kv_halves = (DN + DV) // own_cols
    kv_block = lat_rows * kv_halves
    head_parts = jnp.concatenate(
        [
            q_weight.reshape(own_cols, heads, DQK).transpose(1, 2, 0),
            kvb_weight.reshape(lat_rows, heads, kv_halves, own_cols)
            .transpose(1, 2, 0, 3)
            .reshape(heads, kv_block, own_cols),
            o_weight.reshape(heads, DV, own_cols),
        ],
        axis=1,
    )
    shared_parts = jnp.concatenate(
        [
            shared_gate.reshape(own_cols, groups, hidden).transpose(1, 2, 0),
            shared_up.reshape(own_cols, groups, hidden).transpose(1, 2, 0),
            shared_down.reshape(groups, hidden, own_cols),
        ],
        axis=1,
    )
    small = jnp.concatenate(
        [
            router_weight.T,
            norm1_gain[None, :],
            norm2_gain[None, :],
            widen(kv_gain[None, :], own_cols),
        ],
        axis=0,
    )
    small = jnp.pad(small, [(0, -small.shape[0] % 16), (0, 0)])
    at_kv = DQK
    at_o = at_kv + kv_block
    at_gate = at_o + DV
    planes, all_planes = heads // 4, groups // 4
    small_swap = Swap(jnp.broadcast_to(small[None], (groups,) + small.shape), True)
    (small_all,), (latent_w,), (got,), (normed1_all,) = exchange(
        [
            small_swap,
            Gather([kva_weight], all_planes),
            Swap(jnp.tile(head_parts, (copies, 1, 1)), pace=4),
            NormGather(layer_in, small_swap, groups, planes),
        ],
        1,
    )
    route_wt = from_blocks(small_all[:, :groups])
    gain_one = small_all[:, groups].reshape(width).astype(jnp.float32)
    gain_two = small_all[:, groups + 1].reshape(width).astype(jnp.float32)
    gain_kv = small_all[:, groups + 2, :lat_rows].reshape(lat_width).astype(jnp.float32)
    latent_w = latent_w.reshape(width, kva_weight.shape[1])
    stat_one = rms_scale(layer_in)
    unit_one = layer_in * stat_one

    cosine, sine_part = rope_tables(seq_len, DR)
    turn_cos = jnp.concatenate([cosine, cosine], axis=-1)
    turn_sin = jnp.concatenate([-sine_part, sine_part], axis=-1)
    by_seq = (heads, seq_len, -1)
    fold = 2

    def rotated(block, cos_ref, sin_ref, sign):
        flipped = jnp.concatenate([block[:, DR // 2 :], block[:, : DR // 2]], axis=-1)
        reps = block.shape[0] // seq_len
        cos_rows = jnp.concatenate([cos_ref[...]] * reps, axis=0)
        sin_rows = jnp.concatenate([sin_ref[...]] * reps, axis=0)
        return (block * cos_rows + sign * flipped * sin_rows).astype(bf16)

    def attend_forward(refs):
        rows_in, parts, lat_w, kv_gain_ref, cos_ref, sin_ref = refs[:6]
        query_out, key_out, value_out, prob_out, lat_out, latent_out, mixed_out = refs[6:13]
        out_w, query_w, kv_w = refs[13:]

        def assemble():
            for j in range(groups):
                at = slice(j * own_cols, (j + 1) * own_cols)
                query_w[:, at] = parts[j, :at_kv]
                out_w[:, at] = parts[j, at_o:at_gate]
                down = slice(j * lat_rows, (j + 1) * lat_rows)
                for half in range(kv_halves):
                    start = at_kv + half * lat_rows
                    across = slice(half * own_cols, (half + 1) * own_cols)
                    kv_w[down, across] = parts[j, start : start + lat_rows]

        def some(first):
            rows = rows_in[pl.ds(first, fold)].reshape(fold * seq_len, width)
            query = dot_nt(rows, query_w[...])
            query_plain, query_turn = query[:, :DN].astype(bf16), rotated(query[:, DN:], cos_ref, sin_ref, 1.0)
            full = fdot(rows, lat_w[...])
            plain = full[:, :lat_width]
            latent = (plain * rms_scale(plain) * kv_gain_ref[...]).astype(bf16)
            key_turn = rotated(full[:, lat_width:], cos_ref, sin_ref, 1.0)
            key_value = fdot(latent, kv_w[...]).astype(bf16)
            latent_out[pl.ds(first, fold)] = latent.reshape(fold, seq_len, lat_width)
            lat_out[pl.ds(first, fold)] = plain.reshape(fold, seq_len, lat_width)
            ahead = lax.broadcasted_iota(jnp.int32, (seq_len, seq_len), 1) > lax.broadcasted_iota(
                jnp.int32, (seq_len, seq_len), 0
            )
            for k in range(fold):
                at, seq = slice(k * seq_len, (k + 1) * seq_len), first + k
                scores = dot_nt(query_plain[at], key_value[at, :DN])
                scores += dot_nt(query_turn[at], key_turn[at])
                scores = jnp.where(ahead, -1e30, scores * DQK ** (-0.5))
                row_max = jnp.max(scores, axis=-1, keepdims=True)
                total = jnp.sum(jnp.exp(scores - row_max), axis=-1, keepdims=True)
                probs = jnp.exp(scores - (row_max + jnp.log(total)))
                values = key_value[at, DN:]
                prob_out[seq] = probs
                mixed_out[seq] = fdot(probs.astype(bf16), values).astype(bf16)
                query_out[seq, :, :DN], query_out[seq, :, DN:] = query_plain[at], query_turn[at]
                key_out[seq, :, :DN], key_out[seq, :, DN:] = key_value[at, :DN], key_turn[at]
                value_out[seq] = values

        def two(r):
            pl.when(r == 0)(assemble)
            pl.loop(0, 2)(lambda q: some((2 * r + q) * fold))

        return heads // (2 * fold), two

    out_rows = out_grad.astype(bf16)

    def attn_part(part, slot, refs):
        @pl.loop(0, width // 512)
        def _(k):
            cols = part_rows(k * 512, 512)
            part[slot, :, cols] = fdot(refs[12][slot], refs[13][:, cols]).astype(bf16)

    def shaped(last, kind):
        return jax.ShapeDtypeStruct((heads, seq_len, last), kind)

    attended, (shared_got,) = exchange(
        [
            Reduce(
                [normed1_all, got, latent_w, gain_kv[None, :], turn_cos, turn_sin],
                attn_part,
                heads,
                seq_len,
                width,
                extra=[
                    shaped(DQK, bf16),
                    shaped(DQK, bf16),
                    shaped(DV, bf16),
                    shaped(seq_len, jnp.float32),
                    shaped(lat_width, jnp.float32),
                    shaped(lat_width, bf16),
                    shaped(DV, bf16),
                    jax.ShapeDtypeStruct((DV, width), bf16),
                    jax.ShapeDtypeStruct((DQK, width), bf16),
                    jax.ShapeDtypeStruct((lat_width, DN + DV), bf16),
                ],
                prelude=attend_forward,
            ),
            Swap(shared_parts, pace=groups),
        ],
        2,
    )
    attn_sum, query_rows, key_rows, value_rows, att_probs, lat_plain, latent, mixed = attended[:8]
    output_w, query_wt, kvup_w = attended[8:]

    gate_sht = from_blocks(shared_got[:, :hidden])
    up_sht = from_blocks(shared_got[:, hidden : 2 * hidden])
    down_sh = from_blocks(shared_got[:, 2 * hidden :])
    hidden_state = layer_in + attn_sum

    stat_two = rms_scale(hidden_state)
    unit_two = hidden_state * stat_two
    normed2 = (unit_two * gain_two).astype(bf16)
    router_probs = jax.nn.softmax(fsum("td,ed->te", normed2, route_wt), axis=-1)
    experts = jnp.arange(groups, dtype=jnp.int32)
    chosen = jnp.any(routes[:, :, None] == experts[None, None, :], axis=1)
    marked = widen(jnp.where(chosen, router_probs, -1.0), -(-groups // LANES) * LANES)
    room = -(-hidden // 16) * 16

    def stacked(blocks):
        return jnp.pad(blocks, [(0, room - hidden), (0, 0)])

    token_gather = Gather([normed2, out_rows, marked], all_planes)
    experts_op = Experts(
        token_gather,
        [expert_gate[0].T, expert_up[0].T, expert_down[0]],
        jnp.stack([stacked(gate_sht), stacked(up_sht), stacked(down_sh)]),
        capacity,
    )
    grad_reduce = Reduce(
        [],
        None,
        groups,
        seq_len,
        width + marked.shape[1],
        delay=all_planes + 2,
        maker=experts_op,
    )
    _, expert_results, (summed,) = exchange([token_gather, experts_op, grad_reduce], 3)
    out_block, picks, shared_act, shared_sums = expert_results[:4]
    rows_in, cot_in, expert_act, gate_delta, up_delta = (
        x.reshape(groups * capacity, -1) for x in expert_results[4:]
    )
    gate_grad_turn, up_grad_turn, down_grad = expert_weight_grads(
        expert_act, gate_delta, up_delta, rows_in, cot_in
    )
    expert_gate_grad, expert_up_grad = gate_grad_turn.T[None], up_grad_turn.T[None]
    expert_down_grad = down_grad[None]
    shared_grads = (
        shared_sums[:, :hidden]
        .reshape(3 * hidden, groups, own_cols)
        .transpose(1, 0, 2)
    )
    out_left = jnp.concatenate(
        [picks, shared_act.reshape(room, groups, seq_len).transpose(1, 0, 2)], axis=1
    )

    def expert_part(part, slot, refs):
        left, own, held = refs[0], refs[1], refs[-1]
        held[:capacity] = own[slot]

        @pl.loop(0, width // 512)
        def _(k):
            cols = part_rows(k * 512, 512)
            part[slot, :, cols] = dot_tn(left[slot], held[:, cols]).astype(bf16)

    def hold_shared(refs):
        refs[-1][capacity:] = refs[2][...]

    normed2_sum = summed[:, :width]
    prob_grad = summed[:, width : width + groups]
    logit_delta = (
        router_probs * (prob_grad - jnp.sum(router_probs * prob_grad, axis=-1, keepdims=True))
    ).astype(bf16)
    normed2_grad = normed2_sum + fdot(logit_delta, route_wt)
    router_gradt = fsum("te,td->ed", logit_delta, normed2)
    norm2_gain_grad = jnp.sum(normed2_grad * unit_two, axis=0)
    scaled_two = normed2_grad * gain_two
    hidden_grad = out_grad + stat_two * (
        scaled_two - unit_two * jnp.mean(scaled_two * unit_two, axis=-1, keepdims=True)
    )

    hidden_rows = hidden_grad.astype(bf16)
    hidden_gather = Gather([hidden_rows], planes, True)

    def attend_backward(refs):
        rows_in, keys, values, probs, out_w, cos_ref, sin_ref = refs[:7]
        query_to, kv_to, turn_to = refs[9:]
        place, hidden_in = hidden_gather.place, hidden_gather.results[0]

        def some(r):
            level = lax.rem(hidden_gather.level + r // 2, planes)
            first = level * 4 + place.spot(3 - 2 * lax.rem(r, 2))
            second = level * 4 + place.spot(2 - 2 * lax.rem(r, 2))
            slots = [first, second]
            pl.when(r == 0)(lambda: hidden_gather.ready(first, False))
            pl.when(r > 0)(lambda: hidden_gather.ready(first, True))
            hidden_gather.ready(second, True)
            rows = jnp.concatenate([hidden_in[slot] for slot in slots], axis=0)
            mixed_grads = dot_nt(rows, out_w[...]).astype(bf16)
            for k in range(2):
                slot = slots[k]
                mixed_grad = mixed_grads[k * seq_len : (k + 1) * seq_len]
                prob = probs[slot]
                value_grad = dot_tn(prob.astype(bf16), mixed_grad)
                dprob = dot_nt(mixed_grad, values[slot])
                row_delta = jnp.sum(prob * dprob, axis=-1, keepdims=True)
                score_delta = (prob * (dprob - row_delta) * DQK ** (-0.5)).astype(bf16)
                query_grad = fdot(score_delta, keys[slot])
                key_grad = dot_tn(score_delta, rows_in[slot])
                query_to[slot, :, :DN] = query_grad[:, :DN].astype(bf16)
                query_to[slot, :, DN:] = rotated(query_grad[:, DN:], cos_ref, sin_ref, -1.0)
                kv_to[slot, :, :DN] = key_grad[:, :DN].astype(bf16)
                kv_to[slot, :, DN:] = value_grad.astype(bf16)
                turn_to[slot, :, :DR] = key_grad[:, DN:].astype(bf16)
                turn_to[slot, :, DR:] = jnp.zeros((seq_len, LANES - DR), bf16)

        hidden_gather.landed = True
        return 2 * planes, some

    def back_part(part, slot, refs):
        @pl.loop(0, width // 512)
        def _(k):
            cols = part_rows(k * 512, 512)
            part[slot, :, cols] = fdot(refs[9][slot], refs[7][:, cols]).astype(bf16)

        product = dot_nt(refs[10][slot], refs[8][...])
        part[slot, :, width : width + lat_width] = product.astype(bf16)
        part[slot, :, width + lat_width :] = refs[11][slot]

    (hidden_all,), (back, query_delta, kv_delta), (owned_early,) = exchange(
        [
            hidden_gather,
            Reduce(
                [
                    query_rows,
                    key_rows,
                    value_rows,
                    att_probs,
                    output_w,
                    turn_cos,
                    turn_sin,
                    query_wt,
                    kvup_w,
                ],
                back_part,
                heads,
                seq_len,
                width + lat_width + LANES,
                [pltpu.VMEM((heads, seq_len, LANES), bf16)],
                extra=[shaped(DQK, bf16), shaped(DN + DV, bf16)],
                prelude=attend_backward,
                delay=1,
            ),
            Swap(shared_grads, pace=4),
        ],
        5,
    )
    normed1_query = back[:, :width]
    latent_grad = back[:, width : width + lat_width]
    rot_sum = back[:, width + lat_width : width + lat_width + DR]

    own_plain = lax.dynamic_index_in_dim(lat_plain, head, 0, keepdims=False)
    own_stat = rms_scale(own_plain)
    own_unit = own_plain * own_stat
    kv_gain_grad = jnp.sum(latent_grad * own_unit, axis=0)
    scaled_lat = latent_grad * gain_kv
    latent_back = own_stat * (
        scaled_lat - own_unit * jnp.mean(scaled_lat * own_unit, axis=-1, keepdims=True)
    )
    latent_delta = jnp.concatenate(
        [latent_back, rotate_back(rot_sum, cosine, sine_part)], axis=-1
    ).astype(bf16)
    normed1_grad = normed1_query + fsum("tl,dl->td", latent_delta, latent_w)
    norm1_gain_grad = jnp.sum(normed1_grad * unit_one, axis=0)
    scaled_one = normed1_grad * gain_one
    x_grad = hidden_grad + stat_one * (
        scaled_one - unit_one * jnp.mean(scaled_one * unit_one, axis=-1, keepdims=True)
    )

    share = (lat_width + DR) // heads

    def by_owner(row):
        return widen(row.reshape(groups, 1, -1), own_cols)

    small_grads = jnp.concatenate(
        [
            router_gradt.reshape(groups, groups, own_cols).transpose(1, 0, 2),
            by_owner(norm1_gain_grad),
            by_owner(norm2_gain_grad),
            by_owner(kv_gain_grad),
        ],
        axis=1,
    )
    small_grads = jnp.pad(small_grads, [(0, 0), (0, -small_grads.shape[1] % 8), (0, 0)])

    def make_head_grads(op):
        query_ref, rows_ref, mixed_ref, hidden_ref, latent_ref, kv_ref = op.refs
        tokens = heads * seq_len

        def projections(_):
            queries = query_ref[...].reshape(tokens, DQK)
            mixed_rows = mixed_ref[...].reshape(tokens, DV)

            @pl.loop(0, width // 512)
            def _(part):
                cols, first = part_rows(part * 512, 512), part * (512 // own_cols)
                rows = rows_ref[:, :, cols].reshape(tokens, 512)
                hidden_part = hidden_ref[:, :, cols].reshape(tokens, 512)
                of_query = dot_tn(queries, rows).astype(bf16)
                of_out = dot_tn(mixed_rows, hidden_part).astype(bf16)
                for k in range(512 // own_cols):
                    at = slice(k * own_cols, (k + 1) * own_cols)
                    op.source[first + k, :at_kv] = of_query[:, at]
                    op.source[first + k, at_o:at_gate] = of_out[:, at]

        def latents(_):
            lat = latent_ref[...].reshape(tokens, lat_width)
            of_kv = dot_tn(lat, kv_ref[...].reshape(tokens, DN + DV)).astype(bf16)
            for j in range(groups):
                for half in range(kv_halves):
                    start = at_kv + half * lat_rows
                    block = of_kv[
                        j * lat_rows : (j + 1) * lat_rows, half * own_cols : (half + 1) * own_cols
                    ]
                    op.source[j, start : start + lat_rows] = block

        return [projections, latents]

    latent_gather = Gather([latent_delta], planes, True)
    head_swap = MadeSwap(
        [query_delta, normed1_all, mixed, hidden_all, latent, kv_delta],
        (groups, at_gate, own_cols),
        make_head_grads,
        None,
        groups,
    )

    def make_latent_grads(op):
        def product(_):
            pl.loop(0, planes)(latent_gather.receive)
            deltas = latent_gather.results[0][...].reshape(heads * seq_len, lat_width + DR)

            @pl.loop(0, width // 512)
            def _(part):
                cols = part_rows(part * 512, 512)
                rows = head_swap.refs[1][:, :, cols].reshape(heads * seq_len, 512)
                op.extra[0][:, cols] = dot_tn(deltas, rows)

            first = lax.rem(op.place.chip, heads) * share
            mine = op.extra[0][pl.ds(pl.multiple_of(first, 8), share), :].astype(bf16)
            for j in range(groups):
                op.source[j] = mine[:, j * own_cols : (j + 1) * own_cols]

        latent_gather.landed = True
        return [product]

    (latent_delta_all,), (out_sum,), (owned_heads,), (owned_small,), (owned_share,) = exchange(
        [
            latent_gather,
            Reduce(
                [out_left, out_block, stacked(down_sh)],
                expert_part,
                groups,
                seq_len,
                width,
                [pltpu.VMEM((capacity + room, width), bf16)],
                hold_shared,
            ),
            head_swap,
            Swap(small_grads, pace=groups),
            MadeSwap(
                [],
                (groups, share, own_cols),
                make_latent_grads,
                planes + 1,
                groups,
                [pltpu.VMEM((lat_width + DR, width), jnp.float32)],
            ),
        ],
        6,
    )
    (
        layer_out,
        q_grad,
        kvb_grad,
        own_o_grad,
        shared_gate_grad,
        shared_up_grad,
        shared_down_grad,
        kva_turn,
        small_sums,
    ) = finish(
        (heads, at_kv, at_o, lat_rows, hidden, share),
        owned_heads,
        owned_early,
        owned_share,
        owned_small,
        hidden_state,
        out_sum,
    )
    kva_grad, router_grad = kva_turn.T, small_sums[:groups].T
    return (
        layer_out,
        x_grad,
        small_sums[groups],
        q_grad,
        kva_grad,
        small_sums[groups + 2, :lat_rows],
        kvb_grad,
        own_o_grad,
        small_sums[groups + 1],
        router_grad,
        shared_gate_grad,
        shared_up_grad,
        shared_down_grad,
        expert_gate_grad,
        expert_up_grad,
        expert_down_grad,
    )


def on_device(layer_in, *rest):
    groups, heads = lax.axis_size(EXPERT), rest[1].shape[1] // DQK
    one_each = rest[11].shape[0] == 1
    if one_each and fits(groups, heads, *layer_in.shape):
        return by_heads(layer_in, *rest)
    return general(layer_in, *rest)


def solution(mesh):
    in_specs = (
        P(EXPERT, None),
        P(EXPERT),
        P(EXPERT, TENSOR),
        P(EXPERT, None),
        P(EXPERT),
        P(EXPERT, TENSOR),
        P(TENSOR, EXPERT),
        P(EXPERT),
        P(EXPERT, None),
        P(EXPERT, TENSOR),
        P(EXPERT, TENSOR),
        P(TENSOR, EXPERT),
        P(EXPERT, None, TENSOR),
        P(EXPERT, None, TENSOR),
        P(EXPERT, TENSOR, None),
        P(EXPERT, None),
        P(EXPERT, None),
    )
    out_specs = (
        P(EXPERT, None),
        P(EXPERT, None),
        P(EXPERT),
        P(EXPERT, TENSOR),
        P(EXPERT, None),
        P(EXPERT),
        P(EXPERT, TENSOR),
        P(TENSOR, EXPERT),
        P(EXPERT),
        P(EXPERT, None),
        P(EXPERT, TENSOR),
        P(EXPERT, TENSOR),
        P(TENSOR, EXPERT),
        P(EXPERT, None, TENSOR),
        P(EXPERT, None, TENSOR),
        P(EXPERT, TENSOR, None),
    )
    return jax.shard_map(
        on_device, mesh=mesh, in_specs=in_specs, out_specs=out_specs, check_vma=False
    )
```
